32 devices in a mesh: parts: 2 (over y), gx: 4 (over z), gy: 2 (over x), gz: 2 (over core).
Axes of the slice: x: 2, y: 2, z: 4, core: 2. Of those that a mesh axis runs over, the one named last changes fastest.
Arguments:
- volume: bfloat16 [56, 14, 56, 48], P(('parts', 'gx'), 'gy', 'gz'), parts along dimension 0, may hold values from -6 to 6
- w_qkv: bfloat16 [2, 48, 144], replicated, may hold values from -3 to 3
- w_proj: bfloat16 [2, 48, 48], replicated, may hold values from -0.875 to 0.875
- w_up: bfloat16 [2, 48, 192], replicated, may hold values from -0.875 to 0.875
- w_down: bfloat16 [2, 192, 48], replicated, may hold values from -0.4375 to 0.4375
- norm_gain: float32 [2, 2, 48], replicated, may hold values from 0.25 to 1.75
- conv_weight: bfloat16 [27, 48, 48], replicated, may hold values from -0.15625 to 0.15625
- conv_gain: float32 [48], replicated, may hold values from 0.25 to 1.75
Outputs:
- features: bfloat16 [56, 14, 56, 48], P(('parts', 'gx'), 'gy', 'gz'), parts along dimension 0
The draws below stay inside these ranges and needn't reach their ends.
There are 2 independent parts, one for each index of `parts`. The reference program is written for one: setup_inputs(seed, part) draws one part's arguments, and reference() takes and returns one part's arrays. A program takes and returns all parts, laid end to end along the dimension named above; an argument that names none is the same for every part. Nothing has to cross between parts.
All inputs are finite; a program needn't handle non-finite values.
Results may differ from the reference program's by a relative error of at most 0.039.
The reference program's roundings to bfloat16 on the way count: a program that leaves them out, or rounds other values in their place, can miss the bound.
Values may be sent and summed in bfloat16 or wider, within the bound.
No kernel may reach another device: no remote copies, remote signals or barrier semaphores. Data moves between devices by JAX's collectives and lax.ppermute only.
A program may use at most 64 MiB of HBM per device.

```python
import jax
import jax.numpy as jnp
from jax import lax

C = 48
HEADS = 3
MLP_WIDTH = 192
WINDOW = 7
SHIFT = 3
NX = 28
NY = 14
NZ = 56


def draw_w_qkv(key, part):
    spread = C ** (-0.5)
    base = jax.random.normal(key, (2, C, 3 * C), jnp.float32) * spread
    base = jnp.clip(base, -6.0 * spread, 6.0 * spread)
    return base.astype(jnp.bfloat16)


def block_scale(rng, dims, split, smallest, high):
    level = 1.0
    for axis_at, parts in split:
        draws = jax.random.uniform(jax.random.fold_in(jax.random.fold_in(rng, 6), axis_at), (parts,), jnp.float32, smallest / len(split), high / len(split))
        level = level * jnp.repeat(jnp.exp(draws), dims[axis_at] // parts).reshape((-1,) + (1,) * (len(dims) - 1 - axis_at))
    return level


def gaussian(stream_key, shape, scale, bound, shards=(), kind=jnp.bfloat16):
    drawn = scale * jax.random.normal(stream_key, shape, jnp.float32)
    if shards:
        drawn = drawn * block_scale(stream_key, shape, shards, -0.22, 0.18)
    return jnp.clip(drawn, -bound, bound).astype(kind)


def setup_inputs(seed: int = 0, part: int = 0) -> dict:
    key_of = jax.random.split(jax.random.key(seed), 9)
    part_splits = jax.random.split(jax.random.fold_in(key_of[8], part), 9)
    return {
        "volume": gaussian(part_splits[0], (NX, NY, NZ, C), 1.0, 6.0, ((0, 4), (1, 2), (2, 2))),
        "w_qkv": draw_w_qkv(jax.random.fold_in(key_of[8], 71), part),
        "w_proj": gaussian(key_of[2], (2, C, C), C ** -0.5, 0.875),
        "w_up": gaussian(key_of[3], (2, C, MLP_WIDTH), C ** -0.5, 0.875),
        "w_down": gaussian(key_of[4], (2, MLP_WIDTH, C), MLP_WIDTH ** -0.5, 0.4375),
        "norm_gain": jnp.clip(1.0 + 0.15 * jax.random.normal(key_of[5], (2, 2, C), jnp.float32), 0.25, 1.75),
        "conv_weight": gaussian(key_of[6], (27, C, C), (27 * C) ** -0.5, 0.15625),
        "conv_gain": jnp.clip(1.0 + 0.15 * jax.random.normal(key_of[7], (C,), jnp.float32), 0.25, 1.75),
    }


def layer_norm(values, gain):
    values = values.astype(jnp.float32)
    mean = lax.optimization_barrier(jnp.mean(values, -1, keepdims=True))
    centred = values - mean
    spread = lax.optimization_barrier(jnp.mean(centred * centred, -1, keepdims=True))
    return centred * lax.rsqrt(spread + 1e-05) * gain.astype(jnp.float32)

def to_windows(values):
    sx, sy, sz = (values.shape[0], values.shape[1], values.shape[2])
    rest = values.shape[3:]
    shaped = values.reshape((sx // WINDOW, WINDOW, sy // WINDOW, WINDOW, sz // WINDOW, WINDOW) + rest)
    order = (0, 2, 4, 1, 3, 5) + tuple(range(6, 6 + len(rest)))
    return jnp.transpose(shaped, order).reshape((-1, WINDOW ** 3) + rest)

def from_windows(values, sx, sy, sz):
    width = values.shape[-1]
    shaped = values.reshape(sx // WINDOW, sy // WINDOW, sz // WINDOW, WINDOW, WINDOW, WINDOW, width)
    return jnp.transpose(shaped, (0, 3, 1, 4, 2, 5, 6)).reshape(sx, sy, sz, width)

def attend_group(items):
    qkv, labels = items
    group, count, triple = qkv.shape
    width = triple // 3
    query = qkv[..., :width].reshape(group, count, HEADS, -1).astype(jnp.float32)
    keys = qkv[..., width:2 * width].reshape(group, count, HEADS, -1).astype(jnp.float32)
    vals = qkv[..., 2 * width:].reshape(group, count, HEADS, -1).astype(jnp.float32)
    scores = jnp.einsum('gqhd,gkhd->ghqk', query, keys) * (width // HEADS) ** (-0.5)
    same = labels[:, None, :, None] == labels[:, None, None, :]
    scores = jnp.where(same, scores, -1e+30)
    scores = scores - lax.optimization_barrier(jnp.max(scores, -1, keepdims=True))
    weights = jnp.exp(scores)
    probs = (weights / lax.optimization_barrier(jnp.sum(weights, -1, keepdims=True))).astype(jnp.bfloat16)
    mixed = jnp.einsum('ghqk,gkhd->gqhd', probs.astype(jnp.float32), vals)
    return mixed.reshape(group, count, width).astype(jnp.bfloat16)

def attend(qkv, labels):
    total = qkv.shape[0]
    group = 16 if total % 16 == 0 else 1
    result = lax.map(attend_group, (qkv.reshape((total // group, group) + qkv.shape[1:]), labels.reshape(total // group, group, -1)))
    return result.reshape(total, WINDOW ** 3, -1)

def block(state, labels, w_qkv, w_proj, w_up, w_down, gains):
    sx, sy, sz, width = state.shape
    normed = layer_norm(state, gains[0]).astype(jnp.bfloat16).reshape(-1, width)
    qkv = jnp.dot(normed, w_qkv, preferred_element_type=jnp.float32).astype(jnp.bfloat16)
    qkv = qkv.reshape(sx, sy, sz, 3 * width)
    mixed = from_windows(attend(to_windows(qkv), to_windows(labels)), sx, sy, sz).reshape(-1, width)
    flat = state.reshape(-1, width).astype(jnp.float32)
    flat = (flat + jnp.dot(mixed, w_proj, preferred_element_type=jnp.float32)).astype(jnp.bfloat16)
    normed = layer_norm(flat, gains[1]).astype(jnp.bfloat16)
    upper = jax.nn.gelu(jnp.dot(normed, w_up, preferred_element_type=jnp.float32)).astype(jnp.bfloat16)
    flat = (flat.astype(jnp.float32) + jnp.dot(upper, w_down, preferred_element_type=jnp.float32)).astype(jnp.bfloat16)
    return flat.reshape(sx, sy, sz, width)

def region(coords, length):
    return jnp.where(coords < length - WINDOW, 0, jnp.where(coords < length - SHIFT, 1, 2)).astype(jnp.int32)

def make_labels(offsets, local, whole):
    lx = region(offsets[0] + jnp.arange(local[0], dtype=jnp.int32), whole[0])
    ly = region(offsets[1] + jnp.arange(local[1], dtype=jnp.int32), whole[1])
    lz = region(offsets[2] + jnp.arange(local[2], dtype=jnp.int32), whole[2])
    return 9 * lx[:, None, None] + 3 * ly[None, :, None] + lz[None, None, :]

def conv_out(centre, padded, conv_weight, conv_gain):
    sx, sy, sz, width = centre.shape
    total = jnp.zeros((sx * sy * sz, width), jnp.float32)
    for tap in range(27):
        dx, dy, dz = (tap // 9, tap // 3 % 3, tap % 3)
        piece = padded[dx:dx + sx, dy:dy + sy, dz:dz + sz].reshape(-1, width)
        total = total + jnp.dot(piece, conv_weight[tap], preferred_element_type=jnp.float32)
    active = jax.nn.leaky_relu(layer_norm(total, conv_gain), 0.01)
    return (centre.reshape(-1, width).astype(jnp.float32) + active).astype(jnp.bfloat16).reshape(sx, sy, sz, width)

def reference(volume, w_qkv, w_proj, w_up, w_down, norm_gain, conv_weight, conv_gain):
    sx, sy, sz, width = volume.shape
    plain = jnp.zeros((sx, sy, sz), jnp.int32)
    state = block(volume, plain, w_qkv[0], w_proj[0], w_up[0], w_down[0], norm_gain[0])
    state = jnp.roll(state, (-SHIFT, -SHIFT, -SHIFT), (0, 1, 2))
    labels = make_labels((0, 0, 0), (sx, sy, sz), (sx, sy, sz))
    state = block(state, labels, w_qkv[1], w_proj[1], w_up[1], w_down[1], norm_gain[1])
    state = jnp.roll(state, (SHIFT, SHIFT, SHIFT), (0, 1, 2))
    padded = jnp.pad(state, ((1, 1), (1, 1), (1, 1), (0, 0)))
    return conv_out(state, padded, conv_weight, conv_gain)
```

```python
import functools

import jax
import jax.numpy as jnp
import numpy as np
from jax import lax
from jax.experimental import pallas as pl
from jax.experimental.pallas import tpu as pltpu
from jax.sharding import PartitionSpec as P

HEADS = 3
WINDOW = 7
SHIFT = 3
LANES = 128
HALF = 64
ROWS = 8
BIG = -1e30
HIGH = WINDOW - SHIFT
EXT = 2 * WINDOW + 1
BF = jnp.bfloat16
F32 = jnp.float32


def mm(a, b):
    return jnp.dot(a, b, preferred_element_type=F32)


def layer_norm(x, gain, keep, width):
    mean = jnp.sum(x, -1, keepdims=True) * (1.0 / width)
    centred = jnp.where(keep, x - mean, 0.0)
    spread = jnp.sum(centred * centred, -1, keepdims=True) * (1.0 / width)
    return centred * lax.rsqrt(spread + 1e-05) * gain


def gelu(x):
    inner = 0.7978845608028654 * (x + 0.044715 * (x * x * x))
    return (0.5 * x) * (1.0 + jnp.tanh(inner))


def lane_keep(shape, width):
    return lax.broadcasted_iota(jnp.int32, shape, len(shape) - 1) < width


def window_block(tokens, valid, box, wts, width):
    wvq, wk, wp, wup, wdown, gains = wts
    count = tokens.shape[0]
    keep = lane_keep((count, LANES), width)
    normed = layer_norm(tokens, gains[0:1], keep, width).astype(BF)
    vq = mm(normed, wvq).astype(BF)
    kt = lax.dot_general(wk, normed, (((1,), (1,)), ((), ())), preferred_element_type=F32).astype(BF)
    kaug = jnp.concatenate([jnp.zeros((HALF, count), BF), kt, valid.astype(BF)], 0)
    (x0, nx), (y0, ny) = box

    def pick(v):
        v = v.reshape(WINDOW, WINDOW, ROWS, LANES)[x0 : x0 + nx, y0 : y0 + ny]
        return v.reshape(nx * ny * ROWS, LANES)

    nq = nx * ny * ROWS
    full = nx == WINDOW and ny == WINDOW
    vqf = vq.astype(F32)
    qrows = vqf if full else pick(vqf)
    lane = lax.broadcasted_iota(jnp.int32, (nq, LANES), 1)
    head_dim = width // HEADS
    bias_lane = HALF + width
    rhs = jnp.concatenate([vq, jnp.ones((count, LANES), BF)], 1)
    mixed = jnp.zeros((nq, LANES), F32)
    for h in range(HEADS):
        low = HALF + h * head_dim
        inside = (lane >= low) & (lane < low + head_dim)
        qh = jnp.where(inside, qrows, jnp.where(lane == bias_lane, 1.0, 0.0)).astype(BF)
        scores = mm(qh, kaug)
        top = jnp.max(scores, -1, keepdims=True)
        weights = jnp.exp(scores - top).astype(BF)
        out = mm(weights, rhs)
        part = out[:, :LANES] / out[:, LANES:]
        mine = (lane >= h * head_dim) & (lane < (h + 1) * head_dim)
        mixed = jnp.where(mine, part, mixed)
    residual = tokens if full else pick(tokens)
    first = (residual + mm(mixed.astype(BF), wp)).astype(BF).astype(F32)
    keepq = lane < width
    normed = layer_norm(first, gains[1:2], keepq, width).astype(BF)
    upper = gelu(mm(normed, wup)).astype(BF)
    return (first + mm(upper, wdown)).astype(BF).astype(F32)


def first_kernel(width, vol_ref, geo_ref, wvq_ref, wk_ref, wp_ref, wup_ref, wdown_ref, gain_ref, out_ref, raw, done):
    nz = vol_ref.shape[2]
    groups = nz // WINDOW
    spots = WINDOW * WINDOW
    raw[...] = jnp.zeros(raw.shape, F32)
    raw[:, 0:nz, 0:width] = vol_ref[...].astype(F32).reshape(spots, nz, width)
    done[:, nz:, :] = jnp.zeros((spots, done.shape[1] - nz, LANES), F32)
    wts = (wvq_ref[...], wk_ref[...], wp_ref[...], wup_ref[...], wdown_ref[...], gain_ref[...])
    row = geo_ref[0:1, :]
    bias = jnp.where(row < WINDOW, 0.0, BIG)
    top = lax.broadcasted_iota(jnp.int32, (16, spots * ROWS), 0) == 0
    valid = jnp.where(top, bias, 0.0)
    for w in range(groups):
        tokens = raw[:, WINDOW * w : WINDOW * w + ROWS, :].reshape(spots * ROWS, LANES)
        out = window_block(tokens, valid, ((0, WINDOW), (0, WINDOW)), wts, width)
        out = out.reshape(spots, ROWS, LANES)
        done[:, WINDOW * w : WINDOW * (w + 1), :] = out[:, :WINDOW, :]
        if w == 0:
            done[:, nz : nz + SHIFT, :] = out[:, :SHIFT, :]
    pieces = [done[:, SHIFT + WINDOW * w : SHIFT + WINDOW * w + ROWS, :] for w in range(groups)]
    rolled = [pltpu.roll(p.reshape(spots * ROWS, LANES), HALF, 1).reshape(spots, ROWS, LANES) for p in pieces[1::2]]
    joined = [a + b for a, b in zip(pieces[0::2], rolled)]
    packed = jnp.concatenate(joined, 1).astype(BF)
    out_ref[...] = packed.reshape(WINDOW, WINDOW, ROWS * len(joined), LANES)


def second_kernel(
    width, ypieces, flags, geo_ref, own_ref, *refs
):
    y_refs = refs[:ypieces]
    xa_ref, xb_ref, zown_ref = refs[ypieces : ypieces + 3]
    zy_refs = refs[ypieces + 3 : 2 * ypieces + 3]
    rest = refs[2 * ypieces + 3 :]
    zxa_ref, zxb_ref, wvq_ref, wk_ref, wp_ref, wup_ref, wdown_ref, gain_ref, wc_ref, cgain_ref, out_ref = rest[:11]
    ext, post, grid = rest[11:]
    nz = out_ref.shape[2]
    pairs = own_ref.shape[2] // ROWS
    groups = 2 * pairs + 1
    xeven, yeven = flags[0] == 0, flags[1] == 0
    xlo, xhi, ylo, yhi, zlo, zhi = [flags[i] for i in range(2, 8)]

    if ypieces == 1:
        ext[...] = jnp.zeros(ext.shape, F32)

    def place(tile, ztile, x, y, nx, ny):
        spots = nx * ny
        tile = tile.astype(F32).reshape(spots, pairs * ROWS, LANES)
        ztile = ztile.astype(F32).reshape(spots, ROWS, LANES)
        keep = lane_keep((spots, ROWS, LANES), width)

        def put(slot, v):
            ext[slot, pl.ds(x, nx), pl.ds(y, ny)] = jnp.where(keep, v, 0.0).reshape(nx, ny, ROWS, LANES)

        def turn(v):
            return pltpu.roll(v.reshape(spots * ROWS, LANES), HALF, 1).reshape(spots, ROWS, LANES)

        for p in range(pairs):
            piece = tile[:, p * ROWS : (p + 1) * ROWS, :]
            put(1 + 2 * p, piece)
            if p + 1 < pairs:
                put(2 + 2 * p, turn(piece))
        mine = turn(tile[:, (pairs - 1) * ROWS :, :])
        other = turn(ztile)
        low = lax.broadcasted_iota(jnp.int32, (spots, ROWS, LANES), 1) < HIGH
        put(0, jnp.where(low, other, mine))
        put(groups - 1, jnp.where(low, mine, other))

    far = WINDOW + HIGH
    ya = jnp.where(yeven, far, 0)
    yb = jnp.where(yeven, 0, far)
    xa = jnp.where(xeven, far, 0)
    xb = jnp.where(xeven, 0, far)
    ystarts = [ya, yb][:ypieces]
    place(own_ref[...], zown_ref[...], HIGH, HIGH, WINDOW, WINDOW)
    for r, z, y in zip(y_refs, zy_refs, ystarts):
        place(r[...], z[...], HIGH, y, WINDOW, HIGH)
    for r, z, x in ((xa_ref, zxa_ref, xa), (xb_ref, zxb_ref, xb)):
        place(r[:, :WINDOW], z[:, :WINDOW], x, HIGH, HIGH, WINDOW)
        for i, y in enumerate(ystarts):
            at = WINDOW + i * HIGH
            place(r[:, at : at + HIGH], z[:, at : at + HIGH], x, y, HIGH, HIGH)

    wts = (wvq_ref[...], wk_ref[...], wp_ref[...], wup_ref[...], wdown_ref[...], gain_ref[...])
    spots = WINDOW * WINDOW
    row, px, py = geo_ref[0:1, :], geo_ref[1:2, :], geo_ref[2:3, :]
    top = lax.broadcasted_iota(jnp.int32, (16, spots * ROWS), 0) == 0

    def flag(v):
        return jnp.where(v > 0, 1.0, 0.0)

    boxes = ((SHIFT, HIGH), (0, HIGH + 1))
    for wx in range(2):
        for wy in range(2):
            badx = jnp.where(px < HIGH, 1.0 - flag(xlo), 0.0) if wx == 0 else jnp.where(px >= HIGH, 1.0 - flag(xhi), 0.0)
            bady = jnp.where(py < HIGH, 1.0 - flag(ylo), 0.0) if wy == 0 else jnp.where(py >= HIGH, 1.0 - flag(yhi), 0.0)
            bad = badx + bady + jnp.where(row < WINDOW, 0.0, 1.0)
            (bx, nx), (by, ny) = boxes[wx], boxes[wy]
            shape = (nx, ny, ROWS, LANES)
            qx = lax.broadcasted_iota(jnp.int32, shape, 0) + bx
            qy = lax.broadcasted_iota(jnp.int32, shape, 1) + by
            qr = lax.broadcasted_iota(jnp.int32, shape, 2)
            outx = jnp.where(qx < HIGH, 1.0 - flag(xlo), 0.0) if wx == 0 else jnp.where(qx >= HIGH, 1.0 - flag(xhi), 0.0)
            outy = jnp.where(qy < HIGH, 1.0 - flag(ylo), 0.0) if wy == 0 else jnp.where(qy >= HIGH, 1.0 - flag(yhi), 0.0)

            def one(g, carry, wx=wx, wy=wy, bad=bad, bx=bx, nx=nx, by=by, ny=ny, qr=qr, outxy=outx + outy):
                lowbad = jnp.where((g == 0) & (zlo == 0), 1.0, 0.0)
                highbad = jnp.where((g == groups - 1) & (zhi == 0), 1.0, 0.0)
                badz = jnp.where(row < HIGH, lowbad, highbad)
                valid = jnp.where(top & (bad + badz > 0.0), BIG, 0.0)
                tokens = ext[g, WINDOW * wx : WINDOW * (wx + 1), WINDOW * wy : WINDOW * (wy + 1)]
                out = window_block(
                    tokens.reshape(spots * ROWS, LANES), valid, ((bx, nx), (by, ny)), wts, width
                )
                outz = jnp.where(qr < HIGH, lowbad, highbad)
                out = jnp.where(outxy + outz > 0.0, 0.0, out.reshape(nx, ny, ROWS, LANES))
                post[g, HIGH * wx : HIGH * wx + nx, HIGH * wy : HIGH * wy + ny] = out
                return carry

            lax.fori_loop(0, groups, one, 0)

    side = WINDOW + 2
    for g in range(groups):
        grid[:, :, WINDOW * g : WINDOW * (g + 1), :] = post[g, :, :, :WINDOW, :]
    padded = -(-nz // 16) * 16
    cg = cgain_ref[...]
    keep = lane_keep((WINDOW * padded, LANES), width)

    def lhs(x):
        taps = [grid[x, :, SHIFT + d : SHIFT + d + padded, :].reshape(side * padded, LANES) for d in range(3)]
        return jnp.concatenate([taps[0] + pltpu.roll(taps[1], HALF, 1), taps[2]], 1).astype(BF)

    rows = [lhs(x) for x in range(side)]
    for x in range(WINDOW):
        acc = mm(rows[x], wc_ref[0]) + mm(rows[x + 1], wc_ref[1]) + mm(rows[x + 2], wc_ref[2])
        near, second = acc[:, :LANES], acc[:, LANES:]
        turned = pltpu.roll(near, HALF, 1)
        total = near[: WINDOW * padded] + turned[padded : (WINDOW + 1) * padded] + second[2 * padded :]
        total = jnp.where(keep, total, 0.0)
        normed = layer_norm(total, cg, keep, width)
        active = jnp.where(normed >= 0.0, normed, 0.01 * normed)
        centre = grid[x + 1, 1 : 1 + WINDOW, HIGH : HIGH + padded, :].reshape(WINDOW * padded, LANES)
        result = (centre + active).reshape(WINDOW, padded, LANES).astype(BF)
        out_ref[x] = result[:, :nz, :width]


def pad_to(v, rows, cols, r0=0, c0=0):
    return jnp.pad(v, ((r0, rows - r0 - v.shape[0]), (c0, cols - c0 - v.shape[1])))


def block_weights(w_qkv, w_proj, w_up, w_down, gains):
    width = w_proj.shape[0]
    hidden = -(-w_up.shape[1] // LANES) * LANES
    wq, wk, wv = w_qkv[:, :width], w_qkv[:, width : 2 * width], w_qkv[:, 2 * width :]
    scale = (width // HEADS) ** (-0.5)
    wvq = pad_to(wv, LANES, LANES) + pad_to(wq * jnp.asarray(scale, wq.dtype), LANES, LANES, 0, HALF)
    wkt = pad_to(wk.T, width, LANES)
    return (
        wvq,
        wkt,
        pad_to(w_proj, LANES, LANES),
        pad_to(w_up, LANES, hidden),
        pad_to(w_down, hidden, LANES),
        pad_to(gains.astype(F32), gains.shape[0], LANES),
    )


def conv_weights(conv_weight):
    width = conv_weight.shape[-1]
    w = conv_weight.reshape(3, 3, 3, width, width)
    w = jnp.transpose(w, (0, 2, 3, 1, 4))
    w = jnp.pad(w, ((0, 0), (0, 1), (0, HALF - width), (0, 1), (0, HALF - width)))
    return w.reshape(3, 4 * HALF, 4 * HALF)


def geometry():
    t = np.arange(WINDOW * WINDOW * ROWS)
    geo = np.zeros((8, t.size), np.float32)
    geo[0] = t % ROWS
    geo[1] = t // ROWS // WINDOW
    geo[2] = t // ROWS % WINDOW
    return jnp.asarray(geo)


def swap_pairs(count, odd):
    to = list(range(count))
    for i in range(odd, count - 1, 2):
        to[i], to[i + 1] = i + 1, i
    return list(enumerate(to))


def body(volume, w_qkv, w_proj, w_up, w_down, norm_gain, conv_weight, conv_gain):
    sx, sy, sz, width = volume.shape
    spots = sx * sy
    groups = sz // WINDOW
    geo = geometry()
    weights = [block_weights(w_qkv[b], w_proj[b], w_up[b], w_down[b], norm_gain[b]) for b in range(2)]
    wc = conv_weights(conv_weight)
    cg = pad_to(conv_gain.astype(F32)[None, :], 1, LANES)

    packed = pl.pallas_call(
        functools.partial(first_kernel, width),
        out_shape=jax.ShapeDtypeStruct((sx, sy, ROWS * groups // 2, LANES), BF),
        scratch_shapes=[
            pltpu.VMEM((spots, sz + 2 * ROWS - WINDOW + 3, LANES), F32),
            pltpu.VMEM((spots, sz + 12, LANES), F32),
        ],
        name="first_block",
    )(volume, geo, *weights[0])

    index = [lax.axis_index(a) for a in ("gx", "gy", "gz")]
    count = [lax.axis_size(a) for a in ("gx", "gy", "gz")]
    xodd, yodd = index[0] % 2, index[1] % 2

    def cut(v, odd, dim):
        start = jnp.where(odd == 0, SHIFT, 0)
        return lax.dynamic_slice_in_dim(v, start, HIGH, dim)

    def other_core(v):
        return lax.ppermute(v[:, :, -ROWS:, :], "gz", swap_pairs(count[2], 0))

    zown = other_core(packed)
    halves = [0] if count[1] == 2 else [0, 1]
    ys = [lax.ppermute(cut(packed, (yodd + k) % 2, 1), "gy", swap_pairs(count[1], k)) for k in halves]
    zys = [other_core(v) for v in ys]
    wide = jnp.concatenate([packed] + ys, 1)
    xs = [lax.ppermute(cut(wide, (xodd + k) % 2, 0), "gx", swap_pairs(count[0], k)) for k in (0, 1)]
    zxs = [other_core(v) for v in xs]

    flags = jnp.stack(
        [xodd, yodd]
        + [v for i, c in zip(index, count) for v in ((i > 0).astype(jnp.int32), (i < c - 1).astype(jnp.int32))]
    ).astype(jnp.int32)
    side = WINDOW + 2
    vmem = pl.BlockSpec(memory_space=pltpu.VMEM)
    smem = pl.BlockSpec(memory_space=pltpu.SMEM)
    operands = [flags, geo, packed, *ys, *xs, zown, *zys, *zxs, *weights[1], wc, cg]
    return pl.pallas_call(
        functools.partial(second_kernel, width, len(ys)),
        out_shape=jax.ShapeDtypeStruct(volume.shape, volume.dtype),
        in_specs=[smem] + [vmem] * (len(operands) - 1),
        out_specs=vmem,
        scratch_shapes=[
            pltpu.VMEM((groups + 1, EXT, EXT, ROWS, LANES), F32),
            pltpu.VMEM((groups + 1, side, side, ROWS, LANES), F32),
            pltpu.VMEM((side, side, sz + 12, LANES), F32),
        ],
        name="second_block",
    )(*operands)


def solution(mesh):
    placed = (P(("parts", "gx"), "gy", "gz", None), P(), P(), P(), P(), P(), P(), P())
    return jax.shard_map(
        body,
        mesh=mesh,
        in_specs=placed,
        out_specs=P(("parts", "gx"), "gy", "gz", None),
        check_vma=False,
    )
```

```python
import functools

import jax
import jax.numpy as jnp
import numpy as np
from jax import lax
from jax.experimental import pallas as pl
from jax.experimental.pallas import tpu as pltpu
from jax.sharding import PartitionSpec as P

HEADS = 3
WINDOW = 7
SHIFT = 3
LANES = 128
HALF = 64
ROWS = 8
BIG = -1e30
HIGH = WINDOW - SHIFT
EXT = 2 * WINDOW + 1
BF = jnp.bfloat16
F32 = jnp.float32


def mm(a, b):
    return jnp.dot(a, b, preferred_element_type=F32)


def iota(shape, dim):
    return lax.broadcasted_iota(jnp.int32, shape, dim)


def norm_rows(x, gain, keep, width):
    mean = jnp.sum(x, -1, keepdims=True) * (1.0 / width)
    centred = jnp.where(keep, x - mean, 0.0)
    spread = jnp.sum(centred * centred, -1, keepdims=True) * (1.0 / width)
    return centred * lax.rsqrt(spread + 1e-05) * gain


def norm_cols(x, gain, width):
    mean = jnp.sum(x, 0, keepdims=True) * (1.0 / width)
    centred = x - mean
    spread = jnp.sum(centred * centred, 0, keepdims=True) * (1.0 / width)
    return centred * lax.rsqrt(spread + 1e-05) * gain


def gelu(x):
    inner = 0.7978845608028654 * (x + 0.044715 * (x * x * x))
    return (0.5 * x) * (1.0 + jnp.tanh(inner))


def widen(v, lanes):
    w = v.shape[1]
    eye = jnp.where(iota((w, lanes), 0) == iota((w, lanes), 1), 1.0, 0.0).astype(BF)
    return mm(v, eye).astype(BF)


def block_weights(b, wqkv_ref, wproj_ref, wup_ref, wdown_ref, gain_ref):
    wqkv = wqkv_ref[b]
    width, triple = wqkv.shape
    scale = (width // HEADS) ** (-0.5)
    i, j = iota((triple, LANES), 0), iota((triple, LANES), 1)
    take_v = (j < width) & (i == j + 2 * width)
    take_q = (j >= HALF) & (j < HALF + width) & (i == j - HALF)
    place = jnp.where(take_v, 1.0, jnp.where(take_q, scale, 0.0)).astype(BF)
    wvq = mm(wqkv, place).astype(BF)
    o, i = iota((width, triple), 0), iota((width, triple), 1)
    place = jnp.where(i == o + width, 1.0, 0.0).astype(BF)
    wk = lax.dot_general(place, wqkv, (((1,), (1,)), ((), ())), preferred_element_type=F32).astype(BF)
    gains = gain_ref[b]
    diagonal = iota((width, width), 0) == iota((width, width), 1)
    column = jnp.sum(jnp.where(diagonal, gains[0:1], 0.0), 1, keepdims=True)
    return wvq, wk, column, wproj_ref[b], wup_ref[b], wdown_ref[b], gains[1:2]


def make_keys(columns, bias, wts, width):
    wvq, wk, gain = wts[0], wts[1], wts[2]
    normed = norm_cols(columns, gain, width).astype(BF)
    vq = lax.dot_general(normed, wvq, (((0,), (0,)), ((), ())), preferred_element_type=F32)
    kt = mm(wk, normed).astype(BF)
    keys = columns.shape[1]
    top = iota((HALF - width, keys), 0) == 0
    extra = jnp.where(top, bias, 0.0).astype(BF)
    kaug = jnp.concatenate([jnp.zeros((HALF, keys), BF), kt, extra], 0)
    return vq, kaug


def values_of(vq, width):
    return jnp.where(iota(vq.shape, 1) < width, vq, 1.0).astype(BF)


def queries_of(rows, width):
    head_dim = width // HEADS
    lane = iota(rows.shape, 1)
    one = jnp.where(lane == HALF + width, 1.0, 0.0)
    parts = []
    for h in range(HEADS):
        low = HALF + h * head_dim
        parts.append(jnp.where((lane >= low) & (lane < low + head_dim), rows, one))
    return jnp.concatenate(parts, 0).astype(BF)


def attend(queries, kaug, values, width):
    scores = mm(queries, kaug)
    top = jnp.max(scores, -1, keepdims=True)
    weights = jnp.exp(scores - top).astype(BF)
    out = mm(weights, values)
    n = out.shape[0] // HEADS
    head_dim = width // HEADS
    lane = iota((n, LANES), 1)
    lane = jnp.where(lane >= HALF, lane - HALF, lane)
    mixed = out[:n]
    for h in range(1, HEADS):
        mixed = jnp.where(lane >= h * head_dim, out[h * n : (h + 1) * n], mixed)
    return mixed / pltpu.roll(mixed, HALF, 1)


def feed(residual, mixed, wts, width):
    wp, wup, wdown, gain = wts[3:]
    first = (residual[:, :width] + mm(mixed, wp)).astype(BF).astype(F32)
    mean = jnp.sum(first, -1, keepdims=True) * (1.0 / width)
    centred = first - mean
    spread = jnp.sum(centred * centred, -1, keepdims=True) * (1.0 / width)
    normed = (centred * lax.rsqrt(spread + 1e-05) * gain).astype(BF)
    upper = gelu(mm(normed, wup)).astype(BF)
    return (first + mm(upper, wdown)).astype(BF).astype(F32)


def first_kernel(width, vol_ref, geo_ref, wqkv_ref, wproj_ref, wup_ref, wdown_ref, gain_ref, out_ref, raw, tok, qs, ks, vs, mix, done):
    nz = vol_ref.shape[2]
    groups = nz // WINDOW
    spots = WINDOW * WINDOW
    kept = spots - 1
    keys = kept * ROWS
    wts = block_weights(0, wqkv_ref, wproj_ref, wup_ref, wdown_ref, gain_ref)
    raw[...] = jnp.zeros(raw.shape, F32)
    raw[:, 0:nz, 0:width] = vol_ref[...].astype(F32).reshape(spots, nz, width)
    done[...] = jnp.zeros(done.shape, F32)
    bias = jnp.where(geo_ref[8:9, :] < WINDOW, 0.0, BIG)
    for w in range(groups):
        tok[w] = raw[0:kept, WINDOW * w : WINDOW * w + ROWS, :]
        for j in range(WINDOW):
            tok[w, j, WINDOW : WINDOW + 1, :] = raw[kept, WINDOW * w + j : WINDOW * w + j + 1, :]
    for w in range(groups):
        columns = jnp.transpose(tok[w].reshape(keys, LANES))[:width]
        vq, kaug = make_keys(columns, bias, wts, width)
        vs[w] = values_of(vq, width)
        ks[w] = kaug
        qs[w] = queries_of(vq, width)
    for w in range(groups):
        mix[w] = attend(qs[w], ks[w], vs[w], width)
    for w in range(groups):
        out = feed(tok[w].reshape(keys, LANES), mix[w, :, :width].astype(BF), wts, width)
        out = out.reshape(kept, ROWS, width)
        done[0:kept, WINDOW * w : WINDOW * (w + 1), :width] = out[:, :WINDOW, :]
        if w == 0:
            done[0:kept, nz : nz + SHIFT, :width] = out[:, :SHIFT, :]
        for j in range(WINDOW):
            one = out[j, WINDOW : WINDOW + 1, :]
            done[kept, WINDOW * w + j : WINDOW * w + j + 1, :width] = one
            if w == 0 and j < SHIFT:
                done[kept, nz + j : nz + j + 1, :width] = one
    pieces = [done[:, SHIFT + WINDOW * w : SHIFT + WINDOW * w + ROWS, :] for w in range(groups)]
    rolled = [pltpu.roll(p.reshape(spots * ROWS, LANES), HALF, 1).reshape(spots, ROWS, LANES) for p in pieces[1::2]]
    joined = [a + b for a, b in zip(pieces[0::2], rolled)]
    packed = jnp.concatenate(joined, 1).astype(BF)
    out_ref[...] = packed.reshape(WINDOW, WINDOW, ROWS * len(joined), LANES)


BOXES = ((SHIFT, HIGH), (0, HIGH + 1))
COLUMNS = tuple((wx, wy) for wx in range(2) for wy in range(2))


def box_rows(wx, wy):
    return BOXES[wx][1] * BOXES[wy][1] * ROWS


def second_kernel(width, ypieces, flags, geo_ref, own_ref, *refs):
    y_refs = refs[:ypieces]
    xa_ref, xb_ref, zown_ref = refs[ypieces : ypieces + 3]
    zy_refs = refs[ypieces + 3 : 2 * ypieces + 3]
    rest = refs[2 * ypieces + 3 :]
    zxa_ref, zxb_ref, wqkv_ref, wproj_ref, wup_ref, wdown_ref, gain_ref, wconv_ref, cgain_ref, out_ref = rest[:10]
    ext, res, mix, post, grid, wc, ks, vs = rest[10:18]
    qs = rest[18:]
    nz = out_ref.shape[2]
    pairs = own_ref.shape[2] // ROWS
    groups = 2 * pairs + 1
    xeven, yeven = flags[0] == 0, flags[1] == 0
    xlo, xhi, ylo, yhi, zlo, zhi = [flags[i] for i in range(2, 8)]
    spots = WINDOW * WINDOW
    kept = spots - 1
    keys = kept * ROWS
    wts = block_weights(1, wqkv_ref, wproj_ref, wup_ref, wdown_ref, gain_ref)

    ext[...] = jnp.zeros(ext.shape, F32)

    def place(tile, ztile, x, y, nx, ny):
        n = nx * ny
        tile = tile.astype(F32).reshape(n, pairs * ROWS, LANES)
        other = ztile.astype(F32).reshape(n, ROWS, LANES)
        mine = tile[:, (pairs - 1) * ROWS :, :]
        low = iota((n, ROWS, LANES), 1) < HIGH
        upper = iota((n, ROWS, LANES), 2) >= HALF

        def put(slab, v):
            ext[slab, pl.ds(x, nx), pl.ds(y, ny)] = v.reshape(nx, ny, ROWS, LANES)

        for p in range(pairs - 1):
            put(p, tile[:, p * ROWS : (p + 1) * ROWS, :])
        put(pairs - 1, jnp.where(low | ~upper, mine, other))
        put(pairs, jnp.where(low, other, mine))

    far = WINDOW + HIGH
    ya = jnp.where(yeven, far, 0)
    yb = jnp.where(yeven, 0, far)
    xa = jnp.where(xeven, far, 0)
    xb = jnp.where(xeven, 0, far)
    ystarts = [ya, yb][:ypieces]
    place(own_ref[...], zown_ref[...], HIGH, HIGH, WINDOW, WINDOW)
    for r, z, y in zip(y_refs, zy_refs, ystarts):
        place(r[...], z[...], HIGH, y, WINDOW, HIGH)
    for r, z, x in ((xa_ref, zxa_ref, xa), (xb_ref, zxb_ref, xb)):
        place(r[:, :WINDOW], z[:, :WINDOW], x, HIGH, HIGH, WINDOW)
        for i, y in enumerate(ystarts):
            at = WINDOW + i * HIGH
            place(r[:, at : at + HIGH], z[:, at : at + HIGH], x, y, HIGH, HIGH)

    for wx, wy in COLUMNS:
        x0, y0 = WINDOW * wx, WINDOW * wy
        gone = kept * wx
        for slab in range(pairs + 1):
            for j in range(WINDOW):
                to = j + 1 - wx
                ext[slab, x0 + to // WINDOW, y0 + to % WINDOW, WINDOW : WINDOW + 1, :] = ext[
                    slab, x0 + gone // WINDOW, y0 + gone % WINDOW, j : j + 1, :
                ]

    def flag(v):
        return jnp.where(v > 0, 1.0, 0.0)

    nolow = [1.0 - flag(v) for v in (xlo, ylo, zlo)]
    nohigh = [1.0 - flag(v) for v in (xhi, yhi, zhi)]
    for c, (wx, wy) in enumerate(COLUMNS):
        at = 8 * wx
        row, px, py = [geo_ref[at + k : at + k + 1, :] for k in range(3)]
        badx = jnp.where(px < HIGH, nolow[0], 0.0) if wx == 0 else jnp.where(px >= HIGH, nohigh[0], 0.0)
        bady = jnp.where(py < HIGH, nolow[1], 0.0) if wy == 0 else jnp.where(py >= HIGH, nohigh[1], 0.0)
        bad = badx + bady + jnp.where(row < WINDOW, 0.0, 1.0)
        (bx, nx), (by, ny) = BOXES[wx], BOXES[wy]
        offset = sum(box_rows(*COLUMNS[k]) for k in range(c))
        nq = nx * ny * ROWS
        first = ROWS * (1 - wx)
        for slab in range(pairs + 1):
            tokens = ext[slab, WINDOW * wx : WINDOW * (wx + 1), WINDOW * wy : WINDOW * (wy + 1)]
            flat = tokens.reshape(spots * ROWS, LANES)
            turned = jnp.transpose(flat[first : first + keys])
            chosen = tokens[bx : bx + nx, by : by + ny].reshape(nq, LANES)
            for half in range(2):
                if slab == pairs and half == 0:
                    continue
                g = 0 if slab == pairs else 1 + 2 * slab + half
                badz = jnp.zeros_like(bad)
                if g == 0:
                    badz = jnp.where(row < HIGH, nolow[2], 0.0)
                if g == groups - 1:
                    badz = jnp.where(row >= HIGH, nohigh[2], 0.0)
                bias = jnp.where(bad + badz > 0.0, BIG, 0.0)
                vq, kaug = make_keys(turned[HALF * half : HALF * half + width], bias, wts, width)
                vs[c, g] = values_of(vq, width)
                ks[c, g] = kaug
                picked = [
                    vq[ROWS * (WINDOW * x + by) - first : ROWS * (WINDOW * x + by + ny) - first]
                    for x in range(bx, bx + nx)
                ]
                qs[c][g] = queries_of(jnp.concatenate(picked, 0), width)
                res[g, offset : offset + nq] = pltpu.roll(chosen, HALF, 1) if half else chosen

    def attention(g, carry):
        for c, (wx, wy) in enumerate(COLUMNS):
            offset = sum(box_rows(*COLUMNS[k]) for k in range(c))
            mix[g, offset : offset + box_rows(wx, wy)] = attend(qs[c][g], ks[c, g], vs[c, g], width)
        return carry

    lax.fori_loop(0, groups, attention, 0)

    def feeding(g, carry):
        out = feed(res[g], mix[g, :, :width].astype(BF), wts, width)
        lowbad = jnp.where(g == 0, nolow[2], 0.0)
        highbad = jnp.where(g == groups - 1, nohigh[2], 0.0)
        offset = 0
        for wx, wy in COLUMNS:
            (bx, nx), (by, ny) = BOXES[wx], BOXES[wy]
            shape = (nx, ny, ROWS, width)
            qx, qy, qr = iota(shape, 0) + bx, iota(shape, 1) + by, iota(shape, 2)
            outx = jnp.where(qx < HIGH, nolow[0], 0.0) if wx == 0 else jnp.where(qx >= HIGH, nohigh[0], 0.0)
            outy = jnp.where(qy < HIGH, nolow[1], 0.0) if wy == 0 else jnp.where(qy >= HIGH, nohigh[1], 0.0)
            outz = jnp.where(qr < HIGH, lowbad, highbad)
            part = out[offset : offset + nx * ny * ROWS].reshape(shape)
            offset += nx * ny * ROWS
            part = jnp.where(outx + outy + outz > 0.0, 0.0, part)
            post[g, HIGH * wx : HIGH * wx + nx, HIGH * wy : HIGH * wy + ny, :, :width] = part
        return carry

    post[...] = jnp.zeros(post.shape, F32)
    lax.fori_loop(0, groups, feeding, 0)

    wc[...] = jnp.zeros(wc.shape, BF)
    for dx in range(3):
        total = None
        for dy in range(3):
            taps = wconv_ref[9 * dx + 3 * dy : 9 * dx + 3 * dy + 3].reshape(3 * width, width)
            i, j = iota((width, 4 * HALF), 0), iota((width, 4 * HALF), 1)
            place = jnp.where(j == i + HALF * dy, 1.0, 0.0).astype(BF)
            part = mm(taps, place)
            total = part if total is None else total + part
        for dz in range(3):
            wc[dx, HALF * dz : HALF * dz + width] = total[width * dz : width * (dz + 1)].astype(BF)

    side = WINDOW + 2
    for g in range(groups):
        grid[:, :, WINDOW * g : WINDOW * (g + 1), :] = post[g, :, :, :WINDOW, :]
    padded = -(-nz // 16) * 16
    cg = cgain_ref[...]

    def lhs(x):
        taps = [grid[x, :, SHIFT + d : SHIFT + d + padded, :].reshape(side * padded, LANES) for d in range(3)]
        return jnp.concatenate([taps[0] + pltpu.roll(taps[1], HALF, 1), taps[2]], 1).astype(BF)

    rows = [lhs(x) for x in range(side)]
    for x in range(WINDOW):
        acc = mm(rows[x], wc[0]) + mm(rows[x + 1], wc[1]) + mm(rows[x + 2], wc[2])
        near, second = acc[:, :LANES], acc[:, LANES:]
        turned = pltpu.roll(near, HALF, 1)
        total = near[: WINDOW * padded] + turned[padded : (WINDOW + 1) * padded] + second[2 * padded :]
        total = total[:, :width]
        mean = jnp.sum(total, -1, keepdims=True) * (1.0 / width)
        centred = total - mean
        spread = jnp.sum(centred * centred, -1, keepdims=True) * (1.0 / width)
        normed = centred * lax.rsqrt(spread + 1e-05) * cg
        active = jnp.where(normed >= 0.0, normed, 0.01 * normed)
        centre = grid[x + 1, 1 : 1 + WINDOW, HIGH : HIGH + padded, :].reshape(WINDOW * padded, LANES)
        result = (centre[:, :width] + active).reshape(WINDOW, padded, width).astype(BF)
        out_ref[x] = result[:, :nz]


def geometry():
    kept = WINDOW * WINDOW - 1
    geo = np.full((16, kept * ROWS), WINDOW, np.float32)
    for v in range(2):
        gone = kept * v
        for i in range(kept):
            spot = i + 1 - v
            for r in range(ROWS):
                t = i * ROWS + r
                if r < WINDOW:
                    geo[8 * v : 8 * v + 3, t] = r, spot // WINDOW, spot % WINDOW
                elif i < WINDOW:
                    geo[8 * v : 8 * v + 3, t] = i, gone // WINDOW, gone % WINDOW
                else:
                    geo[8 * v + 1 : 8 * v + 3, t] = spot // WINDOW, spot % WINDOW
    return jnp.asarray(geo)


def swap_pairs(count, odd):
    to = list(range(count))
    for i in range(odd, count - 1, 2):
        to[i], to[i + 1] = i + 1, i
    return list(enumerate(to))


def body(volume, w_qkv, w_proj, w_up, w_down, norm_gain, conv_weight, conv_gain):
    sx, sy, sz, width = volume.shape
    spots = sx * sy
    groups = sz // WINDOW
    geo = geometry()
    keys = (spots - 1) * ROWS
    weights = (w_qkv, w_proj, w_up, w_down, norm_gain)

    packed = pl.pallas_call(
        functools.partial(first_kernel, width),
        out_shape=jax.ShapeDtypeStruct((sx, sy, ROWS * groups // 2, LANES), BF),
        scratch_shapes=[
            pltpu.VMEM((spots, sz + 12, LANES), F32),
            pltpu.VMEM((groups, spots - 1, ROWS, LANES), F32),
            pltpu.VMEM((groups, HEADS * keys, LANES), BF),
            pltpu.VMEM((groups, LANES, keys), BF),
            pltpu.VMEM((groups, keys, LANES), BF),
            pltpu.VMEM((groups, keys, LANES), F32),
            pltpu.VMEM((spots, sz + 12, LANES), F32),
        ],
        name="first_block",
    )(volume, geo, *weights)

    index = [lax.axis_index(a) for a in ("gx", "gy", "gz")]
    count = [lax.axis_size(a) for a in ("gx", "gy", "gz")]
    xodd, yodd = index[0] % 2, index[1] % 2

    def cut(v, odd, dim):
        start = jnp.where(odd == 0, SHIFT, 0)
        return lax.dynamic_slice_in_dim(v, start, HIGH, dim)

    def other_core(v):
        return lax.ppermute(v[:, :, -ROWS:, :], "gz", swap_pairs(count[2], 0))

    zown = other_core(packed)
    halves = [0] if count[1] == 2 else [0, 1]
    ys = [lax.ppermute(cut(packed, (yodd + k) % 2, 1), "gy", swap_pairs(count[1], k)) for k in halves]
    zys = [other_core(v) for v in ys]
    wide = jnp.concatenate([packed] + ys, 1)
    xs = [lax.ppermute(cut(wide, (xodd + k) % 2, 0), "gx", swap_pairs(count[0], k)) for k in (0, 1)]
    zxs = [other_core(v) for v in xs]

    flags = jnp.stack(
        [xodd, yodd]
        + [v for i, c in zip(index, count) for v in ((i > 0).astype(jnp.int32), (i < c - 1).astype(jnp.int32))]
    ).astype(jnp.int32)
    side = WINDOW + 2
    rows = sum(box_rows(*c) for c in COLUMNS)
    vmem = pl.BlockSpec(memory_space=pltpu.VMEM)
    smem = pl.BlockSpec(memory_space=pltpu.SMEM)
    operands = [flags, geo, packed, *ys, *xs, zown, *zys, *zxs, *weights, conv_weight, conv_gain[None, :]]
    return pl.pallas_call(
        functools.partial(second_kernel, width, len(ys)),
        out_shape=jax.ShapeDtypeStruct(volume.shape, volume.dtype),
        in_specs=[smem] + [vmem] * (len(operands) - 1),
        out_specs=vmem,
        scratch_shapes=[
            pltpu.VMEM((groups // 2 + 1, EXT, EXT, ROWS, LANES), F32),
            pltpu.VMEM((groups + 1, rows, LANES), F32),
            pltpu.VMEM((groups + 1, rows, LANES), F32),
            pltpu.VMEM((groups + 1, side, side, ROWS, LANES), F32),
            pltpu.VMEM((side, side, sz + 12, LANES), F32),
            pltpu.VMEM((3, 4 * HALF, 4 * HALF), BF),
            pltpu.VMEM((len(COLUMNS), groups + 1, LANES, keys), BF),
            pltpu.VMEM((len(COLUMNS), groups + 1, keys, LANES), BF),
        ]
        + [pltpu.VMEM((groups + 1, HEADS * box_rows(*c), LANES), BF) for c in COLUMNS],
        name="second_block",
    )(*operands)


def solution(mesh):
    placed = (P(("parts", "gx"), "gy", "gz", None), P(), P(), P(), P(), P(), P(), P())
    return jax.shard_map(
        body,
        mesh=mesh,
        in_specs=placed,
        out_specs=P(("parts", "gx"), "gy", "gz", None),
        check_vma=False,
    )
```

```python
import functools

import jax
import jax.numpy as jnp
import numpy as np
from jax import lax
from jax.experimental import pallas as pl
from jax.experimental.pallas import tpu as pltpu
from jax.sharding import PartitionSpec as P

HEADS = 3
WINDOW = 7
SHIFT = 3
LANES = 128
HALF = 64
ROWS = 8
BIG = -1e30
HIGH = WINDOW - SHIFT
EXT = 2 * WINDOW + 1
BF = jnp.bfloat16
F32 = jnp.float32


def mm(a, b):
    return jnp.dot(a, b, preferred_element_type=F32)


def iota(shape, dim):
    return lax.broadcasted_iota(jnp.int32, shape, dim)


def norm_cols(x, gain, width):
    mean = jnp.sum(x, 0, keepdims=True) * (1.0 / width)
    centred = x - mean
    spread = jnp.sum(centred * centred, 0, keepdims=True) * (1.0 / width)
    return centred * lax.rsqrt(spread + 1e-05) * gain


def gelu(x):
    inner = 0.7978845608028654 * (x + 0.044715 * (x * x * x))
    return (0.5 * x) * (1.0 + jnp.tanh(inner))


def block_weights(b, wqkv_ref, wproj_ref, wup_ref, wdown_ref, gain_ref):
    wqkv = wqkv_ref[b]
    width, triple = wqkv.shape
    scale = (width // HEADS) ** (-0.5)
    i, j = iota((triple, LANES), 0), iota((triple, LANES), 1)
    take_v = (j < width) & (i == j + 2 * width)
    take_q = (j >= HALF) & (j < HALF + width) & (i == j - HALF)
    place = jnp.where(take_v, 1.0, jnp.where(take_q, scale, 0.0)).astype(BF)
    wvq = mm(wqkv, place).astype(BF)
    o, i = iota((width, triple), 0), iota((width, triple), 1)
    place = jnp.where(i == o + width, 1.0, 0.0).astype(BF)
    wk = lax.dot_general(place, wqkv, (((1,), (1,)), ((), ())), preferred_element_type=F32).astype(BF)
    gains = gain_ref[b]
    diagonal = iota((width, width), 0) == iota((width, width), 1)
    column = jnp.sum(jnp.where(diagonal, gains[0:1], 0.0), 1, keepdims=True)
    return wvq, wk, column, wproj_ref[b], wup_ref[b], wdown_ref[b], gains[1:2]


def make_keys(columns, bias, wts, width):
    wvq, wk, gain = wts[0], wts[1], wts[2]
    normed = norm_cols(columns, gain, width).astype(BF)
    vq = lax.dot_general(normed, wvq, (((0,), (0,)), ((), ())), preferred_element_type=F32)
    kt = mm(wk, normed).astype(BF)
    keys = columns.shape[1]
    top = iota((HALF - width, keys), 0) == 0
    extra = jnp.where(top, bias, 0.0).astype(BF)
    kaug = jnp.concatenate([jnp.zeros((HALF, keys), BF), kt, extra], 0)
    return vq, kaug


def values_of(vq, width):
    return jnp.where(iota(vq.shape, 1) < width, vq, 1.0).astype(BF)


def queries_of(rows, width):
    head_dim = width // HEADS
    lane = iota(rows.shape, 1)
    one = jnp.where(lane == HALF + width, 1.0, 0.0)
    parts = []
    for h in range(HEADS):
        low = HALF + h * head_dim
        parts.append(jnp.where((lane >= low) & (lane < low + head_dim), rows, one))
    spare = -len(parts) * rows.shape[0] % 32
    if spare:
        parts.append(jnp.zeros((spare, LANES), F32))
    return jnp.concatenate(parts, 0).astype(BF)


def attend(queries, kaug, values, width, n):
    half = queries.shape[0] // 2
    wide = 2 * LANES
    pair = jnp.concatenate([queries[:half], queries[half:]], 1)
    last = kaug[:, wide:]
    nil = jnp.zeros_like(last)
    both = jnp.concatenate([jnp.concatenate([last, nil], 1), jnp.concatenate([nil, last], 1)], 0)
    front = mm(queries, kaug[:, :wide])
    back = mm(pair, both)
    back = jnp.concatenate([back[:, :LANES], back[:, LANES:]], 0)
    left, right = front[:, :LANES], front[:, LANES:]
    top = jnp.max(jnp.maximum(jnp.maximum(left, right), back), -1, keepdims=True)
    first = jnp.concatenate([jnp.exp(left - top), jnp.exp(right - top)], 1).astype(BF)
    back = jnp.exp(back - top).astype(BF)
    pair = jnp.concatenate([back[:half], back[half:]], 1)
    last = values[wide:]
    nil = jnp.zeros_like(last)
    both = jnp.concatenate([jnp.concatenate([last, nil], 1), jnp.concatenate([nil, last], 1)], 0)
    tail = mm(pair, both)
    out = mm(first, values[:wide]) + jnp.concatenate([tail[:, :LANES], tail[:, LANES:]], 0)
    head_dim = width // HEADS
    lane = iota((n, LANES), 1)
    lane = jnp.where(lane >= HALF, lane - HALF, lane)
    mixed = out[:n]
    for h in range(1, HEADS):
        mixed = jnp.where(lane >= h * head_dim, out[h * n : (h + 1) * n], mixed)
    return mixed / pltpu.roll(mixed, HALF, 1)


def feed(residual, mixed, wts, width):
    wp, wup, wdown, gain = wts[3:]
    first = (residual[:, :width] + mm(mixed, wp)).astype(BF).astype(F32)
    mean = jnp.sum(first, -1, keepdims=True) * (1.0 / width)
    centred = first - mean
    spread = jnp.sum(centred * centred, -1, keepdims=True) * (1.0 / width)
    normed = (centred * lax.rsqrt(spread + 1e-05) * gain).astype(BF)
    upper = gelu(mm(normed, wup)).astype(BF)
    down = lax.dot_general(upper, wdown, (((1,), (1,)), ((), ())), preferred_element_type=F32)
    return (first + down).astype(BF).astype(F32)


def first_kernel(
    width, vol_ref, geo_ref, wqkv_ref, wproj_ref, wup_ref, wdown_ref, gain_ref, out_ref, *refs
):
    y_refs = refs[:-7]
    raw, tok, qs, ks, vs, mix, done = refs[-7:]
    nz = vol_ref.shape[2]
    groups = nz // WINDOW
    spots = WINDOW * WINDOW
    kept = spots - 1
    keys = kept * ROWS
    wts = block_weights(0, wqkv_ref, wproj_ref, wup_ref, wdown_ref, gain_ref)
    raw[:, nz:, :] = jnp.zeros((spots, raw.shape[1] - nz, LANES), F32)
    raw[:, 0:nz, 0:width] = vol_ref[...].astype(F32).reshape(spots, nz, width)
    done[...] = jnp.zeros(done.shape, F32)
    bias = jnp.where(geo_ref[8:9, :] < WINDOW, 0.0, BIG)

    def make(w):
        tok[w] = raw[0:kept, WINDOW * w : WINDOW * w + ROWS, :]
        for j in range(WINDOW):
            tok[w, j, WINDOW : WINDOW + 1, :] = raw[kept, WINDOW * w + j : WINDOW * w + j + 1, :]
        columns = jnp.transpose(tok[w].reshape(keys, LANES))[:width]
        vq, kaug = make_keys(columns, bias, wts, width)
        vs[w] = values_of(vq, width)
        ks[w] = kaug
        qs[w] = queries_of(vq, width)

    def finish(w):
        out = feed(tok[w].reshape(keys, LANES), mix[w, :, :width].astype(BF), wts, width)
        out = out.reshape(kept, ROWS, width)
        done[0:kept, WINDOW * w : WINDOW * (w + 1), :width] = out[:, :WINDOW, :]
        if w == 0:
            done[0:kept, nz : nz + SHIFT, :width] = out[:, :SHIFT, :]
        for j in range(WINDOW):
            one = out[j, WINDOW : WINDOW + 1, :]
            done[kept, WINDOW * w + j : WINDOW * w + j + 1, :width] = one
            if w == 0 and j < SHIFT:
                done[kept, nz + j : nz + j + 1, :width] = one

    make(0)
    for w in range(groups):
        if w + 1 < groups:
            make(w + 1)
        if w > 0:
            finish(w - 1)
        mix[w] = attend(qs[w], ks[w], vs[w], width, keys)
    finish(groups - 1)
    pieces = [done[:, SHIFT + WINDOW * w : SHIFT + WINDOW * w + ROWS, :] for w in range(groups)]
    rolled = [pltpu.roll(p.reshape(spots * ROWS, LANES), HALF, 1).reshape(spots, ROWS, LANES) for p in pieces[1::2]]
    joined = [a + b for a, b in zip(pieces[0::2], rolled)]
    packed = jnp.concatenate(joined, 1).astype(BF)
    out_ref[...] = packed.reshape(WINDOW, WINDOW, ROWS * len(joined), LANES)
    yodd = lax.axis_index("gy") % 2
    for k, y_ref in enumerate(y_refs):
        start = jnp.where((yodd + k) % 2 == 0, SHIFT, 0)
        y_ref[...] = out_ref[:, pl.ds(start, HIGH)]


BOXES = ((SHIFT, HIGH), (0, HIGH + 1))
COLUMNS = tuple((wx, wy) for wx in range(2) for wy in range(2))


def box_rows(wx, wy):
    return BOXES[wx][1] * BOXES[wy][1] * ROWS


def second_kernel(width, ypieces, geo_ref, own_ref, *refs):
    y_refs = refs[:ypieces]
    xa_ref, xb_ref, zown_ref = refs[ypieces : ypieces + 3]
    zy_refs = refs[ypieces + 3 : 2 * ypieces + 3]
    rest = refs[2 * ypieces + 3 :]
    zxa_ref, zxb_ref, wqkv_ref, wproj_ref, wup_ref, wdown_ref, gain_ref, wconv_ref, cgain_ref, out_ref = rest[:10]
    ext, res, mix, grid, wc, tot, ks, vs = rest[10:18]
    qs = rest[18:]
    nz = out_ref.shape[2]
    pairs = own_ref.shape[2] // ROWS
    groups = 2 * pairs + 1
    index = [lax.axis_index(a) for a in ("gx", "gy", "gz")]
    count = [lax.axis_size(a) for a in ("gx", "gy", "gz")]
    xeven, yeven = index[0] % 2 == 0, index[1] % 2 == 0
    spots = WINDOW * WINDOW
    kept = spots - 1
    keys = kept * ROWS
    wts = block_weights(1, wqkv_ref, wproj_ref, wup_ref, wdown_ref, gain_ref)

    def place(tile, ztile, x, y, nx, ny):
        n = nx * ny
        tile = tile.astype(F32).reshape(n, pairs * ROWS, LANES)
        other = ztile.astype(F32).reshape(n, ROWS, LANES)
        mine = tile[:, (pairs - 1) * ROWS :, :]
        low = iota((n, ROWS, LANES), 1) < HIGH
        upper = iota((n, ROWS, LANES), 2) >= HALF

        def put(slab, v):
            ext[slab, pl.ds(x, nx), pl.ds(y, ny)] = v.reshape(nx, ny, ROWS, LANES)

        for p in range(pairs - 1):
            put(p, tile[:, p * ROWS : (p + 1) * ROWS, :])
        put(pairs - 1, jnp.where(low | ~upper, mine, other))
        put(pairs, jnp.where(low, other, mine))

    far = WINDOW + HIGH
    ya = jnp.where(yeven, far, 0)
    yb = jnp.where(yeven, 0, far)
    xa = jnp.where(xeven, far, 0)
    xb = jnp.where(xeven, 0, far)
    ystarts = [ya, yb][:ypieces]
    if ypieces == 1:
        ext[:, :, pl.ds(yb, HIGH)] = jnp.zeros((pairs + 1, EXT, HIGH, ROWS, LANES), F32)
    place(own_ref[...], zown_ref[...], HIGH, HIGH, WINDOW, WINDOW)
    for r, z, y in zip(y_refs, zy_refs, ystarts):
        place(r[...], z[...], HIGH, y, WINDOW, HIGH)
    for r, z, x in ((xa_ref, zxa_ref, xa), (xb_ref, zxb_ref, xb)):
        place(r[:, :WINDOW], z[:, :WINDOW], x, HIGH, HIGH, WINDOW)
        for i, y in enumerate(ystarts):
            at = WINDOW + i * HIGH
            place(r[:, at : at + HIGH], z[:, at : at + HIGH], x, y, HIGH, HIGH)

    for wx, wy in COLUMNS:
        x0, y0 = WINDOW * wx, WINDOW * wy
        gone = kept * wx
        for slab in range(pairs + 1):
            for j in range(WINDOW):
                to = j + 1 - wx
                ext[slab, x0 + to // WINDOW, y0 + to % WINDOW, WINDOW : WINDOW + 1, :] = ext[
                    slab, x0 + gone // WINDOW, y0 + gone % WINDOW, j : j + 1, :
                ]

    nolow = [jnp.where(i > 0, 0.0, 1.0) for i in index]
    nohigh = [jnp.where(i < c - 1, 0.0, 1.0) for i, c in zip(index, count)]
    grid[...] = jnp.zeros(grid.shape, F32)
    offsets = [sum(box_rows(*COLUMNS[k]) for k in range(c)) for c in range(len(COLUMNS))]

    def make(slab, c):
        wx, wy = COLUMNS[c]
        row, px, py = [geo_ref[8 * wx + k : 8 * wx + k + 1, :] for k in range(3)]
        badx = jnp.where(px < HIGH, nolow[0], 0.0) if wx == 0 else jnp.where(px >= HIGH, nohigh[0], 0.0)
        bady = jnp.where(py < HIGH, nolow[1], 0.0) if wy == 0 else jnp.where(py >= HIGH, nohigh[1], 0.0)
        bad = badx + bady + jnp.where(row < WINDOW, 0.0, 1.0)
        (bx, nx), (by, ny) = BOXES[wx], BOXES[wy]
        nq = nx * ny * ROWS
        first = ROWS * (1 - wx)
        tokens = ext[slab, WINDOW * wx : WINDOW * (wx + 1), WINDOW * wy : WINDOW * (wy + 1)]
        flat = tokens.reshape(spots * ROWS, LANES)
        turned = jnp.transpose(flat[first : first + keys])
        chosen = tokens[bx : bx + nx, by : by + ny].reshape(nq, LANES)
        for half in range(2):
            if slab == pairs and half == 0:
                continue
            g = 0 if slab == pairs else 1 + 2 * slab + half
            badz = jnp.zeros_like(bad)
            if g == 0:
                badz = jnp.where(row < HIGH, nolow[2], 0.0)
            if g == groups - 1:
                badz = jnp.where(row >= HIGH, nohigh[2], 0.0)
            bias = jnp.where(bad + badz > 0.0, BIG, 0.0)
            vq, kaug = make_keys(turned[HALF * half : HALF * half + width], bias, wts, width)
            vs[c, g] = values_of(vq, width)
            ks[c, g] = kaug
            picked = [
                vq[ROWS * (WINDOW * x + by) - first : ROWS * (WINDOW * x + by + ny) - first] for x in range(bx, bx + nx)
            ]
            qs[c][g] = queries_of(jnp.concatenate(picked, 0), width)
            res[g, offsets[c] : offsets[c] + nq] = pltpu.roll(chosen, HALF, 1) if half else chosen

    def finish(g, c):
        wx, wy = COLUMNS[c]
        (bx, nx), (by, ny) = BOXES[wx], BOXES[wy]
        span = slice(offsets[c], offsets[c] + nx * ny * ROWS)
        out = feed(res[g, span], mix[g, span, :width].astype(BF), wts, width)
        shape = (nx, ny, ROWS, width)
        qx, qy, qr = iota(shape, 0) + bx, iota(shape, 1) + by, iota(shape, 2)
        outside = jnp.where(qx < HIGH, nolow[0], 0.0) if wx == 0 else jnp.where(qx >= HIGH, nohigh[0], 0.0)
        outside += jnp.where(qy < HIGH, nolow[1], 0.0) if wy == 0 else jnp.where(qy >= HIGH, nohigh[1], 0.0)
        if g == 0:
            outside += jnp.where(qr < HIGH, nolow[2], 0.0)
        if g == groups - 1:
            outside += jnp.where(qr >= HIGH, nohigh[2], 0.0)
        part = jnp.where(outside > 0.0, 0.0, out.reshape(shape))
        x0, y0, z0 = HIGH * wx, HIGH * wy, WINDOW * g
        grid[x0 : x0 + nx, y0 : y0 + ny, z0 : z0 + WINDOW, :width] = part[:, :, :WINDOW]

    cols = range(len(COLUMNS))
    slabs = [pairs] + list(range(pairs))
    for c in cols:
        make(slabs[0], c)
    for g in range(groups):
        for c in cols:
            if g + 1 < len(slabs):
                make(slabs[g + 1], c)
            if g > 0:
                finish(g - 1, c)
            at = offsets[c]
            n = box_rows(*COLUMNS[c])
            mix[g, at : at + n] = attend(qs[c][g], ks[c, g], vs[c, g], width, n)
    for c in cols:
        finish(groups - 1, c)

    wc[...] = jnp.zeros(wc.shape, BF)
    for dx in range(3):
        total = None
        for dy in range(3):
            taps = wconv_ref[9 * dx + 3 * dy : 9 * dx + 3 * dy + 3].reshape(3 * width, width)
            i, j = iota((width, 4 * HALF), 0), iota((width, 4 * HALF), 1)
            place = jnp.where(j == i + HALF * dy, 1.0, 0.0).astype(BF)
            part = mm(taps, place)
            total = part if total is None else total + part
        for dz in range(3):
            at = 4 * HALF * dx + HALF * dz
            wc[at : at + width] = total[width * dz : width * (dz + 1)].astype(BF)

    side = WINDOW + 2
    padded = -(-nz // 16) * 16

    def lhs(x):
        taps = [grid[x, :, SHIFT + d : SHIFT + d + padded, :].reshape(side * padded, LANES) for d in range(3)]
        return jnp.concatenate([taps[0] + pltpu.roll(taps[1], HALF, 1), taps[2]], 1).astype(BF)

    rows = [lhs(x) for x in range(side)]
    acc = mm(jnp.concatenate([jnp.concatenate(rows[x : x + 3], 1) for x in range(WINDOW)], 0), wc[...])
    strip = WINDOW * padded
    for x in range(WINDOW):
        part = acc[x * side * padded : (x + 1) * side * padded]
        near, second = part[:, :LANES], part[:, LANES:]
        turned = pltpu.roll(near[padded : (WINDOW + 1) * padded], HALF, 1)
        tot[x * strip : (x + 1) * strip] = near[:strip] + turned + second[2 * padded :]
    tot[WINDOW * strip :] = jnp.zeros((tot.shape[0] - WINDOW * strip, LANES), F32)
    diagonal = iota((width, width), 0) == iota((width, width), 1)
    cg = jnp.sum(jnp.where(diagonal, cgain_ref[...], 0.0), 1, keepdims=True)
    normed = norm_cols(jnp.transpose(tot[...])[:width], cg, width)
    active = jnp.where(normed >= 0.0, normed, 0.01 * normed)
    active = jnp.transpose(jnp.concatenate([active, jnp.zeros((LANES - width, tot.shape[0]), F32)], 0))
    for x in range(WINDOW):
        centre = grid[x + 1, 1 : 1 + WINDOW, HIGH : HIGH + padded, :].reshape(strip, LANES)
        result = (centre + active[x * strip : (x + 1) * strip]).reshape(WINDOW, padded, LANES).astype(BF)
        out_ref[x] = result[:, :nz, :width]


def geometry():
    kept = WINDOW * WINDOW - 1
    geo = np.full((16, kept * ROWS), WINDOW, np.float32)
    for v in range(2):
        gone = kept * v
        for i in range(kept):
            spot = i + 1 - v
            for r in range(ROWS):
                t = i * ROWS + r
                if r < WINDOW:
                    geo[8 * v : 8 * v + 3, t] = r, spot // WINDOW, spot % WINDOW
                elif i < WINDOW:
                    geo[8 * v : 8 * v + 3, t] = i, gone // WINDOW, gone % WINDOW
                else:
                    geo[8 * v + 1 : 8 * v + 3, t] = spot // WINDOW, spot % WINDOW
    return jnp.asarray(geo)


def exchange(v, axis, odd):
    count, cores = lax.axis_size(axis), lax.axis_size("gz")
    pairs = []
    for i in range(count):
        low = i - (i - odd) % 2
        for c in range(cores):
            if low < 0 or low + 1 >= count:
                to = (i, c ^ 1 if c ^ 1 < cores else c)
            else:
                to = (low + 1 if i == low else low, c)
            pairs.append((i * cores + c, to[0] * cores + to[1]))
    return lax.ppermute(v, (axis, "gz"), pairs)


def body(volume, w_qkv, w_proj, w_up, w_down, norm_gain, conv_weight, conv_gain):
    sx, sy, sz, width = volume.shape
    spots = sx * sy
    groups = sz // WINDOW
    geo = geometry()
    keys = (spots - 1) * ROWS
    weights = (w_qkv, w_proj, w_up, jnp.swapaxes(w_down, 1, 2), norm_gain)
    halves = [0] if lax.axis_size("gy") == 2 else [0, 1]
    tall = ROWS * groups // 2

    packed, *cuts = pl.pallas_call(
        functools.partial(first_kernel, width),
        out_shape=[jax.ShapeDtypeStruct((sx, sy, tall, LANES), BF)]
        + [jax.ShapeDtypeStruct((sx, HIGH, tall, LANES), BF) for _ in halves],
        scratch_shapes=[
            pltpu.VMEM((spots, sz + 12, LANES), F32),
            pltpu.VMEM((groups, spots - 1, ROWS, LANES), F32),
            pltpu.VMEM((groups, HEADS * keys, LANES), BF),
            pltpu.VMEM((groups, LANES, keys), BF),
            pltpu.VMEM((groups, keys, LANES), BF),
            pltpu.VMEM((groups, keys, LANES), F32),
            pltpu.VMEM((spots, sz + 12, LANES), F32),
        ],
        compiler_params=pltpu.CompilerParams(vmem_limit_bytes=24 << 20),
        name="first_block",
    )(volume, geo, *weights)

    xodd = lax.axis_index("gx") % 2

    def cut(v, odd):
        return lax.dynamic_slice_in_dim(v, jnp.where(odd == 0, SHIFT, 0), HIGH, 0)

    def other_core(v):
        return lax.ppermute(v[:, :, -ROWS:, :], "gz", [(0, 1), (1, 0)])

    zown = other_core(packed)
    ys = [exchange(v, "gy", k) for k, v in zip(halves, cuts)]
    zys = [other_core(v) for v in ys]
    wide = jnp.concatenate([packed] + ys, 1)
    xs = [exchange(cut(wide, (xodd + k) % 2), "gx", k) for k in (0, 1)]
    zxs = [other_core(v) for v in xs]

    side = WINDOW + 2
    rows = sum(box_rows(*c) for c in COLUMNS)
    strip = WINDOW * -(-sz // 16) * 16
    operands = [geo, packed, *ys, *xs, zown, *zys, *zxs, *weights, conv_weight, conv_gain[None, :]]
    return pl.pallas_call(
        functools.partial(second_kernel, width, len(ys)),
        out_shape=jax.ShapeDtypeStruct(volume.shape, volume.dtype),
        scratch_shapes=[
            pltpu.VMEM((groups // 2 + 1, EXT, EXT, ROWS, LANES), F32),
            pltpu.VMEM((groups + 1, rows, LANES), F32),
            pltpu.VMEM((groups + 1, rows, LANES), F32),
            pltpu.VMEM((side, side, sz + 12, LANES), F32),
            pltpu.VMEM((3 * 4 * HALF, 4 * HALF), BF),
            pltpu.VMEM((-(-WINDOW * strip // LANES) * LANES, LANES), F32),
            pltpu.VMEM((len(COLUMNS), groups + 1, LANES, keys), BF),
            pltpu.VMEM((len(COLUMNS), groups + 1, keys, LANES), BF),
        ]
        + [pltpu.VMEM((groups + 1, -(-HEADS * box_rows(*c) // 32) * 32, LANES), BF) for c in COLUMNS],
        compiler_params=pltpu.CompilerParams(vmem_limit_bytes=44 << 20),
        name="second_block",
    )(*operands)


def solution(mesh):
    placed = (P(("parts", "gx"), "gy", "gz", None), P(), P(), P(), P(), P(), P(), P())
    return jax.shard_map(
        body,
        mesh=mesh,
        in_specs=placed,
        out_specs=P(("parts", "gx"), "gy", "gz", None),
        check_vma=False,
    )
```

```python
import functools

import jax
import jax.numpy as jnp
import numpy as np
from jax import lax
from jax.experimental import pallas as pl
from jax.experimental.pallas import tpu as pltpu
from jax.sharding import PartitionSpec as P

HEADS = 3
WINDOW = 7
SHIFT = 3
LANES = 128
HALF = 64
ROWS = 8
BIG = -1e30
HIGH = WINDOW - SHIFT
EXT = 2 * WINDOW + 1
BF = jnp.bfloat16
F32 = jnp.float32


def mm(a, b):
    return jnp.dot(a, b, preferred_element_type=F32)


def iota(shape, dim):
    return lax.broadcasted_iota(jnp.int32, shape, dim)


def norm_cols(x, gain, width):
    mean = jnp.sum(x, 0, keepdims=True) * (1.0 / width)
    centred = x - mean
    spread = jnp.sum(centred * centred, 0, keepdims=True) * (1.0 / width)
    return centred * lax.rsqrt(spread + 1e-05) * gain


def twice_gelu(x):
    inner = x * (0.7978845608028654 + (0.7978845608028654 * 0.044715) * (x * x))
    return x + x * jnp.tanh(inner)


def block_weights(b, wqkv_ref, wproj_ref, wup_ref, wdown_ref, gain_ref):
    wqkv = wqkv_ref[b]
    width, triple = wqkv.shape
    scale = (width // HEADS) ** (-0.5)
    i, j = iota((triple, LANES), 0), iota((triple, LANES), 1)
    take_v = (j < width) & (i == j + 2 * width)
    take_q = (j >= HALF) & (j < HALF + width) & (i == j - HALF)
    place = jnp.where(take_v, 1.0, jnp.where(take_q, scale, 0.0)).astype(BF)
    wvq = mm(wqkv, place).astype(BF)
    o, i = iota((width, triple), 0), iota((width, triple), 1)
    place = jnp.where(i == o + width, 1.0, 0.0).astype(BF)
    wk = lax.dot_general(place, wqkv, (((1,), (1,)), ((), ())), preferred_element_type=F32).astype(BF)
    gains = gain_ref[b]
    diagonal = iota((width, width), 0) == iota((width, width), 1)
    column = jnp.sum(jnp.where(diagonal, gains[0:1], 0.0), 1, keepdims=True)
    return wvq, wk, column, wproj_ref[b], wup_ref[b], wdown_ref[b] * jnp.asarray(0.5, BF), gains[1:2]


def make_keys(columns, bias, wts, width):
    wvq, wk, gain = wts[0], wts[1], wts[2]
    normed = norm_cols(columns, gain, width).astype(BF)
    vq = lax.dot_general(normed, wvq, (((0,), (0,)), ((), ())), preferred_element_type=F32)
    kt = mm(wk, normed).astype(BF)
    keys = columns.shape[1]
    top = iota((HALF - width, keys), 0) == 0
    extra = jnp.where(top, bias, 0.0).astype(BF)
    kaug = jnp.concatenate([jnp.zeros((HALF, keys), BF), kt, extra], 0)
    return vq, kaug


def values_of(vq, width):
    return jnp.where(iota(vq.shape, 1) < width, vq, 1.0).astype(BF)


def queries_of(rows, width):
    head_dim = width // HEADS
    lane = iota(rows.shape, 1)
    one = jnp.where(lane == HALF + width, 1.0, 0.0)
    parts = []
    for h in range(HEADS):
        low = HALF + h * head_dim
        parts.append(jnp.where((lane >= low) & (lane < low + head_dim), rows, one))
    spare = -len(parts) * rows.shape[0] % 32
    if spare:
        parts.append(jnp.zeros((spare, LANES), F32))
    return jnp.concatenate(parts, 0).astype(BF)


def attend(jobs, width):
    head_dim = width // HEADS
    jobs = list(jobs)
    ahead = mm(jobs[0][0][...], jobs[0][1][...])
    for i, (_, _, values, n, store) in enumerate(jobs):
        scores = ahead
        if i + 1 < len(jobs):
            ahead = mm(jobs[i + 1][0][...], jobs[i + 1][1][...])
        top = jnp.max(scores, -1, keepdims=True)
        weights = jnp.exp(scores - top).astype(BF)
        out = mm(weights, values[...])
        lane = iota((n, LANES), 1)
        lane = jnp.where(lane >= HALF, lane - HALF, lane)
        mixed = out[:n]
        for h in range(1, HEADS):
            mixed = jnp.where(lane >= h * head_dim, out[h * n : (h + 1) * n], mixed)
        store(mixed / pltpu.roll(mixed, HALF, 1))


def feed(residual, mixed, wts, width):
    wp, wup, wdown, gain = wts[3:]
    first = (residual[:, :width] + mm(mixed, wp)).astype(BF).astype(F32)
    mean = jnp.sum(first, -1, keepdims=True) * (1.0 / width)
    centred = first - mean
    spread = jnp.sum(centred * centred, -1, keepdims=True) * (1.0 / width)
    normed = (centred * lax.rsqrt(spread + 1e-05) * gain).astype(BF)
    upper = twice_gelu(mm(normed, wup)).astype(BF)
    down = lax.dot_general(upper, wdown, (((1,), (1,)), ((), ())), preferred_element_type=F32)
    return (first + down).astype(BF).astype(F32)


def first_kernel(
    width, vol_ref, geo_ref, wqkv_ref, wproj_ref, wup_ref, wdown_ref, gain_ref, out_ref, *refs
):
    y_refs = refs[:-7]
    raw, tok, qs, ks, vs, mix, done = refs[-7:]
    nz = vol_ref.shape[2]
    groups = nz // WINDOW
    spots = WINDOW * WINDOW
    kept = spots - 1
    keys = kept * ROWS
    wts = block_weights(0, wqkv_ref, wproj_ref, wup_ref, wdown_ref, gain_ref)
    raw[:, nz:, :] = jnp.zeros((spots, raw.shape[1] - nz, LANES), F32)
    raw[:, 0:nz, 0:width] = vol_ref[...].astype(F32).reshape(spots, nz, width)
    done[...] = jnp.zeros(done.shape, F32)
    bias = jnp.where(geo_ref[8:9, :] < WINDOW, 0.0, BIG)

    def make(w):
        tok[w] = raw[0:kept, WINDOW * w : WINDOW * w + ROWS, :]
        for j in range(WINDOW):
            tok[w, j, WINDOW : WINDOW + 1, :] = raw[kept, WINDOW * w + j : WINDOW * w + j + 1, :]
        columns = jnp.transpose(tok[w].reshape(keys, LANES))[:width]
        vq, kaug = make_keys(columns, bias, wts, width)
        vs[w] = values_of(vq, width)
        ks[w] = kaug
        qs[w] = queries_of(vq, width)

    def finish(w0, n):
        span = slice(w0, w0 + n)
        out = feed(
            tok[span].reshape(n * keys, LANES), mix[span].reshape(n * keys, LANES)[:, :width].astype(BF), wts, width
        )
        out = out.reshape(n, kept, ROWS, width)
        for w in range(w0, w0 + n):
            done[0:kept, WINDOW * w : WINDOW * (w + 1), :width] = out[w - w0, :, :WINDOW, :]
            if w == 0:
                done[0:kept, nz : nz + SHIFT, :width] = out[w - w0, :, :SHIFT, :]
            for j in range(WINDOW):
                one = out[w - w0, j, WINDOW : WINDOW + 1, :]
                done[kept, WINDOW * w + j : WINDOW * w + j + 1, :width] = one
                if w == 0 and j < SHIFT:
                    done[kept, nz + j : nz + j + 1, :width] = one

    for w in range(groups):
        make(w)

    def keep(w):
        def store(v):
            mix[w] = v

        return store

    attend([(qs.at[w], ks.at[w], vs.at[w], keys, keep(w)) for w in range(groups)], width)
    for w in range(0, groups, 2):
        finish(w, min(2, groups - w))
    pieces = [done[:, SHIFT + WINDOW * w : SHIFT + WINDOW * w + ROWS, :] for w in range(groups)]
    rolled = [pltpu.roll(p.reshape(spots * ROWS, LANES), HALF, 1).reshape(spots, ROWS, LANES) for p in pieces[1::2]]
    joined = [a + b for a, b in zip(pieces[0::2], rolled)]
    packed = jnp.concatenate(joined, 1).astype(BF)
    out_ref[...] = packed.reshape(WINDOW, WINDOW, ROWS * len(joined), LANES)
    yodd = lax.axis_index("gy") % 2
    for k, y_ref in enumerate(y_refs):
        start = jnp.where((yodd + k) % 2 == 0, SHIFT, 0)
        y_ref[...] = out_ref[:, pl.ds(start, HIGH)]


BOXES = ((SHIFT, HIGH), (0, HIGH + 1))
COLUMNS = tuple((wx, wy) for wx in range(2) for wy in range(2))


def box_rows(wx, wy):
    return BOXES[wx][1] * BOXES[wy][1] * ROWS


def second_kernel(width, ypieces, geo_ref, own_ref, *refs):
    y_refs = refs[:ypieces]
    xa_ref, xb_ref, zown_ref = refs[ypieces : ypieces + 3]
    zy_refs = refs[ypieces + 3 : 2 * ypieces + 3]
    rest = refs[2 * ypieces + 3 :]
    zxa_ref, zxb_ref, wqkv_ref, wproj_ref, wup_ref, wdown_ref, gain_ref, wconv_ref, cgain_ref, out_ref = rest[:10]
    ext, res, mix, grid, wc, tot, ks, vs = rest[10:18]
    qs = rest[18:]
    nz = out_ref.shape[2]
    pairs = own_ref.shape[2] // ROWS
    groups = 2 * pairs + 1
    index = [lax.axis_index(a) for a in ("gx", "gy", "gz")]
    count = [lax.axis_size(a) for a in ("gx", "gy", "gz")]
    xeven, yeven = index[0] % 2 == 0, index[1] % 2 == 0
    spots = WINDOW * WINDOW
    kept = spots - 1
    keys = kept * ROWS
    wts = block_weights(1, wqkv_ref, wproj_ref, wup_ref, wdown_ref, gain_ref)

    def place(tile, ztile, x, y, nx, ny):
        n = nx * ny
        tile = tile.astype(F32).reshape(n, pairs * ROWS, LANES)
        other = ztile.astype(F32).reshape(n, ROWS, LANES)
        mine = tile[:, (pairs - 1) * ROWS :, :]
        low = iota((n, ROWS, LANES), 1) < HIGH
        upper = iota((n, ROWS, LANES), 2) >= HALF

        def put(slab, v):
            ext[slab, pl.ds(x, nx), pl.ds(y, ny)] = v.reshape(nx, ny, ROWS, LANES)

        for p in range(pairs - 1):
            put(p, tile[:, p * ROWS : (p + 1) * ROWS, :])
        put(pairs - 1, jnp.where(low | ~upper, mine, other))
        put(pairs, jnp.where(low, other, mine))

    far = WINDOW + HIGH
    ya = jnp.where(yeven, far, 0)
    yb = jnp.where(yeven, 0, far)
    xa = jnp.where(xeven, far, 0)
    xb = jnp.where(xeven, 0, far)
    ystarts = [ya, yb][:ypieces]
    if ypieces == 1:
        ext[:, :, pl.ds(yb, HIGH)] = jnp.zeros((pairs + 1, EXT, HIGH, ROWS, LANES), F32)
    place(own_ref[...], zown_ref[...], HIGH, HIGH, WINDOW, WINDOW)
    for r, z, y in zip(y_refs, zy_refs, ystarts):
        place(r[...], z[...], HIGH, y, WINDOW, HIGH)
    for r, z, x in ((xa_ref, zxa_ref, xa), (xb_ref, zxb_ref, xb)):
        place(r[:, :WINDOW], z[:, :WINDOW], x, HIGH, HIGH, WINDOW)
        for i, y in enumerate(ystarts):
            at = WINDOW + i * HIGH
            place(r[:, at : at + HIGH], z[:, at : at + HIGH], x, y, HIGH, HIGH)

    for wx, wy in COLUMNS:
        x0, y0 = WINDOW * wx, WINDOW * wy
        gone = kept * wx
        for slab in range(pairs + 1):
            for j in range(WINDOW):
                to = j + 1 - wx
                ext[slab, x0 + to // WINDOW, y0 + to % WINDOW, WINDOW : WINDOW + 1, :] = ext[
                    slab, x0 + gone // WINDOW, y0 + gone % WINDOW, j : j + 1, :
                ]

    nolow = [jnp.where(i > 0, 0.0, 1.0) for i in index]
    nohigh = [jnp.where(i < c - 1, 0.0, 1.0) for i, c in zip(index, count)]
    grid[...] = jnp.zeros(grid.shape, F32)
    offsets = [sum(box_rows(*COLUMNS[k]) for k in range(c)) for c in range(len(COLUMNS))]

    def make(slab, c):
        wx, wy = COLUMNS[c]
        row, px, py = [geo_ref[8 * wx + k : 8 * wx + k + 1, :] for k in range(3)]
        badx = jnp.where(px < HIGH, nolow[0], 0.0) if wx == 0 else jnp.where(px >= HIGH, nohigh[0], 0.0)
        bady = jnp.where(py < HIGH, nolow[1], 0.0) if wy == 0 else jnp.where(py >= HIGH, nohigh[1], 0.0)
        bad = badx + bady + jnp.where(row < WINDOW, 0.0, 1.0)
        (bx, nx), (by, ny) = BOXES[wx], BOXES[wy]
        nq = nx * ny * ROWS
        first = ROWS * (1 - wx)
        tokens = ext[slab, WINDOW * wx : WINDOW * (wx + 1), WINDOW * wy : WINDOW * (wy + 1)]
        flat = tokens.reshape(spots * ROWS, LANES)
        turned = jnp.transpose(flat[first : first + keys])
        chosen = tokens[bx : bx + nx, by : by + ny].reshape(nq, LANES)
        for half in range(2):
            if slab == pairs and half == 0:
                continue
            g = 0 if slab == pairs else 1 + 2 * slab + half
            badz = jnp.zeros_like(bad)
            if g == 0:
                badz = jnp.where(row < HIGH, nolow[2], 0.0)
            if g == groups - 1:
                badz = jnp.where(row >= HIGH, nohigh[2], 0.0)
            bias = jnp.where(bad + badz > 0.0, BIG, 0.0)
            vq, kaug = make_keys(turned[HALF * half : HALF * half + width], bias, wts, width)
            vs[c, g] = values_of(vq, width)
            ks[c, g] = kaug
            picked = [
                vq[ROWS * (WINDOW * x + by) - first : ROWS * (WINDOW * x + by + ny) - first] for x in range(bx, bx + nx)
            ]
            qs[c][g] = queries_of(jnp.concatenate(picked, 0), width)
            res[g, offsets[c] : offsets[c] + nq] = pltpu.roll(chosen, HALF, 1) if half else chosen

    def finish(g):
        out = feed(res[g], mix[g, :, :width].astype(BF), wts, width)
        for c, (wx, wy) in enumerate(COLUMNS):
            (bx, nx), (by, ny) = BOXES[wx], BOXES[wy]
            part = out[offsets[c] : offsets[c] + nx * ny * ROWS].reshape(nx, ny, ROWS, width)
            x0, y0, z0 = HIGH * wx, HIGH * wy, WINDOW * g
            grid[x0 : x0 + nx, y0 : y0 + ny, z0 : z0 + WINDOW, :width] = part[:, :, :WINDOW]

    cols = range(len(COLUMNS))
    slabs = [pairs] + list(range(pairs))
    for slab in slabs:
        for c in cols:
            make(slab, c)

    def keep(g, c):
        n = box_rows(*COLUMNS[c])

        def store(v):
            mix[g, offsets[c] : offsets[c] + n] = v

        return n, store

    attend([(qs[c].at[g], ks.at[c, g], vs.at[c, g], *keep(g, c)) for g in range(groups) for c in cols], width)
    for g in range(groups):
        finish(g)

    last = WINDOW + 1

    def clear(when, *at):
        @pl.when(when)
        def _():
            grid[at] = jnp.zeros_like(grid[at])

    clear(index[0] == 0, slice(0, 1))
    clear(index[0] == count[0] - 1, slice(last, last + 1))
    clear(index[1] == 0, slice(None), slice(0, 1))
    clear(index[1] == count[1] - 1, slice(None), slice(last, last + 1))
    clear(index[2] == 0, slice(None), slice(None), slice(SHIFT, HIGH))
    clear(index[2] == count[2] - 1, slice(None), slice(None), slice(HIGH + nz, HIGH + nz + 1))

    wc[...] = jnp.zeros(wc.shape, BF)
    for dx in range(3):
        total = None
        for dy in range(3):
            taps = wconv_ref[9 * dx + 3 * dy : 9 * dx + 3 * dy + 3].reshape(3 * width, width)
            i, j = iota((width, 4 * HALF), 0), iota((width, 4 * HALF), 1)
            place = jnp.where(j == i + HALF * dy, 1.0, 0.0).astype(BF)
            part = mm(taps, place)
            total = part if total is None else total + part
        for dz in range(3):
            at = 4 * HALF * dx + HALF * dz
            wc[at : at + width] = total[width * dz : width * (dz + 1)].astype(BF)

    side = WINDOW + 2
    padded = -(-nz // 16) * 16

    def lhs(x):
        taps = [grid[x, :, SHIFT + d : SHIFT + d + padded, :].reshape(side * padded, LANES) for d in range(3)]
        return jnp.concatenate([taps[0] + pltpu.roll(taps[1], HALF, 1), taps[2]], 1).astype(BF)

    rows = [lhs(x) for x in range(side)]
    acc = mm(jnp.concatenate([jnp.concatenate(rows[x : x + 3], 1) for x in range(WINDOW)], 0), wc[...])
    strip = WINDOW * padded
    for x in range(WINDOW):
        part = acc[x * side * padded : (x + 1) * side * padded]
        near, second = part[:, :LANES], part[:, LANES:]
        turned = pltpu.roll(near[padded : (WINDOW + 1) * padded], HALF, 1)
        tot[x * strip : (x + 1) * strip] = near[:strip] + turned + second[2 * padded :]
    tot[WINDOW * strip :] = jnp.zeros((tot.shape[0] - WINDOW * strip, LANES), F32)
    diagonal = iota((width, width), 0) == iota((width, width), 1)
    cg = jnp.sum(jnp.where(diagonal, cgain_ref[...], 0.0), 1, keepdims=True)
    normed = norm_cols(jnp.transpose(tot[...])[:width], cg, width)
    active = jnp.where(normed >= 0.0, normed, 0.01 * normed)
    active = jnp.transpose(jnp.concatenate([active, jnp.zeros((LANES - width, tot.shape[0]), F32)], 0))
    for x in range(WINDOW):
        centre = grid[x + 1, 1 : 1 + WINDOW, HIGH : HIGH + padded, :].reshape(strip, LANES)
        result = (centre + active[x * strip : (x + 1) * strip]).reshape(WINDOW, padded, LANES).astype(BF)
        out_ref[x] = result[:, :nz, :width]


def geometry():
    kept = WINDOW * WINDOW - 1
    geo = np.full((16, kept * ROWS), WINDOW, np.float32)
    for v in range(2):
        gone = kept * v
        for i in range(kept):
            spot = i + 1 - v
            for r in range(ROWS):
                t = i * ROWS + r
                if r < WINDOW:
                    geo[8 * v : 8 * v + 3, t] = r, spot // WINDOW, spot % WINDOW
                elif i < WINDOW:
                    geo[8 * v : 8 * v + 3, t] = i, gone // WINDOW, gone % WINDOW
                else:
                    geo[8 * v + 1 : 8 * v + 3, t] = spot // WINDOW, spot % WINDOW
    return jnp.asarray(geo)


def exchange(v, axis, odd):
    count, cores = lax.axis_size(axis), lax.axis_size("gz")
    pairs = []
    for i in range(count):
        low = i - (i - odd) % 2
        for c in range(cores):
            if low < 0 or low + 1 >= count:
                to = (i, c ^ 1 if c ^ 1 < cores else c)
            else:
                to = (low + 1 if i == low else low, c)
            pairs.append((i * cores + c, to[0] * cores + to[1]))
    return lax.ppermute(v, (axis, "gz"), pairs)


def body(volume, w_qkv, w_proj, w_up, w_down, norm_gain, conv_weight, conv_gain):
    sx, sy, sz, width = volume.shape
    spots = sx * sy
    groups = sz // WINDOW
    geo = geometry()
    keys = (spots - 1) * ROWS
    weights = (w_qkv, w_proj, w_up, jnp.swapaxes(w_down, 1, 2), norm_gain)
    halves = [0] if lax.axis_size("gy") == 2 else [0, 1]
    tall = ROWS * groups // 2

    packed, *cuts = pl.pallas_call(
        functools.partial(first_kernel, width),
        out_shape=[jax.ShapeDtypeStruct((sx, sy, tall, LANES), BF)]
        + [jax.ShapeDtypeStruct((sx, HIGH, tall, LANES), BF) for _ in halves],
        scratch_shapes=[
            pltpu.VMEM((spots, sz + 12, LANES), F32),
            pltpu.VMEM((groups, spots - 1, ROWS, LANES), F32),
            pltpu.VMEM((groups, HEADS * keys, LANES), BF),
            pltpu.VMEM((groups, LANES, keys), BF),
            pltpu.VMEM((groups, keys, LANES), BF),
            pltpu.VMEM((groups, keys, LANES), F32),
            pltpu.VMEM((spots, sz + 12, LANES), F32),
        ],
        compiler_params=pltpu.CompilerParams(vmem_limit_bytes=24 << 20),
        name="first_block",
    )(volume, geo, *weights)

    xodd = lax.axis_index("gx") % 2

    def cut(v, odd):
        return lax.dynamic_slice_in_dim(v, jnp.where(odd == 0, SHIFT, 0), HIGH, 0)

    def other_core(v):
        return lax.ppermute(v[:, :, -ROWS:, :], "gz", [(0, 1), (1, 0)])

    zown = other_core(packed)
    ys = [exchange(v, "gy", k) for k, v in zip(halves, cuts)]
    zys = [other_core(v) for v in ys]
    wide = jnp.concatenate([packed] + ys, 1)
    xs = [exchange(cut(wide, (xodd + k) % 2), "gx", k) for k in (0, 1)]
    zxs = [other_core(v) for v in xs]

    side = WINDOW + 2
    rows = sum(box_rows(*c) for c in COLUMNS)
    strip = WINDOW * -(-sz // 16) * 16
    operands = [geo, packed, *ys, *xs, zown, *zys, *zxs, *weights, conv_weight, conv_gain[None, :]]
    return pl.pallas_call(
        functools.partial(second_kernel, width, len(ys)),
        out_shape=jax.ShapeDtypeStruct(volume.shape, volume.dtype),
        scratch_shapes=[
            pltpu.VMEM((groups // 2 + 1, EXT, EXT, ROWS, LANES), F32),
            pltpu.VMEM((groups + 1, rows, LANES), F32),
            pltpu.VMEM((groups + 1, rows, LANES), F32),
            pltpu.VMEM((side, side, sz + 12, LANES), F32),
            pltpu.VMEM((3 * 4 * HALF, 4 * HALF), BF),
            pltpu.VMEM((-(-WINDOW * strip // LANES) * LANES, LANES), F32),
            pltpu.VMEM((len(COLUMNS), groups + 1, LANES, keys), BF),
            pltpu.VMEM((len(COLUMNS), groups + 1, keys, LANES), BF),
        ]
        + [pltpu.VMEM((groups + 1, -(-HEADS * box_rows(*c) // 32) * 32, LANES), BF) for c in COLUMNS],
        compiler_params=pltpu.CompilerParams(vmem_limit_bytes=44 << 20),
        name="second_block",
    )(*operands)


def solution(mesh):
    placed = (P(("parts", "gx"), "gy", "gz", None), P(), P(), P(), P(), P(), P(), P())
    return jax.shard_map(
        body,
        mesh=mesh,
        in_specs=placed,
        out_specs=P(("parts", "gx"), "gy", "gz", None),
        check_vma=False,
    )
```

```python
import functools

import jax
import jax.numpy as jnp
import numpy as np
from jax import lax
from jax.experimental import pallas as pl
from jax.experimental.pallas import tpu as pltpu
from jax.sharding import PartitionSpec as P

HEADS = 3
WINDOW = 7
SHIFT = 3
LANES = 128
HALF = 64
ROWS = 8
BIG = -1e30
HIGH = WINDOW - SHIFT
EXT = 2 * WINDOW + 1
BF = jnp.bfloat16
F32 = jnp.float32


def mm(a, b):
    return jnp.dot(a, b, preferred_element_type=F32)


def iota(shape, dim):
    return lax.broadcasted_iota(jnp.int32, shape, dim)


def norm_cols(x, gain, width):
    mean = jnp.sum(x, 0, keepdims=True) * (1.0 / width)
    centred = x - mean
    spread = jnp.sum(centred * centred, 0, keepdims=True) * (1.0 / width)
    return centred * lax.rsqrt(spread + 1e-05) * gain


def twice_gelu(x):
    inner = x * (0.7978845608028654 + (0.7978845608028654 * 0.044715) * (x * x))
    return x + x * jnp.tanh(inner)


def block_weights(b, wqkv_ref, wproj_ref, wup_ref, wdown_ref, gain_ref):
    wqkv = wqkv_ref[b]
    width, triple = wqkv.shape
    scale = (width // HEADS) ** (-0.5)
    i, j = iota((triple, LANES), 0), iota((triple, LANES), 1)
    take_v = (j < width) & (i == j + 2 * width)
    take_q = (j >= HALF) & (j < HALF + width) & (i == j - HALF)
    place = jnp.where(take_v, 1.0, jnp.where(take_q, scale, 0.0)).astype(BF)
    wvq = mm(wqkv, place).astype(BF)
    o, i = iota((width, triple), 0), iota((width, triple), 1)
    place = jnp.where(i == o + width, 1.0, 0.0).astype(BF)
    wk = lax.dot_general(place, wqkv, (((1,), (1,)), ((), ())), preferred_element_type=F32).astype(BF)
    gains = gain_ref[b]
    diagonal = iota((width, width), 0) == iota((width, width), 1)
    column = jnp.sum(jnp.where(diagonal, gains[0:1], 0.0), 1, keepdims=True)
    return wvq, wk, column, wproj_ref[b], wup_ref[b], wdown_ref[b] * jnp.asarray(0.5, BF), gains[1:2]


def make_keys(columns, bias, wts, width):
    wvq, wk, gain = wts[0], wts[1], wts[2]
    normed = norm_cols(columns, gain, width).astype(BF)
    vq = lax.dot_general(normed, wvq, (((0,), (0,)), ((), ())), preferred_element_type=F32)
    kt = mm(wk, normed).astype(BF)
    keys = columns.shape[1]
    top = iota((HALF - width, keys), 0) == 0
    extra = jnp.where(top, bias, 0.0).astype(BF)
    kaug = jnp.concatenate([jnp.zeros((HALF, keys), BF), kt, extra], 0)
    return vq, kaug


def values_of(vq, width):
    return jnp.where(iota(vq.shape, 1) < width, vq, 1.0).astype(BF)


def queries_of(rows, width):
    head_dim = width // HEADS
    lane = iota(rows.shape, 1)
    one = jnp.where(lane == HALF + width, 1.0, 0.0)
    parts = []
    for h in range(HEADS):
        low = HALF + h * head_dim
        parts.append(jnp.where((lane >= low) & (lane < low + head_dim), rows, one))
    spare = -len(parts) * rows.shape[0] % 32
    if spare:
        parts.append(jnp.zeros((spare, LANES), F32))
    return jnp.concatenate(parts, 0).astype(BF)


def attend(jobs, width):
    head_dim = width // HEADS
    jobs = list(jobs)
    ahead = mm(jobs[0][0][...], jobs[0][1][...])
    for i, (_, _, values, n, store) in enumerate(jobs):
        scores = ahead
        if i + 1 < len(jobs):
            ahead = mm(jobs[i + 1][0][...], jobs[i + 1][1][...])
        top = jnp.max(scores, -1, keepdims=True)
        weights = jnp.exp(scores - top).astype(BF)
        out = mm(weights, values[...])
        lane = iota((n, LANES), 1)
        lane = jnp.where(lane >= HALF, lane - HALF, lane)
        mixed = out[:n]
        for h in range(1, HEADS):
            mixed = jnp.where(lane >= h * head_dim, out[h * n : (h + 1) * n], mixed)
        store(mixed / pltpu.roll(mixed, HALF, 1))


def feed(residual, mixed, wts, width):
    wp, wup, wdown, gain = wts[3:]
    first = (residual[:, :width] + mm(mixed, wp)).astype(BF).astype(F32)
    mean = jnp.sum(first, -1, keepdims=True) * (1.0 / width)
    centred = first - mean
    spread = jnp.sum(centred * centred, -1, keepdims=True) * (1.0 / width)
    normed = (centred * lax.rsqrt(spread + 1e-05) * gain).astype(BF)
    upper = twice_gelu(mm(normed, wup)).astype(BF)
    down = lax.dot_general(upper, wdown, (((1,), (1,)), ((), ())), preferred_element_type=F32)
    return (first + down).astype(BF).astype(F32)


def first_kernel(width, ny, *refs):
    hbm, out_ref = refs[:7], refs[7]
    y_refs, x_refs = refs[8 : 8 + ny], refs[8 + ny : 10 + ny]
    copies = refs[10 + ny : 17 + ny]
    sems = refs[17 + ny]
    raw, tok, qs, ks, vs, mix, done = refs[18 + ny :]
    moves = [pltpu.make_async_copy(h, v, sems.at[i]) for i, (h, v) in enumerate(zip(hbm, copies))]
    for m in moves:
        m.start()
    for m in moves[1:]:
        m.wait()
    vol_ref, geo_ref, wqkv_ref, wproj_ref, wup_ref, wdown_ref, gain_ref = copies
    nz = vol_ref.shape[2]
    groups = nz // WINDOW
    spots = WINDOW * WINDOW
    kept = spots - 1
    keys = kept * ROWS
    wts = block_weights(0, wqkv_ref, wproj_ref, wup_ref, wdown_ref, gain_ref)
    done[...] = jnp.zeros(done.shape, F32)
    moves[0].wait()
    raw[:, nz:, :] = jnp.zeros((spots, raw.shape[1] - nz, LANES), F32)
    raw[:, 0:nz, 0:width] = vol_ref[...].astype(F32).reshape(spots, nz, width)
    bias = jnp.where(geo_ref[8:9, :] < WINDOW, 0.0, BIG)

    def make(w):
        tok[w] = raw[0:kept, WINDOW * w : WINDOW * w + ROWS, :]
        for j in range(WINDOW):
            tok[w, j, WINDOW : WINDOW + 1, :] = raw[kept, WINDOW * w + j : WINDOW * w + j + 1, :]
        columns = jnp.transpose(tok[w].reshape(keys, LANES))[:width]
        vq, kaug = make_keys(columns, bias, wts, width)
        vs[w] = values_of(vq, width)
        ks[w] = kaug
        qs[w] = queries_of(vq, width)

    def finish(w0, n):
        span = slice(w0, w0 + n)
        out = feed(
            tok[span].reshape(n * keys, LANES), mix[span].reshape(n * keys, LANES)[:, :width].astype(BF), wts, width
        )
        out = out.reshape(n, kept, ROWS, width)
        for w in range(w0, w0 + n):
            done[0:kept, WINDOW * w : WINDOW * (w + 1), :width] = out[w - w0, :, :WINDOW, :]
            if w == 0:
                done[0:kept, nz : nz + SHIFT, :width] = out[w - w0, :, :SHIFT, :]
            for j in range(WINDOW):
                one = out[w - w0, j, WINDOW : WINDOW + 1, :]
                done[kept, WINDOW * w + j : WINDOW * w + j + 1, :width] = one
                if w == 0 and j < SHIFT:
                    done[kept, nz + j : nz + j + 1, :width] = one

    for w in range(groups):
        make(w)

    def keep(w):
        def store(v):
            mix[w] = v

        return store

    attend([(qs.at[w], ks.at[w], vs.at[w], keys, keep(w)) for w in range(groups)], width)
    for w in range(0, groups, 2):
        finish(w, min(2, groups - w))
    pieces = [done[:, SHIFT + WINDOW * w : SHIFT + WINDOW * w + ROWS, :] for w in range(groups)]
    rolled = [pltpu.roll(p.reshape(spots * ROWS, LANES), HALF, 1).reshape(spots, ROWS, LANES) for p in pieces[1::2]]
    joined = [a + b for a, b in zip(pieces[0::2], rolled)]
    packed = jnp.concatenate(joined, 1).astype(BF)
    out_ref[...] = packed.reshape(WINDOW, WINDOW, ROWS * len(joined), LANES)
    yodd = lax.axis_index("gy") % 2
    for k, y_ref in enumerate(y_refs):
        start = jnp.where((yodd + k) % 2 == 0, SHIFT, 0)
        y_ref[...] = out_ref[:, pl.ds(start, HIGH)]
    xodd = lax.axis_index("gx") % 2
    for k, x_ref in enumerate(x_refs):
        start = jnp.where((xodd + k) % 2 == 0, SHIFT, 0)
        x_ref[...] = out_ref[pl.ds(start, HIGH)]


BOXES = ((SHIFT, HIGH), (0, HIGH + 1))
COLUMNS = tuple((wx, wy) for wx in range(2) for wy in range(2))


def box_rows(wx, wy):
    return BOXES[wx][1] * BOXES[wy][1] * ROWS


def second_kernel(width, ypieces, geo_ref, *refs):
    x_refs = refs[:6]
    y_refs = [refs[6 * i : 6 * i + 6] for i in range(1, ypieces + 1)]
    rest = refs[6 * (ypieces + 1) :]
    wqkv_ref, wproj_ref, wup_ref, wdown_ref, gain_ref, wconv_ref, cgain_ref, out_ref = rest[:8]
    ext, res, mix, grid, wc, tot, ks, vs = rest[8:16]
    qs = rest[16:]
    nz = out_ref.shape[2]
    pairs = x_refs[0].shape[2] // ROWS
    groups = 2 * pairs + 1
    index = [lax.axis_index(a) for a in ("gx", "gy", "gz")]
    count = [lax.axis_size(a) for a in ("gx", "gy", "gz")]
    xeven, yeven = index[0] % 2 == 0, index[1] % 2 == 0
    spots = WINDOW * WINDOW
    kept = spots - 1
    keys = kept * ROWS
    wts = block_weights(1, wqkv_ref, wproj_ref, wup_ref, wdown_ref, gain_ref)

    def place(tile, ztile, x, y, nx, ny):
        n = nx * ny
        tile = tile.astype(F32).reshape(n, pairs * ROWS, LANES)
        other = ztile.astype(F32).reshape(n, ROWS, LANES)
        mine = tile[:, (pairs - 1) * ROWS :, :]
        low = iota((n, ROWS, LANES), 1) < HIGH
        upper = iota((n, ROWS, LANES), 2) >= HALF

        def put(slab, v):
            ext[slab, pl.ds(x, nx), pl.ds(y, ny)] = v.reshape(nx, ny, ROWS, LANES)

        for p in range(pairs - 1):
            put(p, tile[:, p * ROWS : (p + 1) * ROWS, :])
        put(pairs - 1, jnp.where(low | ~upper, mine, other))
        put(pairs, jnp.where(low, other, mine))

    far = WINDOW + HIGH
    ya = jnp.where(yeven, far, 0)
    yb = jnp.where(yeven, 0, far)
    xa = jnp.where(xeven, far, 0)
    xb = jnp.where(xeven, 0, far)
    ystarts = [ya, yb][:ypieces]
    if ypieces == 1:
        ext[:, :, pl.ds(yb, HIGH)] = jnp.zeros((pairs + 1, EXT, HIGH, ROWS, LANES), F32)
    for y, ny, pieces in ((HIGH, WINDOW, x_refs), *zip(ystarts, [HIGH] * ypieces, y_refs)):
        for i, (x, nx) in enumerate(((HIGH, WINDOW), (xa, HIGH), (xb, HIGH))):
            place(pieces[i][...], pieces[i + 3][...], x, y, nx, ny)

    for wx, wy in COLUMNS:
        x0, y0 = WINDOW * wx, WINDOW * wy
        gone = kept * wx
        for slab in range(pairs + 1):
            for j in range(WINDOW):
                to = j + 1 - wx
                ext[slab, x0 + to // WINDOW, y0 + to % WINDOW, WINDOW : WINDOW + 1, :] = ext[
                    slab, x0 + gone // WINDOW, y0 + gone % WINDOW, j : j + 1, :
                ]

    nolow = [jnp.where(i > 0, 0.0, 1.0) for i in index]
    nohigh = [jnp.where(i < c - 1, 0.0, 1.0) for i, c in zip(index, count)]
    grid[...] = jnp.zeros(grid.shape, F32)
    offsets = [sum(box_rows(*COLUMNS[k]) for k in range(c)) for c in range(len(COLUMNS))]

    def make(slab, c):
        wx, wy = COLUMNS[c]
        row, px, py = [geo_ref[8 * wx + k : 8 * wx + k + 1, :] for k in range(3)]
        badx = jnp.where(px < HIGH, nolow[0], 0.0) if wx == 0 else jnp.where(px >= HIGH, nohigh[0], 0.0)
        bady = jnp.where(py < HIGH, nolow[1], 0.0) if wy == 0 else jnp.where(py >= HIGH, nohigh[1], 0.0)
        bad = badx + bady + jnp.where(row < WINDOW, 0.0, 1.0)
        (bx, nx), (by, ny) = BOXES[wx], BOXES[wy]
        nq = nx * ny * ROWS
        first = ROWS * (1 - wx)
        tokens = ext[slab, WINDOW * wx : WINDOW * (wx + 1), WINDOW * wy : WINDOW * (wy + 1)]
        flat = tokens.reshape(spots * ROWS, LANES)
        turned = jnp.transpose(flat[first : first + keys])
        chosen = tokens[bx : bx + nx, by : by + ny].reshape(nq, LANES)
        for half in range(2):
            if slab == pairs and half == 0:
                continue
            g = 0 if slab == pairs else 1 + 2 * slab + half
            badz = jnp.zeros_like(bad)
            if g == 0:
                badz = jnp.where(row < HIGH, nolow[2], 0.0)
            if g == groups - 1:
                badz = jnp.where(row >= HIGH, nohigh[2], 0.0)
            bias = jnp.where(bad + badz > 0.0, BIG, 0.0)
            vq, kaug = make_keys(turned[HALF * half : HALF * half + width], bias, wts, width)
            vs[c, g] = values_of(vq, width)
            ks[c, g] = kaug
            picked = [
                vq[ROWS * (WINDOW * x + by) - first : ROWS * (WINDOW * x + by + ny) - first] for x in range(bx, bx + nx)
            ]
            qs[c][g] = queries_of(jnp.concatenate(picked, 0), width)
            res[g, offsets[c] : offsets[c] + nq] = pltpu.roll(chosen, HALF, 1) if half else chosen

    def finish(g):
        out = feed(res[g], mix[g, :, :width].astype(BF), wts, width)
        for c, (wx, wy) in enumerate(COLUMNS):
            (bx, nx), (by, ny) = BOXES[wx], BOXES[wy]
            part = out[offsets[c] : offsets[c] + nx * ny * ROWS].reshape(nx, ny, ROWS, width)
            x0, y0, z0 = HIGH * wx, HIGH * wy, WINDOW * g
            grid[x0 : x0 + nx, y0 : y0 + ny, z0 : z0 + WINDOW, :width] = part[:, :, :WINDOW]

    cols = range(len(COLUMNS))
    slabs = [pairs] + list(range(pairs))
    for slab in slabs:
        for c in cols:
            make(slab, c)

    def keep(g, c):
        n = box_rows(*COLUMNS[c])

        def store(v):
            mix[g, offsets[c] : offsets[c] + n] = v

        return n, store

    attend([(qs[c].at[g], ks.at[c, g], vs.at[c, g], *keep(g, c)) for g in range(groups) for c in cols], width)
    for g in range(groups):
        finish(g)

    last = WINDOW + 1

    def clear(when, *at):
        @pl.when(when)
        def _():
            grid[at] = jnp.zeros_like(grid[at])

    clear(index[0] == 0, slice(0, 1))
    clear(index[0] == count[0] - 1, slice(last, last + 1))
    clear(index[1] == 0, slice(None), slice(0, 1))
    clear(index[1] == count[1] - 1, slice(None), slice(last, last + 1))
    clear(index[2] == 0, slice(None), slice(None), slice(SHIFT, HIGH))
    clear(index[2] == count[2] - 1, slice(None), slice(None), slice(HIGH + nz, HIGH + nz + 1))

    wc[...] = jnp.zeros(wc.shape, BF)
    for dx in range(3):
        total = None
        for dy in range(3):
            taps = wconv_ref[9 * dx + 3 * dy : 9 * dx + 3 * dy + 3].reshape(3 * width, width)
            i, j = iota((width, 4 * HALF), 0), iota((width, 4 * HALF), 1)
            place = jnp.where(j == i + HALF * dy, 1.0, 0.0).astype(BF)
            part = mm(taps, place)
            total = part if total is None else total + part
        for dz in range(3):
            at = 4 * HALF * dx + HALF * dz
            wc[at : at + width] = total[width * dz : width * (dz + 1)].astype(BF)

    side = WINDOW + 2
    padded = -(-nz // 16) * 16

    def lhs(x):
        taps = [grid[x, :, SHIFT + d : SHIFT + d + padded, :].reshape(side * padded, LANES) for d in range(3)]
        return jnp.concatenate([taps[0] + pltpu.roll(taps[1], HALF, 1), taps[2]], 1).astype(BF)

    rows = [lhs(x) for x in range(side)]
    acc = mm(jnp.concatenate([jnp.concatenate(rows[x : x + 3], 1) for x in range(WINDOW)], 0), wc[...])
    strip = WINDOW * padded
    for x in range(WINDOW):
        part = acc[x * side * padded : (x + 1) * side * padded]
        near, second = part[:, :LANES], part[:, LANES:]
        turned = pltpu.roll(near[padded : (WINDOW + 1) * padded], HALF, 1)
        tot[x * strip : (x + 1) * strip] = near[:strip] + turned + second[2 * padded :]
    tot[WINDOW * strip :] = jnp.zeros((tot.shape[0] - WINDOW * strip, LANES), F32)
    diagonal = iota((width, width), 0) == iota((width, width), 1)
    cg = jnp.sum(jnp.where(diagonal, cgain_ref[...], 0.0), 1, keepdims=True)
    normed = norm_cols(jnp.transpose(tot[...])[:width], cg, width)
    active = jnp.where(normed >= 0.0, normed, 0.01 * normed)
    active = jnp.transpose(jnp.concatenate([active, jnp.zeros((LANES - width, tot.shape[0]), F32)], 0))
    for x in range(WINDOW):
        centre = grid[x + 1, 1 : 1 + WINDOW, HIGH : HIGH + padded, :].reshape(strip, LANES)
        result = (centre + active[x * strip : (x + 1) * strip]).reshape(WINDOW, padded, LANES).astype(BF)
        out_ref[x] = result[:, :nz, :width]


def geometry():
    kept = WINDOW * WINDOW - 1
    geo = np.full((16, kept * ROWS), WINDOW, np.float32)
    for v in range(2):
        gone = kept * v
        for i in range(kept):
            spot = i + 1 - v
            for r in range(ROWS):
                t = i * ROWS + r
                if r < WINDOW:
                    geo[8 * v : 8 * v + 3, t] = r, spot // WINDOW, spot % WINDOW
                elif i < WINDOW:
                    geo[8 * v : 8 * v + 3, t] = i, gone // WINDOW, gone % WINDOW
                else:
                    geo[8 * v + 1 : 8 * v + 3, t] = spot // WINDOW, spot % WINDOW
    return jnp.asarray(geo)


def exchange(v, axis, odd):
    count, cores = lax.axis_size(axis), lax.axis_size("gz")
    pairs = []
    for i in range(count):
        low = i - (i - odd) % 2
        for c in range(cores):
            if low < 0 or low + 1 >= count:
                to = (i, c ^ 1 if c ^ 1 < cores else c)
            else:
                to = (low + 1 if i == low else low, c)
            pairs.append((i * cores + c, to[0] * cores + to[1]))
    return lax.ppermute(v, (axis, "gz"), pairs)


def body(volume, w_qkv, w_proj, w_up, w_down, norm_gain, conv_weight, conv_gain):
    sx, sy, sz, width = volume.shape
    spots = sx * sy
    groups = sz // WINDOW
    geo = geometry()
    keys = (spots - 1) * ROWS
    weights = (w_qkv, w_proj, w_up, jnp.swapaxes(w_down, 1, 2), norm_gain)
    halves = [0] if lax.axis_size("gy") == 2 else [0, 1]
    tall = ROWS * groups // 2

    operands = (volume, geo, *weights)
    packed, *cuts = pl.pallas_call(
        functools.partial(first_kernel, width, len(halves)),
        out_shape=[jax.ShapeDtypeStruct((sx, sy, tall, LANES), BF)]
        + [jax.ShapeDtypeStruct((sx, HIGH, tall, LANES), BF) for _ in halves]
        + [jax.ShapeDtypeStruct((HIGH, sy, tall, LANES), BF) for _ in range(2)],
        in_specs=[pl.BlockSpec(memory_space=pltpu.HBM)] * len(operands),
        scratch_shapes=[pltpu.VMEM(v.shape, v.dtype) for v in operands]
        + [
            pltpu.SemaphoreType.DMA((len(operands),)),
            pltpu.VMEM((spots, sz + 12, LANES), F32),
            pltpu.VMEM((groups, spots - 1, ROWS, LANES), F32),
            pltpu.VMEM((groups, HEADS * keys, LANES), BF),
            pltpu.VMEM((groups, LANES, keys), BF),
            pltpu.VMEM((groups, keys, LANES), BF),
            pltpu.VMEM((groups, keys, LANES), F32),
            pltpu.VMEM((spots, sz + 12, LANES), F32),
        ],
        compiler_params=pltpu.CompilerParams(vmem_limit_bytes=24 << 20),
        name="first_block",
    )(*[pltpu.with_memory_space_constraint(v, pltpu.HBM) for v in operands])

    xodd = lax.axis_index("gx") % 2

    def cut(v, odd):
        return lax.dynamic_slice_in_dim(v, jnp.where(odd == 0, SHIFT, 0), HIGH, 0)

    def other_core(v):
        return lax.ppermute(v[:, :, -ROWS:, :], "gz", [(0, 1), (1, 0)])

    ys = [exchange(v, "gy", k) for k, v in zip(halves, cuts)]
    xs = [exchange(v, "gx", k) for k, v in enumerate(cuts[len(halves) :])]
    zs = [other_core(v) for v in (packed, *xs)]
    corners = [[exchange(cut(v, (xodd + k) % 2), "gx", k) for k in (0, 1)] for v in ys]
    zcorners = [[other_core(v) for v in (y, *c)] for y, c in zip(ys, corners)]

    side = WINDOW + 2
    rows = sum(box_rows(*c) for c in COLUMNS)
    strip = WINDOW * -(-sz // 16) * 16
    flat = [v for y, c, z in zip(ys, corners, zcorners) for v in (y, *c, *z)]
    operands = [geo, packed, *xs, *zs, *flat, *weights, conv_weight, conv_gain[None, :]]
    return pl.pallas_call(
        functools.partial(second_kernel, width, len(ys)),
        out_shape=jax.ShapeDtypeStruct(volume.shape, volume.dtype),
        scratch_shapes=[
            pltpu.VMEM((groups // 2 + 1, EXT, EXT, ROWS, LANES), F32),
            pltpu.VMEM((groups + 1, rows, LANES), F32),
            pltpu.VMEM((groups + 1, rows, LANES), F32),
            pltpu.VMEM((side, side, sz + 12, LANES), F32),
            pltpu.VMEM((3 * 4 * HALF, 4 * HALF), BF),
            pltpu.VMEM((-(-WINDOW * strip // LANES) * LANES, LANES), F32),
            pltpu.VMEM((len(COLUMNS), groups + 1, LANES, keys), BF),
            pltpu.VMEM((len(COLUMNS), groups + 1, keys, LANES), BF),
        ]
        + [pltpu.VMEM((groups + 1, -(-HEADS * box_rows(*c) // 32) * 32, LANES), BF) for c in COLUMNS],
        compiler_params=pltpu.CompilerParams(vmem_limit_bytes=26 << 20),
        name="second_block",
    )(*operands)


def solution(mesh):
    placed = (P(("parts", "gx"), "gy", "gz", None), P(), P(), P(), P(), P(), P(), P())
    return jax.shard_map(
        body,
        mesh=mesh,
        in_specs=placed,
        out_specs=P(("parts", "gx"), "gy", "gz", None),
        check_vma=False,
    )
```

```python
import functools

import jax
import jax.numpy as jnp
import numpy as np
from jax import lax
from jax.experimental import pallas as pl
from jax.experimental.pallas import tpu as pltpu
from jax.sharding import PartitionSpec as P

HEADS = 3
WINDOW = 7
SHIFT = 3
LANES = 128
HALF = 64
ROWS = 8
BIG = -1e30
HIGH = WINDOW - SHIFT
EXT = 2 * WINDOW + 1
BF = jnp.bfloat16
F32 = jnp.float32


def mm(a, b):
    return jnp.dot(a, b, preferred_element_type=F32)


def iota(shape, dim):
    return lax.broadcasted_iota(jnp.int32, shape, dim)


def norm_cols(x, gain, width):
    mean = jnp.sum(x, 0, keepdims=True) * (1.0 / width)
    centred = x - mean
    spread = jnp.sum(centred * centred, 0, keepdims=True) * (1.0 / width)
    return centred * lax.rsqrt(spread + 1e-05) * gain


def twice_gelu(x):
    inner = x * (0.7978845608028654 + (0.7978845608028654 * 0.044715) * (x * x))
    return x + x * jnp.tanh(inner)


def block_weights(b, wqkv_ref, wproj_ref, wup_ref, wdown_ref, gain_ref):
    wqkv = wqkv_ref[b]
    width, triple = wqkv.shape
    scale = (width // HEADS) ** (-0.5)
    i, j = iota((triple, LANES), 0), iota((triple, LANES), 1)
    take_v = (j < width) & (i == j + 2 * width)
    take_q = (j >= HALF) & (j < HALF + width) & (i == j - HALF)
    place = jnp.where(take_v, 1.0, jnp.where(take_q, scale, 0.0)).astype(BF)
    wvq = mm(wqkv, place).astype(BF)
    o, i = iota((width, triple), 0), iota((width, triple), 1)
    place = jnp.where(i == o + width, 1.0, 0.0).astype(BF)
    wk = lax.dot_general(place, wqkv, (((1,), (1,)), ((), ())), preferred_element_type=F32).astype(BF)
    gains = gain_ref[b]
    diagonal = iota((width, width), 0) == iota((width, width), 1)
    first, second = [jnp.sum(jnp.where(diagonal, gains[k : k + 1], 0.0), 1, keepdims=True) for k in range(2)]
    i, j = iota((width, LANES), 0), iota((width, LANES), 1)
    spread = jnp.where(i == j, 1.0, 0.0).astype(BF)
    wp = lax.dot_general(wproj_ref[b], spread, (((0,), (0,)), ((), ())), preferred_element_type=F32)
    wp = (wp + jnp.where(j == i + HALF, 1.0, 0.0)).astype(BF)
    return wvq, wk, first, wp, wup_ref[b], wdown_ref[b] * jnp.asarray(0.5, BF), second


def make_keys(columns, bias, wts, width):
    wvq, wk, gain = wts[0], wts[1], wts[2]
    normed = norm_cols(columns, gain, width).astype(BF)
    vq = lax.dot_general(normed, wvq, (((0,), (0,)), ((), ())), preferred_element_type=F32)
    kt = mm(wk, normed).astype(BF)
    keys = columns.shape[1]
    top = iota((HALF - width, keys), 0) == 0
    extra = jnp.where(top, bias, 0.0).astype(BF)
    kaug = jnp.concatenate([jnp.zeros((HALF, keys), BF), kt, extra], 0)
    return vq, kaug


def values_of(vq, width):
    return jnp.where(iota(vq.shape, 1) < width, vq, 1.0).astype(BF)


def queries_of(rows, width):
    head_dim = width // HEADS
    lane = iota(rows.shape, 1)
    one = jnp.where(lane == HALF + width, 1.0, 0.0)
    parts = []
    for h in range(HEADS):
        low = HALF + h * head_dim
        parts.append(jnp.where((lane >= low) & (lane < low + head_dim), rows, one))
    spare = -len(parts) * rows.shape[0] % 32
    if spare:
        parts.append(jnp.zeros((spare, LANES), F32))
    return jnp.concatenate(parts, 0).astype(BF)


def attend(jobs, width):
    head_dim = width // HEADS
    jobs = list(jobs)
    ahead = mm(jobs[0][0][...], jobs[0][1][...])
    for i, (_, _, values, n, store) in enumerate(jobs):
        scores = ahead
        if i + 1 < len(jobs):
            ahead = mm(jobs[i + 1][0][...], jobs[i + 1][1][...])
        top = jnp.max(scores, -1, keepdims=True)
        weights = jnp.exp(scores - top).astype(BF)
        out = mm(weights, values[...])
        lane = iota((n, LANES), 1)
        lane = jnp.where(lane >= HALF, lane - HALF, lane)
        mixed = out[:n]
        for h in range(1, HEADS):
            mixed = jnp.where(lane >= h * head_dim, out[h * n : (h + 1) * n], mixed)
        store(mixed / pltpu.roll(mixed, HALF, 1))


def feed(first, wts, width):
    wup, wdown, gain = wts[4:]
    first = first.astype(BF).astype(F32)
    normed = norm_cols(first, gain, width).astype(BF)
    upper = lax.dot_general(wup, normed, (((0,), (0,)), ((), ())), preferred_element_type=F32)
    return (first + mm(wdown, twice_gelu(upper).astype(BF))).astype(BF).astype(F32)


def against_rows(w, rows):
    return lax.dot_general(w, rows, (((1,), (1,)), ((), ())), preferred_element_type=F32)


def first_kernel(width, ny, *refs):
    hbm, out_ref = refs[:7], refs[7]
    y_refs, x_refs = refs[8 : 8 + ny], refs[8 + ny : 10 + ny]
    copies = refs[10 + ny : 17 + ny]
    sems = refs[17 + ny]
    raw, tok, qs, ks, vs, mix, held, done = refs[18 + ny :]
    moves = [pltpu.make_async_copy(h, v, sems.at[i]) for i, (h, v) in enumerate(zip(hbm, copies))]
    for m in moves:
        m.start()
    for m in moves[1:]:
        m.wait()
    vol_ref, geo_ref, wqkv_ref, wproj_ref, wup_ref, wdown_ref, gain_ref = copies
    nz = vol_ref.shape[2]
    groups = nz // WINDOW
    spots = WINDOW * WINDOW
    kept = spots - 1
    keys = kept * ROWS
    wts = block_weights(0, wqkv_ref, wproj_ref, wup_ref, wdown_ref, gain_ref)
    done[...] = jnp.zeros(done.shape, F32)
    moves[0].wait()
    raw[:, nz:, :] = jnp.zeros((spots, raw.shape[1] - nz, LANES), F32)
    raw[:, 0:nz, 0:width] = vol_ref[...].astype(F32).reshape(spots, nz, width)
    bias = jnp.where(geo_ref[8:9, :] < WINDOW, 0.0, BIG)

    def make(w):
        tok[w] = raw[0:kept, WINDOW * w : WINDOW * w + ROWS, :]
        for j in range(WINDOW):
            tok[w, j, WINDOW : WINDOW + 1, :] = raw[kept, WINDOW * w + j : WINDOW * w + j + 1, :]
        columns = jnp.transpose(tok[w].reshape(keys, LANES))[:width]
        held[:, keys * w : keys * (w + 1)] = columns
        vq, kaug = make_keys(columns, bias, wts, width)
        vs[w] = values_of(vq, width)
        ks[w] = kaug
        qs[w] = queries_of(vq, width)

    def finish(w0, n):
        mixed = mix[w0 : w0 + n].reshape(n * keys, LANES)[:, :width].astype(BF)
        first = held[:, keys * w0 : keys * (w0 + n)] + against_rows(wts[3][:, :width], mixed)
        out = feed(first, wts, width)
        out = jnp.transpose(jnp.concatenate([out, jnp.zeros((LANES - width, n * keys), F32)], 0))[:, :width]
        out = out.reshape(n, kept, ROWS, width)
        for w in range(w0, w0 + n):
            done[0:kept, WINDOW * w : WINDOW * (w + 1), :width] = out[w - w0, :, :WINDOW, :]
            if w == 0:
                done[0:kept, nz : nz + SHIFT, :width] = out[w - w0, :, :SHIFT, :]
            for j in range(WINDOW):
                one = out[w - w0, j, WINDOW : WINDOW + 1, :]
                done[kept, WINDOW * w + j : WINDOW * w + j + 1, :width] = one
                if w == 0 and j < SHIFT:
                    done[kept, nz + j : nz + j + 1, :width] = one

    for w in range(groups):
        make(w)

    def keep(w):
        def store(v):
            mix[w] = v

        return store

    attend([(qs.at[w], ks.at[w], vs.at[w], keys, keep(w)) for w in range(groups)], width)
    for w in range(0, groups, 2):
        finish(w, min(2, groups - w))
    pieces = [done[:, SHIFT + WINDOW * w : SHIFT + WINDOW * w + ROWS, :] for w in range(groups)]
    rolled = [pltpu.roll(p.reshape(spots * ROWS, LANES), HALF, 1).reshape(spots, ROWS, LANES) for p in pieces[1::2]]
    joined = [a + b for a, b in zip(pieces[0::2], rolled)]
    packed = jnp.concatenate(joined, 1).astype(BF)
    out_ref[...] = packed.reshape(WINDOW, WINDOW, ROWS * len(joined), LANES)
    yodd = lax.axis_index("gy") % 2
    for k, y_ref in enumerate(y_refs):
        start = jnp.where((yodd + k) % 2 == 0, SHIFT, 0)
        y_ref[...] = out_ref[:, pl.ds(start, HIGH)]
    xodd = lax.axis_index("gx") % 2
    for k, x_ref in enumerate(x_refs):
        start = jnp.where((xodd + k) % 2 == 0, SHIFT, 0)
        x_ref[...] = out_ref[pl.ds(start, HIGH)]


CHUNKS = 2
BOXES = ((SHIFT, HIGH), (0, HIGH + 1))
COLUMNS = tuple((wx, wy) for wx in range(2) for wy in range(2))


def box_rows(wx, wy):
    return BOXES[wx][1] * BOXES[wy][1] * ROWS


def second_kernel(width, ypieces, geo_ref, *refs):
    x_refs = refs[:6]
    y_refs = [refs[6 * i : 6 * i + 6] for i in range(1, ypieces + 1)]
    rest = refs[6 * (ypieces + 1) :]
    wqkv_ref, wproj_ref, wup_ref, wdown_ref, gain_ref, wconv_ref, cgain_ref, out_ref = rest[:8]
    ext, mix, grid, wc, tot, ks, vs = rest[8:15]
    qs = rest[15:]
    nz = out_ref.shape[2]
    pairs = x_refs[0].shape[2] // ROWS
    groups = 2 * pairs + 1
    index = [lax.axis_index(a) for a in ("gx", "gy", "gz")]
    count = [lax.axis_size(a) for a in ("gx", "gy", "gz")]
    xeven, yeven = index[0] % 2 == 0, index[1] % 2 == 0
    spots = WINDOW * WINDOW
    kept = spots - 1
    keys = kept * ROWS
    wts = block_weights(1, wqkv_ref, wproj_ref, wup_ref, wdown_ref, gain_ref)

    def place(tile, ztile, x, y, nx, ny):
        n = nx * ny
        tile = tile.astype(F32).reshape(n, pairs * ROWS, LANES)
        other = ztile.astype(F32).reshape(n, ROWS, LANES)
        mine = tile[:, (pairs - 1) * ROWS :, :]
        low = iota((n, ROWS, LANES), 1) < HIGH
        upper = iota((n, ROWS, LANES), 2) >= HALF

        def put(slab, v):
            ext[slab, pl.ds(x, nx), pl.ds(y, ny)] = v.reshape(nx, ny, ROWS, LANES)

        for p in range(pairs - 1):
            put(p, tile[:, p * ROWS : (p + 1) * ROWS, :])
        put(pairs - 1, jnp.where(low | ~upper, mine, other))
        put(pairs, jnp.where(low, other, mine))

    far = WINDOW + HIGH
    ya = jnp.where(yeven, far, 0)
    yb = jnp.where(yeven, 0, far)
    xa = jnp.where(xeven, far, 0)
    xb = jnp.where(xeven, 0, far)
    ystarts = [ya, yb][:ypieces]
    if ypieces == 1:
        ext[:, :, pl.ds(yb, HIGH)] = jnp.zeros((pairs + 1, EXT, HIGH, ROWS, LANES), F32)
    for y, ny, pieces in ((HIGH, WINDOW, x_refs), *zip(ystarts, [HIGH] * ypieces, y_refs)):
        for i, (x, nx) in enumerate(((HIGH, WINDOW), (xa, HIGH), (xb, HIGH))):
            place(pieces[i][...], pieces[i + 3][...], x, y, nx, ny)

    for wx, wy in COLUMNS:
        x0, y0 = WINDOW * wx, WINDOW * wy
        gone = kept * wx
        for slab in range(pairs + 1):
            for j in range(WINDOW):
                to = j + 1 - wx
                ext[slab, x0 + to // WINDOW, y0 + to % WINDOW, WINDOW : WINDOW + 1, :] = ext[
                    slab, x0 + gone // WINDOW, y0 + gone % WINDOW, j : j + 1, :
                ]

    nolow = [jnp.where(i > 0, 0.0, 1.0) for i in index]
    nohigh = [jnp.where(i < c - 1, 0.0, 1.0) for i, c in zip(index, count)]
    depth = grid.shape[2]
    grid[:, :, WINDOW * groups :] = jnp.zeros((WINDOW + 2, WINDOW + 2, depth - WINDOW * groups, LANES), F32)
    offsets = [sum(box_rows(*COLUMNS[k]) for k in range(c)) for c in range(len(COLUMNS))]
    per = sum(box_rows(*c) for c in COLUMNS)
    total = mix.shape[0]
    if total > per * groups:
        mix[per * groups :] = jnp.zeros((total - per * groups, LANES), F32)

    def make(slab, c):
        wx, wy = COLUMNS[c]
        row, px, py = [geo_ref[8 * wx + k : 8 * wx + k + 1, :] for k in range(3)]
        badx = jnp.where(px < HIGH, nolow[0], 0.0) if wx == 0 else jnp.where(px >= HIGH, nohigh[0], 0.0)
        bady = jnp.where(py < HIGH, nolow[1], 0.0) if wy == 0 else jnp.where(py >= HIGH, nohigh[1], 0.0)
        bad = badx + bady + jnp.where(row < WINDOW, 0.0, 1.0)
        (bx, nx), (by, ny) = BOXES[wx], BOXES[wy]
        nq = nx * ny * ROWS
        first = ROWS * (1 - wx)
        tokens = ext[slab, WINDOW * wx : WINDOW * (wx + 1), WINDOW * wy : WINDOW * (wy + 1)]
        flat = tokens.reshape(spots * ROWS, LANES)
        turned = jnp.transpose(flat[first : first + keys])
        chosen = tokens[bx : bx + nx, by : by + ny].reshape(nq, LANES)
        for half in range(2):
            if slab == pairs and half == 0:
                continue
            g = 0 if slab == pairs else 1 + 2 * slab + half
            badz = jnp.zeros_like(bad)
            if g == 0:
                badz = jnp.where(row < HIGH, nolow[2], 0.0)
            if g == groups - 1:
                badz = jnp.where(row >= HIGH, nohigh[2], 0.0)
            bias = jnp.where(bad + badz > 0.0, BIG, 0.0)
            vq, kaug = make_keys(turned[HALF * half : HALF * half + width], bias, wts, width)
            vs[c, g] = values_of(vq, width)
            ks[c, g] = kaug
            picked = [
                vq[ROWS * (WINDOW * x + by) - first : ROWS * (WINDOW * x + by + ny) - first] for x in range(bx, bx + nx)
            ]
            qs[c][g] = queries_of(jnp.concatenate(picked, 0), width)
            at = per * g + offsets[c]
            mix[at : at + nq, HALF:] = (chosen if half else pltpu.roll(chosen, HALF, 1))[:, HALF:]

    def finish(start, stop):
        out = feed(against_rows(wts[3], mix[start:stop].astype(BF)), wts, width)
        nil = jnp.zeros((HALF - width, stop - start), F32)
        out = jnp.transpose(jnp.concatenate([out, nil, out, nil], 0))
        for g in range(groups):
            for c, (wx, wy) in enumerate(COLUMNS):
                (bx, nx), (by, ny) = BOXES[wx], BOXES[wy]
                for x in range(nx):
                    for y in range(ny):
                        at = per * g + offsets[c] + ROWS * (x * ny + y) - start
                        if 0 <= at < stop - start:
                            grid[HIGH * wx + x, HIGH * wy + y, WINDOW * g : WINDOW * (g + 1), :] = out[
                                at : at + WINDOW
                            ]

    cols = range(len(COLUMNS))
    slabs = [pairs] + list(range(pairs))
    for slab in slabs:
        for c in cols:
            make(slab, c)

    def keep(g, c):
        n = box_rows(*COLUMNS[c])

        def store(v):
            at = per * g + offsets[c]
            mix[at : at + n, :HALF] = v[:, :HALF]

        return n, store

    attend([(qs[c].at[g], ks.at[c, g], vs.at[c, g], *keep(g, c)) for g in range(groups) for c in cols], width)
    chunk = total // CHUNKS
    for start in range(0, total, chunk):
        finish(start, start + chunk)

    last = WINDOW + 1

    def clear(when, *at):
        @pl.when(when)
        def _():
            grid[at] = jnp.zeros_like(grid[at])

    clear(index[0] == 0, slice(0, 1))
    clear(index[0] == count[0] - 1, slice(last, last + 1))
    clear(index[1] == 0, slice(None), slice(0, 1))
    clear(index[1] == count[1] - 1, slice(None), slice(last, last + 1))
    clear(index[2] == 0, slice(None), slice(None), slice(SHIFT, HIGH))
    clear(index[2] == count[2] - 1, slice(None), slice(None), slice(HIGH + nz, HIGH + nz + 1))

    wc[...] = jnp.zeros(wc.shape, BF)
    for dx in range(3):
        total = None
        for dy in range(3):
            taps = wconv_ref[9 * dx + 3 * dy : 9 * dx + 3 * dy + 3].reshape(3 * width, width)
            i, j = iota((width, 4 * HALF), 0), iota((width, 4 * HALF), 1)
            place = jnp.where(j == i + HALF * dy, 1.0, 0.0).astype(BF)
            part = mm(taps, place)
            total = part if total is None else total + part
        for dz in range(3):
            at = 4 * HALF * dx + HALF * dz
            wc[at : at + width] = total[width * dz : width * (dz + 1)].astype(BF)

    side = WINDOW + 2
    padded = -(-nz // 16) * 16

    def lhs(x):
        taps = [grid[x, :, SHIFT + d : SHIFT + d + padded, :].reshape(side * padded, LANES) for d in range(3)]
        lower = iota(taps[0].shape, 1) < HALF
        return jnp.concatenate([jnp.where(lower, taps[0], taps[1]), taps[2]], 1).astype(BF)

    rows = [lhs(x) for x in range(side)]
    acc = mm(jnp.concatenate([jnp.concatenate(rows[x : x + 3], 1) for x in range(WINDOW)], 0), wc[...])
    strip = WINDOW * padded
    for x in range(WINDOW):
        part = acc[x * side * padded : (x + 1) * side * padded]
        near, second = part[:, :LANES], part[:, LANES:]
        turned = pltpu.roll(near[padded : (WINDOW + 1) * padded], HALF, 1)
        tot[x * strip : (x + 1) * strip] = near[:strip] + turned + second[2 * padded :]
    tot[WINDOW * strip :] = jnp.zeros((tot.shape[0] - WINDOW * strip, LANES), F32)
    diagonal = iota((width, width), 0) == iota((width, width), 1)
    cg = jnp.sum(jnp.where(diagonal, cgain_ref[...], 0.0), 1, keepdims=True)
    normed = norm_cols(jnp.transpose(tot[...])[:width], cg, width)
    active = jnp.where(normed >= 0.0, normed, 0.01 * normed)
    active = jnp.transpose(jnp.concatenate([active, jnp.zeros((LANES - width, tot.shape[0]), F32)], 0))
    for x in range(WINDOW):
        centre = grid[x + 1, 1 : 1 + WINDOW, HIGH : HIGH + padded, :].reshape(strip, LANES)
        result = (centre + active[x * strip : (x + 1) * strip]).reshape(WINDOW, padded, LANES).astype(BF)
        out_ref[x] = result[:, :nz, :width]


def geometry():
    kept = WINDOW * WINDOW - 1
    geo = np.full((16, kept * ROWS), WINDOW, np.float32)
    for v in range(2):
        gone = kept * v
        for i in range(kept):
            spot = i + 1 - v
            for r in range(ROWS):
                t = i * ROWS + r
                if r < WINDOW:
                    geo[8 * v : 8 * v + 3, t] = r, spot // WINDOW, spot % WINDOW
                elif i < WINDOW:
                    geo[8 * v : 8 * v + 3, t] = i, gone // WINDOW, gone % WINDOW
                else:
                    geo[8 * v + 1 : 8 * v + 3, t] = spot // WINDOW, spot % WINDOW
    return jnp.asarray(geo)


def exchange(v, axis, odd):
    count, cores = lax.axis_size(axis), lax.axis_size("gz")
    pairs = []
    for i in range(count):
        low = i - (i - odd) % 2
        for c in range(cores):
            if low < 0 or low + 1 >= count:
                to = (i, c ^ 1 if c ^ 1 < cores else c)
            else:
                to = (low + 1 if i == low else low, c)
            pairs.append((i * cores + c, to[0] * cores + to[1]))
    return lax.ppermute(v, (axis, "gz"), pairs)


def body(volume, w_qkv, w_proj, w_up, w_down, norm_gain, conv_weight, conv_gain):
    sx, sy, sz, width = volume.shape
    spots = sx * sy
    groups = sz // WINDOW
    geo = geometry()
    keys = (spots - 1) * ROWS
    weights = (w_qkv, w_proj, w_up, jnp.swapaxes(w_down, 1, 2), norm_gain)
    halves = [0] if lax.axis_size("gy") == 2 else [0, 1]
    tall = ROWS * groups // 2

    operands = (volume, geo, *weights)
    packed, *cuts = pl.pallas_call(
        functools.partial(first_kernel, width, len(halves)),
        out_shape=[jax.ShapeDtypeStruct((sx, sy, tall, LANES), BF)]
        + [jax.ShapeDtypeStruct((sx, HIGH, tall, LANES), BF) for _ in halves]
        + [jax.ShapeDtypeStruct((HIGH, sy, tall, LANES), BF) for _ in range(2)],
        in_specs=[pl.BlockSpec(memory_space=pltpu.HBM)] * len(operands),
        scratch_shapes=[pltpu.VMEM(v.shape, v.dtype) for v in operands]
        + [
            pltpu.SemaphoreType.DMA((len(operands),)),
            pltpu.VMEM((spots, sz + 12, LANES), F32),
            pltpu.VMEM((groups, spots - 1, ROWS, LANES), F32),
            pltpu.VMEM((groups, HEADS * keys, LANES), BF),
            pltpu.VMEM((groups, LANES, keys), BF),
            pltpu.VMEM((groups, keys, LANES), BF),
            pltpu.VMEM((groups, keys, LANES), F32),
            pltpu.VMEM((width, groups * keys), F32),
            pltpu.VMEM((spots, sz + 12, LANES), F32),
        ],
        compiler_params=pltpu.CompilerParams(vmem_limit_bytes=24 << 20),
        name="first_block",
    )(*[pltpu.with_memory_space_constraint(v, pltpu.HBM) for v in operands])

    xodd = lax.axis_index("gx") % 2

    def cut(v, odd):
        return lax.dynamic_slice_in_dim(v, jnp.where(odd == 0, SHIFT, 0), HIGH, 0)

    def other_core(v):
        return lax.ppermute(v[:, :, -ROWS:, :], "gz", [(0, 1), (1, 0)])

    ys = [exchange(v, "gy", k) for k, v in zip(halves, cuts)]
    xs = [exchange(v, "gx", k) for k, v in enumerate(cuts[len(halves) :])]
    zs = [other_core(v) for v in (packed, *xs)]
    corners = [[exchange(cut(v, (xodd + k) % 2), "gx", k) for k in (0, 1)] for v in ys]
    zcorners = [[other_core(v) for v in (y, *c)] for y, c in zip(ys, corners)]

    side = WINDOW + 2
    rows = sum(box_rows(*c) for c in COLUMNS)
    strip = WINDOW * -(-sz // 16) * 16
    flat = [v for y, c, z in zip(ys, corners, zcorners) for v in (y, *c, *z)]
    operands = [geo, packed, *xs, *zs, *flat, *weights, conv_weight, conv_gain[None, :]]
    return pl.pallas_call(
        functools.partial(second_kernel, width, len(ys)),
        out_shape=jax.ShapeDtypeStruct(volume.shape, volume.dtype),
        scratch_shapes=[
            pltpu.VMEM((groups // 2 + 1, EXT, EXT, ROWS, LANES), F32),
            pltpu.VMEM((-(-(groups + 1) * rows // (CHUNKS * LANES)) * CHUNKS * LANES, LANES), F32),
            pltpu.VMEM((side, side, sz + 12, LANES), F32),
            pltpu.VMEM((3 * 4 * HALF, 4 * HALF), BF),
            pltpu.VMEM((-(-WINDOW * strip // LANES) * LANES, LANES), F32),
            pltpu.VMEM((len(COLUMNS), groups + 1, LANES, keys), BF),
            pltpu.VMEM((len(COLUMNS), groups + 1, keys, LANES), BF),
        ]
        + [pltpu.VMEM((groups + 1, -(-HEADS * box_rows(*c) // 32) * 32, LANES), BF) for c in COLUMNS],
        compiler_params=pltpu.CompilerParams(vmem_limit_bytes=26 << 20),
        name="second_block",
    )(*operands)


def solution(mesh):
    placed = (P(("parts", "gx"), "gy", "gz", None), P(), P(), P(), P(), P(), P(), P())
    return jax.shard_map(
        body,
        mesh=mesh,
        in_specs=placed,
        out_specs=P(("parts", "gx"), "gy", "gz", None),
        check_vma=False,
    )
```

```python
import functools

import jax
import jax.numpy as jnp
import numpy as np
from jax import lax
from jax.experimental import pallas as pl
from jax.experimental.pallas import tpu as pltpu
from jax.sharding import PartitionSpec as P

HEADS = 3
WINDOW = 7
SHIFT = 3
LANES = 128
HALF = 64
ROWS = 8
BIG = -1e30
HIGH = WINDOW - SHIFT
EXT = 2 * WINDOW + 1
BF = jnp.bfloat16
F32 = jnp.float32


def mm(a, b):
    return jnp.dot(a, b, preferred_element_type=F32)


def iota(shape, dim):
    return lax.broadcasted_iota(jnp.int32, shape, dim)


def norm_cols(x, gain, width):
    mean = jnp.sum(x, 0, keepdims=True) * (1.0 / width)
    centred = x - mean
    spread = jnp.sum(centred * centred, 0, keepdims=True) * (1.0 / width)
    return centred * lax.rsqrt(spread + 1e-05) * gain


def twice_gelu(x):
    inner = x * (0.7978845608028654 + (0.7978845608028654 * 0.044715) * (x * x))
    return x + x * jnp.tanh(inner)


def block_weights(b, wqkv_ref, wproj_ref, wup_ref, wdown_ref, gain_ref):
    wqkv = wqkv_ref[b]
    width, triple = wqkv.shape
    scale = (width // HEADS) ** (-0.5)
    i, j = iota((triple, LANES), 0), iota((triple, LANES), 1)
    take_v = (j < width) & (i == j + 2 * width)
    take_q = (j >= HALF) & (j < HALF + width) & (i == j - HALF)
    place = jnp.where(take_v, 1.0, jnp.where(take_q, scale, 0.0)).astype(BF)
    wvq = mm(wqkv, place).astype(BF)
    o, i = iota((width, triple), 0), iota((width, triple), 1)
    place = jnp.where(i == o + width, 1.0, 0.0).astype(BF)
    wk = lax.dot_general(place, wqkv, (((1,), (1,)), ((), ())), preferred_element_type=F32).astype(BF)
    gains = gain_ref[b]
    diagonal = iota((width, width), 0) == iota((width, width), 1)
    first, second = [jnp.sum(jnp.where(diagonal, gains[k : k + 1], 0.0), 1, keepdims=True) for k in range(2)]
    i, j = iota((width, LANES), 0), iota((width, LANES), 1)
    spread = jnp.where(i == j, 1.0, 0.0).astype(BF)
    wp = lax.dot_general(wproj_ref[b], spread, (((0,), (0,)), ((), ())), preferred_element_type=F32)
    wp = (wp + jnp.where(j == i + HALF, 1.0, 0.0)).astype(BF)
    return wvq, wk, first, wp, wup_ref[b], wdown_ref[b] * jnp.asarray(0.5, BF), second


def make_keys(columns, bias, wts, width):
    wvq, wk, gain = wts[0], wts[1], wts[2]
    normed = norm_cols(columns, gain, width).astype(BF)
    vq = lax.dot_general(normed, wvq, (((0,), (0,)), ((), ())), preferred_element_type=F32)
    kt = mm(wk, normed).astype(BF)
    keys = columns.shape[1]
    top = iota((HALF - width, keys), 0) == 0
    extra = jnp.where(top, bias, 0.0).astype(BF)
    kaug = jnp.concatenate([jnp.zeros((HALF, keys), BF), kt, extra], 0)
    return vq, kaug


def values_of(vq, width):
    return jnp.where(iota(vq.shape, 1) < width, vq, 1.0).astype(BF)


def queries_of(rows, width):
    head_dim = width // HEADS
    lane = iota(rows.shape, 1)
    one = jnp.where(lane == HALF + width, 1.0, 0.0)
    parts = []
    for h in range(HEADS):
        low = HALF + h * head_dim
        parts.append(jnp.where((lane >= low) & (lane < low + head_dim), rows, one))
    spare = -len(parts) * rows.shape[0] % 32
    if spare:
        parts.append(jnp.zeros((spare, LANES), F32))
    return jnp.concatenate(parts, 0).astype(BF)


def attend(jobs, width):
    head_dim = width // HEADS
    jobs = list(jobs)
    ahead = mm(jobs[0][0][...], jobs[0][1][...])
    for i, (_, _, values, n, store) in enumerate(jobs):
        scores = ahead
        if i + 1 < len(jobs):
            ahead = mm(jobs[i + 1][0][...], jobs[i + 1][1][...])
        top = jnp.max(scores, -1, keepdims=True)
        weights = jnp.exp(scores - top).astype(BF)
        out = mm(weights, values[...])
        lane = iota((n, LANES), 1)
        lane = jnp.where(lane >= HALF, lane - HALF, lane)
        mixed = out[:n]
        for h in range(1, HEADS):
            mixed = jnp.where(lane >= h * head_dim, out[h * n : (h + 1) * n], mixed)
        store(mixed / pltpu.roll(mixed, HALF, 1))


def feed(first, wts, width):
    wup, wdown, gain = wts[4:]
    first = first.astype(BF).astype(F32)
    normed = norm_cols(first, gain, width).astype(BF)
    upper = lax.dot_general(wup, normed, (((0,), (0,)), ((), ())), preferred_element_type=F32)
    return (first + mm(wdown, twice_gelu(upper).astype(BF))).astype(BF).astype(F32)


def against_rows(w, rows):
    return lax.dot_general(w, rows, (((1,), (1,)), ((), ())), preferred_element_type=F32)


def first_kernel(width, ny, *refs):
    hbm, out_ref = refs[:7], refs[7]
    y_refs, x_refs = refs[8 : 8 + ny], refs[8 + ny : 10 + ny]
    copies = refs[10 + ny : 17 + ny]
    sems = refs[17 + ny]
    raw, tok, qs, ks, vs, mix, held, done = refs[18 + ny :]
    moves = [pltpu.make_async_copy(h, v, sems.at[i]) for i, (h, v) in enumerate(zip(hbm, copies))]
    for m in moves:
        m.start()
    for m in moves[1:]:
        m.wait()
    vol_ref, geo_ref, wqkv_ref, wproj_ref, wup_ref, wdown_ref, gain_ref = copies
    nz = vol_ref.shape[2]
    groups = nz // WINDOW
    spots = WINDOW * WINDOW
    kept = spots - 1
    keys = kept * ROWS
    wts = block_weights(0, wqkv_ref, wproj_ref, wup_ref, wdown_ref, gain_ref)
    done[...] = jnp.zeros(done.shape, F32)
    moves[0].wait()
    raw[:, nz:, :] = jnp.zeros((spots, raw.shape[1] - nz, LANES), F32)
    raw[:, 0:nz, 0:width] = vol_ref[...].astype(F32).reshape(spots, nz, width)
    bias = jnp.where(geo_ref[8:9, :] < WINDOW, 0.0, BIG)

    def make(w):
        tok[w] = raw[0:kept, WINDOW * w : WINDOW * w + ROWS, :]
        for j in range(WINDOW):
            tok[w, j, WINDOW : WINDOW + 1, :] = raw[kept, WINDOW * w + j : WINDOW * w + j + 1, :]
        columns = jnp.transpose(tok[w].reshape(keys, LANES))[:width]
        held[:, keys * w : keys * (w + 1)] = columns
        vq, kaug = make_keys(columns, bias, wts, width)
        vs[w] = values_of(vq, width)
        ks[w] = kaug
        qs[w] = queries_of(vq, width)

    def finish(w0, n):
        mixed = mix[w0 : w0 + n].reshape(n * keys, LANES)[:, :width].astype(BF)
        first = held[:, keys * w0 : keys * (w0 + n)] + against_rows(wts[3][:, :width], mixed)
        out = feed(first, wts, width)
        out = jnp.transpose(jnp.concatenate([out, jnp.zeros((LANES - width, n * keys), F32)], 0))[:, :width]
        out = out.reshape(n, kept, ROWS, width)
        for w in range(w0, w0 + n):
            done[0:kept, WINDOW * w : WINDOW * (w + 1), :width] = out[w - w0, :, :WINDOW, :]
            if w == 0:
                done[0:kept, nz : nz + SHIFT, :width] = out[w - w0, :, :SHIFT, :]
            for j in range(WINDOW):
                one = out[w - w0, j, WINDOW : WINDOW + 1, :]
                done[kept, WINDOW * w + j : WINDOW * w + j + 1, :width] = one
                if w == 0 and j < SHIFT:
                    done[kept, nz + j : nz + j + 1, :width] = one

    for w in range(groups):
        make(w)

    def keep(w):
        def store(v):
            mix[w] = v

        return store

    attend([(qs.at[w], ks.at[w], vs.at[w], keys, keep(w)) for w in range(groups)], width)
    for w in range(0, groups, 2):
        finish(w, min(2, groups - w))
    pieces = [done[:, SHIFT + WINDOW * w : SHIFT + WINDOW * w + ROWS, :] for w in range(groups)]
    rolled = [pltpu.roll(p.reshape(spots * ROWS, LANES), HALF, 1).reshape(spots, ROWS, LANES) for p in pieces[1::2]]
    joined = [a + b for a, b in zip(pieces[0::2], rolled)]
    packed = jnp.concatenate(joined, 1).astype(BF)
    out_ref[...] = packed.reshape(WINDOW, WINDOW, ROWS * len(joined), LANES)
    yodd = lax.axis_index("gy") % 2
    for k, y_ref in enumerate(y_refs):
        start = jnp.where((yodd + k) % 2 == 0, SHIFT, 0)
        y_ref[...] = out_ref[:, pl.ds(start, HIGH)]
    xodd = lax.axis_index("gx") % 2
    for k, x_ref in enumerate(x_refs):
        start = jnp.where((xodd + k) % 2 == 0, SHIFT, 0)
        x_ref[...] = out_ref[pl.ds(start, HIGH)]


CHUNKS = 2
BOXES = ((SHIFT, HIGH), (0, HIGH + 1))
COLUMNS = tuple((wx, wy) for wx in range(2) for wy in range(2))


def box_rows(wx, wy):
    return BOXES[wx][1] * BOXES[wy][1] * ROWS


def position():
    index = [lax.axis_index(a) for a in ("gx", "gy", "gz")]
    count = [lax.axis_size(a) for a in ("gx", "gy", "gz")]
    return index, count


def place_all(ext, split, pieces, shared):
    for tile, other, x, y in pieces:
        nx, ny = tile.shape[:2]
        n = nx * ny
        tile = tile.astype(F32).reshape(n, tile.shape[2], LANES)
        if other is not None:
            other = other.astype(F32).reshape(n, ROWS, LANES)
        for slab, v in enumerate(split(tile, other)):
            ext[slab, pl.ds(x, nx), pl.ds(y, ny)] = v.reshape(nx, ny, ROWS, LANES)
    for wx, wy in shared:
        x0, y0 = WINDOW * wx, WINDOW * wy
        gone = (WINDOW * WINDOW - 1) * wx
        for slab in range(ext.shape[0]):
            for j in range(WINDOW):
                to = j + 1 - wx
                ext[slab, x0 + to // WINDOW, y0 + to % WINDOW, WINDOW : WINDOW + 1, :] = ext[
                    slab, x0 + gone // WINDOW, y0 + gone % WINDOW, j : j + 1, :
                ]


def window_attention(width, groups, cols, work, base, geo_ref, wts, ext, mix, ks, vs, qs):
    index, count = position()
    spots = WINDOW * WINDOW
    keys = (spots - 1) * ROWS
    nolow = [jnp.where(i > 0, 0.0, 1.0) for i in index]
    nohigh = [jnp.where(i < c - 1, 0.0, 1.0) for i, c in zip(index, count)]
    offsets = [sum(box_rows(*COLUMNS[k]) for k in range(c)) for c in range(len(COLUMNS))]
    per = sum(box_rows(*c) for c in COLUMNS)

    def turn(slab, c):
        wx, wy = COLUMNS[c]
        first = ROWS * (1 - wx)
        tokens = ext[slab, WINDOW * wx : WINDOW * (wx + 1), WINDOW * wy : WINDOW * (wy + 1)]
        flat = tokens.reshape(spots * ROWS, LANES)
        return tokens, jnp.transpose(flat[first : first + keys])

    def make(slab, c, tokens, turned):
        wx, wy = COLUMNS[c]
        row, px, py = [geo_ref[8 * wx + k : 8 * wx + k + 1, :] for k in range(3)]
        badx = jnp.where(px < HIGH, nolow[0], 0.0) if wx == 0 else jnp.where(px >= HIGH, nohigh[0], 0.0)
        bady = jnp.where(py < HIGH, nolow[1], 0.0) if wy == 0 else jnp.where(py >= HIGH, nohigh[1], 0.0)
        bad = badx + bady + jnp.where(row < WINDOW, 0.0, 1.0)
        (bx, nx), (by, ny) = BOXES[wx], BOXES[wy]
        nq = nx * ny * ROWS
        first = ROWS * (1 - wx)
        chosen = tokens[bx : bx + nx, by : by + ny].reshape(nq, LANES)
        for slot, (at, half, g) in enumerate(work):
            if at != slab:
                continue
            badz = jnp.zeros_like(bad)
            if g == 0:
                badz = jnp.where(row < HIGH, nolow[2], 0.0)
            if g == groups - 1:
                badz = jnp.where(row >= HIGH, nohigh[2], 0.0)
            bias = jnp.where(bad + badz > 0.0, BIG, 0.0)
            vq, kaug = make_keys(turned[HALF * half : HALF * half + width], bias, wts, width)
            vs[c, slot] = values_of(vq, width)
            ks[c, slot] = kaug
            picked = [
                vq[ROWS * (WINDOW * x + by) - first : ROWS * (WINDOW * x + by + ny) - first] for x in range(bx, bx + nx)
            ]
            qs[c][slot] = queries_of(jnp.concatenate(picked, 0), width)
            start = per * (g - base) + offsets[c]
            mix[start : start + nq, HALF:] = (chosen if half else pltpu.roll(chosen, HALF, 1))[:, HALF:]

    order = [(slab, c) for slab in sorted({w[0] for w in work}) for c in cols]
    ahead = turn(*order[0])
    for i, at in enumerate(order):
        now = ahead
        if i + 1 < len(order):
            ahead = turn(*order[i + 1])
        make(*at, *now)

    def job(slot, c):
        n = box_rows(*COLUMNS[c])
        start = per * (work[slot][2] - base) + offsets[c]

        def store(v):
            mix[start : start + n, :HALF] = v[:, :HALF]

        return qs[c].at[slot], ks.at[c, slot], vs.at[c, slot], n, store

    attend([job(slot, c) for slot in range(len(work)) for c in cols], width)


def inner_kernel(width, ypieces, part, geo_ref, *refs):
    pieces = refs[:3] if part < 0 else refs[: 3 * (ypieces + 1)]
    rest = refs[len(pieces) :]
    if part > 0:
        rest = rest[1:]
    wqkv_ref, wproj_ref, wup_ref, wdown_ref, gain_ref, mix, ext, ks, vs = rest[:9]
    qs = rest[9:]
    pairs = pieces[0].shape[2] // ROWS
    work = [(p, half, 1 + 2 * p + half) for p in range(pairs) for half in range(2)][:-1]
    index, _ = position()
    far = WINDOW + HIGH
    xa, xb = [jnp.where(index[0] % 2 == k, far, 0) for k in (0, 1)]
    ys = [jnp.where(index[1] % 2 == k, far, 0) for k in range(2)]
    wts = block_weights(1, wqkv_ref, wproj_ref, wup_ref, wdown_ref, gain_ref)
    if part > 0:
        mix[...] = refs[len(pieces)][...]
    tiles = []
    for k, y in enumerate([HIGH] + ys[: len(pieces) // 3 - 1]):
        for i, x in enumerate((HIGH, xa, xb)):
            tiles.append((pieces[3 * k + i][...], None, x, y))
    if part < 0:
        mix[...] = jnp.zeros(mix.shape, F32)
        ext[:, :, pl.ds(ys[1], HIGH)] = jnp.zeros((pairs, EXT, HIGH, ROWS, LANES), F32)

    def split(tile, other):
        return [tile[:, p * ROWS : (p + 1) * ROWS, :] for p in range(pairs)]

    def run(cols):
        place_all(ext, split, tiles, [COLUMNS[c] for c in cols])
        window_attention(width, 2 * pairs + 1, cols, work, 1, geo_ref, wts, ext, mix, ks, vs, qs)

    if part == 0:
        run(range(len(COLUMNS)))
    else:
        for side in range(2):

            @pl.when(index[1] % 2 == side)
            def _(side=side):
                wy = side if part < 0 else 1 - side
                run([c for c, col in enumerate(COLUMNS) if col[1] == wy])


def last_kernel(width, ypieces, geo_ref, inner_ref, *refs):
    pieces = refs[: 6 * (ypieces + 1)]
    rest = refs[6 * (ypieces + 1) :]
    wqkv_ref, wproj_ref, wup_ref, wdown_ref, gain_ref, wconv_ref, cgain_ref, out_ref = rest[:8]
    ext, mix, grid, wc, tot, ks, vs = rest[8:15]
    qs = rest[15:]
    nz = out_ref.shape[2]
    pairs = pieces[0].shape[2] // ROWS
    groups = 2 * pairs + 1
    index, count = position()
    far = WINDOW + HIGH
    xa, xb = [jnp.where(index[0] % 2 == k, far, 0) for k in (0, 1)]
    ys = [jnp.where(index[1] % 2 == k, far, 0) for k in range(2)]
    wts = block_weights(1, wqkv_ref, wproj_ref, wup_ref, wdown_ref, gain_ref)
    tiles = []
    for k, y in enumerate([HIGH] + ys[:ypieces]):
        for i, x in enumerate((HIGH, xa, xb)):
            tiles.append((pieces[6 * k + i][:, :, -ROWS:, :], pieces[6 * k + 3 + i][...], x, y))
    if ypieces == 1:
        ext[:, :, pl.ds(ys[1], HIGH)] = jnp.zeros((2, EXT, HIGH, ROWS, LANES), F32)

    def split(mine, other):
        low = iota(mine.shape, 1) < HIGH
        return jnp.where(low, mine, other), jnp.where(low, other, mine)

    per = sum(box_rows(*c) for c in COLUMNS)
    offsets = [sum(box_rows(*COLUMNS[k]) for k in range(c)) for c in range(len(COLUMNS))]
    total = mix.shape[0]
    mix[per : per * (groups - 1)] = inner_ref[...]
    if total > per * groups:
        mix[per * groups :] = jnp.zeros((total - per * groups, LANES), F32)
    cols = range(len(COLUMNS))
    place_all(ext, split, tiles, COLUMNS)
    window_attention(width, groups, cols, [(0, 1, groups - 1), (1, 1, 0)], 0, geo_ref, wts, ext, mix, ks, vs, qs)
    depth = grid.shape[2]
    grid[:, :, WINDOW * groups :] = jnp.zeros((WINDOW + 2, WINDOW + 2, depth - WINDOW * groups, LANES), F32)

    def finish(start, stop):
        out = feed(against_rows(wts[3], mix[start:stop].astype(BF)), wts, width)
        nil = jnp.zeros((HALF - width, stop - start), F32)
        out = jnp.transpose(jnp.concatenate([out, nil, out, nil], 0))
        for g in range(groups):
            for c, (wx, wy) in enumerate(COLUMNS):
                (bx, nx), (by, ny) = BOXES[wx], BOXES[wy]
                for x in range(nx):
                    for y in range(ny):
                        at = per * g + offsets[c] + ROWS * (x * ny + y) - start
                        if 0 <= at < stop - start:
                            grid[HIGH * wx + x, HIGH * wy + y, WINDOW * g : WINDOW * (g + 1), :] = out[
                                at : at + WINDOW
                            ]

    chunk = total // CHUNKS
    for start in range(0, total, chunk):
        finish(start, start + chunk)

    last = WINDOW + 1

    def clear(when, *at):
        @pl.when(when)
        def _():
            grid[at] = jnp.zeros_like(grid[at])

    clear(index[0] == 0, slice(0, 1))
    clear(index[0] == count[0] - 1, slice(last, last + 1))
    clear(index[1] == 0, slice(None), slice(0, 1))
    clear(index[1] == count[1] - 1, slice(None), slice(last, last + 1))
    clear(index[2] == 0, slice(None), slice(None), slice(SHIFT, HIGH))
    clear(index[2] == count[2] - 1, slice(None), slice(None), slice(HIGH + nz, HIGH + nz + 1))

    wc[...] = jnp.zeros(wc.shape, BF)
    for dx in range(3):
        total = None
        for dy in range(3):
            taps = wconv_ref[9 * dx + 3 * dy : 9 * dx + 3 * dy + 3].reshape(3 * width, width)
            i, j = iota((width, 4 * HALF), 0), iota((width, 4 * HALF), 1)
            place = jnp.where(j == i + HALF * dy, 1.0, 0.0).astype(BF)
            part = mm(taps, place)
            total = part if total is None else total + part
        for dz in range(3):
            at = 4 * HALF * dx + HALF * dz
            wc[at : at + width] = total[width * dz : width * (dz + 1)].astype(BF)

    side = WINDOW + 2
    padded = -(-nz // 16) * 16

    def lhs(x):
        taps = [grid[x, :, SHIFT + d : SHIFT + d + padded, :].reshape(side * padded, LANES) for d in range(3)]
        lower = iota(taps[0].shape, 1) < HALF
        return jnp.concatenate([jnp.where(lower, taps[0], taps[1]), taps[2]], 1).astype(BF)

    rows = [lhs(x) for x in range(side)]
    acc = mm(jnp.concatenate([jnp.concatenate(rows[x : x + 3], 1) for x in range(WINDOW)], 0), wc[...])
    strip = WINDOW * padded
    for x in range(WINDOW):
        part = acc[x * side * padded : (x + 1) * side * padded]
        near, second = part[:, :LANES], part[:, LANES:]
        turned = pltpu.roll(near[padded : (WINDOW + 1) * padded], HALF, 1)
        tot[x * strip : (x + 1) * strip] = near[:strip] + turned + second[2 * padded :]
    tot[WINDOW * strip :] = jnp.zeros((tot.shape[0] - WINDOW * strip, LANES), F32)
    diagonal = iota((width, width), 0) == iota((width, width), 1)
    cg = jnp.sum(jnp.where(diagonal, cgain_ref[...], 0.0), 1, keepdims=True)
    normed = norm_cols(jnp.transpose(tot[...])[:width], cg, width)
    active = jnp.where(normed >= 0.0, normed, 0.01 * normed)
    active = jnp.transpose(jnp.concatenate([active, jnp.zeros((LANES - width, tot.shape[0]), F32)], 0))
    for x in range(WINDOW):
        centre = grid[x + 1, 1 : 1 + WINDOW, HIGH : HIGH + padded, :].reshape(strip, LANES)
        result = (centre + active[x * strip : (x + 1) * strip]).reshape(WINDOW, padded, LANES).astype(BF)
        out_ref[x] = result[:, :nz, :width]


def geometry():
    kept = WINDOW * WINDOW - 1
    geo = np.full((16, kept * ROWS), WINDOW, np.float32)
    for v in range(2):
        gone = kept * v
        for i in range(kept):
            spot = i + 1 - v
            for r in range(ROWS):
                t = i * ROWS + r
                if r < WINDOW:
                    geo[8 * v : 8 * v + 3, t] = r, spot // WINDOW, spot % WINDOW
                elif i < WINDOW:
                    geo[8 * v : 8 * v + 3, t] = i, gone // WINDOW, gone % WINDOW
                else:
                    geo[8 * v + 1 : 8 * v + 3, t] = spot // WINDOW, spot % WINDOW
    return jnp.asarray(geo)


def exchange(v, axis, odd):
    count, cores = lax.axis_size(axis), lax.axis_size("gz")
    pairs = []
    for i in range(count):
        low = i - (i - odd) % 2
        for c in range(cores):
            if low < 0 or low + 1 >= count:
                to = (i, c ^ 1 if c ^ 1 < cores else c)
            else:
                to = (low + 1 if i == low else low, c)
            pairs.append((i * cores + c, to[0] * cores + to[1]))
    return lax.ppermute(v, (axis, "gz"), pairs)


def body(volume, w_qkv, w_proj, w_up, w_down, norm_gain, conv_weight, conv_gain):
    sx, sy, sz, width = volume.shape
    spots = sx * sy
    groups = sz // WINDOW
    geo = geometry()
    keys = (spots - 1) * ROWS
    weights = (w_qkv, w_proj, w_up, jnp.swapaxes(w_down, 1, 2), norm_gain)
    halves = [0] if lax.axis_size("gy") == 2 else [0, 1]
    tall = ROWS * groups // 2

    operands = (volume, geo, *weights)
    packed, *cuts = pl.pallas_call(
        functools.partial(first_kernel, width, len(halves)),
        out_shape=[jax.ShapeDtypeStruct((sx, sy, tall, LANES), BF)]
        + [jax.ShapeDtypeStruct((sx, HIGH, tall, LANES), BF) for _ in halves]
        + [jax.ShapeDtypeStruct((HIGH, sy, tall, LANES), BF) for _ in range(2)],
        in_specs=[pl.BlockSpec(memory_space=pltpu.HBM)] * len(operands),
        scratch_shapes=[pltpu.VMEM(v.shape, v.dtype) for v in operands]
        + [
            pltpu.SemaphoreType.DMA((len(operands),)),
            pltpu.VMEM((spots, sz + 12, LANES), F32),
            pltpu.VMEM((groups, spots - 1, ROWS, LANES), F32),
            pltpu.VMEM((groups, HEADS * keys, LANES), BF),
            pltpu.VMEM((groups, LANES, keys), BF),
            pltpu.VMEM((groups, keys, LANES), BF),
            pltpu.VMEM((groups, keys, LANES), F32),
            pltpu.VMEM((width, groups * keys), F32),
            pltpu.VMEM((spots, sz + 12, LANES), F32),
        ],
        compiler_params=pltpu.CompilerParams(vmem_limit_bytes=24 << 20),
        name="first_block",
    )(*[pltpu.with_memory_space_constraint(v, pltpu.HBM) for v in operands])

    xodd = lax.axis_index("gx") % 2

    def cut(v, odd):
        return lax.dynamic_slice_in_dim(v, jnp.where(odd == 0, SHIFT, 0), HIGH, 0)

    def other_core(v):
        return lax.ppermute(v[:, :, -ROWS:, :], "gz", [(0, 1), (1, 0)])

    ys = [exchange(v, "gy", k) for k, v in zip(halves, cuts)]
    xs = [exchange(v, "gx", k) for k, v in enumerate(cuts[len(halves) :])]
    zs = [other_core(v) for v in (packed, *xs)]
    corners = [[exchange(cut(v, (xodd + k) % 2), "gx", k) for k in (0, 1)] for v in ys]
    zcorners = [[other_core(v) for v in (y, *c)] for y, c in zip(ys, corners)]

    side = WINDOW + 2
    rows = sum(box_rows(*c) for c in COLUMNS)
    strip = WINDOW * -(-sz // 16) * 16

    def buffers(slots):
        return [
            pltpu.VMEM((len(COLUMNS), slots, LANES, keys), BF),
            pltpu.VMEM((len(COLUMNS), slots, keys, LANES), BF),
        ] + [pltpu.VMEM((slots, -(-HEADS * box_rows(*c) // 32) * 32, LANES), BF) for c in COLUMNS]

    def inner(part, operands, name):
        return pl.pallas_call(
            functools.partial(inner_kernel, width, len(ys), part),
            out_shape=jax.ShapeDtypeStruct((rows * (groups - 1), LANES), F32),
            scratch_shapes=[pltpu.VMEM((groups // 2, EXT, EXT, ROWS, LANES), F32)] + buffers(groups - 1),
            compiler_params=pltpu.CompilerParams(vmem_limit_bytes=20 << 20),
            cost_estimate=pl.CostEstimate(flops=2 * 10**9, transcendentals=0, bytes_accessed=10**6),
            name=name,
        )(*operands)

    near = [packed, *xs]
    wide = [v for y, c in zip(ys, corners) for v in (y, *c)]
    if len(ys) == 1:
        early = inner(-1, [geo, *near, *weights], "free_windows")
        done = inner(1, [geo, *near, *wide, early, *weights], "inner_windows")
    else:
        done = inner(0, [geo, *near, *wide, *weights], "inner_windows")

    flat = [v for y, c, z in zip(ys, corners, zcorners) for v in (y, *c, *z)]
    operands = [geo, done, *near, *zs, *flat, *weights, conv_weight, conv_gain[None, :]]
    return pl.pallas_call(
        functools.partial(last_kernel, width, len(ys)),
        out_shape=jax.ShapeDtypeStruct(volume.shape, volume.dtype),
        scratch_shapes=[
            pltpu.VMEM((2, EXT, EXT, ROWS, LANES), F32),
            pltpu.VMEM((-(-(groups + 1) * rows // (CHUNKS * LANES)) * CHUNKS * LANES, LANES), F32),
            pltpu.VMEM((side, side, sz + 12, LANES), F32),
            pltpu.VMEM((3 * 4 * HALF, 4 * HALF), BF),
            pltpu.VMEM((-(-WINDOW * strip // LANES) * LANES, LANES), F32),
        ]
        + buffers(2),
        compiler_params=pltpu.CompilerParams(vmem_limit_bytes=26 << 20),
        name="last_windows",
    )(*operands)


def solution(mesh):
    placed = (P(("parts", "gx"), "gy", "gz", None), P(), P(), P(), P(), P(), P(), P())
    return jax.shard_map(
        body,
        mesh=mesh,
        in_specs=placed,
        out_specs=P(("parts", "gx"), "gy", "gz", None),
        check_vma=False,
    )
```

```python
import functools

import jax
import jax.numpy as jnp
import numpy as np
from jax import lax
from jax.experimental import pallas as pl
from jax.experimental.pallas import tpu as pltpu
from jax.sharding import PartitionSpec as P

HEADS = 3
WINDOW = 7
SHIFT = 3
LANES = 128
HALF = 64
ROWS = 8
BIG = -1e30
HIGH = WINDOW - SHIFT
EXT = 2 * WINDOW + 1
BF = jnp.bfloat16
F32 = jnp.float32


def mm(a, b):
    return jnp.dot(a, b, preferred_element_type=F32)


def iota(shape, dim):
    return lax.broadcasted_iota(jnp.int32, shape, dim)


def norm_cols(x, gain, width):
    mean = jnp.sum(x, 0, keepdims=True) * (1.0 / width)
    centred = x - mean
    spread = jnp.sum(centred * centred, 0, keepdims=True) * (1.0 / width)
    return centred * lax.rsqrt(spread + 1e-05) * gain


def twice_gelu(x):
    inner = x * (0.7978845608028654 + (0.7978845608028654 * 0.044715) * (x * x))
    return x + x * jnp.tanh(inner)


def block_weights(b, wqkv_ref, wproj_ref, wup_ref, wdown_ref, gain_ref):
    wqkv = wqkv_ref[b]
    width, triple = wqkv.shape
    scale = (width // HEADS) ** (-0.5)
    i, j = iota((triple, LANES), 0), iota((triple, LANES), 1)
    take_v = (j < width) & (i == j + 2 * width)
    take_q = (j >= HALF) & (j < HALF + width) & (i == j - HALF)
    place = jnp.where(take_v, 1.0, jnp.where(take_q, scale, 0.0)).astype(BF)
    wvq = mm(wqkv, place).astype(BF)
    o, i = iota((width, triple), 0), iota((width, triple), 1)
    place = jnp.where(i == o + width, 1.0, 0.0).astype(BF)
    wk = lax.dot_general(place, wqkv, (((1,), (1,)), ((), ())), preferred_element_type=F32).astype(BF)
    gains = gain_ref[b]
    diagonal = iota((width, width), 0) == iota((width, width), 1)
    first, second = [jnp.sum(jnp.where(diagonal, gains[k : k + 1], 0.0), 1, keepdims=True) for k in range(2)]
    i, j = iota((width, LANES), 0), iota((width, LANES), 1)
    spread = jnp.where(i == j, 1.0, 0.0).astype(BF)
    wp = lax.dot_general(wproj_ref[b], spread, (((0,), (0,)), ((), ())), preferred_element_type=F32)
    wp = (wp + jnp.where(j == i + HALF, 1.0, 0.0)).astype(BF)
    return wvq, wk, first, wp, wup_ref[b], wdown_ref[b] * jnp.asarray(0.5, BF), second


def make_keys(columns, bias, wts, width):
    wvq, wk, gain = wts[0], wts[1], wts[2]
    normed = norm_cols(columns, gain, width).astype(BF)
    vq = lax.dot_general(normed, wvq, (((0,), (0,)), ((), ())), preferred_element_type=F32)
    kt = mm(wk, normed).astype(BF)
    keys = columns.shape[1]
    top = iota((HALF - width, keys), 0) == 0
    extra = jnp.where(top, bias, 0.0).astype(BF)
    kaug = jnp.concatenate([jnp.zeros((HALF, keys), BF), kt, extra], 0)
    return vq, kaug


def values_of(vq, width):
    return jnp.where(iota(vq.shape, 1) < width, vq, 1.0).astype(BF)


def queries_of(rows, width):
    head_dim = width // HEADS
    lane = iota(rows.shape, 1)
    one = jnp.where(lane == HALF + width, 1.0, 0.0)
    parts = []
    for h in range(HEADS):
        low = HALF + h * head_dim
        parts.append(jnp.where((lane >= low) & (lane < low + head_dim), rows, one))
    spare = -len(parts) * rows.shape[0] % 32
    if spare:
        parts.append(jnp.zeros((spare, LANES), F32))
    return jnp.concatenate(parts, 0).astype(BF)


def attend(jobs, width):
    head_dim = width // HEADS
    jobs = list(jobs)
    ahead = mm(jobs[0][0][...], jobs[0][1][...])
    for i, (_, _, values, n, store) in enumerate(jobs):
        scores = ahead
        if i + 1 < len(jobs):
            ahead = mm(jobs[i + 1][0][...], jobs[i + 1][1][...])
        top = jnp.max(scores, -1, keepdims=True)
        weights = jnp.exp(scores - top).astype(BF)
        out = mm(weights, values[...])
        lane = iota((n, LANES), 1)
        lane = jnp.where(lane >= HALF, lane - HALF, lane)
        mixed = out[:n]
        for h in range(1, HEADS):
            mixed = jnp.where(lane >= h * head_dim, out[h * n : (h + 1) * n], mixed)
        store(mixed / pltpu.roll(mixed, HALF, 1))


def feed(first, wts, width):
    wup, wdown, gain = wts[4:]
    first = first.astype(BF).astype(F32)
    normed = norm_cols(first, gain, width).astype(BF)
    upper = lax.dot_general(wup, normed, (((0,), (0,)), ((), ())), preferred_element_type=F32)
    return (first + mm(wdown, twice_gelu(upper).astype(BF))).astype(BF).astype(F32)


def against_rows(w, rows):
    return lax.dot_general(w, rows, (((1,), (1,)), ((), ())), preferred_element_type=F32)


def first_kernel(width, ny, *refs):
    hbm, out_ref = refs[:7], refs[7]
    y_refs, x_refs = refs[8 : 8 + ny], refs[8 + ny : 10 + ny]
    copies = refs[10 + ny : 17 + ny]
    sems = refs[17 + ny]
    raw, tok, qs, ks, vs, mix, held, done = refs[18 + ny :]
    moves = [pltpu.make_async_copy(h, v, sems.at[i]) for i, (h, v) in enumerate(zip(hbm, copies))]
    for m in moves:
        m.start()
    for m in moves[1:]:
        m.wait()
    vol_ref, geo_ref, wqkv_ref, wproj_ref, wup_ref, wdown_ref, gain_ref = copies
    nz = vol_ref.shape[2]
    groups = nz // WINDOW
    spots = WINDOW * WINDOW
    kept = spots - 1
    keys = kept * ROWS
    wts = block_weights(0, wqkv_ref, wproj_ref, wup_ref, wdown_ref, gain_ref)
    done[...] = jnp.zeros(done.shape, F32)
    moves[0].wait()
    raw[:, nz:, :] = jnp.zeros((spots, raw.shape[1] - nz, LANES), F32)
    raw[:, 0:nz, 0:width] = vol_ref[...].astype(F32).reshape(spots, nz, width)
    bias = jnp.where(geo_ref[8:9, :] < WINDOW, 0.0, BIG)

    def make(w):
        tok[w] = raw[0:kept, WINDOW * w : WINDOW * w + ROWS, :]
        for j in range(WINDOW):
            tok[w, j, WINDOW : WINDOW + 1, :] = raw[kept, WINDOW * w + j : WINDOW * w + j + 1, :]
        columns = jnp.transpose(tok[w].reshape(keys, LANES))[:width]
        held[:, keys * w : keys * (w + 1)] = columns
        vq, kaug = make_keys(columns, bias, wts, width)
        vs[w] = values_of(vq, width)
        ks[w] = kaug
        qs[w] = queries_of(vq, width)

    def finish(w0, n):
        mixed = mix[w0 : w0 + n].reshape(n * keys, LANES)[:, :width].astype(BF)
        first = held[:, keys * w0 : keys * (w0 + n)] + against_rows(wts[3][:, :width], mixed)
        out = feed(first, wts, width)
        out = jnp.transpose(jnp.concatenate([out, jnp.zeros((LANES - width, n * keys), F32)], 0))[:, :width]
        out = out.reshape(n, kept, ROWS, width)
        for w in range(w0, w0 + n):
            done[0:kept, WINDOW * w : WINDOW * (w + 1), :width] = out[w - w0, :, :WINDOW, :]
            if w == 0:
                done[0:kept, nz : nz + SHIFT, :width] = out[w - w0, :, :SHIFT, :]
            for j in range(WINDOW):
                one = out[w - w0, j, WINDOW : WINDOW + 1, :]
                done[kept, WINDOW * w + j : WINDOW * w + j + 1, :width] = one
                if w == 0 and j < SHIFT:
                    done[kept, nz + j : nz + j + 1, :width] = one

    for w in range(groups):
        make(w)

    def keep(w):
        def store(v):
            mix[w] = v

        return store

    attend([(qs.at[w], ks.at[w], vs.at[w], keys, keep(w)) for w in range(groups)], width)
    for w in range(0, groups, 2):
        finish(w, min(2, groups - w))
    pieces = [done[:, SHIFT + WINDOW * w : SHIFT + WINDOW * w + ROWS, :] for w in range(groups)]
    rolled = [pltpu.roll(p.reshape(spots * ROWS, LANES), HALF, 1).reshape(spots, ROWS, LANES) for p in pieces[1::2]]
    joined = [a + b for a, b in zip(pieces[0::2], rolled)]
    packed = jnp.concatenate(joined, 1).astype(BF)
    out_ref[...] = packed.reshape(WINDOW, WINDOW, ROWS * len(joined), LANES)
    yodd = lax.axis_index("gy") % 2
    for k, y_ref in enumerate(y_refs):
        start = jnp.where((yodd + k) % 2 == 0, SHIFT, 0)
        y_ref[...] = out_ref[:, pl.ds(start, HIGH)]
    xodd = lax.axis_index("gx") % 2
    for k, x_ref in enumerate(x_refs):
        start = jnp.where((xodd + k) % 2 == 0, SHIFT, 0)
        x_ref[...] = out_ref[pl.ds(start, HIGH)]


CHUNKS = 2
BOXES = ((SHIFT, HIGH), (0, HIGH + 1))
COLUMNS = tuple((wx, wy) for wx in range(2) for wy in range(2))


def box_rows(wx, wy):
    return BOXES[wx][1] * BOXES[wy][1] * ROWS


def position():
    index = [lax.axis_index(a) for a in ("gx", "gy", "gz")]
    count = [lax.axis_size(a) for a in ("gx", "gy", "gz")]
    return index, count


def place_all(ext, split, pieces, shared):
    for tile, other, x, y in pieces:
        nx, ny = tile.shape[:2]
        n = nx * ny
        tile = tile.astype(F32).reshape(n, tile.shape[2], LANES)
        if other is not None:
            other = other.astype(F32).reshape(n, ROWS, LANES)
        for slab, v in enumerate(split(tile, other)):
            ext[slab, pl.ds(x, nx), pl.ds(y, ny)] = v.reshape(nx, ny, ROWS, LANES)
    for wx, wy in shared:
        x0, y0 = WINDOW * wx, WINDOW * wy
        gone = (WINDOW * WINDOW - 1) * wx
        for slab in range(ext.shape[0]):
            for j in range(WINDOW):
                to = j + 1 - wx
                ext[slab, x0 + to // WINDOW, y0 + to % WINDOW, WINDOW : WINDOW + 1, :] = ext[
                    slab, x0 + gone // WINDOW, y0 + gone % WINDOW, j : j + 1, :
                ]


def window_attention(width, groups, cols, work, base, geo_ref, wts, ext, mix, ks, vs, qs):
    index, count = position()
    spots = WINDOW * WINDOW
    keys = (spots - 1) * ROWS
    nolow = [jnp.where(i > 0, 0.0, 1.0) for i in index]
    nohigh = [jnp.where(i < c - 1, 0.0, 1.0) for i, c in zip(index, count)]
    offsets = [sum(box_rows(*COLUMNS[k]) for k in range(c)) for c in range(len(COLUMNS))]
    per = sum(box_rows(*c) for c in COLUMNS)

    def turn(slab, c):
        wx, wy = COLUMNS[c]
        first = ROWS * (1 - wx)
        tokens = ext[slab, WINDOW * wx : WINDOW * (wx + 1), WINDOW * wy : WINDOW * (wy + 1)]
        flat = tokens.reshape(spots * ROWS, LANES)
        return tokens, jnp.transpose(flat[first : first + keys])

    def make(slab, c, tokens, turned):
        wx, wy = COLUMNS[c]
        row, px, py = [geo_ref[8 * wx + k : 8 * wx + k + 1, :] for k in range(3)]
        badx = jnp.where(px < HIGH, nolow[0], 0.0) if wx == 0 else jnp.where(px >= HIGH, nohigh[0], 0.0)
        bady = jnp.where(py < HIGH, nolow[1], 0.0) if wy == 0 else jnp.where(py >= HIGH, nohigh[1], 0.0)
        bad = badx + bady + jnp.where(row < WINDOW, 0.0, 1.0)
        (bx, nx), (by, ny) = BOXES[wx], BOXES[wy]
        nq = nx * ny * ROWS
        first = ROWS * (1 - wx)
        chosen = tokens[bx : bx + nx, by : by + ny].reshape(nq, LANES)
        for slot, (at, half, g) in enumerate(work):
            if at != slab:
                continue
            badz = jnp.zeros_like(bad)
            if g == 0:
                badz = jnp.where(row < HIGH, nolow[2], 0.0)
            if g == groups - 1:
                badz = jnp.where(row >= HIGH, nohigh[2], 0.0)
            bias = jnp.where(bad + badz > 0.0, BIG, 0.0)
            vq, kaug = make_keys(turned[HALF * half : HALF * half + width], bias, wts, width)
            vs[c, slot] = values_of(vq, width)
            ks[c, slot] = kaug
            picked = [
                vq[ROWS * (WINDOW * x + by) - first : ROWS * (WINDOW * x + by + ny) - first] for x in range(bx, bx + nx)
            ]
            qs[c][slot] = queries_of(jnp.concatenate(picked, 0), width)
            start = per * (g - base) + offsets[c]
            mix[start : start + nq, HALF:] = (chosen if half else pltpu.roll(chosen, HALF, 1))[:, HALF:]

    order = [(slab, c) for slab in sorted({w[0] for w in work}) for c in cols]
    ahead = turn(*order[0])
    for i, at in enumerate(order):
        now = ahead
        if i + 1 < len(order):
            ahead = turn(*order[i + 1])
        make(*at, *now)

    def job(slot, c):
        n = box_rows(*COLUMNS[c])
        start = per * (work[slot][2] - base) + offsets[c]

        def store(v):
            mix[start : start + n, :HALF] = v[:, :HALF]

        return qs[c].at[slot], ks.at[c, slot], vs.at[c, slot], n, store

    attend([job(slot, c) for slot in range(len(work)) for c in cols], width)


def inner_kernel(width, ypieces, part, geo_ref, *refs):
    pieces = refs[:3] if part < 0 else refs[: 3 * (ypieces + 1)]
    rest = refs[len(pieces) :]
    if part > 0:
        rest = rest[1:]
    wqkv_ref, wproj_ref, wup_ref, wdown_ref, gain_ref, mix, ext, ks, vs = rest[:9]
    qs = rest[9:]
    pairs = pieces[0].shape[2] // ROWS
    work = [(p, half, 1 + 2 * p + half) for p in range(pairs) for half in range(2)][:-1]
    index, _ = position()
    far = WINDOW + HIGH
    xa, xb = [jnp.where(index[0] % 2 == k, far, 0) for k in (0, 1)]
    ys = [jnp.where(index[1] % 2 == k, far, 0) for k in range(2)]
    wts = block_weights(1, wqkv_ref, wproj_ref, wup_ref, wdown_ref, gain_ref)
    if part > 0:
        mix[...] = refs[len(pieces)][...]
    tiles = []
    for k, y in enumerate([HIGH] + ys[: len(pieces) // 3 - 1]):
        for i, x in enumerate((HIGH, xa, xb)):
            tiles.append((pieces[3 * k + i][...], None, x, y))
    if part < 0:
        mix[...] = jnp.zeros(mix.shape, F32)
        ext[:, :, pl.ds(ys[1], HIGH)] = jnp.zeros((pairs, EXT, HIGH, ROWS, LANES), F32)

    def split(tile, other):
        return [tile[:, p * ROWS : (p + 1) * ROWS, :] for p in range(pairs)]

    def run(cols):
        place_all(ext, split, tiles, [COLUMNS[c] for c in cols])
        window_attention(width, 2 * pairs + 1, cols, work, 1, geo_ref, wts, ext, mix, ks, vs, qs)

    if part == 0:
        run(range(len(COLUMNS)))
    else:
        for side in range(2):

            @pl.when(index[1] % 2 == side)
            def _(side=side):
                wy = side if part < 0 else 1 - side
                run([c for c, col in enumerate(COLUMNS) if col[1] == wy])


def last_kernel(width, ypieces, geo_ref, inner_ref, *refs):
    pieces = refs[: 4 * (ypieces + 1)]
    rest = refs[4 * (ypieces + 1) :]
    wqkv_ref, wproj_ref, wup_ref, wdown_ref, gain_ref, wconv_hbm, cgain_hbm, out_ref = rest[:8]
    ext, mix, grid, wc, tot, wconv_ref, cgain_ref, sems, ks, vs = rest[8:18]
    qs = rest[18:]
    moves = [
        pltpu.make_async_copy(wconv_hbm, wconv_ref, sems.at[0]),
        pltpu.make_async_copy(cgain_hbm, cgain_ref, sems.at[1]),
    ]
    for m in moves:
        m.start()
    nz = out_ref.shape[2]
    pairs = pieces[0].shape[2] // ROWS
    groups = 2 * pairs + 1
    index, count = position()
    far = WINDOW + HIGH
    xa, xb = [jnp.where(index[0] % 2 == k, far, 0) for k in (0, 1)]
    ys = [jnp.where(index[1] % 2 == k, far, 0) for k in range(2)]
    wts = block_weights(1, wqkv_ref, wproj_ref, wup_ref, wdown_ref, gain_ref)
    tiles = []
    for k, y in enumerate([HIGH] + ys[:ypieces]):
        at = 0
        for i, x in enumerate((HIGH, xa, xb)):
            mine = pieces[4 * k + i][:, :, -ROWS:, :]
            tiles.append((mine, pieces[4 * k + 3][at : at + mine.shape[0]], x, y))
            at += mine.shape[0]
    if ypieces == 1:
        ext[:, :, pl.ds(ys[1], HIGH)] = jnp.zeros((2, EXT, HIGH, ROWS, LANES), F32)

    def split(mine, other):
        low = iota(mine.shape, 1) < HIGH
        return jnp.where(low, mine, other), jnp.where(low, other, mine)

    per = sum(box_rows(*c) for c in COLUMNS)
    offsets = [sum(box_rows(*COLUMNS[k]) for k in range(c)) for c in range(len(COLUMNS))]
    total = mix.shape[0]
    mix[per : per * (groups - 1)] = inner_ref[...]
    if total > per * groups:
        mix[per * groups :] = jnp.zeros((total - per * groups, LANES), F32)
    cols = range(len(COLUMNS))
    place_all(ext, split, tiles, COLUMNS)
    window_attention(width, groups, cols, [(0, 1, groups - 1), (1, 1, 0)], 0, geo_ref, wts, ext, mix, ks, vs, qs)
    depth = grid.shape[2]
    grid[:, :, WINDOW * groups :] = jnp.zeros((WINDOW + 2, WINDOW + 2, depth - WINDOW * groups, LANES), F32)

    def finish(start, stop):
        out = feed(against_rows(wts[3], mix[start:stop].astype(BF)), wts, width)
        nil = jnp.zeros((HALF - width, stop - start), F32)
        out = jnp.transpose(jnp.concatenate([out, nil, out, nil], 0))
        for g in range(groups):
            for c, (wx, wy) in enumerate(COLUMNS):
                (bx, nx), (by, ny) = BOXES[wx], BOXES[wy]
                for x in range(nx):
                    for y in range(ny):
                        at = per * g + offsets[c] + ROWS * (x * ny + y) - start
                        if 0 <= at < stop - start:
                            grid[HIGH * wx + x, HIGH * wy + y, WINDOW * g : WINDOW * (g + 1), :] = out[
                                at : at + WINDOW
                            ]

    chunk = total // CHUNKS
    for start in range(0, total, chunk):
        finish(start, start + chunk)

    last = WINDOW + 1

    def clear(when, *at):
        @pl.when(when)
        def _():
            grid[at] = jnp.zeros_like(grid[at])

    clear(index[0] == 0, slice(0, 1))
    clear(index[0] == count[0] - 1, slice(last, last + 1))
    clear(index[1] == 0, slice(None), slice(0, 1))
    clear(index[1] == count[1] - 1, slice(None), slice(last, last + 1))
    clear(index[2] == 0, slice(None), slice(None), slice(SHIFT, HIGH))
    clear(index[2] == count[2] - 1, slice(None), slice(None), slice(HIGH + nz, HIGH + nz + 1))

    for m in moves:
        m.wait()
    wc[...] = jnp.zeros(wc.shape, BF)
    for dx in range(3):
        total = None
        for dy in range(3):
            taps = wconv_ref[9 * dx + 3 * dy : 9 * dx + 3 * dy + 3].reshape(3 * width, width)
            i, j = iota((width, 4 * HALF), 0), iota((width, 4 * HALF), 1)
            place = jnp.where(j == i + HALF * dy, 1.0, 0.0).astype(BF)
            part = mm(taps, place)
            total = part if total is None else total + part
        for dz in range(3):
            at = 4 * HALF * dx + HALF * dz
            wc[at : at + width] = total[width * dz : width * (dz + 1)].astype(BF)

    side = WINDOW + 2
    padded = -(-nz // 16) * 16

    def lhs(x):
        taps = [grid[x, :, SHIFT + d : SHIFT + d + padded, :].reshape(side * padded, LANES) for d in range(3)]
        lower = iota(taps[0].shape, 1) < HALF
        return jnp.concatenate([jnp.where(lower, taps[0], taps[1]), taps[2]], 1).astype(BF)

    rows = [lhs(x) for x in range(side)]
    acc = mm(jnp.concatenate([jnp.concatenate(rows[x : x + 3], 1) for x in range(WINDOW)], 0), wc[...])
    strip = WINDOW * padded
    for x in range(WINDOW):
        part = acc[x * side * padded : (x + 1) * side * padded]
        near, second = part[:, :LANES], part[:, LANES:]
        turned = pltpu.roll(near[padded : (WINDOW + 1) * padded], HALF, 1)
        tot[x * strip : (x + 1) * strip] = near[:strip] + turned + second[2 * padded :]
    tot[WINDOW * strip :] = jnp.zeros((tot.shape[0] - WINDOW * strip, LANES), F32)
    diagonal = iota((width, width), 0) == iota((width, width), 1)
    cg = jnp.sum(jnp.where(diagonal, cgain_ref[...], 0.0), 1, keepdims=True)
    normed = norm_cols(jnp.transpose(tot[...])[:width], cg, width)
    active = jnp.where(normed >= 0.0, normed, 0.01 * normed)
    active = jnp.transpose(jnp.concatenate([active, jnp.zeros((LANES - width, tot.shape[0]), F32)], 0))
    for x in range(WINDOW):
        centre = grid[x + 1, 1 : 1 + WINDOW, HIGH : HIGH + padded, :].reshape(strip, LANES)
        result = (centre + active[x * strip : (x + 1) * strip]).reshape(WINDOW, padded, LANES).astype(BF)
        out_ref[x] = result[:, :nz, :width]


def geometry():
    kept = WINDOW * WINDOW - 1
    geo = np.full((16, kept * ROWS), WINDOW, np.float32)
    for v in range(2):
        gone = kept * v
        for i in range(kept):
            spot = i + 1 - v
            for r in range(ROWS):
                t = i * ROWS + r
                if r < WINDOW:
                    geo[8 * v : 8 * v + 3, t] = r, spot // WINDOW, spot % WINDOW
                elif i < WINDOW:
                    geo[8 * v : 8 * v + 3, t] = i, gone // WINDOW, gone % WINDOW
                else:
                    geo[8 * v + 1 : 8 * v + 3, t] = spot // WINDOW, spot % WINDOW
    return jnp.asarray(geo)


def exchange(v, axis, odd):
    count, cores = lax.axis_size(axis), lax.axis_size("gz")
    pairs = []
    for i in range(count):
        low = i - (i - odd) % 2
        for c in range(cores):
            if low < 0 or low + 1 >= count:
                to = (i, c ^ 1 if c ^ 1 < cores else c)
            else:
                to = (low + 1 if i == low else low, c)
            pairs.append((i * cores + c, to[0] * cores + to[1]))
    return lax.ppermute(v, (axis, "gz"), pairs)


def body(volume, w_qkv, w_proj, w_up, w_down, norm_gain, conv_weight, conv_gain):
    sx, sy, sz, width = volume.shape
    spots = sx * sy
    groups = sz // WINDOW
    geo = geometry()
    keys = (spots - 1) * ROWS
    weights = (w_qkv, w_proj, w_up, jnp.swapaxes(w_down, 1, 2), norm_gain)
    halves = [0] if lax.axis_size("gy") == 2 else [0, 1]
    tall = ROWS * groups // 2

    operands = (volume, geo, *weights)
    packed, *cuts = pl.pallas_call(
        functools.partial(first_kernel, width, len(halves)),
        out_shape=[jax.ShapeDtypeStruct((sx, sy, tall, LANES), BF)]
        + [jax.ShapeDtypeStruct((sx, HIGH, tall, LANES), BF) for _ in halves]
        + [jax.ShapeDtypeStruct((HIGH, sy, tall, LANES), BF) for _ in range(2)],
        in_specs=[pl.BlockSpec(memory_space=pltpu.HBM)] * len(operands),
        scratch_shapes=[pltpu.VMEM(v.shape, v.dtype) for v in operands]
        + [
            pltpu.SemaphoreType.DMA((len(operands),)),
            pltpu.VMEM((spots, sz + 12, LANES), F32),
            pltpu.VMEM((groups, spots - 1, ROWS, LANES), F32),
            pltpu.VMEM((groups, HEADS * keys, LANES), BF),
            pltpu.VMEM((groups, LANES, keys), BF),
            pltpu.VMEM((groups, keys, LANES), BF),
            pltpu.VMEM((groups, keys, LANES), F32),
            pltpu.VMEM((width, groups * keys), F32),
            pltpu.VMEM((spots, sz + 12, LANES), F32),
        ],
        compiler_params=pltpu.CompilerParams(vmem_limit_bytes=24 << 20),
        name="first_block",
    )(*[pltpu.with_memory_space_constraint(v, pltpu.HBM) for v in operands])

    xodd = lax.axis_index("gx") % 2

    def cut(v, odd):
        return lax.dynamic_slice_in_dim(v, jnp.where(odd == 0, SHIFT, 0), HIGH, 0)

    def other_core(v):
        return lax.ppermute(v, "gz", [(0, 1), (1, 0)])

    ys = [exchange(v, "gy", k) for k, v in zip(halves, cuts)]
    xs = [exchange(v, "gx", k) for k, v in enumerate(cuts[len(halves) :])]
    corners = [[exchange(cut(v, (xodd + k) % 2), "gx", k) for k in (0, 1)] for v in ys]

    side = WINDOW + 2
    rows = sum(box_rows(*c) for c in COLUMNS)
    strip = WINDOW * -(-sz // 16) * 16

    def buffers(slots):
        return [
            pltpu.VMEM((len(COLUMNS), slots, LANES, keys), BF),
            pltpu.VMEM((len(COLUMNS), slots, keys, LANES), BF),
        ] + [pltpu.VMEM((slots, -(-HEADS * box_rows(*c) // 32) * 32, LANES), BF) for c in COLUMNS]

    def inner(part, operands, name):
        return pl.pallas_call(
            functools.partial(inner_kernel, width, len(ys), part),
            out_shape=jax.ShapeDtypeStruct((rows * (groups - 1), LANES), F32),
            scratch_shapes=[pltpu.VMEM((groups // 2, EXT, EXT, ROWS, LANES), F32)] + buffers(groups - 1),
            compiler_params=pltpu.CompilerParams(vmem_limit_bytes=20 << 20),
            cost_estimate=pl.CostEstimate(flops=2 * 10**9, transcendentals=0, bytes_accessed=10**6),
            name=name,
        )(*operands)

    def edge(parts, name):
        def kernel(*refs):
            at = 0
            for r in refs[:-1]:
                refs[-1][at : at + r.shape[0]] = r[:, :, -ROWS:, :]
                at += r.shape[0]

        shape = (sum(p.shape[0] for p in parts),) + (parts[0].shape[1], ROWS, LANES)
        return pl.pallas_call(
            kernel,
            out_shape=jax.ShapeDtypeStruct(shape, BF),
            compiler_params=pltpu.CompilerParams(vmem_limit_bytes=4 << 20),
            name=name,
        )(*parts)

    near = [packed, *xs]
    wide = [v for y, c in zip(ys, corners) for v in (y, *c)]
    if len(ys) == 1:
        early = inner(-1, [geo, *near, *weights], "free_windows")
        rows_first = lax.optimization_barrier((early, *near))
        zs = other_core(edge(rows_first[1:], "near_edge"))
        zcorners = [other_core(edge([y, *c], "far_edge")) for y, c in zip(ys, corners)]
        done = inner(1, [geo, *near, *wide, early, *weights], "inner_windows")
    else:
        zs = other_core(edge(near, "near_edge"))
        zcorners = [other_core(edge([y, *c], "far_edge")) for y, c in zip(ys, corners)]
        done = inner(0, [geo, *near, *wide, *weights], "inner_windows")

    flat = [v for y, c, z in zip(ys, corners, zcorners) for v in (y, *c, z)]
    conv = [pltpu.with_memory_space_constraint(v, pltpu.HBM) for v in (conv_weight, conv_gain[None, :])]
    operands = [geo, done, *near, zs, *flat, *weights, *conv]
    vmem = pl.BlockSpec(memory_space=pltpu.VMEM)
    hbm = pl.BlockSpec(memory_space=pltpu.HBM)
    return pl.pallas_call(
        functools.partial(last_kernel, width, len(ys)),
        out_shape=jax.ShapeDtypeStruct(volume.shape, volume.dtype),
        in_specs=[vmem] * (len(operands) - 2) + [hbm] * 2,
        scratch_shapes=[
            pltpu.VMEM((2, EXT, EXT, ROWS, LANES), F32),
            pltpu.VMEM((-(-(groups + 1) * rows // (CHUNKS * LANES)) * CHUNKS * LANES, LANES), F32),
            pltpu.VMEM((side, side, sz + 12, LANES), F32),
            pltpu.VMEM((3 * 4 * HALF, 4 * HALF), BF),
            pltpu.VMEM((-(-WINDOW * strip // LANES) * LANES, LANES), F32),
            pltpu.VMEM(conv[0].shape, conv[0].dtype),
            pltpu.VMEM(conv[1].shape, conv[1].dtype),
            pltpu.SemaphoreType.DMA((2,)),
        ]
        + buffers(2),
        compiler_params=pltpu.CompilerParams(vmem_limit_bytes=26 << 20),
        name="last_windows",
    )(*operands)


def solution(mesh):
    placed = (P(("parts", "gx"), "gy", "gz", None), P(), P(), P(), P(), P(), P(), P())
    return jax.shard_map(
        body,
        mesh=mesh,
        in_specs=placed,
        out_specs=P(("parts", "gx"), "gy", "gz", None),
        check_vma=False,
    )
```

```python
import functools

import jax
import jax.numpy as jnp
import numpy as np
from jax import lax
from jax.experimental import pallas as pl
from jax.experimental.pallas import tpu as pltpu
from jax.sharding import PartitionSpec as P

HEADS = 3
WINDOW = 7
SHIFT = 3
LANES = 128
HALF = 64
ROWS = 8
BIG = -1e30
HIGH = WINDOW - SHIFT
EXT = 2 * WINDOW + 1
BF = jnp.bfloat16
F32 = jnp.float32


def mm(a, b):
    return jnp.dot(a, b, preferred_element_type=F32)


def iota(shape, dim):
    return lax.broadcasted_iota(jnp.int32, shape, dim)


def norm_cols(x, gain, width):
    mean = jnp.sum(x, 0, keepdims=True) * (1.0 / width)
    centred = x - mean
    spread = jnp.sum(centred * centred, 0, keepdims=True) * (1.0 / width)
    return centred * lax.rsqrt(spread + 1e-05) * gain


def twice_gelu(x):
    inner = x * (0.7978845608028654 + (0.7978845608028654 * 0.044715) * (x * x))
    return x + x * jnp.tanh(inner)


def block_weights(b, wqkv_ref, wproj_ref, wup_ref, wdown_ref, gain_ref):
    wqkv = wqkv_ref[b]
    width, triple = wqkv.shape
    scale = (width // HEADS) ** (-0.5)
    i, j = iota((triple, LANES), 0), iota((triple, LANES), 1)
    take_v = (j < width) & (i == j + 2 * width)
    take_q = (j >= HALF) & (j < HALF + width) & (i == j - HALF)
    place = jnp.where(take_v, 1.0, jnp.where(take_q, scale, 0.0)).astype(BF)
    wvq = mm(wqkv, place).astype(BF)
    o, i = iota((width, triple), 0), iota((width, triple), 1)
    place = jnp.where(i == o + width, 1.0, 0.0).astype(BF)
    wk = lax.dot_general(place, wqkv, (((1,), (1,)), ((), ())), preferred_element_type=F32).astype(BF)
    gains = gain_ref[b]
    diagonal = iota((width, width), 0) == iota((width, width), 1)
    first, second = [jnp.sum(jnp.where(diagonal, gains[k : k + 1], 0.0), 1, keepdims=True) for k in range(2)]
    i, j = iota((width, LANES), 0), iota((width, LANES), 1)
    spread = jnp.where(i == j, 1.0, 0.0).astype(BF)
    wp = lax.dot_general(wproj_ref[b], spread, (((0,), (0,)), ((), ())), preferred_element_type=F32)
    wp = (wp + jnp.where(j == i + HALF, 1.0, 0.0)).astype(BF)
    return wvq, wk, first, wp, wup_ref[b], wdown_ref[b] * jnp.asarray(0.5, BF), second


def make_keys(columns, bias, wts, width):
    wvq, wk, gain = wts[0], wts[1], wts[2]
    normed = norm_cols(columns, gain, width).astype(BF)
    vq = lax.dot_general(normed, wvq, (((0,), (0,)), ((), ())), preferred_element_type=F32)
    kt = mm(wk, normed).astype(BF)
    keys = columns.shape[1]
    top = iota((HALF - width, keys), 0) == 0
    extra = jnp.where(top, bias, 0.0).astype(BF)
    kaug = jnp.concatenate([jnp.zeros((HALF, keys), BF), kt, extra], 0)
    return vq, kaug


def values_of(vq, width):
    return jnp.where(iota(vq.shape, 1) < width, vq, 1.0).astype(BF)


def queries_of(rows, width):
    head_dim = width // HEADS
    lane = iota(rows.shape, 1)
    one = jnp.where(lane == HALF + width, 1.0, 0.0)
    parts = []
    for h in range(HEADS):
        low = HALF + h * head_dim
        parts.append(jnp.where((lane >= low) & (lane < low + head_dim), rows, one))
    spare = -len(parts) * rows.shape[0] % 32
    if spare:
        parts.append(jnp.zeros((spare, LANES), F32))
    return jnp.concatenate(parts, 0).astype(BF)


def attend(jobs, width, between=None):
    head_dim = width // HEADS
    jobs = list(jobs)
    ahead = mm(jobs[0][0][...], jobs[0][1][...])
    for i, (_, _, values, n, store) in enumerate(jobs):
        scores = ahead
        if i + 1 < len(jobs):
            ahead = mm(jobs[i + 1][0][...], jobs[i + 1][1][...])
        if between is not None:
            between(i)
        top = jnp.max(scores, -1, keepdims=True)
        weights = jnp.exp(scores - top).astype(BF)
        out = mm(weights, values[...])
        lane = iota((n, LANES), 1)
        lane = jnp.where(lane >= HALF, lane - HALF, lane)
        mixed = out[:n]
        for h in range(1, HEADS):
            mixed = jnp.where(lane >= h * head_dim, out[h * n : (h + 1) * n], mixed)
        store(mixed / pltpu.roll(mixed, HALF, 1))


def feed(first, wts, width):
    wup, wdown, gain = wts[4:]
    first = first.astype(BF).astype(F32)
    normed = norm_cols(first, gain, width).astype(BF)
    upper = lax.dot_general(wup, normed, (((0,), (0,)), ((), ())), preferred_element_type=F32)
    return (first + mm(wdown, twice_gelu(upper).astype(BF))).astype(BF).astype(F32)


def against_rows(w, rows):
    return lax.dot_general(w, rows, (((1,), (1,)), ((), ())), preferred_element_type=F32)


def first_kernel(width, ny, *refs):
    hbm, out_ref = refs[:7], refs[7]
    y_refs, x_refs = refs[8 : 8 + ny], refs[8 + ny : 10 + ny]
    copies = refs[10 + ny : 17 + ny]
    sems = refs[17 + ny]
    raw, tok, qs, ks, vs, mix, held, done = refs[18 + ny :]
    moves = [pltpu.make_async_copy(h, v, sems.at[i]) for i, (h, v) in enumerate(zip(hbm, copies))]
    for m in moves:
        m.start()
    for m in moves[1:]:
        m.wait()
    vol_ref, geo_ref, wqkv_ref, wproj_ref, wup_ref, wdown_ref, gain_ref = copies
    nz = vol_ref.shape[2]
    groups = nz // WINDOW
    spots = WINDOW * WINDOW
    kept = spots - 1
    keys = kept * ROWS
    wts = block_weights(0, wqkv_ref, wproj_ref, wup_ref, wdown_ref, gain_ref)
    done[...] = jnp.zeros(done.shape, F32)
    moves[0].wait()
    raw[:, nz:, :] = jnp.zeros((spots, raw.shape[1] - nz, LANES), F32)
    raw[:, 0:nz, 0:width] = vol_ref[...].astype(F32).reshape(spots, nz, width)
    bias = jnp.where(geo_ref[8:9, :] < WINDOW, 0.0, BIG)

    def make(w):
        tok[w] = raw[0:kept, WINDOW * w : WINDOW * w + ROWS, :]
        for j in range(WINDOW):
            tok[w, j, WINDOW : WINDOW + 1, :] = raw[kept, WINDOW * w + j : WINDOW * w + j + 1, :]
        columns = jnp.transpose(tok[w].reshape(keys, LANES))[:width]
        held[:, keys * w : keys * (w + 1)] = columns
        vq, kaug = make_keys(columns, bias, wts, width)
        vs[w] = values_of(vq, width)
        ks[w] = kaug
        qs[w] = queries_of(vq, width)

    def finish(w0, n):
        mixed = mix[w0 : w0 + n].reshape(n * keys, LANES)[:, :width].astype(BF)
        first = held[:, keys * w0 : keys * (w0 + n)] + against_rows(wts[3][:, :width], mixed)
        out = feed(first, wts, width)
        out = jnp.transpose(jnp.concatenate([out, jnp.zeros((LANES - width, n * keys), F32)], 0))[:, :width]
        out = out.reshape(n, kept, ROWS, width)
        for w in range(w0, w0 + n):
            done[0:kept, WINDOW * w : WINDOW * (w + 1), :width] = out[w - w0, :, :WINDOW, :]
            if w == 0:
                done[0:kept, nz : nz + SHIFT, :width] = out[w - w0, :, :SHIFT, :]
            for j in range(WINDOW):
                one = out[w - w0, j, WINDOW : WINDOW + 1, :]
                done[kept, WINDOW * w + j : WINDOW * w + j + 1, :width] = one
                if w == 0 and j < SHIFT:
                    done[kept, nz + j : nz + j + 1, :width] = one

    for w in range(groups):
        make(w)

    def keep(w):
        def store(v):
            mix[w] = v

        return store

    attend([(qs.at[w], ks.at[w], vs.at[w], keys, keep(w)) for w in range(groups)], width)
    finish(0, groups)
    pieces = [done[:, SHIFT + WINDOW * w : SHIFT + WINDOW * w + ROWS, :] for w in range(groups)]
    rolled = [pltpu.roll(p.reshape(spots * ROWS, LANES), HALF, 1).reshape(spots, ROWS, LANES) for p in pieces[1::2]]
    joined = [a + b for a, b in zip(pieces[0::2], rolled)]
    packed = jnp.concatenate(joined, 1).astype(BF)
    out_ref[...] = packed.reshape(WINDOW, WINDOW, ROWS * len(joined), LANES)
    yodd = lax.axis_index("gy") % 2
    for k, y_ref in enumerate(y_refs):
        start = jnp.where((yodd + k) % 2 == 0, SHIFT, 0)
        y_ref[...] = out_ref[:, pl.ds(start, HIGH)]
    xodd = lax.axis_index("gx") % 2
    for k, x_ref in enumerate(x_refs):
        start = jnp.where((xodd + k) % 2 == 0, SHIFT, 0)
        x_ref[...] = out_ref[pl.ds(start, HIGH)]


BOXES = ((SHIFT, HIGH), (0, HIGH + 1))
COLUMNS = tuple((wx, wy) for wx in range(2) for wy in range(2))


def box_rows(wx, wy):
    return BOXES[wx][1] * BOXES[wy][1] * ROWS


def layout(cols):
    sizes = [box_rows(*COLUMNS[c]) for c in cols]
    return {c: sum(sizes[:i]) for i, c in enumerate(cols)}, sum(sizes)


def half_columns(wy):
    return [c for c, column in enumerate(COLUMNS) if column[1] == wy]


def up(n, m):
    return -(-n // m) * m


def feed_rows(mix, stop, wts, width):
    out = feed(against_rows(wts[3], mix[:stop].astype(BF)), wts, width)
    nil = jnp.zeros((HALF - width, stop), F32)
    return jnp.transpose(jnp.concatenate([out, nil, out, nil], 0))


def position():
    index = [lax.axis_index(a) for a in ("gx", "gy", "gz")]
    count = [lax.axis_size(a) for a in ("gx", "gy", "gz")]
    return index, count


def place_all(ext, split, pieces, shared):
    for tile, other, x, y in pieces:
        nx, ny = tile.shape[:2]
        n = nx * ny
        tile = tile.astype(F32).reshape(n, tile.shape[2], LANES)
        if other is not None:
            other = other.astype(F32).reshape(n, ROWS, LANES)
        for slab, v in enumerate(split(tile, other)):
            ext[slab, pl.ds(x, nx), pl.ds(y, ny)] = v.reshape(nx, ny, ROWS, LANES)
    for wx, wy in shared:
        x0, y0 = WINDOW * wx, WINDOW * wy
        gone = (WINDOW * WINDOW - 1) * wx
        for slab in range(ext.shape[0]):
            for j in range(WINDOW):
                to = j + 1 - wx
                ext[slab, x0 + to // WINDOW, y0 + to % WINDOW, WINDOW : WINDOW + 1, :] = ext[
                    slab, x0 + gone // WINDOW, y0 + gone % WINDOW, j : j + 1, :
                ]


def window_attention(width, groups, cols, work, start_of, geo_ref, wts, ext, mix, ks, vs, qs, between=None):
    index, count = position()
    spots = WINDOW * WINDOW
    keys = (spots - 1) * ROWS
    nolow = [jnp.where(i > 0, 0.0, 1.0) for i in index]
    nohigh = [jnp.where(i < c - 1, 0.0, 1.0) for i, c in zip(index, count)]

    def turn(slab, c):
        wx, wy = COLUMNS[c]
        first = ROWS * (1 - wx)
        tokens = ext[slab, WINDOW * wx : WINDOW * (wx + 1), WINDOW * wy : WINDOW * (wy + 1)]
        flat = tokens.reshape(spots * ROWS, LANES)
        return tokens, jnp.transpose(flat[first : first + keys])

    def make(slab, c, tokens, turned):
        wx, wy = COLUMNS[c]
        row, px, py = [geo_ref[8 * wx + k : 8 * wx + k + 1, :] for k in range(3)]
        badx = jnp.where(px < HIGH, nolow[0], 0.0) if wx == 0 else jnp.where(px >= HIGH, nohigh[0], 0.0)
        bady = jnp.where(py < HIGH, nolow[1], 0.0) if wy == 0 else jnp.where(py >= HIGH, nohigh[1], 0.0)
        bad = badx + bady + jnp.where(row < WINDOW, 0.0, 1.0)
        (bx, nx), (by, ny) = BOXES[wx], BOXES[wy]
        nq = nx * ny * ROWS
        first = ROWS * (1 - wx)
        chosen = tokens[bx : bx + nx, by : by + ny].reshape(nq, LANES)
        for slot, (at, half, g) in enumerate(work):
            if at != slab:
                continue
            badz = jnp.zeros_like(bad)
            if g == 0:
                badz = jnp.where(row < HIGH, nolow[2], 0.0)
            if g == groups - 1:
                badz = jnp.where(row >= HIGH, nohigh[2], 0.0)
            bias = jnp.where(bad + badz > 0.0, BIG, 0.0)
            vq, kaug = make_keys(turned[HALF * half : HALF * half + width], bias, wts, width)
            vs[c, slot] = values_of(vq, width)
            ks[c, slot] = kaug
            picked = [
                vq[ROWS * (WINDOW * x + by) - first : ROWS * (WINDOW * x + by + ny) - first] for x in range(bx, bx + nx)
            ]
            qs[c][slot] = queries_of(jnp.concatenate(picked, 0), width)
            start = start_of(g, c)
            mix[start : start + nq, HALF:] = (chosen if half else pltpu.roll(chosen, HALF, 1))[:, HALF:]

    order = [(slab, c) for slab in sorted({w[0] for w in work}) for c in cols]
    ahead = turn(*order[0])
    for i, at in enumerate(order):
        now = ahead
        if i + 1 < len(order):
            ahead = turn(*order[i + 1])
        make(*at, *now)

    def job(slot, c):
        n = box_rows(*COLUMNS[c])
        start = start_of(work[slot][2], c)

        def store(v):
            mix[start : start + n, :HALF] = v[:, :HALF]

        return qs[c].at[slot], ks.at[c, slot], vs.at[c, slot], n, store

    attend([job(slot, c) for slot in range(len(work)) for c in cols], width, between)


def inner_kernel(width, ypieces, part, geo_ref, *refs):
    pieces = refs[:3] if part < 0 else refs[: 3 * (ypieces + 1)]
    rest = refs[len(pieces) :]
    wqkv_ref, wproj_ref, wup_ref, wdown_ref, gain_ref, out_ref, mix, ext, ks, vs = rest[:10]
    qs = rest[10:]
    pairs = pieces[0].shape[2] // ROWS
    work = [(p, half, 1 + 2 * p + half) for p in range(pairs) for half in range(2)][:-1]
    index, _ = position()
    far = WINDOW + HIGH
    xa, xb = [jnp.where(index[0] % 2 == k, far, 0) for k in (0, 1)]
    ys = [jnp.where(index[1] % 2 == k, far, 0) for k in range(2)]
    wts = block_weights(1, wqkv_ref, wproj_ref, wup_ref, wdown_ref, gain_ref)
    tiles = []
    for k, y in enumerate([HIGH] + ys[: len(pieces) // 3 - 1]):
        for i, x in enumerate((HIGH, xa, xb)):
            tiles.append((pieces[3 * k + i][...], None, x, y))
    if part < 0:
        ext[:, :, pl.ds(ys[1], HIGH)] = jnp.zeros((pairs, EXT, HIGH, ROWS, LANES), F32)

    def split(tile, other):
        return [tile[:, p * ROWS : (p + 1) * ROWS, :] for p in range(pairs)]

    def run(cols):
        places, rows = layout(cols)
        used = rows * len(work)
        rows_ref = mix if part < 0 else out_ref
        rest = rows_ref.shape[0] - used
        if rest:
            rows_ref[used:] = jnp.zeros((rest, LANES), F32)
        place_all(ext, split, tiles, [COLUMNS[c] for c in cols])
        start = lambda g, c: rows * (g - 1) + places[c]
        window_attention(width, 2 * pairs + 1, cols, work, start, geo_ref, wts, ext, rows_ref, ks, vs, qs)
        if part < 0:
            stop = up(used, LANES)
            out_ref[:stop] = feed_rows(mix, stop, wts, width)
            if stop < out_ref.shape[0]:
                out_ref[stop:] = jnp.zeros((out_ref.shape[0] - stop, LANES), F32)

    if part == 0:
        run(list(range(len(COLUMNS))))
    else:
        for side in range(2):

            @pl.when(index[1] % 2 == side)
            def _(side=side):
                run(half_columns(side if part < 0 else 1 - side))


def last_kernel(width, ypieces, geo_ref, inner_ref, *refs):
    early = ypieces == 1
    if early:
        free_ref, *refs = refs
    pieces = refs[: 4 * (ypieces + 1)]
    rest = refs[4 * (ypieces + 1) :]
    wqkv_ref, wproj_ref, wup_ref, wdown_ref, gain_ref, wconv_hbm, cgain_hbm, out_ref = rest[:8]
    ext, mix, fed, grid, wc, tot, wconv_ref, cgain_ref, sems, ks, vs = rest[8:19]
    qs = rest[19:]
    moves = [
        pltpu.make_async_copy(wconv_hbm, wconv_ref, sems.at[0]),
        pltpu.make_async_copy(cgain_hbm, cgain_ref, sems.at[1]),
    ]
    for m in moves:
        m.start()
    nz = out_ref.shape[2]
    pairs = pieces[0].shape[2] // ROWS
    groups = 2 * pairs + 1
    index, count = position()
    far = WINDOW + HIGH
    xa, xb = [jnp.where(index[0] % 2 == k, far, 0) for k in (0, 1)]
    ys = [jnp.where(index[1] % 2 == k, far, 0) for k in range(2)]
    wts = block_weights(1, wqkv_ref, wproj_ref, wup_ref, wdown_ref, gain_ref)
    tiles = []
    for k, y in enumerate([HIGH] + ys[:ypieces]):
        at = 0
        for i, x in enumerate((HIGH, xa, xb)):
            mine = pieces[4 * k + i][:, :, -ROWS:, :]
            tiles.append((mine, pieces[4 * k + 3][at : at + mine.shape[0]], x, y))
            at += mine.shape[0]
    if ypieces == 1:
        ext[:, :, pl.ds(ys[1], HIGH)] = jnp.zeros((2, EXT, HIGH, ROWS, LANES), F32)

    def split(mine, other):
        low = iota(mine.shape, 1) < HIGH
        return jnp.where(low, mine, other), jnp.where(low, other, mine)

    cols = list(range(len(COLUMNS)))
    offsets, per = layout(cols)
    depth = grid.shape[2]
    grid[:, :, WINDOW * groups :] = jnp.zeros((WINDOW + 2, WINDOW + 2, depth - WINDOW * groups, LANES), F32)

    def scatter(g, rows, base, cols):
        places, _ = layout(cols)
        for c in cols:
            wx, wy = COLUMNS[c]
            (_, nx), (_, ny) = BOXES[wx], BOXES[wy]
            for x in range(nx):
                for y in range(ny):
                    at = base + places[c] + ROWS * (x * ny + y)
                    grid[HIGH * wx + x, HIGH * wy + y, WINDOW * g : WINDOW * (g + 1), :] = rows[at : at + WINDOW]

    used = 2 * per
    stop = up(used, LANES)
    mix[used:stop] = jnp.zeros((stop - used, LANES), F32)
    fed[...] = feed_rows(inner_ref, inner_ref.shape[0], wts, width)
    place_all(ext, split, tiles, COLUMNS)
    work = [(0, 1, groups - 1), (1, 1, 0)]
    start = lambda g, c: (per if g else 0) + offsets[c]
    window_attention(width, groups, cols, work, start, geo_ref, wts, ext, mix, ks, vs, qs)
    out = feed_rows(mix, stop, wts, width)
    scatter(0, out, 0, cols)
    scatter(groups - 1, out, per, cols)
    if early:
        for side in range(2):

            @pl.when(index[1] % 2 == side)
            def _(side=side):
                for wy, rows in ((side, free_ref), (1 - side, fed)):
                    half = half_columns(wy)
                    for g in range(1, groups - 1):
                        scatter(g, rows, layout(half)[1] * (g - 1), half)

    else:
        for g in range(1, groups - 1):
            scatter(g, fed, per * (g - 1), cols)

    last = WINDOW + 1

    def clear(when, *at):
        @pl.when(when)
        def _():
            grid[at] = jnp.zeros_like(grid[at])

    clear(index[0] == 0, slice(0, 1))
    clear(index[0] == count[0] - 1, slice(last, last + 1))
    clear(index[1] == 0, slice(None), slice(0, 1))
    clear(index[1] == count[1] - 1, slice(None), slice(last, last + 1))
    clear(index[2] == 0, slice(None), slice(None), slice(SHIFT, HIGH))
    clear(index[2] == count[2] - 1, slice(None), slice(None), slice(HIGH + nz, HIGH + nz + 1))

    for m in moves:
        m.wait()
    wc[...] = jnp.zeros(wc.shape, BF)
    for dx in range(3):
        total = None
        for dy in range(3):
            taps = wconv_ref[9 * dx + 3 * dy : 9 * dx + 3 * dy + 3].reshape(3 * width, width)
            i, j = iota((width, 4 * HALF), 0), iota((width, 4 * HALF), 1)
            place = jnp.where(j == i + HALF * dy, 1.0, 0.0).astype(BF)
            part = mm(taps, place)
            total = part if total is None else total + part
        for dz in range(3):
            at = 4 * HALF * dx + HALF * dz
            wc[at : at + width] = total[width * dz : width * (dz + 1)].astype(BF)

    side = WINDOW + 2
    padded = -(-nz // 16) * 16

    def lhs(x):
        taps = [grid[x, :, SHIFT + d : SHIFT + d + padded, :].reshape(side * padded, LANES) for d in range(3)]
        lower = iota(taps[0].shape, 1) < HALF
        return jnp.concatenate([jnp.where(lower, taps[0], taps[1]), taps[2]], 1).astype(BF)

    rows = [lhs(x) for x in range(side)]
    acc = mm(jnp.concatenate([jnp.concatenate(rows[x : x + 3], 1) for x in range(WINDOW)], 0), wc[...])
    strip = WINDOW * padded
    for x in range(WINDOW):
        part = acc[x * side * padded : (x + 1) * side * padded]
        near, second = part[:, :LANES], part[:, LANES:]
        turned = pltpu.roll(near[padded : (WINDOW + 1) * padded], HALF, 1)
        tot[x * strip : (x + 1) * strip] = near[:strip] + turned + second[2 * padded :]
    tot[WINDOW * strip :] = jnp.zeros((tot.shape[0] - WINDOW * strip, LANES), F32)
    diagonal = iota((width, width), 0) == iota((width, width), 1)
    cg = jnp.sum(jnp.where(diagonal, cgain_ref[...], 0.0), 1, keepdims=True)
    normed = norm_cols(jnp.transpose(tot[...])[:width], cg, width)
    active = jnp.where(normed >= 0.0, normed, 0.01 * normed)
    active = jnp.transpose(jnp.concatenate([active, jnp.zeros((LANES - width, tot.shape[0]), F32)], 0))
    for x in range(WINDOW):
        centre = grid[x + 1, 1 : 1 + WINDOW, HIGH : HIGH + padded, :].reshape(strip, LANES)
        result = (centre + active[x * strip : (x + 1) * strip]).reshape(WINDOW, padded, LANES).astype(BF)
        out_ref[x] = result[:, :nz, :width]


def geometry():
    kept = WINDOW * WINDOW - 1
    geo = np.full((16, kept * ROWS), WINDOW, np.float32)
    for v in range(2):
        gone = kept * v
        for i in range(kept):
            spot = i + 1 - v
            for r in range(ROWS):
                t = i * ROWS + r
                if r < WINDOW:
                    geo[8 * v : 8 * v + 3, t] = r, spot // WINDOW, spot % WINDOW
                elif i < WINDOW:
                    geo[8 * v : 8 * v + 3, t] = i, gone // WINDOW, gone % WINDOW
                else:
                    geo[8 * v + 1 : 8 * v + 3, t] = spot // WINDOW, spot % WINDOW
    return jnp.asarray(geo)


def exchange(v, axis, odd):
    count, cores = lax.axis_size(axis), lax.axis_size("gz")
    pairs = []
    for i in range(count):
        low = i - (i - odd) % 2
        for c in range(cores):
            if low < 0 or low + 1 >= count:
                to = (i, c ^ 1 if c ^ 1 < cores else c)
            else:
                to = (low + 1 if i == low else low, c)
            pairs.append((i * cores + c, to[0] * cores + to[1]))
    return lax.ppermute(v, (axis, "gz"), pairs)


def body(volume, w_qkv, w_proj, w_up, w_down, norm_gain, conv_weight, conv_gain):
    sx, sy, sz, width = volume.shape
    spots = sx * sy
    groups = sz // WINDOW
    geo = geometry()
    keys = (spots - 1) * ROWS
    weights = (w_qkv, w_proj, w_up, jnp.swapaxes(w_down, 1, 2), norm_gain)
    halves = [0] if lax.axis_size("gy") == 2 else [0, 1]
    tall = ROWS * groups // 2

    operands = (volume, geo, *weights)
    packed, *cuts = pl.pallas_call(
        functools.partial(first_kernel, width, len(halves)),
        out_shape=[jax.ShapeDtypeStruct((sx, sy, tall, LANES), BF)]
        + [jax.ShapeDtypeStruct((sx, HIGH, tall, LANES), BF) for _ in halves]
        + [jax.ShapeDtypeStruct((HIGH, sy, tall, LANES), BF) for _ in range(2)],
        in_specs=[pl.BlockSpec(memory_space=pltpu.HBM)] * len(operands),
        scratch_shapes=[pltpu.VMEM(v.shape, v.dtype) for v in operands]
        + [
            pltpu.SemaphoreType.DMA((len(operands),)),
            pltpu.VMEM((spots, sz + 12, LANES), F32),
            pltpu.VMEM((groups, spots - 1, ROWS, LANES), F32),
            pltpu.VMEM((groups, HEADS * keys, LANES), BF),
            pltpu.VMEM((groups, LANES, keys), BF),
            pltpu.VMEM((groups, keys, LANES), BF),
            pltpu.VMEM((groups, keys, LANES), F32),
            pltpu.VMEM((width, groups * keys), F32),
            pltpu.VMEM((spots, sz + 12, LANES), F32),
        ],
        compiler_params=pltpu.CompilerParams(vmem_limit_bytes=24 << 20),
        name="first_block",
    )(*[pltpu.with_memory_space_constraint(v, pltpu.HBM) for v in operands])

    xodd = lax.axis_index("gx") % 2

    def cut(v, odd):
        return lax.dynamic_slice_in_dim(v, jnp.where(odd == 0, SHIFT, 0), HIGH, 0)

    def other_core(v):
        return lax.ppermute(v, "gz", [(0, 1), (1, 0)])

    ys = [exchange(v, "gy", k) for k, v in zip(halves, cuts)]
    xs = [exchange(v, "gx", k) for k, v in enumerate(cuts[len(halves) :])]
    corners = [[exchange(cut(v, (xodd + k) % 2), "gx", k) for k in (0, 1)] for v in ys]

    side = WINDOW + 2
    rows = sum(box_rows(*c) for c in COLUMNS)
    strip = WINDOW * -(-sz // 16) * 16

    def buffers(slots):
        return [
            pltpu.VMEM((len(COLUMNS), slots, LANES, keys), BF),
            pltpu.VMEM((len(COLUMNS), slots, keys, LANES), BF),
        ] + [pltpu.VMEM((slots, -(-HEADS * box_rows(*c) // 32) * 32, LANES), BF) for c in COLUMNS]

    span = up(max(layout(half_columns(k))[1] for k in range(2)) * (groups - 1), LANES)

    def inner(part, operands, name):
        return pl.pallas_call(
            functools.partial(inner_kernel, width, len(ys), part),
            out_shape=jax.ShapeDtypeStruct((span if part else up(rows * (groups - 1), LANES), LANES), F32),
            scratch_shapes=[
                pltpu.VMEM((span, LANES), F32),
                pltpu.VMEM((groups // 2, EXT, EXT, ROWS, LANES), F32),
            ]
            + buffers(groups - 1),
            compiler_params=pltpu.CompilerParams(vmem_limit_bytes=20 << 20),
            cost_estimate=pl.CostEstimate(flops=2 * 10**9, transcendentals=0, bytes_accessed=10**6),
            name=name,
        )(*operands)

    def edge(parts, name):
        def kernel(*refs):
            at = 0
            for r in refs[:-1]:
                refs[-1][at : at + r.shape[0]] = r[:, :, -ROWS:, :]
                at += r.shape[0]

        shape = (sum(p.shape[0] for p in parts),) + (parts[0].shape[1], ROWS, LANES)
        return pl.pallas_call(
            kernel,
            out_shape=jax.ShapeDtypeStruct(shape, BF),
            compiler_params=pltpu.CompilerParams(vmem_limit_bytes=4 << 20),
            name=name,
        )(*parts)

    near = [packed, *xs]
    wide = [v for y, c in zip(ys, corners) for v in (y, *c)]
    if len(ys) == 1:
        early = inner(-1, [geo, *near, *weights], "free_windows")
        rows_first = lax.optimization_barrier((early, *near))
        zs = other_core(edge(rows_first[1:], "near_edge"))
        zcorners = [other_core(edge([y, *c], "far_edge")) for y, c in zip(ys, corners)]
        done = inner(1, [geo, *near, *wide, *weights], "inner_windows")
        done = [done, early]
    else:
        zs = other_core(edge(near, "near_edge"))
        zcorners = [other_core(edge([y, *c], "far_edge")) for y, c in zip(ys, corners)]
        done = [inner(0, [geo, *near, *wide, *weights], "inner_windows")]

    flat = [v for y, c, z in zip(ys, corners, zcorners) for v in (y, *c, z)]
    conv = [pltpu.with_memory_space_constraint(v, pltpu.HBM) for v in (conv_weight, conv_gain[None, :])]
    operands = [geo, *done, *near, zs, *flat, *weights, *conv]
    vmem = pl.BlockSpec(memory_space=pltpu.VMEM)
    hbm = pl.BlockSpec(memory_space=pltpu.HBM)
    return pl.pallas_call(
        functools.partial(last_kernel, width, len(ys)),
        out_shape=jax.ShapeDtypeStruct(volume.shape, volume.dtype),
        in_specs=[vmem] * (len(operands) - 2) + [hbm] * 2,
        scratch_shapes=[
            pltpu.VMEM((2, EXT, EXT, ROWS, LANES), F32),
            pltpu.VMEM((up(2 * rows, LANES), LANES), F32),
            pltpu.VMEM(done[0].shape, F32),
            pltpu.VMEM((side, side, sz + 12, LANES), F32),
            pltpu.VMEM((3 * 4 * HALF, 4 * HALF), BF),
            pltpu.VMEM((-(-WINDOW * strip // LANES) * LANES, LANES), F32),
            pltpu.VMEM(conv[0].shape, conv[0].dtype),
            pltpu.VMEM(conv[1].shape, conv[1].dtype),
            pltpu.SemaphoreType.DMA((2,)),
        ]
        + buffers(2),
        compiler_params=pltpu.CompilerParams(vmem_limit_bytes=26 << 20),
        name="last_windows",
    )(*operands)


def solution(mesh):
    placed = (P(("parts", "gx"), "gy", "gz", None), P(), P(), P(), P(), P(), P(), P())
    return jax.shard_map(
        body,
        mesh=mesh,
        in_specs=placed,
        out_specs=P(("parts", "gx"), "gy", "gz", None),
        check_vma=False,
    )
```

```python
import functools

import jax
import jax.numpy as jnp
import numpy as np
from jax import lax
from jax.experimental import pallas as pl
from jax.experimental.pallas import tpu as pltpu
from jax.sharding import PartitionSpec as P


HEADS = 3
WINDOW = 7
SHIFT = 3
LANES = 128
HALF = 64
ROWS = 8
BIG = -1e30
HIGH = WINDOW - SHIFT
EXT = 2 * WINDOW + 1
BF = jnp.bfloat16
F32 = jnp.float32


def mm(a, b):
    return jnp.dot(a, b, preferred_element_type=F32)


def iota(shape, dim):
    return lax.broadcasted_iota(jnp.int32, shape, dim)


def norm_cols(x, gain, width):
    mean = jnp.sum(x, 0, keepdims=True) * (1.0 / width)
    centred = x - mean
    spread = jnp.sum(centred * centred, 0, keepdims=True) * (1.0 / width)
    return centred * lax.rsqrt(spread + 1e-05) * gain


def twice_gelu(x):
    inner = x * (0.7978845608028654 + (0.7978845608028654 * 0.044715) * (x * x))
    return x + x * jnp.tanh(inner)


def block_weights(b, wqkv_ref, wproj_ref, wup_ref, wdown_ref, gain_ref):
    wqkv = wqkv_ref[b]
    width, triple = wqkv.shape
    scale = (width // HEADS) ** (-0.5)
    i, j = iota((triple, LANES), 0), iota((triple, LANES), 1)
    take_v = (j < width) & (i == j + 2 * width)
    take_q = (j >= HALF) & (j < HALF + width) & (i == j - HALF)
    place = jnp.where(take_v, 1.0, jnp.where(take_q, scale, 0.0)).astype(BF)
    wvq = mm(wqkv, place).astype(BF)
    o, i = iota((width, triple), 0), iota((width, triple), 1)
    place = jnp.where(i == o + width, 1.0, 0.0).astype(BF)
    wk = lax.dot_general(place, wqkv, (((1,), (1,)), ((), ())), preferred_element_type=F32).astype(BF)
    gains = gain_ref[b]
    diagonal = iota((width, width), 0) == iota((width, width), 1)
    first, second = [jnp.sum(jnp.where(diagonal, gains[k : k + 1], 0.0), 1, keepdims=True) for k in range(2)]
    i, j = iota((width, LANES), 0), iota((width, LANES), 1)
    spread = jnp.where(i == j, 1.0, 0.0).astype(BF)
    wp = lax.dot_general(wproj_ref[b], spread, (((0,), (0,)), ((), ())), preferred_element_type=F32)
    wp = (wp + jnp.where(j == i + HALF, 1.0, 0.0)).astype(BF)
    return wvq, wk, first, wp, wup_ref[b], wdown_ref[b] * jnp.asarray(0.5, BF), second


def make_keys(columns, bias, wts, width):
    wvq, wk, gain = wts[0], wts[1], wts[2]
    normed = norm_cols(columns, gain, width).astype(BF)
    vq = lax.dot_general(normed, wvq, (((0,), (0,)), ((), ())), preferred_element_type=F32)
    kt = mm(wk, normed).astype(BF)
    keys = columns.shape[1]
    top = iota((HALF - width, keys), 0) == 0
    extra = jnp.where(top, bias, 0.0).astype(BF)
    kaug = jnp.concatenate([jnp.zeros((HALF, keys), BF), kt, extra], 0)
    return vq, kaug


def values_of(vq, width):
    return jnp.where(iota(vq.shape, 1) < width, vq, 1.0).astype(BF)


def queries_of(rows, width):
    head_dim = width // HEADS
    lane = iota(rows.shape, 1)
    one = jnp.where(lane == HALF + width, 1.0, 0.0)
    parts = []
    for h in range(HEADS):
        low = HALF + h * head_dim
        parts.append(jnp.where((lane >= low) & (lane < low + head_dim), rows, one))
    spare = -len(parts) * rows.shape[0] % 32
    if spare:
        parts.append(jnp.zeros((spare, LANES), F32))
    return jnp.concatenate(parts, 0).astype(BF)


def attend(jobs, width, between=None):
    head_dim = width // HEADS
    jobs = list(jobs)
    ahead = mm(jobs[0][0][...], jobs[0][1][...])
    for i, (_, _, values, n, store) in enumerate(jobs):
        scores = ahead
        if i + 1 < len(jobs):
            ahead = mm(jobs[i + 1][0][...], jobs[i + 1][1][...])
        if between is not None:
            between(i)
        top = jnp.max(scores, -1, keepdims=True)
        weights = jnp.exp(scores - top).astype(BF)
        out = mm(weights, values[...])
        lane = iota((n, LANES), 1)
        lane = jnp.where(lane >= HALF, lane - HALF, lane)
        mixed = out[:n]
        for h in range(1, HEADS):
            mixed = jnp.where(lane >= h * head_dim, out[h * n : (h + 1) * n], mixed)
        store(mixed / pltpu.roll(mixed, HALF, 1))


def feed(first, wts, width):
    wup, wdown, gain = wts[4:]
    first = first.astype(BF).astype(F32)
    normed = norm_cols(first, gain, width).astype(BF)
    upper = lax.dot_general(wup, normed, (((0,), (0,)), ((), ())), preferred_element_type=F32)
    return (first + mm(wdown, twice_gelu(upper).astype(BF))).astype(BF).astype(F32)


def against_rows(w, rows):
    return lax.dot_general(w, rows, (((1,), (1,)), ((), ())), preferred_element_type=F32)


def first_kernel(width, ny, *refs):
    hbm, out_ref = refs[:7], refs[7]
    y_refs, x_refs = refs[8 : 8 + ny], refs[8 + ny : 10 + ny]
    copies = refs[10 + ny : 17 + ny]
    sems = refs[17 + ny]
    raw, tok, qs, ks, vs, mix, held, done = refs[18 + ny :]
    moves = [pltpu.make_async_copy(h, v, sems.at[i]) for i, (h, v) in enumerate(zip(hbm, copies))]
    for m in moves:
        m.start()
    for m in moves[1:]:
        m.wait()
    vol_ref, geo_ref, wqkv_ref, wproj_ref, wup_ref, wdown_ref, gain_ref = copies
    nz = vol_ref.shape[2]
    groups = nz // WINDOW
    spots = WINDOW * WINDOW
    kept = spots - 1
    keys = kept * ROWS
    wts = block_weights(0, wqkv_ref, wproj_ref, wup_ref, wdown_ref, gain_ref)
    done[...] = jnp.zeros(done.shape, F32)
    moves[0].wait()
    raw[:, nz:, :] = jnp.zeros((spots, raw.shape[1] - nz, LANES), F32)
    raw[:, 0:nz, 0:width] = vol_ref[...].astype(F32).reshape(spots, nz, width)
    bias = jnp.where(geo_ref[8:9, :] < WINDOW, 0.0, BIG)

    def make(w):
        tok[w] = raw[0:kept, WINDOW * w : WINDOW * w + ROWS, :]
        for j in range(WINDOW):
            tok[w, j, WINDOW : WINDOW + 1, :] = raw[kept, WINDOW * w + j : WINDOW * w + j + 1, :]
        columns = jnp.transpose(tok[w].reshape(keys, LANES))[:width]
        held[:, keys * w : keys * (w + 1)] = columns
        vq, kaug = make_keys(columns, bias, wts, width)
        vs[w] = values_of(vq, width)
        ks[w] = kaug
        qs[w] = queries_of(vq, width)

    def finish(w0, n):
        mixed = mix[w0 : w0 + n].reshape(n * keys, LANES)[:, :width].astype(BF)
        first = held[:, keys * w0 : keys * (w0 + n)] + against_rows(wts[3][:, :width], mixed)
        out = feed(first, wts, width)
        out = jnp.transpose(jnp.concatenate([out, jnp.zeros((LANES - width, n * keys), F32)], 0))[:, :width]
        out = out.reshape(n, kept, ROWS, width)
        for w in range(w0, w0 + n):
            done[0:kept, WINDOW * w : WINDOW * (w + 1), :width] = out[w - w0, :, :WINDOW, :]
            if w == 0:
                done[0:kept, nz : nz + SHIFT, :width] = out[w - w0, :, :SHIFT, :]
            for j in range(WINDOW):
                one = out[w - w0, j, WINDOW : WINDOW + 1, :]
                done[kept, WINDOW * w + j : WINDOW * w + j + 1, :width] = one
                if w == 0 and j < SHIFT:
                    done[kept, nz + j : nz + j + 1, :width] = one

    for w in range(groups):
        make(w)

    def keep(w):
        def store(v):
            mix[w] = v

        return store

    attend([(qs.at[w], ks.at[w], vs.at[w], keys, keep(w)) for w in range(groups)], width)
    finish(0, groups)
    pieces = [done[:, SHIFT + WINDOW * w : SHIFT + WINDOW * w + ROWS, :] for w in range(groups)]
    rolled = [pltpu.roll(p.reshape(spots * ROWS, LANES), HALF, 1).reshape(spots, ROWS, LANES) for p in pieces[1::2]]
    joined = [a + b for a, b in zip(pieces[0::2], rolled)]
    packed = jnp.concatenate(joined, 1).astype(BF)
    out_ref[...] = packed.reshape(WINDOW, WINDOW, ROWS * len(joined), LANES)
    yodd = lax.axis_index("gy") % 2
    for k, y_ref in enumerate(y_refs):
        start = jnp.where((yodd + k) % 2 == 0, SHIFT, 0)
        y_ref[...] = out_ref[:, pl.ds(start, HIGH)]
    xodd = lax.axis_index("gx") % 2
    for k, x_ref in enumerate(x_refs):
        start = jnp.where((xodd + k) % 2 == 0, SHIFT, 0)
        x_ref[...] = out_ref[pl.ds(start, HIGH)]


BOXES = ((SHIFT, HIGH), (0, HIGH + 1))
COLUMNS = tuple((wx, wy) for wx in range(2) for wy in range(2))


def box_rows(wx, wy):
    return BOXES[wx][1] * BOXES[wy][1] * ROWS


def layout(cols):
    sizes = [box_rows(*COLUMNS[c]) for c in cols]
    return {c: sum(sizes[:i]) for i, c in enumerate(cols)}, sum(sizes)


def half_columns(wy):
    return [c for c, column in enumerate(COLUMNS) if column[1] == wy]


def up(n, m):
    return -(-n // m) * m


def feed_rows(mix, stop, wts, width):
    out = feed(against_rows(wts[3], mix[:stop].astype(BF)), wts, width)
    nil = jnp.zeros((HALF - width, stop), F32)
    return jnp.transpose(jnp.concatenate([out, nil, out, nil], 0))


def position():
    index = [lax.axis_index(a) for a in ("gx", "gy", "gz")]
    count = [lax.axis_size(a) for a in ("gx", "gy", "gz")]
    return index, count


def place_all(ext, split, pieces, shared):
    for tile, other, x, y in pieces:
        nx, ny = tile.shape[:2]
        n = nx * ny
        tile = tile.astype(F32).reshape(n, tile.shape[2], LANES)
        if other is not None:
            other = other.astype(F32).reshape(n, ROWS, LANES)
        for slab, v in enumerate(split(tile, other)):
            ext[slab, pl.ds(x, nx), pl.ds(y, ny)] = v.reshape(nx, ny, ROWS, LANES)
    for wx, wy in shared:
        x0, y0 = WINDOW * wx, WINDOW * wy
        gone = (WINDOW * WINDOW - 1) * wx
        for slab in range(ext.shape[0]):
            for j in range(WINDOW):
                to = j + 1 - wx
                ext[slab, x0 + to // WINDOW, y0 + to % WINDOW, WINDOW : WINDOW + 1, :] = ext[
                    slab, x0 + gone // WINDOW, y0 + gone % WINDOW, j : j + 1, :
                ]


def window_attention(width, groups, cols, work, start_of, geo_ref, wts, ext, mix, ks, vs, qs, between=None):
    index, count = position()
    spots = WINDOW * WINDOW
    keys = (spots - 1) * ROWS
    nolow = [jnp.where(i > 0, 0.0, 1.0) for i in index]
    nohigh = [jnp.where(i < c - 1, 0.0, 1.0) for i, c in zip(index, count)]

    def turn(slab, c):
        wx, wy = COLUMNS[c]
        first = ROWS * (1 - wx)
        tokens = ext[slab, WINDOW * wx : WINDOW * (wx + 1), WINDOW * wy : WINDOW * (wy + 1)]
        flat = tokens.reshape(spots * ROWS, LANES)
        return tokens, jnp.transpose(flat[first : first + keys])

    def make(slab, c, tokens, turned):
        wx, wy = COLUMNS[c]
        row, px, py = [geo_ref[8 * wx + k : 8 * wx + k + 1, :] for k in range(3)]
        badx = jnp.where(px < HIGH, nolow[0], 0.0) if wx == 0 else jnp.where(px >= HIGH, nohigh[0], 0.0)
        bady = jnp.where(py < HIGH, nolow[1], 0.0) if wy == 0 else jnp.where(py >= HIGH, nohigh[1], 0.0)
        bad = badx + bady + jnp.where(row < WINDOW, 0.0, 1.0)
        (bx, nx), (by, ny) = BOXES[wx], BOXES[wy]
        nq = nx * ny * ROWS
        first = ROWS * (1 - wx)
        chosen = tokens[bx : bx + nx, by : by + ny].reshape(nq, LANES)
        for slot, (at, half, g) in enumerate(work):
            if at != slab:
                continue
            badz = jnp.zeros_like(bad)
            if g == 0:
                badz = jnp.where(row < HIGH, nolow[2], 0.0)
            if g == groups - 1:
                badz = jnp.where(row >= HIGH, nohigh[2], 0.0)
            bias = jnp.where(bad + badz > 0.0, BIG, 0.0)
            vq, kaug = make_keys(turned[HALF * half : HALF * half + width], bias, wts, width)
            vs[c, slot] = values_of(vq, width)
            ks[c, slot] = kaug
            picked = [
                vq[ROWS * (WINDOW * x + by) - first : ROWS * (WINDOW * x + by + ny) - first] for x in range(bx, bx + nx)
            ]
            qs[c][slot] = queries_of(jnp.concatenate(picked, 0), width)
            start = start_of(g, c)
            mix[start : start + nq, HALF:] = (chosen if half else pltpu.roll(chosen, HALF, 1))[:, HALF:]

    order = [(slab, c) for slab in sorted({w[0] for w in work}) for c in cols]
    ahead = turn(*order[0])
    for i, at in enumerate(order):
        now = ahead
        if i + 1 < len(order):
            ahead = turn(*order[i + 1])
        make(*at, *now)

    def job(slot, c):
        n = box_rows(*COLUMNS[c])
        start = start_of(work[slot][2], c)

        def store(v):
            mix[start : start + n, :HALF] = v[:, :HALF]

        return qs[c].at[slot], ks.at[c, slot], vs.at[c, slot], n, store

    attend([job(slot, c) for slot in range(len(work)) for c in cols], width, between)


def inner_kernel(width, ypieces, part, geo_ref, *refs):
    pieces = refs[:3] if part < 0 else refs[: 3 * (ypieces + 1)]
    rest = refs[len(pieces) :]
    wqkv_ref, wproj_ref, wup_ref, wdown_ref, gain_ref, out_ref, mix, ext, ks, vs = rest[:10]
    qs = rest[10:]
    pairs = pieces[0].shape[2] // ROWS
    work = [(p, half, 1 + 2 * p + half) for p in range(pairs) for half in range(2)][:-1]
    index, _ = position()
    far = WINDOW + HIGH
    xa, xb = [jnp.where(index[0] % 2 == k, far, 0) for k in (0, 1)]
    ys = [jnp.where(index[1] % 2 == k, far, 0) for k in range(2)]
    wts = block_weights(1, wqkv_ref, wproj_ref, wup_ref, wdown_ref, gain_ref)
    tiles = []
    for k, y in enumerate([HIGH] + ys[: len(pieces) // 3 - 1]):
        for i, x in enumerate((HIGH, xa, xb)):
            tiles.append((pieces[3 * k + i][...], None, x, y))
    if part < 0:
        ext[:, :, pl.ds(ys[1], HIGH)] = jnp.zeros((pairs, EXT, HIGH, ROWS, LANES), F32)

    def split(tile, other):
        return [tile[:, p * ROWS : (p + 1) * ROWS, :] for p in range(pairs)]

    def run(cols):
        places, rows = layout(cols)
        used = rows * len(work)
        rows_ref = mix if part < 0 else out_ref
        rest = rows_ref.shape[0] - used
        if rest:
            rows_ref[used:] = jnp.zeros((rest, LANES), F32)
        place_all(ext, split, tiles, [COLUMNS[c] for c in cols])
        start = lambda g, c: rows * (g - 1) + places[c]
        window_attention(width, 2 * pairs + 1, cols, work, start, geo_ref, wts, ext, rows_ref, ks, vs, qs)
        if part < 0:
            stop = up(used, LANES)
            out_ref[:stop] = feed_rows(mix, stop, wts, width)
            if stop < out_ref.shape[0]:
                out_ref[stop:] = jnp.zeros((out_ref.shape[0] - stop, LANES), F32)

    if part == 0:
        run(list(range(len(COLUMNS))))
    else:
        for side in range(2):

            @pl.when(index[1] % 2 == side)
            def _(side=side):
                run(half_columns(side if part < 0 else 1 - side))


def last_kernel(width, ypieces, geo_ref, inner_ref, *refs):
    early = ypieces == 1
    if early:
        free_ref, *refs = refs
    pieces = refs[: 4 * (ypieces + 1)]
    rest = refs[4 * (ypieces + 1) :]
    wqkv_ref, wproj_ref, wup_ref, wdown_ref, gain_ref, wconv_hbm, cgain_hbm, out_ref = rest[:8]
    ext, mix, fed, grid, wc, tot, wconv_ref, cgain_ref, sems, ks, vs = rest[8:19]
    qs = rest[19:]
    moves = [
        pltpu.make_async_copy(wconv_hbm, wconv_ref, sems.at[0]),
        pltpu.make_async_copy(cgain_hbm, cgain_ref, sems.at[1]),
    ]
    for m in moves:
        m.start()
    nz = out_ref.shape[2]
    pairs = pieces[0].shape[2] // ROWS
    groups = 2 * pairs + 1
    index, count = position()
    far = WINDOW + HIGH
    xa, xb = [jnp.where(index[0] % 2 == k, far, 0) for k in (0, 1)]
    ys = [jnp.where(index[1] % 2 == k, far, 0) for k in range(2)]
    wts = block_weights(1, wqkv_ref, wproj_ref, wup_ref, wdown_ref, gain_ref)
    tiles = []
    for k, y in enumerate([HIGH] + ys[:ypieces]):
        at = 0
        for i, x in enumerate((HIGH, xa, xb)):
            mine = pieces[4 * k + i][:, :, -ROWS:, :]
            tiles.append((mine, pieces[4 * k + 3][at : at + mine.shape[0]], x, y))
            at += mine.shape[0]
    if ypieces == 1:
        ext[:, :, pl.ds(ys[1], HIGH)] = jnp.zeros((2, EXT, HIGH, ROWS, LANES), F32)

    def split(mine, other):
        low = iota(mine.shape, 1) < HIGH
        return jnp.where(low, mine, other), jnp.where(low, other, mine)

    cols = list(range(len(COLUMNS)))
    offsets, per = layout(cols)
    depth = grid.shape[2]
    grid[:, :, WINDOW * groups :] = jnp.zeros((WINDOW + 2, WINDOW + 2, depth - WINDOW * groups, LANES), F32)

    def scatter(g, rows, base, cols):
        places, _ = layout(cols)
        for c in cols:
            wx, wy = COLUMNS[c]
            (_, nx), (_, ny) = BOXES[wx], BOXES[wy]
            for x in range(nx):
                for y in range(ny):
                    at = base + places[c] + ROWS * (x * ny + y)
                    grid[HIGH * wx + x, HIGH * wy + y, WINDOW * g : WINDOW * (g + 1), :] = rows[at : at + WINDOW]

    used = 2 * per
    stop = up(used, LANES)
    mix[used:stop] = jnp.zeros((stop - used, LANES), F32)
    fed[...] = feed_rows(inner_ref, inner_ref.shape[0], wts, width)
    place_all(ext, split, tiles, COLUMNS)
    work = [(0, 1, groups - 1), (1, 1, 0)]
    start = lambda g, c: (per if g else 0) + offsets[c]
    window_attention(width, groups, cols, work, start, geo_ref, wts, ext, mix, ks, vs, qs)
    out = feed_rows(mix, stop, wts, width)
    scatter(0, out, 0, cols)
    scatter(groups - 1, out, per, cols)
    if early:
        for side in range(2):

            @pl.when(index[1] % 2 == side)
            def _(side=side):
                for wy, rows in ((side, free_ref), (1 - side, fed)):
                    half = half_columns(wy)
                    for g in range(1, groups - 1):
                        scatter(g, rows, layout(half)[1] * (g - 1), half)

    else:
        for g in range(1, groups - 1):
            scatter(g, fed, per * (g - 1), cols)

    last = WINDOW + 1

    def clear(when, *at):
        @pl.when(when)
        def _():
            grid[at] = jnp.zeros_like(grid[at])

    clear(index[0] == 0, slice(0, 1))
    clear(index[0] == count[0] - 1, slice(last, last + 1))
    clear(index[1] == 0, slice(None), slice(0, 1))
    clear(index[1] == count[1] - 1, slice(None), slice(last, last + 1))
    clear(index[2] == 0, slice(None), slice(None), slice(SHIFT, HIGH))
    clear(index[2] == count[2] - 1, slice(None), slice(None), slice(HIGH + nz, HIGH + nz + 1))

    for m in moves:
        m.wait()
    wc[...] = jnp.zeros(wc.shape, BF)
    for dx in range(3):
        total = None
        for dy in range(3):
            taps = wconv_ref[9 * dx + 3 * dy : 9 * dx + 3 * dy + 3].reshape(3 * width, width)
            i, j = iota((width, 4 * HALF), 0), iota((width, 4 * HALF), 1)
            place = jnp.where(j == i + HALF * dy, 1.0, 0.0).astype(BF)
            part = mm(taps, place)
            total = part if total is None else total + part
        for dz in range(3):
            at = 4 * HALF * dx + HALF * dz
            wc[at : at + width] = total[width * dz : width * (dz + 1)].astype(BF)

    side = WINDOW + 2
    padded = -(-nz // 16) * 16

    def lhs(x):
        taps = [grid[x, :, SHIFT + d : SHIFT + d + padded, :].reshape(side * padded, LANES) for d in range(3)]
        lower = iota(taps[0].shape, 1) < HALF
        return jnp.concatenate([jnp.where(lower, taps[0], taps[1]), taps[2]], 1).astype(BF)

    rows = [lhs(x) for x in range(side)]
    acc = mm(jnp.concatenate([jnp.concatenate(rows[x : x + 3], 1) for x in range(WINDOW)], 0), wc[...])
    strip = WINDOW * padded
    for x in range(WINDOW):
        part = acc[x * side * padded : (x + 1) * side * padded]
        near, second = part[:, :LANES], part[:, LANES:]
        turned = pltpu.roll(near[padded : (WINDOW + 1) * padded], HALF, 1)
        tot[x * strip : (x + 1) * strip] = near[:strip] + turned + second[2 * padded :]
    tot[WINDOW * strip :] = jnp.zeros((tot.shape[0] - WINDOW * strip, LANES), F32)
    diagonal = iota((width, width), 0) == iota((width, width), 1)
    cg = jnp.sum(jnp.where(diagonal, cgain_ref[...], 0.0), 1, keepdims=True)
    normed = norm_cols(jnp.transpose(tot[...])[:width], cg, width)
    active = jnp.where(normed >= 0.0, normed, 0.01 * normed)
    active = jnp.transpose(jnp.concatenate([active, jnp.zeros((LANES - width, tot.shape[0]), F32)], 0))
    for x in range(WINDOW):
        centre = grid[x + 1, 1 : 1 + WINDOW, HIGH : HIGH + padded, :].reshape(strip, LANES)
        result = (centre + active[x * strip : (x + 1) * strip]).reshape(WINDOW, padded, LANES).astype(BF)
        out_ref[x] = result[:, :nz, :width]


def geometry():
    kept = WINDOW * WINDOW - 1
    geo = np.full((16, kept * ROWS), WINDOW, np.float32)
    for v in range(2):
        gone = kept * v
        for i in range(kept):
            spot = i + 1 - v
            for r in range(ROWS):
                t = i * ROWS + r
                if r < WINDOW:
                    geo[8 * v : 8 * v + 3, t] = r, spot // WINDOW, spot % WINDOW
                elif i < WINDOW:
                    geo[8 * v : 8 * v + 3, t] = i, gone // WINDOW, gone % WINDOW
                else:
                    geo[8 * v + 1 : 8 * v + 3, t] = spot // WINDOW, spot % WINDOW
    return jnp.asarray(geo)


def exchange(v, axis, odd):
    count, cores = lax.axis_size(axis), lax.axis_size("gz")
    pairs = []
    for i in range(count):
        low = i - (i - odd) % 2
        for c in range(cores):
            if low < 0 or low + 1 >= count:
                to = (i, c ^ 1 if c ^ 1 < cores else c)
            else:
                to = (low + 1 if i == low else low, c)
            pairs.append((i * cores + c, to[0] * cores + to[1]))
    return lax.ppermute(v, (axis, "gz"), pairs)


def body(volume, w_qkv, w_proj, w_up, w_down, norm_gain, conv_weight, conv_gain):
    sx, sy, sz, width = volume.shape
    spots = sx * sy
    groups = sz // WINDOW
    geo = geometry()
    keys = (spots - 1) * ROWS
    weights = (w_qkv, w_proj, w_up, jnp.swapaxes(w_down, 1, 2), norm_gain)
    halves = [0] if lax.axis_size("gy") == 2 else [0, 1]
    tall = ROWS * groups // 2

    operands = (volume, geo, *weights)
    packed, *cuts = pl.pallas_call(
        functools.partial(first_kernel, width, len(halves)),
        out_shape=[jax.ShapeDtypeStruct((sx, sy, tall, LANES), BF)]
        + [jax.ShapeDtypeStruct((sx, HIGH, tall, LANES), BF) for _ in halves]
        + [jax.ShapeDtypeStruct((HIGH, sy, tall, LANES), BF) for _ in range(2)],
        in_specs=[pl.BlockSpec(memory_space=pltpu.HBM)] * len(operands),
        scratch_shapes=[pltpu.VMEM(v.shape, v.dtype) for v in operands]
        + [
            pltpu.SemaphoreType.DMA((len(operands),)),
            pltpu.VMEM((spots, sz + 12, LANES), F32),
            pltpu.VMEM((groups, spots - 1, ROWS, LANES), F32),
            pltpu.VMEM((groups, HEADS * keys, LANES), BF),
            pltpu.VMEM((groups, LANES, keys), BF),
            pltpu.VMEM((groups, keys, LANES), BF),
            pltpu.VMEM((groups, keys, LANES), F32),
            pltpu.VMEM((width, groups * keys), F32),
            pltpu.VMEM((spots, sz + 12, LANES), F32),
        ],
        compiler_params=pltpu.CompilerParams(vmem_limit_bytes=24 << 20),
        name="first_block",
    )(*[pltpu.with_memory_space_constraint(v, pltpu.HBM) for v in operands])

    xodd = lax.axis_index("gx") % 2

    def cut(v, odd):
        return lax.dynamic_slice_in_dim(v, jnp.where(odd == 0, SHIFT, 0), HIGH, 0)

    def other_core(v):
        return lax.ppermute(v, "gz", [(0, 1), (1, 0)])

    ys = [exchange(v, "gy", k) for k, v in zip(halves, cuts)]
    xs = [exchange(v, "gx", k) for k, v in enumerate(cuts[len(halves) :])]
    corners = [[exchange(cut(v, (xodd + k) % 2), "gx", k) for k in (0, 1)] for v in ys]

    side = WINDOW + 2
    rows = sum(box_rows(*c) for c in COLUMNS)
    strip = WINDOW * -(-sz // 16) * 16

    def buffers(slots):
        return [
            pltpu.VMEM((len(COLUMNS), slots, LANES, keys), BF),
            pltpu.VMEM((len(COLUMNS), slots, keys, LANES), BF),
        ] + [pltpu.VMEM((slots, -(-HEADS * box_rows(*c) // 32) * 32, LANES), BF) for c in COLUMNS]

    span = up(max(layout(half_columns(k))[1] for k in range(2)) * (groups - 1), LANES)

    def inner(part, operands):
        return pl.pallas_call(
            functools.partial(inner_kernel, width, len(ys), part),
            out_shape=jax.ShapeDtypeStruct((span if part else up(rows * (groups - 1), LANES), LANES), F32),
            scratch_shapes=[
                pltpu.VMEM((span, LANES), F32),
                pltpu.VMEM((groups // 2, EXT, EXT, ROWS, LANES), F32),
            ]
            + buffers(groups - 1),
            compiler_params=pltpu.CompilerParams(vmem_limit_bytes=20 << 20),
            cost_estimate=pl.CostEstimate(flops=2 * 10**9, transcendentals=0, bytes_accessed=10**6),
        )(*operands)

    def edge(parts):
        def kernel(*refs):
            at = 0
            for r in refs[:-1]:
                refs[-1][at : at + r.shape[0]] = r[:, :, -ROWS:, :]
                at += r.shape[0]

        shape = (sum(p.shape[0] for p in parts),) + (parts[0].shape[1], ROWS, LANES)
        return pl.pallas_call(
            kernel,
            out_shape=jax.ShapeDtypeStruct(shape, BF),
            compiler_params=pltpu.CompilerParams(vmem_limit_bytes=4 << 20),
        )(*parts)

    near = [packed, *xs]
    wide = [v for y, c in zip(ys, corners) for v in (y, *c)]
    if len(ys) == 1:
        early = inner(-1, [geo, *near, *weights])
        rows_first = lax.optimization_barrier((early, *near))
        zs = other_core(edge(rows_first[1:]))
        zcorners = [other_core(edge([y, *c])) for y, c in zip(ys, corners)]
        done = inner(1, [geo, *near, *wide, *weights])
        done = [done, early]
    else:
        zs = other_core(edge(near))
        zcorners = [other_core(edge([y, *c])) for y, c in zip(ys, corners)]
        done = [inner(0, [geo, *near, *wide, *weights])]

    flat = [v for y, c, z in zip(ys, corners, zcorners) for v in (y, *c, z)]
    conv = [pltpu.with_memory_space_constraint(v, pltpu.HBM) for v in (conv_weight, conv_gain[None, :])]
    operands = [geo, *done, *near, zs, *flat, *weights, *conv]
    vmem = pl.BlockSpec(memory_space=pltpu.VMEM)
    hbm = pl.BlockSpec(memory_space=pltpu.HBM)
    return pl.pallas_call(
        functools.partial(last_kernel, width, len(ys)),
        out_shape=jax.ShapeDtypeStruct(volume.shape, volume.dtype),
        in_specs=[vmem] * (len(operands) - 2) + [hbm] * 2,
        scratch_shapes=[
            pltpu.VMEM((2, EXT, EXT, ROWS, LANES), F32),
            pltpu.VMEM((up(2 * rows, LANES), LANES), F32),
            pltpu.VMEM(done[0].shape, F32),
            pltpu.VMEM((side, side, sz + 12, LANES), F32),
            pltpu.VMEM((3 * 4 * HALF, 4 * HALF), BF),
            pltpu.VMEM((-(-WINDOW * strip // LANES) * LANES, LANES), F32),
            pltpu.VMEM(conv[0].shape, conv[0].dtype),
            pltpu.VMEM(conv[1].shape, conv[1].dtype),
            pltpu.SemaphoreType.DMA((2,)),
        ]
        + buffers(2),
        compiler_params=pltpu.CompilerParams(vmem_limit_bytes=26 << 20),
        name="last_windows",
    )(*operands)


def solution(mesh):
    placed = (P(("parts", "gx"), "gy", "gz", None), P(), P(), P(), P(), P(), P(), P())

    return jax.shard_map(
        body,
        mesh=mesh,
        in_specs=placed,
        out_specs=P(("parts", "gx"), "gy", "gz", None),
        check_vma=False,
    )
```

```python
import functools

import jax
import jax.numpy as jnp
import numpy as np
from jax import lax
from jax.experimental import pallas as pl
from jax.experimental.pallas import tpu as pltpu
from jax.sharding import PartitionSpec as P


HEADS = 3
WINDOW = 7
SHIFT = 3
LANES = 128
HALF = 64
ROWS = 8
BIG = -1e30
HIGH = WINDOW - SHIFT
EXT = 2 * WINDOW + 1
BF = jnp.bfloat16
F32 = jnp.float32


def mm(a, b):
    return jnp.dot(a, b, preferred_element_type=F32)


def iota(shape, dim):
    return lax.broadcasted_iota(jnp.int32, shape, dim)


def norm_cols(x, gain, width):
    mean = jnp.sum(x, 0, keepdims=True) * (1.0 / width)
    centred = x - mean
    spread = jnp.sum(centred * centred, 0, keepdims=True) * (1.0 / width)
    return centred * lax.rsqrt(spread + 1e-05) * gain


def twice_gelu(x):
    inner = x * (0.7978845608028654 + (0.7978845608028654 * 0.044715) * (x * x))
    return x + x * jnp.tanh(inner)


def block_weights(b, wqkv_ref, wproj_ref, wup_ref, wdown_ref, gain_ref):
    wqkv = wqkv_ref[b]
    width, triple = wqkv.shape
    scale = (width // HEADS) ** (-0.5)
    i, j = iota((triple, LANES), 0), iota((triple, LANES), 1)
    take_v = (j < width) & (i == j + 2 * width)
    take_q = (j >= HALF) & (j < HALF + width) & (i == j - HALF)
    place = jnp.where(take_v, 1.0, jnp.where(take_q, scale, 0.0)).astype(BF)
    wvq = mm(wqkv, place).astype(BF)
    o, i = iota((width, triple), 0), iota((width, triple), 1)
    place = jnp.where(i == o + width, 1.0, 0.0).astype(BF)
    wk = lax.dot_general(place, wqkv, (((1,), (1,)), ((), ())), preferred_element_type=F32).astype(BF)
    gains = gain_ref[b]
    diagonal = iota((width, width), 0) == iota((width, width), 1)
    first, second = [jnp.sum(jnp.where(diagonal, gains[k : k + 1], 0.0), 1, keepdims=True) for k in range(2)]
    i, j = iota((width, LANES), 0), iota((width, LANES), 1)
    spread = jnp.where(i == j, 1.0, 0.0).astype(BF)
    wp = lax.dot_general(wproj_ref[b], spread, (((0,), (0,)), ((), ())), preferred_element_type=F32)
    wp = (wp + jnp.where(j == i + HALF, 1.0, 0.0)).astype(BF)
    return wvq, wk, first, wp, wup_ref[b], wdown_ref[b] * jnp.asarray(0.5, BF), second


def make_keys(columns, bias, wts, width):
    wvq, wk, gain = wts[0], wts[1], wts[2]
    normed = norm_cols(columns, gain, width).astype(BF)
    vq = lax.dot_general(normed, wvq, (((0,), (0,)), ((), ())), preferred_element_type=F32)
    kt = mm(wk, normed).astype(BF)
    keys = columns.shape[1]
    top = iota((HALF - width, keys), 0) == 0
    extra = jnp.where(top, bias, 0.0).astype(BF)
    kaug = jnp.concatenate([jnp.zeros((HALF, keys), BF), kt, extra], 0)
    return vq, kaug


def values_of(vq, width):
    return jnp.where(iota(vq.shape, 1) < width, vq, 1.0).astype(BF)


def queries_of(rows, width):
    head_dim = width // HEADS
    lane = iota(rows.shape, 1)
    one = jnp.where(lane == HALF + width, 1.0, 0.0)
    parts = []
    for h in range(HEADS):
        low = HALF + h * head_dim
        parts.append(jnp.where((lane >= low) & (lane < low + head_dim), rows, one))
    spare = -len(parts) * rows.shape[0] % 32
    if spare:
        parts.append(jnp.zeros((spare, LANES), F32))
    return jnp.concatenate(parts, 0).astype(BF)


def attend(jobs, width, between=None):
    head_dim = width // HEADS
    jobs = list(jobs)
    ahead = mm(jobs[0][0][...], jobs[0][1][...])
    for i, (_, _, values, n, store) in enumerate(jobs):
        scores = ahead
        if i + 1 < len(jobs):
            ahead = mm(jobs[i + 1][0][...], jobs[i + 1][1][...])
        if between is not None:
            between(i)
        top = jnp.max(scores, -1, keepdims=True)
        weights = jnp.exp(scores - top).astype(BF)
        out = mm(weights, values[...])
        lane = iota((n, LANES), 1)
        lane = jnp.where(lane >= HALF, lane - HALF, lane)
        mixed = out[:n]
        for h in range(1, HEADS):
            mixed = jnp.where(lane >= h * head_dim, out[h * n : (h + 1) * n], mixed)
        store(mixed / pltpu.roll(mixed, HALF, 1))


def feed(first, wts, width):
    wup, wdown, gain = wts[4:]
    first = first.astype(BF).astype(F32)
    normed = norm_cols(first, gain, width).astype(BF)
    upper = lax.dot_general(wup, normed, (((0,), (0,)), ((), ())), preferred_element_type=F32)
    return (first + mm(wdown, twice_gelu(upper).astype(BF))).astype(BF).astype(F32)


def against_rows(w, rows):
    return lax.dot_general(w, rows, (((1,), (1,)), ((), ())), preferred_element_type=F32)


def first_kernel(width, ny, *refs):
    hbm, out_ref = refs[:7], refs[7]
    y_refs, x_refs = refs[8 : 8 + ny], refs[8 + ny : 10 + ny]
    copies = refs[10 + ny : 17 + ny]
    sems = refs[17 + ny]
    raw, tok, qs, ks, vs, mix, held, done = refs[18 + ny :]
    moves = [pltpu.make_async_copy(h, v, sems.at[i]) for i, (h, v) in enumerate(zip(hbm, copies))]
    for m in moves:
        m.start()
    for m in moves[1:]:
        m.wait()
    vol_ref, geo_ref, wqkv_ref, wproj_ref, wup_ref, wdown_ref, gain_ref = copies
    nz = vol_ref.shape[2]
    groups = nz // WINDOW
    spots = WINDOW * WINDOW
    kept = spots - 1
    keys = kept * ROWS
    wts = block_weights(0, wqkv_ref, wproj_ref, wup_ref, wdown_ref, gain_ref)
    done[...] = jnp.zeros(done.shape, F32)
    moves[0].wait()
    raw[:, nz:, :] = jnp.zeros((spots, raw.shape[1] - nz, LANES), F32)
    raw[:, 0:nz, 0:width] = vol_ref[...].astype(F32).reshape(spots, nz, width)
    bias = jnp.where(geo_ref[8:9, :] < WINDOW, 0.0, BIG)

    def make(w):
        tok[w] = raw[0:kept, WINDOW * w : WINDOW * w + ROWS, :]
        for j in range(WINDOW):
            tok[w, j, WINDOW : WINDOW + 1, :] = raw[kept, WINDOW * w + j : WINDOW * w + j + 1, :]
        columns = jnp.transpose(tok[w].reshape(keys, LANES))[:width]
        held[:, keys * w : keys * (w + 1)] = columns
        vq, kaug = make_keys(columns, bias, wts, width)
        vs[w] = values_of(vq, width)
        ks[w] = kaug
        qs[w] = queries_of(vq, width)

    def finish(w0, n):
        mixed = mix[w0 : w0 + n].reshape(n * keys, LANES)[:, :width].astype(BF)
        first = held[:, keys * w0 : keys * (w0 + n)] + against_rows(wts[3][:, :width], mixed)
        out = feed(first, wts, width)
        out = jnp.transpose(jnp.concatenate([out, jnp.zeros((LANES - width, n * keys), F32)], 0))[:, :width]
        out = out.reshape(n, kept, ROWS, width)
        for w in range(w0, w0 + n):
            done[0:kept, WINDOW * w : WINDOW * (w + 1), :width] = out[w - w0, :, :WINDOW, :]
            if w == 0:
                done[0:kept, nz : nz + SHIFT, :width] = out[w - w0, :, :SHIFT, :]
            for j in range(WINDOW):
                one = out[w - w0, j, WINDOW : WINDOW + 1, :]
                done[kept, WINDOW * w + j : WINDOW * w + j + 1, :width] = one
                if w == 0 and j < SHIFT:
                    done[kept, nz + j : nz + j + 1, :width] = one

    for w in range(groups):
        make(w)

    def keep(w):
        def store(v):
            mix[w] = v

        return store

    attend([(qs.at[w], ks.at[w], vs.at[w], keys, keep(w)) for w in range(groups)], width)
    finish(0, groups)
    pieces = [done[:, SHIFT + WINDOW * w : SHIFT + WINDOW * w + ROWS, :] for w in range(groups)]
    rolled = [pltpu.roll(p.reshape(spots * ROWS, LANES), HALF, 1).reshape(spots, ROWS, LANES) for p in pieces[1::2]]
    joined = [a + b for a, b in zip(pieces[0::2], rolled)]
    packed = jnp.concatenate(joined, 1).astype(BF)
    out_ref[...] = packed.reshape(WINDOW, WINDOW, ROWS * len(joined), LANES)
    yodd = lax.axis_index("gy") % 2
    for k, y_ref in enumerate(y_refs):
        start = jnp.where((yodd + k) % 2 == 0, SHIFT, 0)
        y_ref[...] = out_ref[:, pl.ds(start, HIGH)]
    xodd = lax.axis_index("gx") % 2
    for k, x_ref in enumerate(x_refs):
        start = jnp.where((xodd + k) % 2 == 0, SHIFT, 0)
        x_ref[...] = out_ref[pl.ds(start, HIGH)]


BOXES = ((SHIFT, HIGH), (0, HIGH + 1))
COLUMNS = tuple((wx, wy) for wx in range(2) for wy in range(2))


def box_rows(wx, wy):
    return BOXES[wx][1] * BOXES[wy][1] * ROWS


def layout(cols, size=lambda n: n):
    sizes = [size(box_rows(*COLUMNS[c])) for c in cols]
    return {c: sum(sizes[:i]) for i, c in enumerate(cols)}, sum(sizes)


def half_columns(wy):
    return [c for c, column in enumerate(COLUMNS) if column[1] == wy]


def up(n, m):
    return -(-n // m) * m


def feed_rows(mix, stop, wts, width):
    out = feed(against_rows(wts[3], mix[:stop].astype(BF)), wts, width)
    nil = jnp.zeros((HALF - width, stop), F32)
    return jnp.transpose(jnp.concatenate([out, nil, out, nil], 0))


def position():
    index = [lax.axis_index(a) for a in ("gx", "gy", "gz")]
    count = [lax.axis_size(a) for a in ("gx", "gy", "gz")]
    return index, count


def place_all(ext, split, pieces, shared):
    for tile, other, x, y in pieces:
        nx, ny = tile.shape[:2]
        n = nx * ny
        tile = tile.astype(F32).reshape(n, tile.shape[2], LANES)
        if other is not None:
            other = other.astype(F32).reshape(n, ROWS, LANES)
        for slab, v in enumerate(split(tile, other)):
            ext[slab, pl.ds(x, nx), pl.ds(y, ny)] = v.reshape(nx, ny, ROWS, LANES)
    for wx, wy in shared:
        x0, y0 = WINDOW * wx, WINDOW * wy
        gone = (WINDOW * WINDOW - 1) * wx
        for slab in range(ext.shape[0]):
            for j in range(WINDOW):
                to = j + 1 - wx
                ext[slab, x0 + to // WINDOW, y0 + to % WINDOW, WINDOW : WINDOW + 1, :] = ext[
                    slab, x0 + gone // WINDOW, y0 + gone % WINDOW, j : j + 1, :
                ]


def squeezed(rows):
    return up(rows // ROWS, 2) // 2 * ROWS


def squeeze(rows):
    n = rows.shape[0] // ROWS
    if n % 2:
        rows = jnp.concatenate([rows, jnp.zeros((ROWS, LANES), F32)], 0)
    m = (n + 1) // 2
    pairs = rows.reshape(m, 2, ROWS, LANES)
    even, odd = [pairs[:, k].reshape(m * ROWS, LANES) for k in (0, 1)]
    low = iota((m * ROWS, LANES), 0) % ROWS < HIGH
    return jnp.where(low, pltpu.roll(even, m * ROWS - SHIFT, 0), pltpu.roll(odd, 1, 0))


def window_attention(width, groups, cols, work, start_of, geo_ref, wts, ext, mix, ks, vs, qs, short=()):
    index, count = position()
    spots = WINDOW * WINDOW
    keys = (spots - 1) * ROWS
    nolow = [jnp.where(i > 0, 0.0, 1.0) for i in index]
    nohigh = [jnp.where(i < c - 1, 0.0, 1.0) for i, c in zip(index, count)]

    def turn(slab, c):
        wx, wy = COLUMNS[c]
        first = ROWS * (1 - wx)
        tokens = ext[slab, WINDOW * wx : WINDOW * (wx + 1), WINDOW * wy : WINDOW * (wy + 1)]
        flat = tokens.reshape(spots * ROWS, LANES)
        return tokens, jnp.transpose(flat[first : first + keys])

    def make(slab, c, tokens, turned):
        wx, wy = COLUMNS[c]
        row, px, py = [geo_ref[8 * wx + k : 8 * wx + k + 1, :] for k in range(3)]
        badx = jnp.where(px < HIGH, nolow[0], 0.0) if wx == 0 else jnp.where(px >= HIGH, nohigh[0], 0.0)
        bady = jnp.where(py < HIGH, nolow[1], 0.0) if wy == 0 else jnp.where(py >= HIGH, nohigh[1], 0.0)
        bad = badx + bady + jnp.where(row < WINDOW, 0.0, 1.0)
        (bx, nx), (by, ny) = BOXES[wx], BOXES[wy]
        nq = nx * ny * ROWS
        first = ROWS * (1 - wx)
        chosen = tokens[bx : bx + nx, by : by + ny].reshape(nq, LANES)
        for slot, (at, half, g) in enumerate(work):
            if at != slab:
                continue
            badz = jnp.zeros_like(bad)
            if g == 0:
                badz = jnp.where(row < HIGH, nolow[2], 0.0)
            if g == groups - 1:
                badz = jnp.where(row >= HIGH, nohigh[2], 0.0)
            bias = jnp.where(bad + badz > 0.0, BIG, 0.0)
            vq, kaug = make_keys(turned[HALF * half : HALF * half + width], bias, wts, width)
            vs[c, slot] = values_of(vq, width)
            ks[c, slot] = kaug
            picked = [
                vq[ROWS * (WINDOW * x + by) - first : ROWS * (WINDOW * x + by + ny) - first] for x in range(bx, bx + nx)
            ]
            picked, residual = jnp.concatenate(picked, 0), chosen
            if g in short:
                picked, residual = squeeze(picked), squeeze(residual)
            queries = queries_of(picked, width)
            qs[c][slot, 0 : queries.shape[0]] = queries
            start = start_of(g, c)
            residual = residual if half else pltpu.roll(residual, HALF, 1)
            mix[start : start + residual.shape[0], HALF:] = residual[:, HALF:]

    order = [(slab, c) for slab in sorted({w[0] for w in work}) for c in cols]
    ahead = turn(*order[0])
    for i, at in enumerate(order):
        now = ahead
        if i + 1 < len(order):
            ahead = turn(*order[i + 1])
        make(*at, *now)

    def job(slot, c):
        n = box_rows(*COLUMNS[c])
        if work[slot][2] in short:
            n = squeezed(n)
        start = start_of(work[slot][2], c)

        def store(v):
            mix[start : start + n, :HALF] = v[:, :HALF]

        return qs[c].at[slot, 0 : up(HEADS * n, 32)], ks.at[c, slot], vs.at[c, slot], n, store

    attend([job(slot, c) for slot in range(len(work)) for c in cols], width)


def prepare_kernel(wqkv_ref, wproj_ref, wup_ref, wdown_ref, gain_ref, wconv_ref, cgain_ref, *outs):
    for out, value in zip(outs, block_weights(1, wqkv_ref, wproj_ref, wup_ref, wdown_ref, gain_ref)):
        out[...] = value
    cg_ref, wc = outs[7], outs[8]
    width = wproj_ref.shape[1]
    diagonal = iota((width, width), 0) == iota((width, width), 1)
    cg_ref[...] = jnp.sum(jnp.where(diagonal, cgain_ref[...], 0.0), 1, keepdims=True)
    wc[...] = jnp.zeros(wc.shape, BF)
    for dx in range(3):
        total = None
        for dy in range(3):
            taps = wconv_ref[9 * dx + 3 * dy : 9 * dx + 3 * dy + 3].reshape(3 * width, width)
            i, j = iota((width, 4 * HALF), 0), iota((width, 4 * HALF), 1)
            place = jnp.where(j == i + HALF * dy, 1.0, 0.0).astype(BF)
            part = mm(taps, place)
            total = part if total is None else total + part
        for dz in range(3):
            at = 4 * HALF * dx + HALF * dz
            wc[at : at + width] = total[width * dz : width * (dz + 1)].astype(BF)


def inner_kernel(width, ypieces, part, geo_ref, *refs):
    pieces = refs[:3] if part < 0 else refs[: 3 * (ypieces + 1)]
    rest = refs[len(pieces) :]
    wts = [r[...] for r in rest[:7]]
    out_ref, mix, ext, ks, vs = rest[7:12]
    qs = rest[12:]
    pairs = pieces[0].shape[2] // ROWS
    work = [(p, half, 1 + 2 * p + half) for p in range(pairs) for half in range(2)][:-1]
    index, _ = position()
    far = WINDOW + HIGH
    xa, xb = [jnp.where(index[0] % 2 == k, far, 0) for k in (0, 1)]
    ys = [jnp.where(index[1] % 2 == k, far, 0) for k in range(2)]
    tiles = []
    for k, y in enumerate([HIGH] + ys[: len(pieces) // 3 - 1]):
        for i, x in enumerate((HIGH, xa, xb)):
            tiles.append((pieces[3 * k + i][...], None, x, y))
    if part < 0:
        ext[:, :, pl.ds(ys[1], HIGH)] = jnp.zeros((pairs, EXT, HIGH, ROWS, LANES), F32)

    def split(tile, other):
        return [tile[:, p * ROWS : (p + 1) * ROWS, :] for p in range(pairs)]

    def run(cols):
        places, rows = layout(cols)
        used = rows * len(work)
        rows_ref = mix if part < 0 else out_ref
        rest = rows_ref.shape[0] - used
        if rest:
            rows_ref[used:] = jnp.zeros((rest, LANES), F32)
        place_all(ext, split, tiles, [COLUMNS[c] for c in cols])
        start = lambda g, c: rows * (g - 1) + places[c]
        window_attention(width, 2 * pairs + 1, cols, work, start, geo_ref, wts, ext, rows_ref, ks, vs, qs)
        if part < 0:
            stop = up(used, LANES)
            out_ref[:stop] = feed_rows(mix, stop, wts, width)
            if stop < out_ref.shape[0]:
                out_ref[stop:] = jnp.zeros((out_ref.shape[0] - stop, LANES), F32)

    if part == 0:
        run(list(range(len(COLUMNS))))
    else:
        for side in range(2):

            @pl.when(index[1] % 2 == side)
            def _(side=side):
                run(half_columns(side if part < 0 else 1 - side))


def last_kernel(width, ypieces, geo_ref, inner_ref, *refs):
    early = ypieces == 1
    if early:
        free_ref, *refs = refs
    pieces = refs[: 4 * (ypieces + 1)]
    rest = refs[4 * (ypieces + 1) :]
    wts = [r[...] for r in rest[:7]]
    cg_ref, wc, out_ref, ext, mix, fed, grid, tot, ks, vs = rest[7:17]
    qs = rest[17:]
    nz = out_ref.shape[2]
    pairs = pieces[0].shape[2] // ROWS
    groups = 2 * pairs + 1
    index, count = position()
    far = WINDOW + HIGH
    xa, xb = [jnp.where(index[0] % 2 == k, far, 0) for k in (0, 1)]
    ys = [jnp.where(index[1] % 2 == k, far, 0) for k in range(2)]
    tiles = []
    for k, y in enumerate([HIGH] + ys[:ypieces]):
        at = 0
        for i, x in enumerate((HIGH, xa, xb)):
            mine = pieces[4 * k + i][:, :, -ROWS:, :]
            tiles.append((mine, pieces[4 * k + 3][at : at + mine.shape[0]], x, y))
            at += mine.shape[0]
    if ypieces == 1:
        ext[:, :, pl.ds(ys[1], HIGH)] = jnp.zeros((2, EXT, HIGH, ROWS, LANES), F32)

    def split(mine, other):
        low = iota(mine.shape, 1) < HIGH
        return jnp.where(low, mine, other), jnp.where(low, other, mine)

    cols = list(range(len(COLUMNS)))
    offsets, per = layout(cols)
    depth = grid.shape[2]
    grid[:, :, WINDOW * groups :] = jnp.zeros((WINDOW + 2, WINDOW + 2, depth - WINDOW * groups, LANES), F32)

    def scatter(g, rows, base, cols):
        places, _ = layout(cols)
        for c in cols:
            wx, wy = COLUMNS[c]
            (_, nx), (_, ny) = BOXES[wx], BOXES[wy]
            for x in range(nx):
                for y in range(ny):
                    at = base + places[c] + ROWS * (x * ny + y)
                    grid[HIGH * wx + x, HIGH * wy + y, WINDOW * g : WINDOW * (g + 1), :] = rows[at : at + WINDOW]

    places, lowest = layout(cols, squeezed)
    used = lowest + per
    stop = up(used, LANES)
    mix[used:stop] = jnp.zeros((stop - used, LANES), F32)
    fed[...] = feed_rows(inner_ref, inner_ref.shape[0], wts, width)
    place_all(ext, split, tiles, COLUMNS)
    work = [(0, 1, groups - 1), (1, 1, 0)]
    start = lambda g, c: lowest + offsets[c] if g else places[c]
    window_attention(width, groups, cols, work, start, geo_ref, wts, ext, mix, ks, vs, qs, (0,))
    out = feed_rows(mix, stop, wts, width)
    for c, (wx, wy) in enumerate(COLUMNS):
        (_, nx), (_, ny) = BOXES[wx], BOXES[wy]
        for i in range(nx * ny):
            at = places[c] + HIGH * i
            grid[HIGH * wx + i // ny, HIGH * wy + i % ny, SHIFT:WINDOW, :] = out[at : at + HIGH]
    scatter(groups - 1, out, lowest, cols)
    if early:
        for side in range(2):

            @pl.when(index[1] % 2 == side)
            def _(side=side):
                for wy, rows in ((side, free_ref), (1 - side, fed)):
                    half = half_columns(wy)
                    for g in range(1, groups - 1):
                        scatter(g, rows, layout(half)[1] * (g - 1), half)

    else:
        for g in range(1, groups - 1):
            scatter(g, fed, per * (g - 1), cols)

    last = WINDOW + 1

    def clear(when, *at):
        @pl.when(when)
        def _():
            grid[at] = jnp.zeros_like(grid[at])

    clear(index[0] == 0, slice(0, 1))
    clear(index[0] == count[0] - 1, slice(last, last + 1))
    clear(index[1] == 0, slice(None), slice(0, 1))
    clear(index[1] == count[1] - 1, slice(None), slice(last, last + 1))
    clear(index[2] == 0, slice(None), slice(None), slice(SHIFT, HIGH))
    clear(index[2] == count[2] - 1, slice(None), slice(None), slice(HIGH + nz, HIGH + nz + 1))

    side = WINDOW + 2
    padded = -(-nz // 16) * 16

    def lhs(x):
        taps = [grid[x, :, SHIFT + d : SHIFT + d + padded, :].reshape(side * padded, LANES) for d in range(3)]
        lower = iota(taps[0].shape, 1) < HALF
        return jnp.concatenate([jnp.where(lower, taps[0], taps[1]), taps[2]], 1).astype(BF)

    rows = [lhs(x) for x in range(side)]
    acc = mm(jnp.concatenate([jnp.concatenate(rows[x : x + 3], 1) for x in range(WINDOW)], 0), wc[...])
    strip = WINDOW * padded
    for x in range(WINDOW):
        part = acc[x * side * padded : (x + 1) * side * padded]
        near, second = part[:, :LANES], part[:, LANES:]
        turned = pltpu.roll(near[padded : (WINDOW + 1) * padded], HALF, 1)
        tot[x * strip : (x + 1) * strip] = near[:strip] + turned + second[2 * padded :]
    tot[WINDOW * strip :] = jnp.zeros((tot.shape[0] - WINDOW * strip, LANES), F32)
    normed = norm_cols(jnp.transpose(tot[...])[:width], cg_ref[...], width)
    active = jnp.where(normed >= 0.0, normed, 0.01 * normed)
    active = jnp.transpose(jnp.concatenate([active, jnp.zeros((LANES - width, tot.shape[0]), F32)], 0))
    for x in range(WINDOW):
        centre = grid[x + 1, 1 : 1 + WINDOW, HIGH : HIGH + padded, :].reshape(strip, LANES)
        result = (centre + active[x * strip : (x + 1) * strip]).reshape(WINDOW, padded, LANES).astype(BF)
        out_ref[x] = result[:, :nz, :width]


def geometry():
    kept = WINDOW * WINDOW - 1
    geo = np.full((16, kept * ROWS), WINDOW, np.float32)
    for v in range(2):
        gone = kept * v
        for i in range(kept):
            spot = i + 1 - v
            for r in range(ROWS):
                t = i * ROWS + r
                if r < WINDOW:
                    geo[8 * v : 8 * v + 3, t] = r, spot // WINDOW, spot % WINDOW
                elif i < WINDOW:
                    geo[8 * v : 8 * v + 3, t] = i, gone // WINDOW, gone % WINDOW
                else:
                    geo[8 * v + 1 : 8 * v + 3, t] = spot // WINDOW, spot % WINDOW
    return jnp.asarray(geo)


def exchange(v, axis, odd):
    count, cores = lax.axis_size(axis), lax.axis_size("gz")
    pairs = []
    for i in range(count):
        low = i - (i - odd) % 2
        for c in range(cores):
            if low < 0 or low + 1 >= count:
                to = (i, c ^ 1 if c ^ 1 < cores else c)
            else:
                to = (low + 1 if i == low else low, c)
            pairs.append((i * cores + c, to[0] * cores + to[1]))
    return lax.ppermute(v, (axis, "gz"), pairs)


def body(volume, w_qkv, w_proj, w_up, w_down, norm_gain, conv_weight, conv_gain):
    sx, sy, sz, width = volume.shape
    spots = sx * sy
    groups = sz // WINDOW
    geo = geometry()
    keys = (spots - 1) * ROWS
    weights = (w_qkv, w_proj, w_up, jnp.swapaxes(w_down, 1, 2), norm_gain)
    halves = [0] if lax.axis_size("gy") == 2 else [0, 1]
    tall = ROWS * groups // 2

    operands = (volume, geo, *weights)
    packed, *cuts = pl.pallas_call(
        functools.partial(first_kernel, width, len(halves)),
        out_shape=[jax.ShapeDtypeStruct((sx, sy, tall, LANES), BF)]
        + [jax.ShapeDtypeStruct((sx, HIGH, tall, LANES), BF) for _ in halves]
        + [jax.ShapeDtypeStruct((HIGH, sy, tall, LANES), BF) for _ in range(2)],
        in_specs=[pl.BlockSpec(memory_space=pltpu.HBM)] * len(operands),
        scratch_shapes=[pltpu.VMEM(v.shape, v.dtype) for v in operands]
        + [
            pltpu.SemaphoreType.DMA((len(operands),)),
            pltpu.VMEM((spots, sz + 12, LANES), F32),
            pltpu.VMEM((groups, spots - 1, ROWS, LANES), F32),
            pltpu.VMEM((groups, HEADS * keys, LANES), BF),
            pltpu.VMEM((groups, LANES, keys), BF),
            pltpu.VMEM((groups, keys, LANES), BF),
            pltpu.VMEM((groups, keys, LANES), F32),
            pltpu.VMEM((width, groups * keys), F32),
            pltpu.VMEM((spots, sz + 12, LANES), F32),
        ],
        compiler_params=pltpu.CompilerParams(vmem_limit_bytes=24 << 20),
        name="first_block",
    )(*[pltpu.with_memory_space_constraint(v, pltpu.HBM) for v in operands])

    xodd = lax.axis_index("gx") % 2

    def cut(v, odd):
        return lax.dynamic_slice_in_dim(v, jnp.where(odd == 0, SHIFT, 0), HIGH, 0)

    def other_core(v):
        return lax.ppermute(v, "gz", [(0, 1), (1, 0)])

    ys = [exchange(v, "gy", k) for k, v in zip(halves, cuts)]
    xs = [exchange(v, "gx", k) for k, v in enumerate(cuts[len(halves) :])]
    corners = [[exchange(cut(v, (xodd + k) % 2), "gx", k) for k in (0, 1)] for v in ys]

    side = WINDOW + 2
    rows = sum(box_rows(*c) for c in COLUMNS)
    strip = WINDOW * -(-sz // 16) * 16

    def buffers(slots):
        return [
            pltpu.VMEM((len(COLUMNS), slots, LANES, keys), BF),
            pltpu.VMEM((len(COLUMNS), slots, keys, LANES), BF),
        ] + [pltpu.VMEM((slots, -(-HEADS * box_rows(*c) // 32) * 32, LANES), BF) for c in COLUMNS]

    span = up(max(layout(half_columns(k))[1] for k in range(2)) * (groups - 1), LANES)

    def inner(part, operands):
        return pl.pallas_call(
            functools.partial(inner_kernel, width, len(ys), part),
            out_shape=jax.ShapeDtypeStruct((span if part else up(rows * (groups - 1), LANES), LANES), F32),
            scratch_shapes=[
                pltpu.VMEM((span, LANES), F32),
                pltpu.VMEM((groups // 2, EXT, EXT, ROWS, LANES), F32),
            ]
            + buffers(groups - 1),
            compiler_params=pltpu.CompilerParams(vmem_limit_bytes=20 << 20),
            cost_estimate=pl.CostEstimate(flops=2 * 10**9, transcendentals=0, bytes_accessed=10**6),
        )(*operands)

    hidden = w_up.shape[2]
    column = jax.ShapeDtypeStruct((width, 1), F32)
    ready = pl.pallas_call(
        prepare_kernel,
        out_shape=[
            jax.ShapeDtypeStruct((width, LANES), BF),
            jax.ShapeDtypeStruct((width, width), BF),
            column,
            jax.ShapeDtypeStruct((width, LANES), BF),
            jax.ShapeDtypeStruct((width, hidden), BF),
            jax.ShapeDtypeStruct((width, hidden), BF),
            column,
            column,
            jax.ShapeDtypeStruct((3 * 4 * HALF, 4 * HALF), BF),
        ],
        compiler_params=pltpu.CompilerParams(vmem_limit_bytes=8 << 20),
        name="prepare",
    )(*weights, conv_weight, conv_gain[None, :])
    block = ready[:7]

    def edge(parts):
        def kernel(*refs):
            at = 0
            for r in refs[:-1]:
                refs[-1][at : at + r.shape[0]] = r[:, :, -ROWS:, :]
                at += r.shape[0]

        shape = (sum(p.shape[0] for p in parts),) + (parts[0].shape[1], ROWS, LANES)
        return pl.pallas_call(
            kernel,
            out_shape=jax.ShapeDtypeStruct(shape, BF),
            compiler_params=pltpu.CompilerParams(vmem_limit_bytes=4 << 20),
        )(*parts)

    near = [packed, *xs]
    wide = [v for y, c in zip(ys, corners) for v in (y, *c)]
    if len(ys) == 1:
        early = inner(-1, [geo, *near, *block])
        rows_first = lax.optimization_barrier((early, *near))
        zs = other_core(edge(rows_first[1:]))
        zcorners = [other_core(edge([y, *c])) for y, c in zip(ys, corners)]
        done = inner(1, [geo, *near, *wide, *block])
        done = [done, early]
    else:
        zs = other_core(edge(near))
        zcorners = [other_core(edge([y, *c])) for y, c in zip(ys, corners)]
        done = [inner(0, [geo, *near, *wide, *block])]

    flat = [v for y, c, z in zip(ys, corners, zcorners) for v in (y, *c, z)]
    operands = [geo, *done, *near, zs, *flat, *ready]
    return pl.pallas_call(
        functools.partial(last_kernel, width, len(ys)),
        out_shape=jax.ShapeDtypeStruct(volume.shape, volume.dtype),
        scratch_shapes=[
            pltpu.VMEM((2, EXT, EXT, ROWS, LANES), F32),
            pltpu.VMEM((up(layout(range(len(COLUMNS)), squeezed)[1] + rows, LANES), LANES), F32),
            pltpu.VMEM(done[0].shape, F32),
            pltpu.VMEM((side, side, sz + 12, LANES), F32),
            pltpu.VMEM((-(-WINDOW * strip // LANES) * LANES, LANES), F32),
        ]
        + buffers(2),
        compiler_params=pltpu.CompilerParams(vmem_limit_bytes=26 << 20),
        name="last_windows",
    )(*operands)


def solution(mesh):
    placed = (P(("parts", "gx"), "gy", "gz", None), P(), P(), P(), P(), P(), P(), P())

    return jax.shard_map(
        body,
        mesh=mesh,
        in_specs=placed,
        out_specs=P(("parts", "gx"), "gy", "gz", None),
        check_vma=False,
    )
```

```python
import functools

import jax
import jax.numpy as jnp
import numpy as np
from jax import lax
from jax.experimental import pallas as pl
from jax.experimental.pallas import tpu as pltpu
from jax.sharding import PartitionSpec as P


HEADS = 3
WINDOW = 7
SHIFT = 3
LANES = 128
HALF = 64
ROWS = 8
BIG = -1e30
HIGH = WINDOW - SHIFT
EXT = 2 * WINDOW + 1
BF = jnp.bfloat16
F32 = jnp.float32


def mm(a, b):
    return jnp.dot(a, b, preferred_element_type=F32)


def iota(shape, dim):
    return lax.broadcasted_iota(jnp.int32, shape, dim)


def norm_cols(x, gain, width):
    mean = jnp.sum(x, 0, keepdims=True) * (1.0 / width)
    centred = x - mean
    spread = jnp.sum(centred * centred, 0, keepdims=True) * (1.0 / width)
    return centred * lax.rsqrt(spread + 1e-05) * gain


def twice_gelu(x):
    inner = x * (0.7978845608028654 + (0.7978845608028654 * 0.044715) * (x * x))
    return x + x * jnp.tanh(inner)


def block_weights(b, wqkv_ref, wproj_ref, wup_ref, wdown_ref, gain_ref):
    wqkv = wqkv_ref[b]
    width, triple = wqkv.shape
    scale = (width // HEADS) ** (-0.5)
    i, j = iota((triple, LANES), 0), iota((triple, LANES), 1)
    take_v = (j < width) & (i == j + 2 * width)
    take_q = (j >= HALF) & (j < HALF + width) & (i == j - HALF)
    place = jnp.where(take_v, 1.0, jnp.where(take_q, scale, 0.0)).astype(BF)
    wvq = mm(wqkv, place).astype(BF)
    o, i = iota((width, triple), 0), iota((width, triple), 1)
    place = jnp.where(i == o + width, 1.0, 0.0).astype(BF)
    wk = lax.dot_general(place, wqkv, (((1,), (1,)), ((), ())), preferred_element_type=F32).astype(BF)
    gains = gain_ref[b]
    diagonal = iota((width, width), 0) == iota((width, width), 1)
    first, second = [jnp.sum(jnp.where(diagonal, gains[k : k + 1], 0.0), 1, keepdims=True) for k in range(2)]
    i, j = iota((width, LANES), 0), iota((width, LANES), 1)
    spread = jnp.where(i == j, 1.0, 0.0).astype(BF)
    wp = lax.dot_general(wproj_ref[b], spread, (((0,), (0,)), ((), ())), preferred_element_type=F32)
    wp = (wp + jnp.where(j == i + HALF, 1.0, 0.0)).astype(BF)
    return wvq, wk, first, wp, wup_ref[b], wdown_ref[b] * jnp.asarray(0.5, BF), second


def make_keys(columns, bias, wts, width):
    wvq, wk, gain = wts[0], wts[1], wts[2]
    normed = norm_cols(columns, gain, width).astype(BF)
    vq = lax.dot_general(normed, wvq, (((0,), (0,)), ((), ())), preferred_element_type=F32)
    kt = mm(wk, normed).astype(BF)
    keys = columns.shape[1]
    top = iota((HALF - width, keys), 0) == 0
    extra = jnp.where(top, bias, 0.0).astype(BF)
    kaug = jnp.concatenate([jnp.zeros((HALF, keys), BF), kt, extra], 0)
    return vq, kaug


def values_of(vq, width):
    return jnp.where(iota(vq.shape, 1) < width, vq, 1.0).astype(BF)


def queries_of(rows, width):
    head_dim = width // HEADS
    lane = iota(rows.shape, 1)
    one = jnp.where(lane == HALF + width, 1.0, 0.0)
    parts = []
    for h in range(HEADS):
        low = HALF + h * head_dim
        parts.append(jnp.where((lane >= low) & (lane < low + head_dim), rows, one))
    spare = -len(parts) * rows.shape[0] % 32
    if spare:
        parts.append(jnp.zeros((spare, LANES), F32))
    return jnp.concatenate(parts, 0).astype(BF)


def attend(jobs, width):
    head_dim = width // HEADS
    jobs = list(jobs)
    ahead = mm(jobs[0][0][...], jobs[0][1][...])
    for i, (_, _, values, n, store) in enumerate(jobs):
        scores = ahead
        if i + 1 < len(jobs):
            ahead = mm(jobs[i + 1][0][...], jobs[i + 1][1][...])
        top = jnp.max(scores, -1, keepdims=True)
        weights = jnp.exp(scores - top).astype(BF)
        out = mm(weights, values[...])
        lane = iota((n, LANES), 1)
        lane = jnp.where(lane >= HALF, lane - HALF, lane)
        mixed = out[:n]
        for h in range(1, HEADS):
            mixed = jnp.where(lane >= h * head_dim, out[h * n : (h + 1) * n], mixed)
        store(mixed / pltpu.roll(mixed, HALF, 1))


def feed(first, wts, width):
    wup, wdown, gain = wts[4:]
    first = first.astype(BF).astype(F32)
    normed = norm_cols(first, gain, width).astype(BF)
    upper = lax.dot_general(wup, normed, (((0,), (0,)), ((), ())), preferred_element_type=F32)
    return (first + mm(wdown, twice_gelu(upper).astype(BF))).astype(BF).astype(F32)


def against_rows(w, rows):
    return lax.dot_general(w, rows, (((1,), (1,)), ((), ())), preferred_element_type=F32)


def first_kernel(width, ny, *refs):
    hbm, out_ref = refs[:7], refs[7]
    y_refs, x_refs = refs[8 : 8 + ny], refs[8 + ny : 10 + ny]
    copies = refs[10 + ny : 17 + ny]
    sems = refs[17 + ny]
    raw, tok, qs, ks, vs, mix, held, done = refs[18 + ny :]
    moves = [pltpu.make_async_copy(h, v, sems.at[i]) for i, (h, v) in enumerate(zip(hbm, copies))]
    for m in moves:
        m.start()
    for m in moves[1:]:
        m.wait()
    vol_ref, geo_ref, wqkv_ref, wproj_ref, wup_ref, wdown_ref, gain_ref = copies
    nz = vol_ref.shape[2]
    groups = nz // WINDOW
    spots = WINDOW * WINDOW
    kept = spots - 1
    keys = kept * ROWS
    wts = block_weights(0, wqkv_ref, wproj_ref, wup_ref, wdown_ref, gain_ref)
    done[...] = jnp.zeros(done.shape, F32)
    moves[0].wait()
    raw[:, nz:, :] = jnp.zeros((spots, raw.shape[1] - nz, LANES), F32)
    raw[:, 0:nz, 0:width] = vol_ref[...].astype(F32).reshape(spots, nz, width)
    bias = jnp.where(geo_ref[8:9, :] < WINDOW, 0.0, BIG)

    def make(w):
        tok[w] = raw[0:kept, WINDOW * w : WINDOW * w + ROWS, :]
        for j in range(WINDOW):
            tok[w, j, WINDOW : WINDOW + 1, :] = raw[kept, WINDOW * w + j : WINDOW * w + j + 1, :]
        columns = jnp.transpose(tok[w].reshape(keys, LANES))[:width]
        held[:, keys * w : keys * (w + 1)] = columns
        vq, kaug = make_keys(columns, bias, wts, width)
        vs[w] = values_of(vq, width)
        ks[w] = kaug
        qs[w] = queries_of(vq, width)

    def finish(w0, n):
        mixed = mix[w0 : w0 + n].reshape(n * keys, LANES)[:, :width].astype(BF)
        first = held[:, keys * w0 : keys * (w0 + n)] + against_rows(wts[3][:, :width], mixed)
        out = feed(first, wts, width)
        out = jnp.transpose(jnp.concatenate([out, jnp.zeros((LANES - width, n * keys), F32)], 0))[:, :width]
        out = out.reshape(n, kept, ROWS, width)
        for w in range(w0, w0 + n):
            done[0:kept, WINDOW * w : WINDOW * (w + 1), :width] = out[w - w0, :, :WINDOW, :]
            if w == 0:
                done[0:kept, nz : nz + SHIFT, :width] = out[w - w0, :, :SHIFT, :]
            for j in range(WINDOW):
                one = out[w - w0, j, WINDOW : WINDOW + 1, :]
                done[kept, WINDOW * w + j : WINDOW * w + j + 1, :width] = one
                if w == 0 and j < SHIFT:
                    done[kept, nz + j : nz + j + 1, :width] = one

    for w in range(groups):
        make(w)

    def keep(w):
        def store(v):
            mix[w] = v

        return store

    attend([(qs.at[w], ks.at[w], vs.at[w], keys, keep(w)) for w in range(groups)], width)
    finish(0, groups)
    pieces = [done[:, SHIFT + WINDOW * w : SHIFT + WINDOW * w + ROWS, :] for w in range(groups)]
    rolled = [pltpu.roll(p.reshape(spots * ROWS, LANES), HALF, 1).reshape(spots, ROWS, LANES) for p in pieces[1::2]]
    joined = [a + b for a, b in zip(pieces[0::2], rolled)]
    packed = jnp.concatenate(joined, 1).astype(BF)
    out_ref[...] = packed.reshape(WINDOW, WINDOW, ROWS * len(joined), LANES)
    yodd = lax.axis_index("gy") % 2
    for k, y_ref in enumerate(y_refs):
        start = jnp.where((yodd + k) % 2 == 0, SHIFT, 0)
        y_ref[...] = out_ref[:, pl.ds(start, HIGH)]
    xodd = lax.axis_index("gx") % 2
    for k, x_ref in enumerate(x_refs):
        start = jnp.where((xodd + k) % 2 == 0, SHIFT, 0)
        x_ref[...] = out_ref[pl.ds(start, HIGH)]


BOXES = ((SHIFT, HIGH), (0, HIGH + 1))
COLUMNS = tuple((wx, wy) for wx in range(2) for wy in range(2))


def box_rows(wx, wy):
    return BOXES[wx][1] * BOXES[wy][1] * ROWS


def layout(cols, size=lambda n: n):
    sizes = [size(box_rows(*COLUMNS[c])) for c in cols]
    return {c: sum(sizes[:i]) for i, c in enumerate(cols)}, sum(sizes)


def half_columns(wy):
    return [c for c, column in enumerate(COLUMNS) if column[1] == wy]


def up(n, m):
    return -(-n // m) * m


def feed_rows(mix, stop, wts, width):
    out = feed(against_rows(wts[3], mix[:stop].astype(BF)), wts, width)
    nil = jnp.zeros((HALF - width, stop), F32)
    return jnp.transpose(jnp.concatenate([out, nil, out, nil], 0))


def position():
    index = [lax.axis_index(a) for a in ("gx", "gy", "gz")]
    count = [lax.axis_size(a) for a in ("gx", "gy", "gz")]
    return index, count


def place_all(ext, split, pieces, shared):
    for tile, other, x, y in pieces:
        nx, ny = tile.shape[:2]
        n = nx * ny
        tile = tile.astype(F32).reshape(n, tile.shape[2], LANES)
        if other is not None:
            other = other.astype(F32).reshape(n, ROWS, LANES)
        for slab, v in enumerate(split(tile, other)):
            ext[slab, pl.ds(x, nx), pl.ds(y, ny)] = v.reshape(nx, ny, ROWS, LANES)
    for wx, wy in shared:
        x0, y0 = WINDOW * wx, WINDOW * wy
        gone = (WINDOW * WINDOW - 1) * wx
        for slab in range(ext.shape[0]):
            for j in range(WINDOW):
                to = j + 1 - wx
                ext[slab, x0 + to // WINDOW, y0 + to % WINDOW, WINDOW : WINDOW + 1, :] = ext[
                    slab, x0 + gone // WINDOW, y0 + gone % WINDOW, j : j + 1, :
                ]


def squeezed(rows):
    return up(rows // ROWS, 2) // 2 * ROWS


def squeeze(rows):
    n = rows.shape[0] // ROWS
    if n % 2:
        rows = jnp.concatenate([rows, jnp.zeros((ROWS, LANES), F32)], 0)
    m = (n + 1) // 2
    pairs = rows.reshape(m, 2, ROWS, LANES)
    even, odd = [pairs[:, k].reshape(m * ROWS, LANES) for k in (0, 1)]
    low = iota((m * ROWS, LANES), 0) % ROWS < HIGH
    return jnp.where(low, pltpu.roll(even, m * ROWS - SHIFT, 0), pltpu.roll(odd, 1, 0))


def window_attention(width, groups, cols, work, start_of, geo_ref, wts, ext, mix, ks, vs, qs, short=()):
    index, count = position()
    spots = WINDOW * WINDOW
    keys = (spots - 1) * ROWS
    nolow = [jnp.where(i > 0, 0.0, 1.0) for i in index]
    nohigh = [jnp.where(i < c - 1, 0.0, 1.0) for i, c in zip(index, count)]

    def turn(slab, c):
        wx, wy = COLUMNS[c]
        first = ROWS * (1 - wx)
        tokens = ext[slab, WINDOW * wx : WINDOW * (wx + 1), WINDOW * wy : WINDOW * (wy + 1)]
        flat = tokens.reshape(spots * ROWS, LANES)
        return tokens, jnp.transpose(flat[first : first + keys])

    def make(slab, c, tokens, turned):
        wx, wy = COLUMNS[c]
        row, px, py = [geo_ref[8 * wx + k : 8 * wx + k + 1, :] for k in range(3)]
        badx = jnp.where(px < HIGH, nolow[0], 0.0) if wx == 0 else jnp.where(px >= HIGH, nohigh[0], 0.0)
        bady = jnp.where(py < HIGH, nolow[1], 0.0) if wy == 0 else jnp.where(py >= HIGH, nohigh[1], 0.0)
        bad = badx + bady + jnp.where(row < WINDOW, 0.0, 1.0)
        (bx, nx), (by, ny) = BOXES[wx], BOXES[wy]
        nq = nx * ny * ROWS
        first = ROWS * (1 - wx)
        chosen = tokens[bx : bx + nx, by : by + ny].reshape(nq, LANES)
        for slot, (at, half, g) in enumerate(work):
            if at != slab:
                continue
            badz = jnp.zeros_like(bad)
            if g == 0:
                badz = jnp.where(row < HIGH, nolow[2], 0.0)
            if g == groups - 1:
                badz = jnp.where(row >= HIGH, nohigh[2], 0.0)
            bias = jnp.where(bad + badz > 0.0, BIG, 0.0)
            vq, kaug = make_keys(turned[HALF * half : HALF * half + width], bias, wts, width)
            vs[c, slot] = values_of(vq, width)
            ks[c, slot] = kaug
            picked = [
                vq[ROWS * (WINDOW * x + by) - first : ROWS * (WINDOW * x + by + ny) - first] for x in range(bx, bx + nx)
            ]
            picked, residual = jnp.concatenate(picked, 0), chosen
            if g in short:
                picked, residual = squeeze(picked), squeeze(residual)
            queries = queries_of(picked, width)
            qs[c][slot, 0 : queries.shape[0]] = queries
            start = start_of(g, c)
            residual = residual if half else pltpu.roll(residual, HALF, 1)
            mix[start : start + residual.shape[0], HALF:] = residual[:, HALF:]

    order = [(slab, c) for slab in sorted({w[0] for w in work}) for c in cols]
    ahead = turn(*order[0])
    for i, at in enumerate(order):
        now = ahead
        if i + 1 < len(order):
            ahead = turn(*order[i + 1])
        make(*at, *now)

    def job(slot, c):
        n = box_rows(*COLUMNS[c])
        if work[slot][2] in short:
            n = squeezed(n)
        start = start_of(work[slot][2], c)

        def store(v):
            mix[start : start + n, :HALF] = v[:, :HALF]

        return qs[c].at[slot, 0 : up(HEADS * n, 32)], ks.at[c, slot], vs.at[c, slot], n, store

    attend([job(slot, c) for slot in range(len(work)) for c in cols], width)


def inner_kernel(width, ypieces, part, geo_ref, *refs):
    pieces = refs[:3] if part < 0 else refs[: 3 * (ypieces + 1)]
    rest = refs[len(pieces) :]
    wqkv_ref, wproj_ref, wup_ref, wdown_ref, gain_ref, out_ref, mix, ext, ks, vs = rest[:10]
    qs = rest[10:]
    pairs = pieces[0].shape[2] // ROWS
    work = [(p, half, 1 + 2 * p + half) for p in range(pairs) for half in range(2)][:-1]
    index, _ = position()
    far = WINDOW + HIGH
    xa, xb = [jnp.where(index[0] % 2 == k, far, 0) for k in (0, 1)]
    ys = [jnp.where(index[1] % 2 == k, far, 0) for k in range(2)]
    wts = block_weights(1, wqkv_ref, wproj_ref, wup_ref, wdown_ref, gain_ref)
    tiles = []
    for k, y in enumerate([HIGH] + ys[: len(pieces) // 3 - 1]):
        for i, x in enumerate((HIGH, xa, xb)):
            tiles.append((pieces[3 * k + i][...], None, x, y))
    if part < 0:
        ext[:, :, pl.ds(ys[1], HIGH)] = jnp.zeros((pairs, EXT, HIGH, ROWS, LANES), F32)

    def split(tile, other):
        return [tile[:, p * ROWS : (p + 1) * ROWS, :] for p in range(pairs)]

    def run(cols):
        places, rows = layout(cols)
        used = rows * len(work)
        rows_ref = mix if part < 0 else out_ref
        rest = rows_ref.shape[0] - used
        if rest:
            rows_ref[used:] = jnp.zeros((rest, LANES), F32)
        place_all(ext, split, tiles, [COLUMNS[c] for c in cols])
        start = lambda g, c: rows * (g - 1) + places[c]
        window_attention(width, 2 * pairs + 1, cols, work, start, geo_ref, wts, ext, rows_ref, ks, vs, qs)
        if part < 0:
            stop = up(used, LANES)
            out_ref[:stop] = feed_rows(mix, stop, wts, width)
            if stop < out_ref.shape[0]:
                out_ref[stop:] = jnp.zeros((out_ref.shape[0] - stop, LANES), F32)

    if part == 0:
        run(list(range(len(COLUMNS))))
    else:
        for side in range(2):

            @pl.when(index[1] % 2 == side)
            def _(side=side):
                run(half_columns(side if part < 0 else 1 - side))


def last_kernel(width, ypieces, geo_ref, inner_ref, *refs):
    early = ypieces == 1
    if early:
        free_ref, *refs = refs
    pieces = refs[: 4 * (ypieces + 1)]
    rest = refs[4 * (ypieces + 1) :]
    wqkv_ref, wproj_ref, wup_ref, wdown_ref, gain_ref, wconv_hbm, cgain_hbm, out_ref = rest[:8]
    ext, mix, fed, grid, wc, tot, wconv_ref, cgain_ref, sems, ks, vs = rest[8:19]
    qs = rest[19:]
    moves = [
        pltpu.make_async_copy(wconv_hbm, wconv_ref, sems.at[0]),
        pltpu.make_async_copy(cgain_hbm, cgain_ref, sems.at[1]),
    ]
    for m in moves:
        m.start()
    nz = out_ref.shape[2]
    pairs = pieces[0].shape[2] // ROWS
    groups = 2 * pairs + 1
    index, count = position()
    far = WINDOW + HIGH
    xa, xb = [jnp.where(index[0] % 2 == k, far, 0) for k in (0, 1)]
    ys = [jnp.where(index[1] % 2 == k, far, 0) for k in range(2)]
    wts = block_weights(1, wqkv_ref, wproj_ref, wup_ref, wdown_ref, gain_ref)
    tiles = []
    for k, y in enumerate([HIGH] + ys[:ypieces]):
        at = 0
        for i, x in enumerate((HIGH, xa, xb)):
            mine = pieces[4 * k + i][:, :, -ROWS:, :]
            tiles.append((mine, pieces[4 * k + 3][at : at + mine.shape[0]], x, y))
            at += mine.shape[0]
    if ypieces == 1:
        ext[:, :, pl.ds(ys[1], HIGH)] = jnp.zeros((2, EXT, HIGH, ROWS, LANES), F32)

    def split(mine, other):
        low = iota(mine.shape, 1) < HIGH
        return jnp.where(low, mine, other), jnp.where(low, other, mine)

    cols = list(range(len(COLUMNS)))
    offsets, per = layout(cols)
    depth = grid.shape[2]
    grid[:, :, WINDOW * groups :] = jnp.zeros((WINDOW + 2, WINDOW + 2, depth - WINDOW * groups, LANES), F32)

    def scatter(g, rows, base, cols):
        places, _ = layout(cols)
        for c in cols:
            wx, wy = COLUMNS[c]
            (_, nx), (_, ny) = BOXES[wx], BOXES[wy]
            for x in range(nx):
                for y in range(ny):
                    at = base + places[c] + ROWS * (x * ny + y)
                    grid[HIGH * wx + x, HIGH * wy + y, WINDOW * g : WINDOW * (g + 1), :] = rows[at : at + WINDOW]

    places, lowest = layout(cols, squeezed)
    used = lowest + per
    stop = up(used, LANES)
    mix[used:stop] = jnp.zeros((stop - used, LANES), F32)
    fed[...] = feed_rows(inner_ref, inner_ref.shape[0], wts, width)
    place_all(ext, split, tiles, COLUMNS)
    work = [(0, 1, groups - 1), (1, 1, 0)]
    start = lambda g, c: lowest + offsets[c] if g else places[c]
    window_attention(width, groups, cols, work, start, geo_ref, wts, ext, mix, ks, vs, qs, (0,))
    out = feed_rows(mix, stop, wts, width)
    for c, (wx, wy) in enumerate(COLUMNS):
        (_, nx), (_, ny) = BOXES[wx], BOXES[wy]
        for i in range(nx * ny):
            at = places[c] + HIGH * i
            grid[HIGH * wx + i // ny, HIGH * wy + i % ny, SHIFT:WINDOW, :] = out[at : at + HIGH]
    scatter(groups - 1, out, lowest, cols)
    if early:
        for side in range(2):

            @pl.when(index[1] % 2 == side)
            def _(side=side):
                for wy, rows in ((side, free_ref), (1 - side, fed)):
                    half = half_columns(wy)
                    for g in range(1, groups - 1):
                        scatter(g, rows, layout(half)[1] * (g - 1), half)

    else:
        for g in range(1, groups - 1):
            scatter(g, fed, per * (g - 1), cols)

    last = WINDOW + 1

    def clear(when, *at):
        @pl.when(when)
        def _():
            grid[at] = jnp.zeros_like(grid[at])

    clear(index[0] == 0, slice(0, 1))
    clear(index[0] == count[0] - 1, slice(last, last + 1))
    clear(index[1] == 0, slice(None), slice(0, 1))
    clear(index[1] == count[1] - 1, slice(None), slice(last, last + 1))
    clear(index[2] == 0, slice(None), slice(None), slice(SHIFT, HIGH))
    clear(index[2] == count[2] - 1, slice(None), slice(None), slice(HIGH + nz, HIGH + nz + 1))

    for m in moves:
        m.wait()
    wc[...] = jnp.zeros(wc.shape, BF)
    for dx in range(3):
        total = None
        for dy in range(3):
            taps = wconv_ref[9 * dx + 3 * dy : 9 * dx + 3 * dy + 3].reshape(3 * width, width)
            i, j = iota((width, 4 * HALF), 0), iota((width, 4 * HALF), 1)
            place = jnp.where(j == i + HALF * dy, 1.0, 0.0).astype(BF)
            part = mm(taps, place)
            total = part if total is None else total + part
        for dz in range(3):
            at = 4 * HALF * dx + HALF * dz
            wc[at : at + width] = total[width * dz : width * (dz + 1)].astype(BF)

    side = WINDOW + 2
    padded = -(-nz // 16) * 16

    def lhs(x):
        taps = [grid[x, :, SHIFT + d : SHIFT + d + padded, :].reshape(side * padded, LANES) for d in range(3)]
        lower = iota(taps[0].shape, 1) < HALF
        return jnp.concatenate([jnp.where(lower, taps[0], taps[1]), taps[2]], 1).astype(BF)

    rows = [lhs(x) for x in range(side)]
    acc = mm(jnp.concatenate([jnp.concatenate(rows[x : x + 3], 1) for x in range(WINDOW)], 0), wc[...])
    strip = WINDOW * padded
    for x in range(WINDOW):
        part = acc[x * side * padded : (x + 1) * side * padded]
        near, second = part[:, :LANES], part[:, LANES:]
        turned = pltpu.roll(near[padded : (WINDOW + 1) * padded], HALF, 1)
        tot[x * strip : (x + 1) * strip] = near[:strip] + turned + second[2 * padded :]
    tot[WINDOW * strip :] = jnp.zeros((tot.shape[0] - WINDOW * strip, LANES), F32)
    diagonal = iota((width, width), 0) == iota((width, width), 1)
    cg = jnp.sum(jnp.where(diagonal, cgain_ref[...], 0.0), 1, keepdims=True)
    normed = norm_cols(jnp.transpose(tot[...])[:width], cg, width)
    active = jnp.where(normed >= 0.0, normed, 0.01 * normed)
    active = jnp.transpose(jnp.concatenate([active, jnp.zeros((LANES - width, tot.shape[0]), F32)], 0))
    for x in range(WINDOW):
        centre = grid[x + 1, 1 : 1 + WINDOW, HIGH : HIGH + padded, :].reshape(strip, LANES)
        result = (centre + active[x * strip : (x + 1) * strip]).reshape(WINDOW, padded, LANES).astype(BF)
        out_ref[x] = result[:, :nz, :width]


def geometry():
    kept = WINDOW * WINDOW - 1
    geo = np.full((16, kept * ROWS), WINDOW, np.float32)
    for v in range(2):
        gone = kept * v
        for i in range(kept):
            spot = i + 1 - v
            for r in range(ROWS):
                t = i * ROWS + r
                if r < WINDOW:
                    geo[8 * v : 8 * v + 3, t] = r, spot // WINDOW, spot % WINDOW
                elif i < WINDOW:
                    geo[8 * v : 8 * v + 3, t] = i, gone // WINDOW, gone % WINDOW
                else:
                    geo[8 * v + 1 : 8 * v + 3, t] = spot // WINDOW, spot % WINDOW
    return jnp.asarray(geo)


def exchange(v, axis, odd):
    count, cores = lax.axis_size(axis), lax.axis_size("gz")
    pairs = []
    for i in range(count):
        low = i - (i - odd) % 2
        for c in range(cores):
            if low < 0 or low + 1 >= count:
                to = (i, c ^ 1 if c ^ 1 < cores else c)
            else:
                to = (low + 1 if i == low else low, c)
            pairs.append((i * cores + c, to[0] * cores + to[1]))
    return lax.ppermute(v, (axis, "gz"), pairs)


def body(volume, w_qkv, w_proj, w_up, w_down, norm_gain, conv_weight, conv_gain):
    sx, sy, sz, width = volume.shape
    spots = sx * sy
    groups = sz // WINDOW
    geo = geometry()
    keys = (spots - 1) * ROWS
    weights = (w_qkv, w_proj, w_up, jnp.swapaxes(w_down, 1, 2), norm_gain)
    halves = [0] if lax.axis_size("gy") == 2 else [0, 1]
    tall = ROWS * groups // 2

    operands = (volume, geo, *weights)
    packed, *cuts = pl.pallas_call(
        functools.partial(first_kernel, width, len(halves)),
        out_shape=[jax.ShapeDtypeStruct((sx, sy, tall, LANES), BF)]
        + [jax.ShapeDtypeStruct((sx, HIGH, tall, LANES), BF) for _ in halves]
        + [jax.ShapeDtypeStruct((HIGH, sy, tall, LANES), BF) for _ in range(2)],
        in_specs=[pl.BlockSpec(memory_space=pltpu.HBM)] * len(operands),
        scratch_shapes=[pltpu.VMEM(v.shape, v.dtype) for v in operands]
        + [
            pltpu.SemaphoreType.DMA((len(operands),)),
            pltpu.VMEM((spots, sz + 12, LANES), F32),
            pltpu.VMEM((groups, spots - 1, ROWS, LANES), F32),
            pltpu.VMEM((groups, HEADS * keys, LANES), BF),
            pltpu.VMEM((groups, LANES, keys), BF),
            pltpu.VMEM((groups, keys, LANES), BF),
            pltpu.VMEM((groups, keys, LANES), F32),
            pltpu.VMEM((width, groups * keys), F32),
            pltpu.VMEM((spots, sz + 12, LANES), F32),
        ],
        compiler_params=pltpu.CompilerParams(vmem_limit_bytes=24 << 20),
        name="first_block",
    )(*[pltpu.with_memory_space_constraint(v, pltpu.HBM) for v in operands])

    xodd = lax.axis_index("gx") % 2

    def cut(v, odd):
        return lax.dynamic_slice_in_dim(v, jnp.where(odd == 0, SHIFT, 0), HIGH, 0)

    def other_core(v):
        return lax.ppermute(v, "gz", [(0, 1), (1, 0)])

    ys = [exchange(v, "gy", k) for k, v in zip(halves, cuts)]
    xs = [exchange(v, "gx", k) for k, v in enumerate(cuts[len(halves) :])]
    corners = [[exchange(cut(v, (xodd + k) % 2), "gx", k) for k in (0, 1)] for v in ys]

    side = WINDOW + 2
    rows = sum(box_rows(*c) for c in COLUMNS)
    strip = WINDOW * -(-sz // 16) * 16

    def buffers(slots):
        return [
            pltpu.VMEM((len(COLUMNS), slots, LANES, keys), BF),
            pltpu.VMEM((len(COLUMNS), slots, keys, LANES), BF),
        ] + [pltpu.VMEM((slots, -(-HEADS * box_rows(*c) // 32) * 32, LANES), BF) for c in COLUMNS]

    span = up(max(layout(half_columns(k))[1] for k in range(2)) * (groups - 1), LANES)

    def inner(part, operands):
        return pl.pallas_call(
            functools.partial(inner_kernel, width, len(ys), part),
            out_shape=jax.ShapeDtypeStruct((span if part else up(rows * (groups - 1), LANES), LANES), F32),
            scratch_shapes=[
                pltpu.VMEM((span, LANES), F32),
                pltpu.VMEM((groups // 2, EXT, EXT, ROWS, LANES), F32),
            ]
            + buffers(groups - 1),
            compiler_params=pltpu.CompilerParams(vmem_limit_bytes=20 << 20),
            cost_estimate=pl.CostEstimate(flops=2 * 10**9, transcendentals=0, bytes_accessed=10**6),
        )(*operands)

    def edge(parts):
        def kernel(*refs):
            at = 0
            for r in refs[:-1]:
                refs[-1][at : at + r.shape[0]] = r[:, :, -ROWS:, :]
                at += r.shape[0]

        shape = (sum(p.shape[0] for p in parts),) + (parts[0].shape[1], ROWS, LANES)
        return pl.pallas_call(
            kernel,
            out_shape=jax.ShapeDtypeStruct(shape, BF),
            compiler_params=pltpu.CompilerParams(vmem_limit_bytes=4 << 20),
        )(*parts)

    near = [packed, *xs]
    wide = [v for y, c in zip(ys, corners) for v in (y, *c)]
    if len(ys) == 1:
        early = inner(-1, [geo, *near, *weights])
        rows_first = lax.optimization_barrier((early, *near))
        zs = other_core(edge(rows_first[1:]))
        zcorners = [other_core(edge([y, *c])) for y, c in zip(ys, corners)]
        done = inner(1, [geo, *near, *wide, *weights])
        done = [done, early]
    else:
        zs = other_core(edge(near))
        zcorners = [other_core(edge([y, *c])) for y, c in zip(ys, corners)]
        done = [inner(0, [geo, *near, *wide, *weights])]

    flat = [v for y, c, z in zip(ys, corners, zcorners) for v in (y, *c, z)]
    conv = [pltpu.with_memory_space_constraint(v, pltpu.HBM) for v in (conv_weight, conv_gain[None, :])]
    operands = [geo, *done, *near, zs, *flat, *weights, *conv]
    vmem = pl.BlockSpec(memory_space=pltpu.VMEM)
    hbm = pl.BlockSpec(memory_space=pltpu.HBM)
    return pl.pallas_call(
        functools.partial(last_kernel, width, len(ys)),
        out_shape=jax.ShapeDtypeStruct(volume.shape, volume.dtype),
        in_specs=[vmem] * (len(operands) - 2) + [hbm] * 2,
        scratch_shapes=[
            pltpu.VMEM((2, EXT, EXT, ROWS, LANES), F32),
            pltpu.VMEM((up(layout(range(len(COLUMNS)), squeezed)[1] + rows, LANES), LANES), F32),
            pltpu.VMEM(done[0].shape, F32),
            pltpu.VMEM((side, side, sz + 12, LANES), F32),
            pltpu.VMEM((3 * 4 * HALF, 4 * HALF), BF),
            pltpu.VMEM((-(-WINDOW * strip // LANES) * LANES, LANES), F32),
            pltpu.VMEM(conv[0].shape, conv[0].dtype),
            pltpu.VMEM(conv[1].shape, conv[1].dtype),
            pltpu.SemaphoreType.DMA((2,)),
        ]
        + buffers(2),
        compiler_params=pltpu.CompilerParams(vmem_limit_bytes=26 << 20),
        name="last_windows",
    )(*operands)


def solution(mesh):
    placed = (P(("parts", "gx"), "gy", "gz", None), P(), P(), P(), P(), P(), P(), P())

    return jax.shard_map(
        body,
        mesh=mesh,
        in_specs=placed,
        out_specs=P(("parts", "gx"), "gy", "gz", None),
        check_vma=False,
    )
```

```python
import functools

import jax
import jax.numpy as jnp
import numpy as np
from jax import lax
from jax.experimental import pallas as pl
from jax.experimental.pallas import tpu as pltpu
from jax.sharding import PartitionSpec as P


HEADS = 3
WINDOW = 7
SHIFT = 3
LANES = 128
HALF = 64
ROWS = 8
BIG = -1e30
HIGH = WINDOW - SHIFT
EXT = 2 * WINDOW + 1
BF = jnp.bfloat16
F32 = jnp.float32


def mm(a, b):
    return jnp.dot(a, b, preferred_element_type=F32)


def iota(shape, dim):
    return lax.broadcasted_iota(jnp.int32, shape, dim)


def norm_cols(x, gain, width):
    mean = jnp.sum(x, 0, keepdims=True) * (1.0 / width)
    centred = x - mean
    spread = jnp.sum(centred * centred, 0, keepdims=True) * (1.0 / width)
    return centred * lax.rsqrt(spread + 1e-05) * gain


def twice_gelu(x):
    inner = x * (0.7978845608028654 + (0.7978845608028654 * 0.044715) * (x * x))
    return x + x * jnp.tanh(inner)


def block_weights(b, wqkv_ref, wproj_ref, wup_ref, wdown_ref, gain_ref):
    wqkv = wqkv_ref[b]
    width, triple = wqkv.shape
    scale = (width // HEADS) ** (-0.5)
    i, j = iota((triple, LANES), 0), iota((triple, LANES), 1)
    take_v = (j < width) & (i == j + 2 * width)
    take_q = (j >= HALF) & (j < HALF + width) & (i == j - HALF)
    place = jnp.where(take_v, 1.0, jnp.where(take_q, scale, 0.0)).astype(BF)
    wvq = mm(wqkv, place).astype(BF)
    o, i = iota((width, triple), 0), iota((width, triple), 1)
    place = jnp.where(i == o + width, 1.0, 0.0).astype(BF)
    wk = lax.dot_general(place, wqkv, (((1,), (1,)), ((), ())), preferred_element_type=F32).astype(BF)
    gains = gain_ref[b]
    diagonal = iota((width, width), 0) == iota((width, width), 1)
    first, second = [jnp.sum(jnp.where(diagonal, gains[k : k + 1], 0.0), 1, keepdims=True) for k in range(2)]
    i, j = iota((width, LANES), 0), iota((width, LANES), 1)
    spread = jnp.where(i == j, 1.0, 0.0).astype(BF)
    wp = lax.dot_general(wproj_ref[b], spread, (((0,), (0,)), ((), ())), preferred_element_type=F32)
    wp = (wp + jnp.where(j == i + HALF, 1.0, 0.0)).astype(BF)
    return wvq, wk, first, wp, wup_ref[b], wdown_ref[b] * jnp.asarray(0.5, BF), second


def make_keys(columns, bias, wts, width):
    wvq, wk, gain = wts[0], wts[1], wts[2]
    normed = norm_cols(columns, gain, width).astype(BF)
    vq = lax.dot_general(normed, wvq, (((0,), (0,)), ((), ())), preferred_element_type=F32)
    kt = mm(wk, normed).astype(BF)
    keys = columns.shape[1]
    top = iota((HALF - width, keys), 0) == 0
    extra = jnp.where(top, bias, 0.0).astype(BF)
    kaug = jnp.concatenate([jnp.zeros((HALF, keys), BF), kt, extra], 0)
    return vq, kaug


def values_of(vq, width):
    return jnp.where(iota(vq.shape, 1) < width, vq, 1.0).astype(BF)


def queries_of(rows, width):
    head_dim = width // HEADS
    lane = iota(rows.shape, 1)
    one = jnp.where(lane == HALF + width, 1.0, 0.0)
    parts = []
    for h in range(HEADS):
        low = HALF + h * head_dim
        parts.append(jnp.where((lane >= low) & (lane < low + head_dim), rows, one))
    spare = -len(parts) * rows.shape[0] % 32
    if spare:
        parts.append(jnp.zeros((spare, LANES), F32))
    return jnp.concatenate(parts, 0).astype(BF)


def attend(jobs, width):
    head_dim = width // HEADS
    jobs = list(jobs)
    ahead = mm(jobs[0][0][...], jobs[0][1][...])
    for i, (_, _, values, n, store) in enumerate(jobs):
        scores = ahead
        if i + 1 < len(jobs):
            ahead = mm(jobs[i + 1][0][...], jobs[i + 1][1][...])
        top = jnp.max(scores, -1, keepdims=True)
        weights = jnp.exp(scores - top).astype(BF)
        out = mm(weights, values[...])
        lane = iota((n, LANES), 1)
        lane = jnp.where(lane >= HALF, lane - HALF, lane)
        mixed = out[:n]
        for h in range(1, HEADS):
            mixed = jnp.where(lane >= h * head_dim, out[h * n : (h + 1) * n], mixed)
        store(mixed / pltpu.roll(mixed, HALF, 1))


def feed(first, wts, width):
    wup, wdown, gain = wts[4:]
    first = first.astype(BF).astype(F32)
    normed = norm_cols(first, gain, width).astype(BF)
    upper = lax.dot_general(wup, normed, (((0,), (0,)), ((), ())), preferred_element_type=F32)
    return (first + mm(wdown, twice_gelu(upper).astype(BF))).astype(BF).astype(F32)


def against_rows(w, rows):
    return lax.dot_general(w, rows, (((1,), (1,)), ((), ())), preferred_element_type=F32)


def first_kernel(width, ny, *refs):
    hbm, out_ref = refs[:7], refs[7]
    y_refs, x_refs = refs[8 : 8 + ny], refs[8 + ny : 10 + ny]
    copies = refs[10 + ny : 17 + ny]
    sems = refs[17 + ny]
    raw, tok, qs, ks, vs, mix, held, done = refs[18 + ny :]
    moves = [pltpu.make_async_copy(h, v, sems.at[i]) for i, (h, v) in enumerate(zip(hbm, copies))]
    for m in moves:
        m.start()
    for m in moves[1:]:
        m.wait()
    vol_ref, geo_ref, wqkv_ref, wproj_ref, wup_ref, wdown_ref, gain_ref = copies
    nz = vol_ref.shape[2]
    groups = nz // WINDOW
    spots = WINDOW * WINDOW
    kept = spots - 1
    keys = kept * ROWS
    wts = block_weights(0, wqkv_ref, wproj_ref, wup_ref, wdown_ref, gain_ref)
    done[...] = jnp.zeros(done.shape, F32)
    moves[0].wait()
    raw[:, nz:, :] = jnp.zeros((spots, raw.shape[1] - nz, LANES), F32)
    raw[:, 0:nz, 0:width] = vol_ref[...].astype(F32).reshape(spots, nz, width)
    bias = jnp.where(geo_ref[8:9, :] < WINDOW, 0.0, BIG)

    def make(w):
        tok[w] = raw[0:kept, WINDOW * w : WINDOW * w + ROWS, :]
        for j in range(WINDOW):
            tok[w, j, WINDOW : WINDOW + 1, :] = raw[kept, WINDOW * w + j : WINDOW * w + j + 1, :]
        columns = jnp.transpose(tok[w].reshape(keys, LANES))[:width]
        held[:, keys * w : keys * (w + 1)] = columns
        vq, kaug = make_keys(columns, bias, wts, width)
        vs[w] = values_of(vq, width)
        ks[w] = kaug
        qs[w] = queries_of(vq, width)

    def finish(w0, n):
        mixed = mix[w0 : w0 + n].reshape(n * keys, LANES)[:, :width].astype(BF)
        first = held[:, keys * w0 : keys * (w0 + n)] + against_rows(wts[3][:, :width], mixed)
        out = feed(first, wts, width)
        out = jnp.transpose(jnp.concatenate([out, jnp.zeros((LANES - width, n * keys), F32)], 0))[:, :width]
        out = out.reshape(n, kept, ROWS, width)
        for w in range(w0, w0 + n):
            done[0:kept, WINDOW * w : WINDOW * (w + 1), :width] = out[w - w0, :, :WINDOW, :]
            if w == 0:
                done[0:kept, nz : nz + SHIFT, :width] = out[w - w0, :, :SHIFT, :]
            for j in range(WINDOW):
                one = out[w - w0, j, WINDOW : WINDOW + 1, :]
                done[kept, WINDOW * w + j : WINDOW * w + j + 1, :width] = one
                if w == 0 and j < SHIFT:
                    done[kept, nz + j : nz + j + 1, :width] = one

    for w in range(groups):
        make(w)

    def keep(w):
        def store(v):
            mix[w] = v

        return store

    attend([(qs.at[w], ks.at[w], vs.at[w], keys, keep(w)) for w in range(groups)], width)
    finish(0, groups)
    pieces = [done[:, SHIFT + WINDOW * w : SHIFT + WINDOW * w + ROWS, :] for w in range(groups)]
    rolled = [pltpu.roll(p.reshape(spots * ROWS, LANES), HALF, 1).reshape(spots, ROWS, LANES) for p in pieces[1::2]]
    joined = [a + b for a, b in zip(pieces[0::2], rolled)]
    packed = jnp.concatenate(joined, 1).astype(BF)
    out_ref[...] = packed.reshape(WINDOW, WINDOW, ROWS * len(joined), LANES)
    yodd = lax.axis_index("gy") % 2
    for k, y_ref in enumerate(y_refs):
        start = jnp.where((yodd + k) % 2 == 0, SHIFT, 0)
        y_ref[...] = out_ref[:, pl.ds(start, HIGH)]
    xodd = lax.axis_index("gx") % 2
    for k, x_ref in enumerate(x_refs):
        start = jnp.where((xodd + k) % 2 == 0, SHIFT, 0)
        x_ref[...] = out_ref[pl.ds(start, HIGH)]


BOXES = ((SHIFT, HIGH), (0, HIGH + 1))
COLUMNS = tuple((wx, wy) for wx in range(2) for wy in range(2))


def box_rows(wx, wy):
    return BOXES[wx][1] * BOXES[wy][1] * ROWS


def layout(cols, size=lambda n: n):
    sizes = [size(box_rows(*COLUMNS[c])) for c in cols]
    return {c: sum(sizes[:i]) for i, c in enumerate(cols)}, sum(sizes)


def half_columns(wy):
    return [c for c, column in enumerate(COLUMNS) if column[1] == wy]


def up(n, m):
    return -(-n // m) * m


def feed_rows(mix, stop, wts, width):
    out = feed(against_rows(wts[3], mix[:stop].astype(BF)), wts, width)
    nil = jnp.zeros((HALF - width, stop), F32)
    return jnp.transpose(jnp.concatenate([out, nil, out, nil], 0))


def position():
    index = [lax.axis_index(a) for a in ("gx", "gy", "gz")]
    count = [lax.axis_size(a) for a in ("gx", "gy", "gz")]
    return index, count


def place_all(ext, split, pieces, shared):
    for tile, other, x, y in pieces:
        nx, ny = tile.shape[:2]
        n = nx * ny
        tile = tile.astype(F32).reshape(n, tile.shape[2], LANES)
        if other is not None:
            other = other.astype(F32).reshape(n, ROWS, LANES)
        for slab, v in enumerate(split(tile, other)):
            ext[slab, pl.ds(x, nx), pl.ds(y, ny)] = v.reshape(nx, ny, ROWS, LANES)
    for wx, wy in shared:
        x0, y0 = WINDOW * wx, WINDOW * wy
        gone = (WINDOW * WINDOW - 1) * wx
        for slab in range(ext.shape[0]):
            for j in range(WINDOW):
                to = j + 1 - wx
                ext[slab, x0 + to // WINDOW, y0 + to % WINDOW, WINDOW : WINDOW + 1, :] = ext[
                    slab, x0 + gone // WINDOW, y0 + gone % WINDOW, j : j + 1, :
                ]


def squeezed(rows):
    return up(rows // ROWS, 2) // 2 * ROWS


def squeeze(rows):
    n = rows.shape[0] // ROWS
    if n % 2:
        rows = jnp.concatenate([rows, jnp.zeros((ROWS, LANES), F32)], 0)
    m = (n + 1) // 2
    pairs = rows.reshape(m, 2, ROWS, LANES)
    even, odd = [pairs[:, k].reshape(m * ROWS, LANES) for k in (0, 1)]
    low = iota((m * ROWS, LANES), 0) % ROWS < HIGH
    return jnp.where(low, pltpu.roll(even, m * ROWS - SHIFT, 0), pltpu.roll(odd, 1, 0))


def window_attention(width, groups, cols, work, start_of, geo_ref, wts, ext, mix, ks, vs, qs, short=()):
    index, count = position()
    spots = WINDOW * WINDOW
    keys = (spots - 1) * ROWS
    nolow = [jnp.where(i > 0, 0.0, 1.0) for i in index]
    nohigh = [jnp.where(i < c - 1, 0.0, 1.0) for i, c in zip(index, count)]

    def turn(slab, c):
        wx, wy = COLUMNS[c]
        first = ROWS * (1 - wx)
        tokens = ext[slab, WINDOW * wx : WINDOW * (wx + 1), WINDOW * wy : WINDOW * (wy + 1)]
        flat = tokens.reshape(spots * ROWS, LANES)
        return tokens, jnp.transpose(flat[first : first + keys])

    def make(slab, c, tokens, turned):
        wx, wy = COLUMNS[c]
        row, px, py = [geo_ref[8 * wx + k : 8 * wx + k + 1, :] for k in range(3)]
        badx = jnp.where(px < HIGH, nolow[0], 0.0) if wx == 0 else jnp.where(px >= HIGH, nohigh[0], 0.0)
        bady = jnp.where(py < HIGH, nolow[1], 0.0) if wy == 0 else jnp.where(py >= HIGH, nohigh[1], 0.0)
        bad = badx + bady + jnp.where(row < WINDOW, 0.0, 1.0)
        (bx, nx), (by, ny) = BOXES[wx], BOXES[wy]
        nq = nx * ny * ROWS
        first = ROWS * (1 - wx)
        chosen = tokens[bx : bx + nx, by : by + ny].reshape(nq, LANES)
        for slot, (at, half, g) in enumerate(work):
            if at != slab:
                continue
            badz = jnp.zeros_like(bad)
            if g == 0:
                badz = jnp.where(row < HIGH, nolow[2], 0.0)
            if g == groups - 1:
                badz = jnp.where(row >= HIGH, nohigh[2], 0.0)
            bias = jnp.where(bad + badz > 0.0, BIG, 0.0)
            vq, kaug = make_keys(turned[HALF * half : HALF * half + width], bias, wts, width)
            vs[c, slot] = values_of(vq, width)
            ks[c, slot] = kaug
            picked = [
                vq[ROWS * (WINDOW * x + by) - first : ROWS * (WINDOW * x + by + ny) - first] for x in range(bx, bx + nx)
            ]
            picked, residual = jnp.concatenate(picked, 0), chosen
            if g in short:
                picked, residual = squeeze(picked), squeeze(residual)
            queries = queries_of(picked, width)
            qs[c][slot, 0 : queries.shape[0]] = queries
            start = start_of(g, c)
            residual = residual if half else pltpu.roll(residual, HALF, 1)
            mix[start : start + residual.shape[0], HALF:] = residual[:, HALF:]

    order = [(slab, c) for slab in sorted({w[0] for w in work}) for c in cols]
    ahead = turn(*order[0])
    for i, at in enumerate(order):
        now = ahead
        if i + 1 < len(order):
            ahead = turn(*order[i + 1])
        make(*at, *now)

    def job(slot, c):
        n = box_rows(*COLUMNS[c])
        if work[slot][2] in short:
            n = squeezed(n)
        start = start_of(work[slot][2], c)

        def store(v):
            mix[start : start + n, :HALF] = v[:, :HALF]

        return qs[c].at[slot, 0 : up(HEADS * n, 32)], ks.at[c, slot], vs.at[c, slot], n, store

    attend([job(slot, c) for slot in range(len(work)) for c in cols], width)


def inner_kernel(width, ypieces, part, geo_ref, *refs):
    pieces = refs[:3] if part < 0 else refs[: 3 * (ypieces + 1)]
    rest = refs[len(pieces) :]
    wqkv_ref, wproj_ref, wup_ref, wdown_ref, gain_ref, out_ref, mix, ext, ks, vs = rest[:10]
    qs = rest[10:]
    pairs = pieces[0].shape[2] // ROWS
    work = [(p, half, 1 + 2 * p + half) for p in range(pairs) for half in range(2)][:-1]
    index, _ = position()
    far = WINDOW + HIGH
    xa, xb = [jnp.where(index[0] % 2 == k, far, 0) for k in (0, 1)]
    ys = [jnp.where(index[1] % 2 == k, far, 0) for k in range(2)]
    wts = block_weights(1, wqkv_ref, wproj_ref, wup_ref, wdown_ref, gain_ref)
    tiles = []
    for k, y in enumerate([HIGH] + ys[: len(pieces) // 3 - 1]):
        for i, x in enumerate((HIGH, xa, xb)):
            tiles.append((pieces[3 * k + i][...], None, x, y))
    if part < 0:
        ext[:, :, pl.ds(ys[1], HIGH)] = jnp.zeros((pairs, EXT, HIGH, ROWS, LANES), F32)

    def split(tile, other):
        return [tile[:, p * ROWS : (p + 1) * ROWS, :] for p in range(pairs)]

    def run(cols):
        places, rows = layout(cols)
        used = rows * len(work)
        rows_ref = mix if part < 0 else out_ref
        rest = rows_ref.shape[0] - used
        if rest:
            rows_ref[used:] = jnp.zeros((rest, LANES), F32)
        place_all(ext, split, tiles, [COLUMNS[c] for c in cols])
        start = lambda g, c: rows * (g - 1) + places[c]
        window_attention(width, 2 * pairs + 1, cols, work, start, geo_ref, wts, ext, rows_ref, ks, vs, qs)
        if part < 0:
            stop = up(used, LANES)
            out_ref[:stop] = feed_rows(mix, stop, wts, width)
            if stop < out_ref.shape[0]:
                out_ref[stop:] = jnp.zeros((out_ref.shape[0] - stop, LANES), F32)

    if part == 0:
        run(list(range(len(COLUMNS))))
    else:
        for side in range(2):

            @pl.when(index[1] % 2 == side)
            def _(side=side):
                run(half_columns(side if part < 0 else 1 - side))


def last_kernel(width, ypieces, geo_ref, inner_ref, *refs):
    early = ypieces == 1
    if early:
        free_ref, *refs = refs
    pieces = refs[: 3 * (ypieces + 1)]
    zs_ref = refs[3 * (ypieces + 1)]
    rest = refs[3 * (ypieces + 1) + 1 :]
    wqkv_ref, wproj_ref, wup_ref, wdown_ref, gain_ref, wconv_hbm, cgain_hbm, out_ref = rest[:8]
    ext, mix, fed, grid, wc, tot, wconv_ref, cgain_ref, sems, ks, vs = rest[8:19]
    qs = rest[19:]
    moves = [
        pltpu.make_async_copy(wconv_hbm, wconv_ref, sems.at[0]),
        pltpu.make_async_copy(cgain_hbm, cgain_ref, sems.at[1]),
    ]
    for m in moves:
        m.start()
    nz = out_ref.shape[2]
    pairs = pieces[0].shape[2] // ROWS
    groups = 2 * pairs + 1
    index, count = position()
    far = WINDOW + HIGH
    xa, xb = [jnp.where(index[0] % 2 == k, far, 0) for k in (0, 1)]
    ys = [jnp.where(index[1] % 2 == k, far, 0) for k in range(2)]
    wts = block_weights(1, wqkv_ref, wproj_ref, wup_ref, wdown_ref, gain_ref)
    tiles, at = [], 0
    for k, y in enumerate([HIGH] + ys[:ypieces]):
        for i, x in enumerate((HIGH, xa, xb)):
            mine = pieces[3 * k + i][:, :, -ROWS:, :]
            n = mine.shape[0] * mine.shape[1]
            tiles.append((mine, zs_ref[at : at + n], x, y))
            at += n
    if ypieces == 1:
        ext[:, :, pl.ds(ys[1], HIGH)] = jnp.zeros((2, EXT, HIGH, ROWS, LANES), F32)

    def split(mine, other):
        low = iota(mine.shape, 1) < HIGH
        return jnp.where(low, mine, other), jnp.where(low, other, mine)

    cols = list(range(len(COLUMNS)))
    offsets, per = layout(cols)
    depth = grid.shape[2]
    grid[:, :, WINDOW * groups :] = jnp.zeros((WINDOW + 2, WINDOW + 2, depth - WINDOW * groups, LANES), F32)

    def scatter(g, rows, base, cols):
        places, _ = layout(cols)
        for c in cols:
            wx, wy = COLUMNS[c]
            (_, nx), (_, ny) = BOXES[wx], BOXES[wy]
            for x in range(nx):
                for y in range(ny):
                    at = base + places[c] + ROWS * (x * ny + y)
                    grid[HIGH * wx + x, HIGH * wy + y, WINDOW * g : WINDOW * (g + 1), :] = rows[at : at + WINDOW]

    places, lowest = layout(cols, squeezed)
    used = lowest + per
    stop = up(used, LANES)
    mix[used:stop] = jnp.zeros((stop - used, LANES), F32)
    fed[...] = feed_rows(inner_ref, inner_ref.shape[0], wts, width)
    place_all(ext, split, tiles, COLUMNS)
    work = [(0, 1, groups - 1), (1, 1, 0)]
    start = lambda g, c: lowest + offsets[c] if g else places[c]
    window_attention(width, groups, cols, work, start, geo_ref, wts, ext, mix, ks, vs, qs, (0,))
    out = feed_rows(mix, stop, wts, width)
    for c, (wx, wy) in enumerate(COLUMNS):
        (_, nx), (_, ny) = BOXES[wx], BOXES[wy]
        for i in range(nx * ny):
            at = places[c] + HIGH * i
            grid[HIGH * wx + i // ny, HIGH * wy + i % ny, SHIFT:WINDOW, :] = out[at : at + HIGH]
    scatter(groups - 1, out, lowest, cols)
    if early:
        for side in range(2):

            @pl.when(index[1] % 2 == side)
            def _(side=side):
                for wy, rows in ((side, free_ref), (1 - side, fed)):
                    half = half_columns(wy)
                    for g in range(1, groups - 1):
                        scatter(g, rows, layout(half)[1] * (g - 1), half)

    else:
        for g in range(1, groups - 1):
            scatter(g, fed, per * (g - 1), cols)

    last = WINDOW + 1

    def clear(when, *at):
        @pl.when(when)
        def _():
            grid[at] = jnp.zeros_like(grid[at])

    clear(index[0] == 0, slice(0, 1))
    clear(index[0] == count[0] - 1, slice(last, last + 1))
    clear(index[1] == 0, slice(None), slice(0, 1))
    clear(index[1] == count[1] - 1, slice(None), slice(last, last + 1))
    clear(index[2] == 0, slice(None), slice(None), slice(SHIFT, HIGH))
    clear(index[2] == count[2] - 1, slice(None), slice(None), slice(HIGH + nz, HIGH + nz + 1))

    for m in moves:
        m.wait()
    wc[...] = jnp.zeros(wc.shape, BF)
    for dx in range(3):
        total = None
        for dy in range(3):
            taps = wconv_ref[9 * dx + 3 * dy : 9 * dx + 3 * dy + 3].reshape(3 * width, width)
            i, j = iota((width, 4 * HALF), 0), iota((width, 4 * HALF), 1)
            place = jnp.where(j == i + HALF * dy, 1.0, 0.0).astype(BF)
            part = mm(taps, place)
            total = part if total is None else total + part
        for dz in range(3):
            at = 4 * HALF * dx + HALF * dz
            wc[at : at + width] = total[width * dz : width * (dz + 1)].astype(BF)

    side = WINDOW + 2
    padded = -(-nz // 16) * 16

    def lhs(x):
        taps = [grid[x, :, SHIFT + d : SHIFT + d + padded, :].reshape(side * padded, LANES) for d in range(3)]
        lower = iota(taps[0].shape, 1) < HALF
        return jnp.concatenate([jnp.where(lower, taps[0], taps[1]), taps[2]], 1).astype(BF)

    rows = [lhs(x) for x in range(side)]
    acc = mm(jnp.concatenate([jnp.concatenate(rows[x : x + 3], 1) for x in range(WINDOW)], 0), wc[...])
    strip = WINDOW * padded
    for x in range(WINDOW):
        part = acc[x * side * padded : (x + 1) * side * padded]
        near, second = part[:, :LANES], part[:, LANES:]
        turned = pltpu.roll(near[padded : (WINDOW + 1) * padded], HALF, 1)
        tot[x * strip : (x + 1) * strip] = near[:strip] + turned + second[2 * padded :]
    tot[WINDOW * strip :] = jnp.zeros((tot.shape[0] - WINDOW * strip, LANES), F32)
    diagonal = iota((width, width), 0) == iota((width, width), 1)
    cg = jnp.sum(jnp.where(diagonal, cgain_ref[...], 0.0), 1, keepdims=True)
    normed = norm_cols(jnp.transpose(tot[...])[:width], cg, width)
    active = jnp.where(normed >= 0.0, normed, 0.01 * normed)
    active = jnp.transpose(jnp.concatenate([active, jnp.zeros((LANES - width, tot.shape[0]), F32)], 0))
    for x in range(WINDOW):
        centre = grid[x + 1, 1 : 1 + WINDOW, HIGH : HIGH + padded, :].reshape(strip, LANES)
        result = (centre + active[x * strip : (x + 1) * strip]).reshape(WINDOW, padded, LANES).astype(BF)
        out_ref[x] = result[:, :nz, :width]


def geometry():
    kept = WINDOW * WINDOW - 1
    geo = np.full((16, kept * ROWS), WINDOW, np.float32)
    for v in range(2):
        gone = kept * v
        for i in range(kept):
            spot = i + 1 - v
            for r in range(ROWS):
                t = i * ROWS + r
                if r < WINDOW:
                    geo[8 * v : 8 * v + 3, t] = r, spot // WINDOW, spot % WINDOW
                elif i < WINDOW:
                    geo[8 * v : 8 * v + 3, t] = i, gone // WINDOW, gone % WINDOW
                else:
                    geo[8 * v + 1 : 8 * v + 3, t] = spot // WINDOW, spot % WINDOW
    return jnp.asarray(geo)


def exchange(v, axis, odd):
    count, cores = lax.axis_size(axis), lax.axis_size("gz")
    pairs = []
    for i in range(count):
        low = i - (i - odd) % 2
        for c in range(cores):
            if low < 0 or low + 1 >= count:
                to = (i, c ^ 1 if c ^ 1 < cores else c)
            else:
                to = (low + 1 if i == low else low, c)
            pairs.append((i * cores + c, to[0] * cores + to[1]))
    return lax.ppermute(v, (axis, "gz"), pairs)


def body(volume, w_qkv, w_proj, w_up, w_down, norm_gain, conv_weight, conv_gain):
    sx, sy, sz, width = volume.shape
    spots = sx * sy
    groups = sz // WINDOW
    geo = geometry()
    keys = (spots - 1) * ROWS
    weights = (w_qkv, w_proj, w_up, jnp.swapaxes(w_down, 1, 2), norm_gain)
    halves = [0] if lax.axis_size("gy") == 2 else [0, 1]
    tall = ROWS * groups // 2

    operands = (volume, geo, *weights)
    packed, *cuts = pl.pallas_call(
        functools.partial(first_kernel, width, len(halves)),
        out_shape=[jax.ShapeDtypeStruct((sx, sy, tall, LANES), BF)]
        + [jax.ShapeDtypeStruct((sx, HIGH, tall, LANES), BF) for _ in halves]
        + [jax.ShapeDtypeStruct((HIGH, sy, tall, LANES), BF) for _ in range(2)],
        in_specs=[pl.BlockSpec(memory_space=pltpu.HBM)] * len(operands),
        scratch_shapes=[pltpu.VMEM(v.shape, v.dtype) for v in operands]
        + [
            pltpu.SemaphoreType.DMA((len(operands),)),
            pltpu.VMEM((spots, sz + 12, LANES), F32),
            pltpu.VMEM((groups, spots - 1, ROWS, LANES), F32),
            pltpu.VMEM((groups, HEADS * keys, LANES), BF),
            pltpu.VMEM((groups, LANES, keys), BF),
            pltpu.VMEM((groups, keys, LANES), BF),
            pltpu.VMEM((groups, keys, LANES), F32),
            pltpu.VMEM((width, groups * keys), F32),
            pltpu.VMEM((spots, sz + 12, LANES), F32),
        ],
        compiler_params=pltpu.CompilerParams(vmem_limit_bytes=24 << 20),
        name="first_block",
    )(*[pltpu.with_memory_space_constraint(v, pltpu.HBM) for v in operands])

    xodd = lax.axis_index("gx") % 2

    def cut(v, odd):
        return lax.dynamic_slice_in_dim(v, jnp.where(odd == 0, SHIFT, 0), HIGH, 0)

    def other_core(v):
        return lax.ppermute(v, "gz", [(0, 1), (1, 0)])

    ys = [exchange(v, "gy", k) for k, v in zip(halves, cuts)]
    xs = [exchange(v, "gx", k) for k, v in enumerate(cuts[len(halves) :])]
    corners = [[exchange(cut(v, (xodd + k) % 2), "gx", k) for k in (0, 1)] for v in ys]

    side = WINDOW + 2
    rows = sum(box_rows(*c) for c in COLUMNS)
    strip = WINDOW * -(-sz // 16) * 16

    def buffers(slots):
        return [
            pltpu.VMEM((len(COLUMNS), slots, LANES, keys), BF),
            pltpu.VMEM((len(COLUMNS), slots, keys, LANES), BF),
        ] + [pltpu.VMEM((slots, -(-HEADS * box_rows(*c) // 32) * 32, LANES), BF) for c in COLUMNS]

    span = up(max(layout(half_columns(k))[1] for k in range(2)) * (groups - 1), LANES)

    def inner(part, operands):
        return pl.pallas_call(
            functools.partial(inner_kernel, width, len(ys), part),
            out_shape=jax.ShapeDtypeStruct((span if part else up(rows * (groups - 1), LANES), LANES), F32),
            scratch_shapes=[
                pltpu.VMEM((span, LANES), F32),
                pltpu.VMEM((groups // 2, EXT, EXT, ROWS, LANES), F32),
            ]
            + buffers(groups - 1),
            compiler_params=pltpu.CompilerParams(vmem_limit_bytes=20 << 20),
            cost_estimate=pl.CostEstimate(flops=2 * 10**9, transcendentals=0, bytes_accessed=10**6),
        )(*operands)

    def edge(parts):
        def kernel(*refs):
            at = 0
            for r in refs[:-1]:
                n = r.shape[0] * r.shape[1]
                refs[-1][at : at + n] = r[:, :, -ROWS:, :].reshape(n, ROWS, LANES)
                at += n

        shape = (sum(p.shape[0] * p.shape[1] for p in parts), ROWS, LANES)
        return pl.pallas_call(
            kernel,
            out_shape=jax.ShapeDtypeStruct(shape, BF),
            compiler_params=pltpu.CompilerParams(vmem_limit_bytes=4 << 20),
        )(*parts)

    near = [packed, *xs]
    wide = [v for y, c in zip(ys, corners) for v in (y, *c)]
    if len(ys) == 1:
        early = inner(-1, [geo, *near, *weights])
        waited = lax.optimization_barrier((early, *near))
        zs = other_core(edge([*waited[1:], *wide]))
        done = inner(1, [geo, *near, *wide, *weights])
        done = [done, early]
    else:
        zs = other_core(edge(near + wide))
        done = [inner(0, [geo, *near, *wide, *weights])]

    conv = [pltpu.with_memory_space_constraint(v, pltpu.HBM) for v in (conv_weight, conv_gain[None, :])]
    operands = [geo, *done, *near, *wide, zs, *weights, *conv]
    vmem = pl.BlockSpec(memory_space=pltpu.VMEM)
    hbm = pl.BlockSpec(memory_space=pltpu.HBM)
    return pl.pallas_call(
        functools.partial(last_kernel, width, len(ys)),
        out_shape=jax.ShapeDtypeStruct(volume.shape, volume.dtype),
        in_specs=[vmem] * (len(operands) - 2) + [hbm] * 2,
        scratch_shapes=[
            pltpu.VMEM((2, EXT, EXT, ROWS, LANES), F32),
            pltpu.VMEM((up(layout(range(len(COLUMNS)), squeezed)[1] + rows, LANES), LANES), F32),
            pltpu.VMEM(done[0].shape, F32),
            pltpu.VMEM((side, side, sz + 12, LANES), F32),
            pltpu.VMEM((3 * 4 * HALF, 4 * HALF), BF),
            pltpu.VMEM((-(-WINDOW * strip // LANES) * LANES, LANES), F32),
            pltpu.VMEM(conv[0].shape, conv[0].dtype),
            pltpu.VMEM(conv[1].shape, conv[1].dtype),
            pltpu.SemaphoreType.DMA((2,)),
        ]
        + buffers(2),
        compiler_params=pltpu.CompilerParams(vmem_limit_bytes=26 << 20),
        name="last_windows",
    )(*operands)


def solution(mesh):
    placed = (P(("parts", "gx"), "gy", "gz", None), P(), P(), P(), P(), P(), P(), P())

    return jax.shard_map(
        body,
        mesh=mesh,
        in_specs=placed,
        out_specs=P(("parts", "gx"), "gy", "gz", None),
        check_vma=False,
    )
```

```python
import functools

import jax
import jax.numpy as jnp
import numpy as np
from jax import lax
from jax.experimental import pallas as pl
from jax.experimental.pallas import tpu as pltpu
from jax.sharding import PartitionSpec as P


HEADS = 3
WINDOW = 7
SHIFT = 3
LANES = 128
HALF = 64
ROWS = 8
BIG = -1e30
HIGH = WINDOW - SHIFT
EXT = 2 * WINDOW + 1
BF = jnp.bfloat16
F32 = jnp.float32


def mm(a, b):
    return jnp.dot(a, b, preferred_element_type=F32)


def iota(shape, dim):
    return lax.broadcasted_iota(jnp.int32, shape, dim)


def norm_cols(x, gain, width):
    mean = jnp.sum(x, 0, keepdims=True) * (1.0 / width)
    centred = x - mean
    spread = jnp.sum(centred * centred, 0, keepdims=True) * (1.0 / width)
    return centred * lax.rsqrt(spread + 1e-05) * gain


def twice_gelu(x):
    inner = x * (0.7978845608028654 + (0.7978845608028654 * 0.044715) * (x * x))
    return x + x * jnp.tanh(inner)


def block_weights(b, wqkv_ref, wproj_ref, wup_ref, wdown_ref, gain_ref):
    wqkv = wqkv_ref[b]
    width, triple = wqkv.shape
    scale = (width // HEADS) ** (-0.5)
    i, j = iota((triple, LANES), 0), iota((triple, LANES), 1)
    take_v = (j < width) & (i == j + 2 * width)
    take_q = (j >= HALF) & (j < HALF + width) & (i == j - HALF)
    place = jnp.where(take_v, 1.0, jnp.where(take_q, scale, 0.0)).astype(BF)
    wvq = mm(wqkv, place).astype(BF)
    o, i = iota((width, triple), 0), iota((width, triple), 1)
    place = jnp.where(i == o + width, 1.0, 0.0).astype(BF)
    wk = lax.dot_general(place, wqkv, (((1,), (1,)), ((), ())), preferred_element_type=F32).astype(BF)
    gains = gain_ref[b]
    diagonal = iota((width, width), 0) == iota((width, width), 1)
    first, second = [jnp.sum(jnp.where(diagonal, gains[k : k + 1], 0.0), 1, keepdims=True) for k in range(2)]
    i, j = iota((width, LANES), 0), iota((width, LANES), 1)
    spread = jnp.where(i == j, 1.0, 0.0).astype(BF)
    wp = lax.dot_general(wproj_ref[b], spread, (((0,), (0,)), ((), ())), preferred_element_type=F32)
    wp = (wp + jnp.where(j == i + HALF, 1.0, 0.0)).astype(BF)
    return wvq, wk, first, wp, wup_ref[b], wdown_ref[b] * jnp.asarray(0.5, BF), second


def make_keys(columns, bias, wts, width):
    wvq, wk, gain = wts[0], wts[1], wts[2]
    normed = norm_cols(columns, gain, width).astype(BF)
    vq = lax.dot_general(normed, wvq, (((0,), (0,)), ((), ())), preferred_element_type=F32)
    kt = mm(wk, normed).astype(BF)
    keys = columns.shape[1]
    top = iota((HALF - width, keys), 0) == 0
    extra = jnp.where(top, bias, 0.0).astype(BF)
    kaug = jnp.concatenate([jnp.zeros((HALF, keys), BF), kt, extra], 0)
    return vq, kaug


def values_of(vq, width):
    return jnp.where(iota(vq.shape, 1) < width, vq, 1.0).astype(BF)


def queries_of(rows, width):
    head_dim = width // HEADS
    lane = iota(rows.shape, 1)
    one = jnp.where(lane == HALF + width, 1.0, 0.0)
    parts = []
    for h in range(HEADS):
        low = HALF + h * head_dim
        parts.append(jnp.where((lane >= low) & (lane < low + head_dim), rows, one))
    spare = -len(parts) * rows.shape[0] % 32
    if spare:
        parts.append(jnp.zeros((spare, LANES), F32))
    return jnp.concatenate(parts, 0).astype(BF)


def attend(jobs, width):
    head_dim = width // HEADS
    jobs = list(jobs)
    ahead = mm(jobs[0][0][...], jobs[0][1][...])
    for i, (_, _, values, n, store) in enumerate(jobs):
        scores = ahead
        if i + 1 < len(jobs):
            ahead = mm(jobs[i + 1][0][...], jobs[i + 1][1][...])
        top = jnp.max(scores, -1, keepdims=True)
        weights = jnp.exp(scores - top).astype(BF)
        out = mm(weights, values[...])
        lane = iota((n, LANES), 1)
        lane = jnp.where(lane >= HALF, lane - HALF, lane)
        mixed = out[:n]
        for h in range(1, HEADS):
            mixed = jnp.where(lane >= h * head_dim, out[h * n : (h + 1) * n], mixed)
        store(mixed / pltpu.roll(mixed, HALF, 1))


def feed(first, wts, width):
    wup, wdown, gain = wts[4:]
    first = first.astype(BF).astype(F32)
    normed = norm_cols(first, gain, width).astype(BF)
    upper = lax.dot_general(wup, normed, (((0,), (0,)), ((), ())), preferred_element_type=F32)
    return (first + mm(wdown, twice_gelu(upper).astype(BF))).astype(BF).astype(F32)


def against_rows(w, rows):
    return lax.dot_general(w, rows, (((1,), (1,)), ((), ())), preferred_element_type=F32)


def first_kernel(width, ny, *refs):
    hbm, out_ref = refs[:7], refs[7]
    y_refs, x_refs = refs[8 : 8 + ny], refs[8 + ny : 10 + ny]
    copies = refs[10 + ny : 17 + ny]
    sems = refs[17 + ny]
    raw, tok, qs, ks, vs, mix, held, done = refs[18 + ny :]
    moves = [pltpu.make_async_copy(h, v, sems.at[i]) for i, (h, v) in enumerate(zip(hbm, copies))]
    for m in moves:
        m.start()
    for m in moves[1:]:
        m.wait()
    vol_ref, geo_ref, wqkv_ref, wproj_ref, wup_ref, wdown_ref, gain_ref = copies
    nz = vol_ref.shape[2]
    groups = nz // WINDOW
    spots = WINDOW * WINDOW
    kept = spots - 1
    keys = kept * ROWS
    wts = block_weights(0, wqkv_ref, wproj_ref, wup_ref, wdown_ref, gain_ref)
    done[...] = jnp.zeros(done.shape, F32)
    moves[0].wait()
    raw[:, nz:, :] = jnp.zeros((spots, raw.shape[1] - nz, LANES), F32)
    raw[:, 0:nz, 0:width] = vol_ref[...].astype(F32).reshape(spots, nz, width)
    bias = jnp.where(geo_ref[8:9, :] < WINDOW, 0.0, BIG)

    def make(w):
        tok[w] = raw[0:kept, WINDOW * w : WINDOW * w + ROWS, :]
        for j in range(WINDOW):
            tok[w, j, WINDOW : WINDOW + 1, :] = raw[kept, WINDOW * w + j : WINDOW * w + j + 1, :]
        columns = jnp.transpose(tok[w].reshape(keys, LANES))[:width]
        held[:, keys * w : keys * (w + 1)] = columns
        vq, kaug = make_keys(columns, bias, wts, width)
        vs[w] = values_of(vq, width)
        ks[w] = kaug
        qs[w] = queries_of(vq, width)

    def finish(w0, n):
        mixed = mix[w0 : w0 + n].reshape(n * keys, LANES)[:, :width].astype(BF)
        first = held[:, keys * w0 : keys * (w0 + n)] + against_rows(wts[3][:, :width], mixed)
        out = feed(first, wts, width)
        nil = jnp.zeros((HALF - width, n * keys), F32)
        out = jnp.transpose(jnp.concatenate([out, nil, out, nil], 0)).reshape(n, kept, ROWS, LANES)
        for w in range(w0, w0 + n):
            done[0:kept, WINDOW * w : WINDOW * (w + 1), :] = out[w - w0, :, :WINDOW, :]
            if w == 0:
                done[0:kept, nz : nz + SHIFT, :] = out[w - w0, :, :SHIFT, :]
            for j in range(WINDOW):
                one = out[w - w0, j, WINDOW : WINDOW + 1, :]
                done[kept, WINDOW * w + j : WINDOW * w + j + 1, :] = one
                if w == 0 and j < SHIFT:
                    done[kept, nz + j : nz + j + 1, :] = one

    for w in range(groups):
        make(w)

    def keep(w):
        def store(v):
            mix[w] = v

        return store

    attend([(qs.at[w], ks.at[w], vs.at[w], keys, keep(w)) for w in range(groups)], width)
    finish(0, groups)
    pieces = [done[:, SHIFT + WINDOW * w : SHIFT + WINDOW * w + ROWS, :] for w in range(groups)]
    lower = iota(pieces[0].shape, 2) < HALF
    joined = [jnp.where(lower, a, b) for a, b in zip(pieces[0::2], pieces[1::2])]
    packed = jnp.concatenate(joined, 1).astype(BF)
    out_ref[...] = packed.reshape(WINDOW, WINDOW, ROWS * len(joined), LANES)
    yodd = lax.axis_index("gy") % 2
    for k, y_ref in enumerate(y_refs):
        start = jnp.where((yodd + k) % 2 == 0, SHIFT, 0)
        y_ref[...] = out_ref[:, pl.ds(start, HIGH)]
    xodd = lax.axis_index("gx") % 2
    for k, x_ref in enumerate(x_refs):
        start = jnp.where((xodd + k) % 2 == 0, SHIFT, 0)
        x_ref[...] = out_ref[pl.ds(start, HIGH)]


BOXES = ((SHIFT, HIGH), (0, HIGH + 1))
COLUMNS = tuple((wx, wy) for wx in range(2) for wy in range(2))


def box_rows(wx, wy):
    return BOXES[wx][1] * BOXES[wy][1] * ROWS


def layout(cols, size=lambda n: n):
    sizes = [size(box_rows(*COLUMNS[c])) for c in cols]
    return {c: sum(sizes[:i]) for i, c in enumerate(cols)}, sum(sizes)


def half_columns(wy):
    return [c for c, column in enumerate(COLUMNS) if column[1] == wy]


def up(n, m):
    return -(-n // m) * m


def feed_rows(mix, stop, wts, width):
    out = feed(against_rows(wts[3], mix[:stop].astype(BF)), wts, width)
    nil = jnp.zeros((HALF - width, stop), F32)
    return jnp.transpose(jnp.concatenate([out, nil, out, nil], 0))


def position():
    index = [lax.axis_index(a) for a in ("gx", "gy", "gz")]
    count = [lax.axis_size(a) for a in ("gx", "gy", "gz")]
    return index, count


def place_all(ext, split, pieces, shared):
    for tile, other, x, y in pieces:
        nx, ny = tile.shape[:2]
        n = nx * ny
        tile = tile.astype(F32).reshape(n, tile.shape[2], LANES)
        if other is not None:
            other = other.astype(F32).reshape(n, ROWS, LANES)
        for slab, v in enumerate(split(tile, other)):
            ext[slab, pl.ds(x, nx), pl.ds(y, ny)] = v.reshape(nx, ny, ROWS, LANES)
    for wx, wy in shared:
        x0, y0 = WINDOW * wx, WINDOW * wy
        gone = (WINDOW * WINDOW - 1) * wx
        for slab in range(ext.shape[0]):
            for j in range(WINDOW):
                to = j + 1 - wx
                ext[slab, x0 + to // WINDOW, y0 + to % WINDOW, WINDOW : WINDOW + 1, :] = ext[
                    slab, x0 + gone // WINDOW, y0 + gone % WINDOW, j : j + 1, :
                ]


def squeezed(rows):
    return up(rows // ROWS, 2) // 2 * ROWS


def squeeze(rows):
    n = rows.shape[0] // ROWS
    if n % 2:
        rows = jnp.concatenate([rows, jnp.zeros((ROWS, LANES), F32)], 0)
    m = (n + 1) // 2
    pairs = rows.reshape(m, 2, ROWS, LANES)
    even, odd = [pairs[:, k].reshape(m * ROWS, LANES) for k in (0, 1)]
    low = iota((m * ROWS, LANES), 0) % ROWS < HIGH
    return jnp.where(low, pltpu.roll(even, m * ROWS - SHIFT, 0), pltpu.roll(odd, 1, 0))


def window_attention(width, groups, cols, work, start_of, geo_ref, wts, ext, mix, ks, vs, qs, short=()):
    index, count = position()
    spots = WINDOW * WINDOW
    keys = (spots - 1) * ROWS
    nolow = [jnp.where(i > 0, 0.0, 1.0) for i in index]
    nohigh = [jnp.where(i < c - 1, 0.0, 1.0) for i, c in zip(index, count)]

    def turn(slab, c):
        wx, wy = COLUMNS[c]
        first = ROWS * (1 - wx)
        tokens = ext[slab, WINDOW * wx : WINDOW * (wx + 1), WINDOW * wy : WINDOW * (wy + 1)]
        flat = tokens.reshape(spots * ROWS, LANES)
        return tokens, jnp.transpose(flat[first : first + keys])

    def make(slab, c, tokens, turned):
        wx, wy = COLUMNS[c]
        row, px, py = [geo_ref[8 * wx + k : 8 * wx + k + 1, :] for k in range(3)]
        badx = jnp.where(px < HIGH, nolow[0], 0.0) if wx == 0 else jnp.where(px >= HIGH, nohigh[0], 0.0)
        bady = jnp.where(py < HIGH, nolow[1], 0.0) if wy == 0 else jnp.where(py >= HIGH, nohigh[1], 0.0)
        bad = badx + bady + jnp.where(row < WINDOW, 0.0, 1.0)
        (bx, nx), (by, ny) = BOXES[wx], BOXES[wy]
        nq = nx * ny * ROWS
        first = ROWS * (1 - wx)
        chosen = tokens[bx : bx + nx, by : by + ny].reshape(nq, LANES)
        for slot, (at, half, g) in enumerate(work):
            if at != slab:
                continue
            badz = jnp.zeros_like(bad)
            if g == 0:
                badz = jnp.where(row < HIGH, nolow[2], 0.0)
            if g == groups - 1:
                badz = jnp.where(row >= HIGH, nohigh[2], 0.0)
            bias = jnp.where(bad + badz > 0.0, BIG, 0.0)
            vq, kaug = make_keys(turned[HALF * half : HALF * half + width], bias, wts, width)
            vs[c, slot] = values_of(vq, width)
            ks[c, slot] = kaug
            picked = [
                vq[ROWS * (WINDOW * x + by) - first : ROWS * (WINDOW * x + by + ny) - first] for x in range(bx, bx + nx)
            ]
            picked, residual = jnp.concatenate(picked, 0), chosen
            if g in short:
                picked, residual = squeeze(picked), squeeze(residual)
            queries = queries_of(picked, width)
            qs[c][slot, 0 : queries.shape[0]] = queries
            start = start_of(g, c)
            residual = residual if half else pltpu.roll(residual, HALF, 1)
            mix[start : start + residual.shape[0], HALF:] = residual[:, HALF:]

    order = [(slab, c) for slab in sorted({w[0] for w in work}) for c in cols]
    ahead = turn(*order[0])
    for i, at in enumerate(order):
        now = ahead
        if i + 1 < len(order):
            ahead = turn(*order[i + 1])
        make(*at, *now)

    def job(slot, c):
        n = box_rows(*COLUMNS[c])
        if work[slot][2] in short:
            n = squeezed(n)
        start = start_of(work[slot][2], c)

        def store(v):
            mix[start : start + n, :HALF] = v[:, :HALF]

        return qs[c].at[slot, 0 : up(HEADS * n, 32)], ks.at[c, slot], vs.at[c, slot], n, store

    attend([job(slot, c) for slot in range(len(work)) for c in cols], width)


def inner_kernel(width, ypieces, part, geo_ref, *refs):
    pieces = refs[:3] if part < 0 else refs[: 3 * (ypieces + 1)]
    rest = refs[len(pieces) :]
    wqkv_ref, wproj_ref, wup_ref, wdown_ref, gain_ref, out_ref, mix, ext, ks, vs = rest[:10]
    qs = rest[10:]
    pairs = pieces[0].shape[2] // ROWS
    work = [(p, half, 1 + 2 * p + half) for p in range(pairs) for half in range(2)][:-1]
    index, _ = position()
    far = WINDOW + HIGH
    xa, xb = [jnp.where(index[0] % 2 == k, far, 0) for k in (0, 1)]
    ys = [jnp.where(index[1] % 2 == k, far, 0) for k in range(2)]
    wts = block_weights(1, wqkv_ref, wproj_ref, wup_ref, wdown_ref, gain_ref)
    tiles = []
    for k, y in enumerate([HIGH] + ys[: len(pieces) // 3 - 1]):
        for i, x in enumerate((HIGH, xa, xb)):
            tiles.append((pieces[3 * k + i][...], None, x, y))
    if part < 0:
        ext[:, :, pl.ds(ys[1], HIGH)] = jnp.zeros((pairs, EXT, HIGH, ROWS, LANES), F32)

    def split(tile, other):
        return [tile[:, p * ROWS : (p + 1) * ROWS, :] for p in range(pairs)]

    def run(cols):
        places, rows = layout(cols)
        used = rows * len(work)
        rows_ref = mix if part < 0 else out_ref
        rest = rows_ref.shape[0] - used
        if rest:
            rows_ref[used:] = jnp.zeros((rest, LANES), F32)
        place_all(ext, split, tiles, [COLUMNS[c] for c in cols])
        start = lambda g, c: rows * (g - 1) + places[c]
        window_attention(width, 2 * pairs + 1, cols, work, start, geo_ref, wts, ext, rows_ref, ks, vs, qs)
        if part < 0:
            stop = up(used, LANES)
            out_ref[:stop] = feed_rows(mix, stop, wts, width)
            if stop < out_ref.shape[0]:
                out_ref[stop:] = jnp.zeros((out_ref.shape[0] - stop, LANES), F32)

    if part == 0:
        run(list(range(len(COLUMNS))))
    else:
        for side in range(2):

            @pl.when(index[1] % 2 == side)
            def _(side=side):
                run(half_columns(side if part < 0 else 1 - side))


def last_kernel(width, ypieces, geo_ref, inner_ref, *refs):
    early = ypieces == 1
    if early:
        free_ref, *refs = refs
    pieces = refs[: 3 * (ypieces + 1)]
    zs_ref = refs[3 * (ypieces + 1)]
    rest = refs[3 * (ypieces + 1) + 1 :]
    wqkv_ref, wproj_ref, wup_ref, wdown_ref, gain_ref, wconv_hbm, cgain_hbm, out_ref = rest[:8]
    ext, mix, fed, grid, wc, tot, wconv_ref, cgain_ref, sems, ks, vs = rest[8:19]
    qs = rest[19:]
    moves = [
        pltpu.make_async_copy(wconv_hbm, wconv_ref, sems.at[0]),
        pltpu.make_async_copy(cgain_hbm, cgain_ref, sems.at[1]),
    ]
    for m in moves:
        m.start()
    nz = out_ref.shape[2]
    pairs = pieces[0].shape[2] // ROWS
    groups = 2 * pairs + 1
    index, count = position()
    far = WINDOW + HIGH
    xa, xb = [jnp.where(index[0] % 2 == k, far, 0) for k in (0, 1)]
    ys = [jnp.where(index[1] % 2 == k, far, 0) for k in range(2)]
    wts = block_weights(1, wqkv_ref, wproj_ref, wup_ref, wdown_ref, gain_ref)
    tiles, at = [], 0
    for k, y in enumerate([HIGH] + ys[:ypieces]):
        for i, x in enumerate((HIGH, xa, xb)):
            mine = pieces[3 * k + i][:, :, -ROWS:, :]
            n = mine.shape[0] * mine.shape[1]
            tiles.append((mine, zs_ref[at : at + n], x, y))
            at += n
    if ypieces == 1:
        ext[:, :, pl.ds(ys[1], HIGH)] = jnp.zeros((2, EXT, HIGH, ROWS, LANES), F32)

    def split(mine, other):
        low = iota(mine.shape, 1) < HIGH
        return jnp.where(low, mine, other), jnp.where(low, other, mine)

    cols = list(range(len(COLUMNS)))
    offsets, per = layout(cols)
    depth = grid.shape[2]
    grid[:, :, WINDOW * groups :] = jnp.zeros((WINDOW + 2, WINDOW + 2, depth - WINDOW * groups, LANES), F32)

    def scatter(g, rows, base, cols):
        places, _ = layout(cols)
        for c in cols:
            wx, wy = COLUMNS[c]
            (_, nx), (_, ny) = BOXES[wx], BOXES[wy]
            for x in range(nx):
                for y in range(ny):
                    at = base + places[c] + ROWS * (x * ny + y)
                    grid[HIGH * wx + x, HIGH * wy + y, WINDOW * g : WINDOW * (g + 1), :] = rows[at : at + WINDOW]

    places, lowest = layout(cols, squeezed)
    used = lowest + per
    stop = up(used, LANES)
    mix[used:stop] = jnp.zeros((stop - used, LANES), F32)
    fed[...] = feed_rows(inner_ref, inner_ref.shape[0], wts, width)
    place_all(ext, split, tiles, COLUMNS)
    work = [(0, 1, groups - 1), (1, 1, 0)]
    start = lambda g, c: lowest + offsets[c] if g else places[c]
    window_attention(width, groups, cols, work, start, geo_ref, wts, ext, mix, ks, vs, qs, (0,))
    out = feed_rows(mix, stop, wts, width)
    for c, (wx, wy) in enumerate(COLUMNS):
        (_, nx), (_, ny) = BOXES[wx], BOXES[wy]
        for i in range(nx * ny):
            at = places[c] + HIGH * i
            grid[HIGH * wx + i // ny, HIGH * wy + i % ny, SHIFT:WINDOW, :] = out[at : at + HIGH]
    scatter(groups - 1, out, lowest, cols)
    if early:
        for side in range(2):

            @pl.when(index[1] % 2 == side)
            def _(side=side):
                for wy, rows in ((side, free_ref), (1 - side, fed)):
                    half = half_columns(wy)
                    for g in range(1, groups - 1):
                        scatter(g, rows, layout(half)[1] * (g - 1), half)

    else:
        for g in range(1, groups - 1):
            scatter(g, fed, per * (g - 1), cols)

    last = WINDOW + 1

    def clear(when, *at):
        @pl.when(when)
        def _():
            grid[at] = jnp.zeros_like(grid[at])

    clear(index[0] == 0, slice(0, 1))
    clear(index[0] == count[0] - 1, slice(last, last + 1))
    clear(index[1] == 0, slice(None), slice(0, 1))
    clear(index[1] == count[1] - 1, slice(None), slice(last, last + 1))
    clear(index[2] == 0, slice(None), slice(None), slice(SHIFT, HIGH))
    clear(index[2] == count[2] - 1, slice(None), slice(None), slice(HIGH + nz, HIGH + nz + 1))

    for m in moves:
        m.wait()
    wc[...] = jnp.zeros(wc.shape, BF)
    for dx in range(3):
        total = None
        for dy in range(3):
            taps = wconv_ref[9 * dx + 3 * dy : 9 * dx + 3 * dy + 3].reshape(3 * width, width)
            i, j = iota((width, 4 * HALF), 0), iota((width, 4 * HALF), 1)
            place = jnp.where(j == i + HALF * dy, 1.0, 0.0).astype(BF)
            part = mm(taps, place)
            total = part if total is None else total + part
        for dz in range(3):
            at = 4 * HALF * dx + HALF * dz
            wc[at : at + width] = total[width * dz : width * (dz + 1)].astype(BF)

    side = WINDOW + 2
    padded = -(-nz // 16) * 16

    def lhs(x):
        taps = [grid[x, :, SHIFT + d : SHIFT + d + padded, :].reshape(side * padded, LANES) for d in range(3)]
        lower = iota(taps[0].shape, 1) < HALF
        return jnp.concatenate([jnp.where(lower, taps[0], taps[1]), taps[2]], 1).astype(BF)

    rows = [lhs(x) for x in range(side)]
    acc = mm(jnp.concatenate([jnp.concatenate(rows[x : x + 3], 1) for x in range(WINDOW)], 0), wc[...])
    strip = WINDOW * padded
    for x in range(WINDOW):
        part = acc[x * side * padded : (x + 1) * side * padded]
        near, second = part[:, :LANES], part[:, LANES:]
        turned = pltpu.roll(near[padded : (WINDOW + 1) * padded], HALF, 1)
        tot[x * strip : (x + 1) * strip] = near[:strip] + turned + second[2 * padded :]
    tot[WINDOW * strip :] = jnp.zeros((tot.shape[0] - WINDOW * strip, LANES), F32)
    diagonal = iota((width, width), 0) == iota((width, width), 1)
    cg = jnp.sum(jnp.where(diagonal, cgain_ref[...], 0.0), 1, keepdims=True)
    normed = norm_cols(jnp.transpose(tot[...])[:width], cg, width)
    active = jnp.where(normed >= 0.0, normed, 0.01 * normed)
    active = jnp.transpose(jnp.concatenate([active, jnp.zeros((LANES - width, tot.shape[0]), F32)], 0))
    for x in range(WINDOW):
        centre = grid[x + 1, 1 : 1 + WINDOW, HIGH : HIGH + padded, :].reshape(strip, LANES)
        result = (centre + active[x * strip : (x + 1) * strip]).reshape(WINDOW, padded, LANES).astype(BF)
        out_ref[x] = result[:, :nz, :width]


def geometry():
    kept = WINDOW * WINDOW - 1
    geo = np.full((16, kept * ROWS), WINDOW, np.float32)
    for v in range(2):
        gone = kept * v
        for i in range(kept):
            spot = i + 1 - v
            for r in range(ROWS):
                t = i * ROWS + r
                if r < WINDOW:
                    geo[8 * v : 8 * v + 3, t] = r, spot // WINDOW, spot % WINDOW
                elif i < WINDOW:
                    geo[8 * v : 8 * v + 3, t] = i, gone // WINDOW, gone % WINDOW
                else:
                    geo[8 * v + 1 : 8 * v + 3, t] = spot // WINDOW, spot % WINDOW
    return jnp.asarray(geo)


def exchange(v, axis, odd):
    count, cores = lax.axis_size(axis), lax.axis_size("gz")
    pairs = []
    for i in range(count):
        low = i - (i - odd) % 2
        for c in range(cores):
            if low < 0 or low + 1 >= count:
                to = (i, c ^ 1 if c ^ 1 < cores else c)
            else:
                to = (low + 1 if i == low else low, c)
            pairs.append((i * cores + c, to[0] * cores + to[1]))
    return lax.ppermute(v, (axis, "gz"), pairs)


def body(volume, w_qkv, w_proj, w_up, w_down, norm_gain, conv_weight, conv_gain):
    sx, sy, sz, width = volume.shape
    spots = sx * sy
    groups = sz // WINDOW
    geo = geometry()
    keys = (spots - 1) * ROWS
    weights = (w_qkv, w_proj, w_up, jnp.swapaxes(w_down, 1, 2), norm_gain)
    halves = [0] if lax.axis_size("gy") == 2 else [0, 1]
    tall = ROWS * groups // 2

    operands = (volume, geo, *weights)
    packed, *cuts = pl.pallas_call(
        functools.partial(first_kernel, width, len(halves)),
        out_shape=[jax.ShapeDtypeStruct((sx, sy, tall, LANES), BF)]
        + [jax.ShapeDtypeStruct((sx, HIGH, tall, LANES), BF) for _ in halves]
        + [jax.ShapeDtypeStruct((HIGH, sy, tall, LANES), BF) for _ in range(2)],
        in_specs=[pl.BlockSpec(memory_space=pltpu.HBM)] * len(operands),
        scratch_shapes=[pltpu.VMEM(v.shape, v.dtype) for v in operands]
        + [
            pltpu.SemaphoreType.DMA((len(operands),)),
            pltpu.VMEM((spots, sz + 12, LANES), F32),
            pltpu.VMEM((groups, spots - 1, ROWS, LANES), F32),
            pltpu.VMEM((groups, HEADS * keys, LANES), BF),
            pltpu.VMEM((groups, LANES, keys), BF),
            pltpu.VMEM((groups, keys, LANES), BF),
            pltpu.VMEM((groups, keys, LANES), F32),
            pltpu.VMEM((width, groups * keys), F32),
            pltpu.VMEM((spots, sz + 12, LANES), F32),
        ],
        compiler_params=pltpu.CompilerParams(vmem_limit_bytes=24 << 20),
        name="first_block",
    )(*[pltpu.with_memory_space_constraint(v, pltpu.HBM) for v in operands])

    xodd = lax.axis_index("gx") % 2

    def cut(v, odd):
        return lax.dynamic_slice_in_dim(v, jnp.where(odd == 0, SHIFT, 0), HIGH, 0)

    def other_core(v):
        return lax.ppermute(v, "gz", [(0, 1), (1, 0)])

    ys = [exchange(v, "gy", k) for k, v in zip(halves, cuts)]
    xs = [exchange(v, "gx", k) for k, v in enumerate(cuts[len(halves) :])]
    corners = [[exchange(cut(v, (xodd + k) % 2), "gx", k) for k in (0, 1)] for v in ys]

    side = WINDOW + 2
    rows = sum(box_rows(*c) for c in COLUMNS)
    strip = WINDOW * -(-sz // 16) * 16

    def buffers(slots):
        return [
            pltpu.VMEM((len(COLUMNS), slots, LANES, keys), BF),
            pltpu.VMEM((len(COLUMNS), slots, keys, LANES), BF),
        ] + [pltpu.VMEM((slots, -(-HEADS * box_rows(*c) // 32) * 32, LANES), BF) for c in COLUMNS]

    span = up(max(layout(half_columns(k))[1] for k in range(2)) * (groups - 1), LANES)

    def inner(part, operands):
        return pl.pallas_call(
            functools.partial(inner_kernel, width, len(ys), part),
            out_shape=jax.ShapeDtypeStruct((span if part else up(rows * (groups - 1), LANES), LANES), F32),
            scratch_shapes=[
                pltpu.VMEM((span, LANES), F32),
                pltpu.VMEM((groups // 2, EXT, EXT, ROWS, LANES), F32),
            ]
            + buffers(groups - 1),
            compiler_params=pltpu.CompilerParams(vmem_limit_bytes=20 << 20),
            cost_estimate=pl.CostEstimate(flops=2 * 10**9, transcendentals=0, bytes_accessed=10**6),
        )(*operands)

    def edge(parts):
        def kernel(*refs):
            at = 0
            for r in refs[:-1]:
                n = r.shape[0] * r.shape[1]
                refs[-1][at : at + n] = r[:, :, -ROWS:, :].reshape(n, ROWS, LANES)
                at += n

        shape = (sum(p.shape[0] * p.shape[1] for p in parts), ROWS, LANES)
        return pl.pallas_call(
            kernel,
            out_shape=jax.ShapeDtypeStruct(shape, BF),
            compiler_params=pltpu.CompilerParams(vmem_limit_bytes=4 << 20),
        )(*parts)

    near = [packed, *xs]
    wide = [v for y, c in zip(ys, corners) for v in (y, *c)]
    if len(ys) == 1:
        early = inner(-1, [geo, *near, *weights])
        waited = lax.optimization_barrier((early, *near))
        zs = other_core(edge([*waited[1:], *wide]))
        done = inner(1, [geo, *near, *wide, *weights])
        done = [done, early]
    else:
        zs = other_core(edge(near + wide))
        done = [inner(0, [geo, *near, *wide, *weights])]

    conv = [pltpu.with_memory_space_constraint(v, pltpu.HBM) for v in (conv_weight, conv_gain[None, :])]
    operands = [geo, *done, *near, *wide, zs, *weights, *conv]
    vmem = pl.BlockSpec(memory_space=pltpu.VMEM)
    hbm = pl.BlockSpec(memory_space=pltpu.HBM)
    return pl.pallas_call(
        functools.partial(last_kernel, width, len(ys)),
        out_shape=jax.ShapeDtypeStruct(volume.shape, volume.dtype),
        in_specs=[vmem] * (len(operands) - 2) + [hbm] * 2,
        scratch_shapes=[
            pltpu.VMEM((2, EXT, EXT, ROWS, LANES), F32),
            pltpu.VMEM((up(layout(range(len(COLUMNS)), squeezed)[1] + rows, LANES), LANES), F32),
            pltpu.VMEM(done[0].shape, F32),
            pltpu.VMEM((side, side, sz + 12, LANES), F32),
            pltpu.VMEM((3 * 4 * HALF, 4 * HALF), BF),
            pltpu.VMEM((-(-WINDOW * strip // LANES) * LANES, LANES), F32),
            pltpu.VMEM(conv[0].shape, conv[0].dtype),
            pltpu.VMEM(conv[1].shape, conv[1].dtype),
            pltpu.SemaphoreType.DMA((2,)),
        ]
        + buffers(2),
        compiler_params=pltpu.CompilerParams(vmem_limit_bytes=26 << 20),
        name="last_windows",
    )(*operands)


def solution(mesh):
    placed = (P(("parts", "gx"), "gy", "gz", None), P(), P(), P(), P(), P(), P(), P())

    return jax.shard_map(
        body,
        mesh=mesh,
        in_specs=placed,
        out_specs=P(("parts", "gx"), "gy", "gz", None),
        check_vma=False,
    )
```
